32 devices in a mesh: dp: 4 (over z), tp: 8 (over y, x, core).
Axes of the slice: x: 2, y: 2, z: 4, core: 2. Of those that a mesh axis runs over, the one named last changes fastest.
Arguments:
- img: bfloat16 [8, 2048, 3072], P('dp'), parts along dimension 0
- txt: bfloat16 [8, 256, 3072], P('dp'), parts along dimension 0
- vec: bfloat16 [8, 3072], P('dp'), parts along dimension 0
- ids: int32 [8, 2304, 3], P('dp'), parts along dimension 0
- img_mod_w: bfloat16 [3072, 6, 3072], P(None, None, 'tp')
- img_mod_b: bfloat16 [6, 3072], P(None, 'tp')
- img_qkv_w: bfloat16 [3072, 3, 3072], P(None, None, 'tp')
- img_qkv_b: bfloat16 [3, 3072], P(None, 'tp')
- img_q_gain: bfloat16 [128], replicated
- img_k_gain: bfloat16 [128], replicated
- img_proj_w: bfloat16 [3072, 3072], P('tp')
- img_proj_b: bfloat16 [3072], replicated
- img_fc1_w: bfloat16 [3072, 12288], P(None, 'tp')
- img_fc1_b: bfloat16 [12288], P('tp')
- img_fc2_w: bfloat16 [12288, 3072], P('tp')
- img_fc2_b: bfloat16 [3072], replicated
- txt_mod_w: bfloat16 [3072, 6, 3072], P(None, None, 'tp')
- txt_mod_b: bfloat16 [6, 3072], P(None, 'tp')
- txt_qkv_w: bfloat16 [3072, 3, 3072], P(None, None, 'tp')
- txt_qkv_b: bfloat16 [3, 3072], P(None, 'tp')
- txt_q_gain: bfloat16 [128], replicated
- txt_k_gain: bfloat16 [128], replicated
- txt_proj_w: bfloat16 [3072, 3072], P('tp')
- txt_proj_b: bfloat16 [3072], replicated
- txt_fc1_w: bfloat16 [3072, 12288], P(None, 'tp')
- txt_fc1_b: bfloat16 [12288], P('tp')
- txt_fc2_w: bfloat16 [12288, 3072], P('tp')
- txt_fc2_b: bfloat16 [3072], replicated
Outputs:
- output 1: bfloat16 [8, 2048, 3072], P('dp'), parts along dimension 0
- output 2: bfloat16 [8, 256, 3072], P('dp'), parts along dimension 0
There are 4 independent parts. The reference program is written for one: setup_inputs(seed, part) draws one part's arguments, and reference() takes and returns one part's arrays. A program takes and returns all parts, laid end to end along the dimension named above; an argument that names none is the same for every part.
All inputs are finite; a program needn't handle non-finite values.
Results may differ from the reference program's by a relative error of at most 0.014405.
Values are sent between devices in bfloat16 or wider.
A program may use at most 1 GiB of HBM per device.

```python
import jax
import jax.numpy as jnp
from jax import lax

D = 3072
HEADS = 24
FF = 12288
HEAD = 128
B = 2
LT = 256
LI = 2048

SEQ_LEN = LT + LI
NORM_EPS = 1e-6
ROPE_THETA = 10000.0
AXES_DIM = (16, 56, 56)


def normal_draw(key, shape, scale):
    return (scale * jax.random.normal(key, shape, jnp.float32)).astype(jnp.bfloat16)


def draw_path(key):
    sub_keys = jax.random.split(key, 12)
    return dict(
        mod_w=normal_draw(sub_keys[0], (D, 6, D), D ** -0.5),
        mod_b=normal_draw(sub_keys[1], (6, D), 0.5),
        qkv_w=normal_draw(sub_keys[2], (D, 3, D), D ** -0.5),
        qkv_b=normal_draw(sub_keys[3], (3, D), 0.5),
        q_gain=jax.random.uniform(sub_keys[4], (HEAD,), jnp.float32, 1.2, 2.2).astype(jnp.bfloat16),
        k_gain=jax.random.uniform(sub_keys[5], (HEAD,), jnp.float32, 1.2, 2.2).astype(jnp.bfloat16),
        proj_w=normal_draw(sub_keys[6], (D, D), D ** -0.5),
        proj_b=normal_draw(sub_keys[7], (D,), 0.5),
        fc1_w=normal_draw(sub_keys[8], (D, FF), D ** -0.5),
        fc1_b=normal_draw(sub_keys[9], (FF,), 0.5),
        fc2_w=normal_draw(sub_keys[10], (FF, D), FF ** -0.5),
        fc2_b=normal_draw(sub_keys[11], (D,), 0.5),
    )


def setup_inputs(seed: int = 0, part: int = 0) -> dict:
    root_key = jax.random.key(seed)
    part_key = jax.random.fold_in(root_key, part)
    act_keys = jax.random.split(part_key, 4)
    inputs = dict(
        img=normal_draw(act_keys[0], (B, LI, D), 1.0),
        txt=normal_draw(act_keys[1], (B, LT, D), 1.0),
        vec=normal_draw(act_keys[2], (B, D), 1.5),
        ids=jax.random.randint(act_keys[3], (B, SEQ_LEN, 3), 0, 64, jnp.int32),
    )
    for path_idx, prefix in enumerate(('img', 'txt')):
        drawn = draw_path(jax.random.fold_in(jax.random.key(seed + 1), path_idx))
        inputs.update({prefix + '_' + field_name: drawn_arr for field_name, drawn_arr in drawn.items()})
    return inputs


def layer_norm(tokens):
    values = tokens.astype(jnp.float32)
    centered = values - jnp.mean(values, axis=-1, keepdims=True)
    variance = jnp.mean(centered * centered, axis=-1, keepdims=True)
    return centered * lax.rsqrt(variance + NORM_EPS)


def modulate(tokens, shift_vec, scale_vec):
    scaled = (1.0 + scale_vec.astype(jnp.float32)[:, None, :]) * layer_norm(tokens)
    return (scaled + shift_vec.astype(jnp.float32)[:, None, :]).astype(jnp.bfloat16)


def rope_tables(ids):
    pieces = []
    for axis_idx, axis_dim in enumerate(AXES_DIM):
        inv_freq = ROPE_THETA ** (-jnp.arange(0, axis_dim, 2, dtype=jnp.float32) / axis_dim)
        pieces.append(ids[:, :, axis_idx, None].astype(jnp.float32) * inv_freq)
    angles = jnp.concatenate(pieces, axis=-1)
    return jnp.cos(angles), jnp.sin(angles)


def apply_rope(values, cos_t, sin_t):
    value_pairs = values.reshape(values.shape[:-1] + (values.shape[-1] // 2, 2))
    even_part = value_pairs[..., 0]
    odd_part = value_pairs[..., 1]
    cos_b = cos_t[:, :, None, :]
    sin_b = sin_t[:, :, None, :]
    rotated = jnp.stack([cos_b * even_part - sin_b * odd_part, sin_b * even_part + cos_b * odd_part], axis=-1)
    return rotated.reshape(values.shape)


def rms_gain(values, gain_vec):
    mean_sq = jnp.mean(values * values, axis=-1, keepdims=True)
    return values * lax.rsqrt(mean_sq + NORM_EPS) * gain_vec.astype(jnp.float32)


def matmul_rows(tokens, weight):
    flat_out = jnp.dot(tokens.reshape(-1, tokens.shape[-1]), weight, preferred_element_type=jnp.float32)
    return flat_out.reshape(tokens.shape[:-1] + (weight.shape[1],))


def modulation(silu_vec, mod_w, mod_b):
    flat_mods = jnp.dot(silu_vec, mod_w.reshape(D, 6 * D), preferred_element_type=jnp.float32)
    return (flat_mods.reshape(B, 6, D) + mod_b.astype(jnp.float32)).astype(jnp.bfloat16)


def path_qkv(tokens, mod_vecs, qkv_w, qkv_b, q_gain, k_gain, cos_t, sin_t):
    length = tokens.shape[1]
    normed = modulate(tokens, mod_vecs[:, 0], mod_vecs[:, 1])
    proj_qkv = matmul_rows(normed, qkv_w.reshape(D, 3 * D)).reshape(B, length, 3, D)
    proj_qkv = (proj_qkv + qkv_b.astype(jnp.float32)).reshape(B, length, 3, HEADS, HEAD)
    query_h = apply_rope(rms_gain(proj_qkv[:, :, 0], q_gain), cos_t, sin_t).astype(jnp.bfloat16)
    key_h = apply_rope(rms_gain(proj_qkv[:, :, 1], k_gain), cos_t, sin_t).astype(jnp.bfloat16)
    value_h = proj_qkv[:, :, 2].astype(jnp.bfloat16)
    return query_h, key_h, value_h


def one_head(operands):
    query_h, key_h, value_h = operands
    scores = jnp.einsum('bqd,bkd->bqk', query_h.astype(jnp.float32), key_h.astype(jnp.float32)) * HEAD ** -0.5
    attn_probs = jax.nn.softmax(scores, axis=-1).astype(jnp.bfloat16)
    head_out = jnp.einsum('bqk,bkd->bqd', attn_probs.astype(jnp.float32), value_h.astype(jnp.float32))
    return head_out.astype(jnp.bfloat16)


def joint_attention(query_h, key_h, value_h):
    per_head = lax.map(one_head, (jnp.moveaxis(query_h, 2, 0), jnp.moveaxis(key_h, 2, 0), jnp.moveaxis(value_h, 2, 0)))
    return jnp.moveaxis(per_head, 0, 2).reshape(B, SEQ_LEN, D)


def add_branch(tokens, gate_vec, summed, bias_vec):
    branch = summed.astype(jnp.float32) + bias_vec.astype(jnp.float32)
    return (tokens.astype(jnp.float32) + gate_vec.astype(jnp.float32)[:, None, :] * branch).astype(jnp.bfloat16)


def mlp_hidden(tokens, mod_vecs, fc1_w, fc1_b):
    normed = modulate(tokens, mod_vecs[:, 3], mod_vecs[:, 4])
    pre_act = matmul_rows(normed, fc1_w) + fc1_b.astype(jnp.float32)
    return jax.nn.gelu(pre_act, approximate=True).astype(jnp.bfloat16)


def reference(img, txt, vec, ids, img_mod_w, img_mod_b, img_qkv_w, img_qkv_b, img_q_gain, img_k_gain, img_proj_w, img_proj_b, img_fc1_w, img_fc1_b, img_fc2_w, img_fc2_b, txt_mod_w, txt_mod_b, txt_qkv_w, txt_qkv_b, txt_q_gain, txt_k_gain, txt_proj_w, txt_proj_b, txt_fc1_w, txt_fc1_b, txt_fc2_w, txt_fc2_b):
    silu_vec = jax.nn.silu(vec.astype(jnp.float32)).astype(jnp.bfloat16)
    img_mods = modulation(silu_vec, img_mod_w, img_mod_b)
    txt_mods = modulation(silu_vec, txt_mod_w, txt_mod_b)
    cos_t, sin_t = rope_tables(ids)
    img_q, img_k, img_v = path_qkv(img, img_mods, img_qkv_w, img_qkv_b, img_q_gain, img_k_gain, cos_t[:, LT:], sin_t[:, LT:])
    txt_q, txt_k, txt_v = path_qkv(txt, txt_mods, txt_qkv_w, txt_qkv_b, txt_q_gain, txt_k_gain, cos_t[:, :LT], sin_t[:, :LT])
    attn_out = joint_attention(jnp.concatenate([txt_q, img_q], axis=1), jnp.concatenate([txt_k, img_k], axis=1), jnp.concatenate([txt_v, img_v], axis=1))
    img_mid = add_branch(img, img_mods[:, 2], matmul_rows(attn_out[:, LT:], img_proj_w), img_proj_b)
    txt_mid = add_branch(txt, txt_mods[:, 2], matmul_rows(attn_out[:, :LT], txt_proj_w), txt_proj_b)
    img_out = add_branch(img_mid, img_mods[:, 5], matmul_rows(mlp_hidden(img_mid, img_mods, img_fc1_w, img_fc1_b), img_fc2_w), img_fc2_b)
    txt_out = add_branch(txt_mid, txt_mods[:, 5], matmul_rows(mlp_hidden(txt_mid, txt_mods, txt_fc1_w, txt_fc1_b), txt_fc2_w), txt_fc2_b)
    return (img_out, txt_out)
```

```python
import functools

import jax
import jax.numpy as jnp
import numpy as np
from jax import lax
from jax.experimental import pallas as pl
from jax.experimental.pallas import tpu as pltpu
from jax.sharding import PartitionSpec as P

HEAD = 128
NORM_EPS = 1e-6
ROPE_THETA = 10000.0
AXES_DIM = (16, 56, 56)
N_IDS = 64
PATH_SPECS = (P(None, None, 'tp'), P(None, 'tp'), P(None, None, 'tp'), P(None, 'tp'), P(None), P(None), P('tp', None), P(None), P(None, 'tp'), P('tp'), P('tp', None), P(None))
F32 = jnp.float32
BF16 = jnp.bfloat16


def rope_table():
    cos = np.zeros((3 * N_IDS, HEAD), np.float32)
    sin = np.zeros((3 * N_IDS, HEAD), np.float32)
    lane = 0
    for axis, dim in enumerate(AXES_DIM):
        inv_freq = np.float32(ROPE_THETA) ** (-np.arange(0, dim, 2, dtype=np.float32) / np.float32(dim))
        angles = np.arange(N_IDS, dtype=np.float32)[:, None] * inv_freq.astype(np.float32)
        rows = slice(axis * N_IDS, (axis + 1) * N_IDS)
        c = np.cos(angles.astype(np.float64)).astype(np.float32)
        s = np.sin(angles.astype(np.float64)).astype(np.float32)
        cos[rows, lane:lane + dim:2] = c
        cos[rows, lane + 1:lane + dim:2] = c
        sin[rows, lane:lane + dim:2] = -s
        sin[rows, lane + 1:lane + dim:2] = s
        lane += dim
    parts = []
    for table in (cos, sin):
        rest = table
        for _ in range(3):
            part = rest.astype(jnp.bfloat16)
            parts.append(np.asarray(part))
            rest = rest - np.asarray(part).astype(np.float32)
    return np.concatenate(parts, axis=1)


def qkv_kernel(heads, x_ref, mod_ref, w_ref, b_ref, gain_ref, ids_ref, tab_ref, *rest):
    out_ref = rest[-1]
    width = heads * HEAD
    rows = x_ref.shape[1]
    x = x_ref[0].astype(F32)
    centered = x - jnp.mean(x, axis=-1, keepdims=True)
    variance = jnp.mean(centered * centered, axis=-1, keepdims=True)
    normed = centered * lax.rsqrt(variance + NORM_EPS)
    shift = mod_ref[0, 0:1, :].astype(F32)
    scale = mod_ref[0, 1:2, :].astype(F32)
    u = ((1.0 + scale) * normed + shift).astype(BF16)

    code = lax.broadcasted_iota(jnp.int32, (N_IDS, rows), 0)
    hot = jnp.concatenate([(ids_ref[0, axis:axis + 1, :] == code).astype(F32).astype(BF16) for axis in range(3)], axis=0)
    parts = lax.dot_general(hot, tab_ref[...], (((0,), (0,)), ((), ())), preferred_element_type=F32)
    cos_t = parts[:, 0:128] + parts[:, 128:256] + parts[:, 256:384]
    sin_t = parts[:, 384:512] + parts[:, 512:640] + parts[:, 640:768]
    even = lax.broadcasted_iota(jnp.int32, (rows, HEAD), 1) % 2 == 0

    for j in range(3):
        a = jnp.dot(u, w_ref[j], preferred_element_type=F32) + b_ref[j:j + 1, :].astype(F32)
        for h in range(heads):
            t = a[:, h * HEAD:(h + 1) * HEAD]
            if j < 2:
                mean_sq = jnp.mean(t * t, axis=-1, keepdims=True)
                t = t * lax.rsqrt(mean_sq + NORM_EPS) * gain_ref[j:j + 1, :]
                swapped = jnp.where(even, pltpu.roll(t, HEAD - 1, 1), pltpu.roll(t, 1, 1))
                t = t * cos_t + swapped * sin_t
            col = j * width + h * HEAD
            out_ref[0, :, col:col + HEAD] = t.astype(BF16)


def qkv_call(x, mods, w3, bias, gains, ids_t, table, base, row_block, first_block, total_rows):
    batch, length, dim = x.shape
    width = w3.shape[2]
    heads = width // HEAD
    steps = length // row_block
    in_specs = [
        pl.BlockSpec((1, row_block, dim), lambda b, r: (b, r, 0)),
        pl.BlockSpec((1, 6, dim), lambda b, r: (b, 0, 0)),
        pl.BlockSpec((3, dim, width), lambda b, r: (0, 0, 0)),
        pl.BlockSpec((3, width), lambda b, r: (0, 0)),
        pl.BlockSpec((2, HEAD), lambda b, r: (0, 0)),
        pl.BlockSpec((1, 3, row_block), lambda b, r: (b, 0, r + first_block)),
        pl.BlockSpec(table.shape, lambda b, r: (0, 0)),
    ]
    args = [x, mods, w3, bias, gains, ids_t, table]
    aliases = {}
    if base is not None:
        in_specs.append(pl.BlockSpec(memory_space=pl.ANY))
        args.append(base)
        aliases = {7: 0}
    flops = 2 * batch * length * dim * 3 * width
    return pl.pallas_call(
        functools.partial(qkv_kernel, heads),
        grid=(batch, steps),
        in_specs=in_specs,
        out_specs=pl.BlockSpec((1, row_block, 3 * width), lambda b, r: (b, r + first_block, 0)),
        out_shape=jax.ShapeDtypeStruct((batch, total_rows, 3 * width), BF16),
        input_output_aliases=aliases,
        compiler_params=pltpu.CompilerParams(dimension_semantics=("arbitrary", "arbitrary"), vmem_limit_bytes=60 * 2**20),
        cost_estimate=pl.CostEstimate(flops=flops, bytes_accessed=2 * batch * length * (dim + 3 * width) + 6 * dim * width, transcendentals=0),
        name="qkv",
    )(*args)


LOG2E = 1.4426950408889634


def attention_kernel(sub, q_ref, k_ref, v_ref, out_ref):
    rows = q_ref.shape[1]
    k = k_ref[0]
    v = v_ref[0]
    factor = HEAD ** -0.5 * LOG2E
    for r in range(0, rows, sub):
        q = q_ref[0, r:r + sub, :]
        s = lax.dot_general(q, k, (((1,), (1,)), ((), ())), preferred_element_type=F32)
        top = jnp.max(s, axis=-1, keepdims=True)
        p = jnp.exp2((s - top) * factor)
        total = jnp.sum(p, axis=-1, keepdims=True)
        o = jnp.dot(p.astype(BF16), v, preferred_element_type=F32)
        out_ref[0, r:r + sub, :] = (o * (1.0 / total)).astype(BF16)


def attention_call(qkv, heads, row_block, sub, first_row, rows):
    batch, total_rows, width3 = qkv.shape
    first = first_row // row_block
    return pl.pallas_call(
        functools.partial(attention_kernel, sub),
        grid=(batch, heads, rows // row_block),
        in_specs=[
            pl.BlockSpec((1, row_block, HEAD), lambda b, h, r: (b, r + first, h)),
            pl.BlockSpec((1, total_rows, HEAD), lambda b, h, r: (b, 0, heads + h)),
            pl.BlockSpec((1, total_rows, HEAD), lambda b, h, r: (b, 0, 2 * heads + h)),
        ],
        out_specs=pl.BlockSpec((1, row_block, HEAD), lambda b, h, r: (b, r, h)),
        out_shape=jax.ShapeDtypeStruct((batch, rows, heads * HEAD), BF16),
        compiler_params=pltpu.CompilerParams(dimension_semantics=("arbitrary",) * 3, vmem_limit_bytes=60 * 2**20),
        cost_estimate=pl.CostEstimate(flops=4 * batch * heads * rows * total_rows * HEAD * 2, bytes_accessed=batch * heads * (2 * rows + 2 * total_rows) * HEAD * 2, transcendentals=batch * heads * rows * total_rows),
        name="attention",
    )(qkv, qkv, qkv)


def layer_norm(tokens):
    values = tokens.astype(F32)
    centered = values - jnp.mean(values, axis=-1, keepdims=True)
    variance = jnp.mean(centered * centered, axis=-1, keepdims=True)
    return centered * lax.rsqrt(variance + NORM_EPS)


def modulate(tokens, shift_vec, scale_vec):
    scaled = (1.0 + scale_vec.astype(F32)[:, None, :]) * layer_norm(tokens)
    return (scaled + shift_vec.astype(F32)[:, None, :]).astype(BF16)


def modulation(silu_vec, weights):
    flat_mods = jnp.einsum('bd,dke->bke', silu_vec, weights[0], preferred_element_type=F32)
    return (flat_mods + weights[1].astype(F32)).astype(BF16)


def project(tokens, weight):
    return jnp.einsum('blk,kd->bld', tokens, weight, preferred_element_type=F32)


def add_branch(tokens, gate_vec, summed, bias_vec):
    branch = summed.astype(F32) + bias_vec.astype(F32)
    return (tokens.astype(F32) + gate_vec.astype(F32)[:, None, :] * branch).astype(BF16)


MESH = pl.DeviceIdType.MESH
(O_CORE, O_FIRST, O_SECOND, O_RELAY, U_CORE, PART_CORE, RS_FIRST, RS_SECOND, OUT_FIRST, OUT_SECOND, OUT_RELAY, CORE_OWN, CORE_FIRST, CORE_SECOND, CORE_RELAY) = range(15)
(L_O, L_X, L_OUT) = range(3)
SLOTS = 4
SEMS = 8


def block_kernel(cfg, o_hbm, x_hbm, ut_hbm, x1t_hbm, wp_hbm, w1t_hbm, w2t_hbm, w1i_hbm, w2i_hbm, vec_ref, fb_ref, out_hbm,
                 wp, w1, w2, obuf, xbuf, x1buf, x1keep, u2, hid, psend, precv, own, chip_sum, rs1, keep2, rs2_out, rs2_in, outb,
                 wsem, lsem, tsem, ssem, rsem):
    batch, txt_chunks, img_chunks, per_img, rows, tile = cfg
    half, quarter, eighth = rows // 2, rows // 4, rows // 8
    dim = wp.shape[0]
    ff = w1.shape[1]
    cols = o_hbm.shape[2]
    total = txt_chunks + img_chunks
    per_txt = txt_chunks // batch

    me = lax.axis_index('tp')
    core = me % 2
    xi = (me // 2) % 2
    yi = me // 4
    partner = me + 1 - 2 * core
    x_next = me + 2 - 4 * xi
    y_next = me + 4 - 8 * yi
    first = x_next * (1 - core) + y_next * core
    second = x_next * core + y_next * (1 - core)
    bit1 = xi * (1 - core) + yi * core
    bit2 = xi * core + yi * (1 - core)

    barrier = pltpu.get_barrier_semaphore()
    for dev in (partner, first, second):
        pl.semaphore_signal(barrier, inc=1, device_id={'tp': dev}, device_id_type=MESH)
    pl.semaphore_wait(barrier, 3)

    def remote(kind, g, src, dst, dev):
        return pltpu.make_async_remote_copy(src_ref=src, dst_ref=dst, send_sem=ssem.at[kind, g % SEMS], recv_sem=rsem.at[kind, g % SEMS], device_id={'tp': dev}, device_id_type=MESH)

    def rows_at(start, size):
        return pl.ds(pl.multiple_of(start, size), size)

    def img_pos(g):
        k = g - txt_chunks
        return k // per_img, (k % per_img) * rows

    def chip_cols(dev):
        return rows_at((dev // 2) * (2 * cols), 2 * cols)

    def own_rows(b1, b2):
        return core * half + b1 * quarter + b2 * eighth

    def o_local(g):
        b, r0 = img_pos(g)
        return pltpu.make_async_copy(o_hbm.at[b, rows_at(r0 + core * half, half), :], obuf.at[g % SLOTS, :, rows_at(me * cols, cols)], lsem.at[L_O, g % SEMS])

    def o_core(g):
        b, r0 = img_pos(g)
        return remote(O_CORE, g, o_hbm.at[b, rows_at(r0 + (1 - core) * half, half), :], obuf.at[g % SLOTS, :, rows_at(me * cols, cols)], partner)

    def o_send(kind, g, owner, dev):
        ref = obuf.at[g % SLOTS, :, chip_cols(owner)]
        return remote(kind, g, ref, ref, dev)

    def x_load(g):
        b, r0 = img_pos(g)
        return pltpu.make_async_copy(x_hbm.at[b, rows_at(r0 + core * half, half), :], xbuf.at[g % 2], lsem.at[L_X, g % SEMS])

    def u_core(g):
        ref = u2.at[g % 2, rows_at(core * half, half), :]
        return remote(U_CORE, g, ref, ref, partner)

    def part_core(g):
        return remote(PART_CORE, g, psend, precv.at[g % 2], partner)

    def rs_first(g):
        return remote(RS_FIRST, g, chip_sum.at[rows_at((1 - bit1) * quarter, quarter), :], rs1.at[g % 2], first)

    def rs_second(g):
        return remote(RS_SECOND, g, rs2_out.at[g % 2], rs2_in.at[g % SLOTS], second)

    def out_ref(g, b1, b2):
        return out_hbm.at[rows_at(g * rows + own_rows(b1, b2), eighth), :]

    def out_send(kind, g, b1, b2, dev):
        ref = out_ref(g, b1, b2)
        mine = kind in (OUT_FIRST, OUT_SECOND, CORE_OWN)
        return remote(kind, g, outb.at[g % SLOTS] if mine else ref, ref, dev)

    def out_local(g):
        return pltpu.make_async_copy(outb.at[g % SLOTS], out_ref(g, bit1, bit2), lsem.at[L_OUT, g % SEMS])

    def txt_load(g):
        b, r0 = g // per_txt, (g % per_txt) * rows
        return (pltpu.make_async_copy(ut_hbm.at[b, rows_at(r0, rows), :], u2.at[g % 2], tsem.at[0, g % 2]),
                pltpu.make_async_copy(x1t_hbm.at[b, rows_at(r0 + own_rows(bit1, bit2), eighth), :], x1keep.at[g % SLOTS], tsem.at[1, g % 2]))

    def w_load(k, src, dst):
        return pltpu.make_async_copy(src, dst, wsem.at[k])

    def select(g):
        txt = (g < txt_chunks).astype(jnp.int32)
        return txt * (g // per_txt) + (1 - txt) * (batch + (g - txt_chunks) // per_img)

    def start_o(g):
        o_local(g).start()
        o_core(g).start()

    def send_o(g):
        o_local(g).wait()
        o_core(g).wait()
        o_send(O_FIRST, g, me, first).start()
        o_send(O_SECOND, g, me, second).start()

    def relay_o(g):
        o_send(O_FIRST, g, first, first).wait_recv()
        o_send(O_RELAY, g, first, second).start()
        x_load(g).start()

    def project(g):
        o_send(O_FIRST, g, me, first).wait_send()
        o_send(O_SECOND, g, me, second).wait_send()
        o_send(O_RELAY, g, first, second).wait_send()
        o_send(O_SECOND, g, second, second).wait_recv()
        o_send(O_RELAY, g, second, second).wait_recv()
        x_load(g).wait()

        @pl.when(g == txt_chunks)
        def _():
            w_load(2, wp_hbm, wp).wait()

        sel = select(g)
        slot = g % SLOTS

        def columns(n, carry):
            at = rows_at(n * tile, tile)
            acc = jnp.dot(obuf[slot], wp[:, at], preferred_element_type=F32)
            branch = acc + vec_ref[sel, 1:2, at]
            x1buf[:, at] = (xbuf[g % 2, :, at].astype(F32) + vec_ref[sel, 0:1, at] * branch).astype(BF16)
            return carry

        lax.fori_loop(0, dim // tile, columns, 0)

        def norm(n, carry):
            at = rows_at(n * 16, 16)
            x = x1buf[at, :].astype(F32)
            centered = x - jnp.mean(x, axis=-1, keepdims=True)
            variance = jnp.mean(centered * centered, axis=-1, keepdims=True)
            normed = centered * lax.rsqrt(variance + NORM_EPS)
            u2[g % 2, rows_at(core * half + n * 16, 16), :] = ((1.0 + vec_ref[sel, 2:3, :]) * normed + vec_ref[sel, 3:4, :]).astype(BF16)
            return carry

        lax.fori_loop(0, half // 16, norm, 0)
        u_core(g).start()
        x1keep[slot] = x1buf[rows_at(bit1 * quarter + bit2 * eighth, eighth), :]

    def mlp(g):
        @pl.when(g < txt_chunks)
        def _():
            for copy in txt_load(g):
                copy.wait()

        @pl.when(g >= txt_chunks)
        def _():
            u_core(g).wait()

        @pl.when(g == 0)
        def _():
            w_load(0, w1t_hbm, w1).wait()
            w_load(1, w2t_hbm, w2).wait()

        @pl.when(g == txt_chunks)
        def _():
            w_load(0, w1i_hbm, w1).wait()
            w_load(1, w2i_hbm, w2).wait()

        path = (g >= txt_chunks).astype(jnp.int32)

        def hidden(n, carry):
            at = rows_at(n * tile, tile)
            acc = jnp.dot(u2[g % 2], w1[:, at], preferred_element_type=F32)
            pre = acc + fb_ref[path, 0:1, at]
            hid[:, at] = jax.nn.gelu(pre, approximate=True).astype(BF16)
            return carry

        lax.fori_loop(0, ff // tile, hidden, 0)

        def theirs(n, carry):
            at = rows_at(n * tile, tile)
            psend[:, at] = jnp.dot(hid[rows_at((1 - core) * half, half), :], w2[:, at], preferred_element_type=F32).astype(BF16)
            return carry

        lax.fori_loop(0, dim // tile, theirs, 0)
        part_core(g).start()

        def mine(n, carry):
            at = rows_at(n * tile, tile)
            own[:, at] = jnp.dot(hid[rows_at(core * half, half), :], w2[:, at], preferred_element_type=F32)
            return carry

        lax.fori_loop(0, dim // tile, mine, 0)

        @pl.when(g == txt_chunks - 1)
        def _():
            w_load(0, w1i_hbm, w1).start()
            w_load(1, w2i_hbm, w2).start()

        part_core(g).wait()

        def add(n, carry):
            at = rows_at(n * 16, 16)
            chip_sum[at, :] = (own[at, :] + precv[g % 2, at, :].astype(F32)).astype(BF16)
            return carry

        lax.fori_loop(0, half // 16, add, 0)
        rs_first(g).start()

    def add_first(g):
        rs_first(g).wait()
        rs2_out[g % 2] = (chip_sum[rows_at(bit1 * quarter + (1 - bit2) * eighth, eighth), :].astype(F32) + rs1[g % 2, rows_at((1 - bit2) * eighth, eighth), :].astype(F32)).astype(BF16)
        rs_second(g).start()
        keep2[g % 2] = chip_sum[rows_at(bit1 * quarter + bit2 * eighth, eighth), :].astype(F32) + rs1[g % 2, rows_at(bit2 * eighth, eighth), :].astype(F32)

    def finish(g):
        rs_second(g).wait()
        sel = select(g)
        branch = keep2[g % 2] + rs2_in[g % SLOTS].astype(F32) + vec_ref[sel, 5:6, :]
        outb[g % SLOTS] = (x1keep[g % SLOTS].astype(F32) + vec_ref[sel, 4:5, :] * branch).astype(BF16)
        out_send(OUT_FIRST, g, bit1, bit2, first).start()
        out_send(OUT_SECOND, g, bit1, bit2, second).start()
        out_send(CORE_OWN, g, bit1, bit2, partner).start()
        out_local(g).start()

    def relay_out(g):
        out_send(OUT_FIRST, g, 1 - bit1, bit2, first).wait_recv()
        out_send(OUT_RELAY, g, 1 - bit1, bit2, second).start()
        out_send(CORE_FIRST, g, 1 - bit1, bit2, partner).start()
        out_send(OUT_SECOND, g, bit1, 1 - bit2, second).wait_recv()
        out_send(CORE_SECOND, g, bit1, 1 - bit2, partner).start()

    def relay_core(g):
        out_send(OUT_RELAY, g, 1 - bit1, 1 - bit2, second).wait_recv()
        out_send(CORE_RELAY, g, 1 - bit1, 1 - bit2, partner).start()

    def drain(g):
        out_local(g).wait()
        out_send(OUT_FIRST, g, bit1, bit2, first).wait_send()
        out_send(OUT_SECOND, g, bit1, bit2, second).wait_send()
        out_send(OUT_RELAY, g, 1 - bit1, bit2, second).wait_send()
        out_send(CORE_OWN, g, bit1, bit2, partner).wait()
        out_send(CORE_FIRST, g, 1 - bit1, bit2, partner).wait()
        out_send(CORE_SECOND, g, bit1, 1 - bit2, partner).wait()
        out_send(CORE_RELAY, g, 1 - bit1, 1 - bit2, partner).wait()

    w_load(0, w1t_hbm, w1).start()
    w_load(1, w2t_hbm, w2).start()
    for g in range(txt_chunks):
        for copy in txt_load(g):
            copy.start()
    w_load(2, wp_hbm, wp).start()

    stages = ((start_o, 4, txt_chunks), (send_o, 3, txt_chunks), (relay_o, 2, txt_chunks), (relay_out, -3, 0), (relay_core, -4, 0), (drain, -5, 0),
              (project, 1, txt_chunks), (add_first, -1, 0), (finish, -2, 0), (mlp, 0, 0))
    lead = 4 - txt_chunks

    def step(i, carry):
        for stage, ahead, lowest in stages:
            g = i - lead + ahead

            @pl.when((g >= lowest) & (g < total))
            def _():
                stage(g)
        return carry

    lax.fori_loop(0, total + lead + 5, step, 0)


def block_call(img_o, x, u_txt, x1_txt, wp, w1t, w2t, w1i, w2i, vecs, fb, rows):
    batch, img_len, dim = x.shape
    txt_len = u_txt.shape[1]
    ff = w1t.shape[1]
    txt_chunks = batch * (txt_len // rows)
    per_img = img_len // rows
    img_chunks = batch * per_img
    assert txt_chunks == 2
    half, quarter, eighth = rows // 2, rows // 4, rows // 8
    cfg = (batch, txt_chunks, img_chunks, per_img, rows, 512)
    total = txt_chunks + img_chunks
    anywhere = pl.BlockSpec(memory_space=pl.ANY)
    flops = 2 * total * rows * 2 * dim * ff + 2 * img_chunks * half * dim * dim
    return pl.pallas_call(
        functools.partial(block_kernel, cfg),
        in_specs=[anywhere] * 9 + [pl.BlockSpec(memory_space=pltpu.VMEM)] * 2,
        out_specs=anywhere,
        out_shape=jax.ShapeDtypeStruct((total * rows, dim), BF16),
        scratch_shapes=[
            pltpu.VMEM((dim, dim), BF16),
            pltpu.VMEM((dim, ff), BF16),
            pltpu.VMEM((ff, dim), BF16),
            pltpu.VMEM((SLOTS, half, dim), BF16),
            pltpu.VMEM((2, half, dim), BF16),
            pltpu.VMEM((half, dim), BF16),
            pltpu.VMEM((SLOTS, eighth, dim), BF16),
            pltpu.VMEM((2, rows, dim), BF16),
            pltpu.VMEM((rows, ff), BF16),
            pltpu.VMEM((half, dim), BF16),
            pltpu.VMEM((2, half, dim), BF16),
            pltpu.VMEM((half, dim), F32),
            pltpu.VMEM((half, dim), BF16),
            pltpu.VMEM((2, quarter, dim), BF16),
            pltpu.VMEM((2, eighth, dim), F32),
            pltpu.VMEM((2, eighth, dim), BF16),
            pltpu.VMEM((SLOTS, eighth, dim), BF16),
            pltpu.VMEM((SLOTS, eighth, dim), BF16),
            pltpu.SemaphoreType.DMA((3,)),
            pltpu.SemaphoreType.DMA((3, SEMS)),
            pltpu.SemaphoreType.DMA((2, 2)),
            pltpu.SemaphoreType.DMA((15, SEMS)),
            pltpu.SemaphoreType.DMA((15, SEMS)),
        ],
        compiler_params=pltpu.CompilerParams(collective_id=0, has_side_effects=True, vmem_limit_bytes=67043328),
        cost_estimate=pl.CostEstimate(flops=flops, bytes_accessed=4 * dim * dim + 8 * dim * ff + 4 * total * rows * dim, transcendentals=0),
        name="block",
    )(img_o, x, u_txt, x1_txt, wp, w1t, w2t, w1i, w2i, vecs, fb)


def local_block(img, txt, vec, ids, img_w, txt_w):
    batch, txt_len = txt.shape[:2]
    img_len = img.shape[1]
    width = img_w[6].shape[0]
    heads = width // HEAD
    proj_w = lax.all_gather(img_w[6], 'tp', axis=0, tiled=True)
    silu_vec = jax.nn.silu(vec.astype(F32)).astype(BF16)
    own_mods = jnp.stack([modulation(silu_vec, img_w), modulation(silu_vec, txt_w)])
    full_mods = lax.all_gather(own_mods, 'tp', axis=3, tiled=True)
    img_mods = full_mods[0]
    txt_mods = full_mods[1]
    table = jnp.asarray(rope_table())
    ids_t = jnp.swapaxes(ids, 1, 2)
    block = min(256, txt_len)
    total = txt_len + img_len

    def gains(w):
        return jnp.stack([w[4], w[5]]).astype(F32)

    def w3(w):
        return jnp.transpose(w[2], (1, 0, 2))

    qkv = qkv_call(txt, txt_mods, w3(txt_w), txt_w[3], gains(txt_w), ids_t, table, None, block, 0, total)
    qkv = qkv_call(img, img_mods, w3(img_w), img_w[3], gains(img_w), ids_t, table, qkv, block, txt_len // block, total)
    txt_o = attention_call(qkv, heads, block, block // 2, 0, txt_len)
    img_o = attention_call(qkv, heads, block, block // 2, txt_len, img_len)
    txt_part = project(txt_o, txt_w[6]).astype(BF16)
    txt_sum = lax.psum(txt_part, 'tp')
    txt_mid = add_branch(txt, txt_mods[:, 2], txt_sum, txt_w[7])
    txt_u = modulate(txt_mid, txt_mods[:, 3], txt_mods[:, 4])

    def vectors(mods, w):
        def rep(bias):
            return jnp.broadcast_to(bias.astype(F32), (batch, bias.shape[0]))
        m = mods.astype(F32)
        zero = jnp.zeros_like(m[:, 0])
        return jnp.stack([m[:, 2], rep(w[7]), m[:, 4], m[:, 3], m[:, 5], rep(w[11]), zero, zero], axis=1)

    vecs = jnp.concatenate([vectors(txt_mods, txt_w), vectors(img_mods, img_w)], axis=0)
    fb = jnp.stack([txt_w[9], img_w[9]]).astype(F32)[:, None, :]
    flat = block_call(img_o, img, txt_u, txt_mid, proj_w, txt_w[8], txt_w[10], img_w[8], img_w[10], vecs, fb, block)
    split = batch * txt_len
    return flat[split:].reshape(img.shape), flat[:split].reshape(txt.shape)


def solution(mesh):
    act_spec = P('dp', None, None)
    mapped = jax.shard_map(local_block, mesh=mesh, in_specs=(act_spec, act_spec, P('dp', None), act_spec, PATH_SPECS, PATH_SPECS), out_specs=(act_spec, act_spec), check_vma=False)

    def forward(img, txt, vec, ids, *weights):
        return mapped(img, txt, vec, ids, weights[:12], weights[12:])

    return forward
```

```python
import functools

import jax
import jax.numpy as jnp
import numpy as np
from jax import lax
from jax.experimental import pallas as pl
from jax.experimental.pallas import tpu as pltpu
from jax.sharding import PartitionSpec as P

HEAD = 128
NORM_EPS = 1e-6
ROPE_THETA = 10000.0
AXES_DIM = (16, 56, 56)
N_IDS = 64
WHOLE = None
PATH_SPECS = (P(WHOLE, WHOLE, 'tp'), P(WHOLE, 'tp'), P(WHOLE, WHOLE, 'tp'), P(WHOLE, 'tp'), P(WHOLE), P(WHOLE), P('tp', WHOLE), P(WHOLE), P(WHOLE, 'tp'), P('tp'), P('tp', WHOLE), P(WHOLE))
F32 = jnp.float32
BF16 = jnp.bfloat16


def rope_table():
    cos = np.zeros((3 * N_IDS, HEAD), np.float32)
    sin = np.zeros((3 * N_IDS, HEAD), np.float32)
    lane = 0
    for axis, dim in enumerate(AXES_DIM):
        inv_freq = np.float32(ROPE_THETA) ** (-np.arange(0, dim, 2, dtype=np.float32) / np.float32(dim))
        angles = np.arange(N_IDS, dtype=np.float32)[:, None] * inv_freq.astype(np.float32)
        rows = slice(axis * N_IDS, (axis + 1) * N_IDS)
        c = np.cos(angles.astype(np.float64)).astype(np.float32)
        s = np.sin(angles.astype(np.float64)).astype(np.float32)
        cos[rows, lane:lane + dim:2] = c
        cos[rows, lane + 1:lane + dim:2] = c
        sin[rows, lane:lane + dim:2] = -s
        sin[rows, lane + 1:lane + dim:2] = s
        lane += dim
    parts = []
    for table in (cos, sin):
        rest = table
        for _ in range(3):
            part = rest.astype(jnp.bfloat16)
            parts.append(np.asarray(part))
            rest = rest - np.asarray(part).astype(np.float32)
    return np.concatenate(parts, axis=1)


MESH = pl.DeviceIdType.MESH


SHIFT1, SCALE1, GATE1, SHIFT2, SCALE2, GATE2, PROJ_B, FC2_B = range(8)
VMEM_BYTES = 67043328


def row_of(ref, sel, row, at=slice(None)):
    return ref[sel, pl.ds(row, 1), at]


def loop(count, body):
    lax.fori_loop(0, count, lambda i, carry: (body(i), carry)[-1], 0)


def normalize(x):
    centered = x - jnp.mean(x, axis=-1, keepdims=True)
    variance = jnp.mean(centered * centered, axis=-1, keepdims=True)
    return centered * lax.rsqrt(variance + NORM_EPS)


def modulated(x, vec_ref, sel, shift, scale):
    return ((1.0 + row_of(vec_ref, sel, scale)) * normalize(x) + row_of(vec_ref, sel, shift)).astype(BF16)


def mods_kernel(vec_ref, bt_ref, bi_ref, pt_ref, pi_ref, ft_ref, fi_ref, wt_hbm, wi_hbm, out_ref, wbuf, early, late, wsem, ssem, rsem):
    me = lax.axis_index('tp')
    batch, dim = vec_ref.shape
    width = wbuf.shape[3]
    n_dev = early.shape[0]
    barrier = pltpu.get_barrier_semaphore()
    for d in range(1, n_dev):
        pl.semaphore_signal(barrier, inc=1, device_id={'tp': (me + d) % n_dev}, device_id_type=MESH)

    def load(path, k):
        return pltpu.make_async_copy((wt_hbm, wi_hbm)[path].at[k], wbuf.at[path, k], wsem.at[path, k])

    for k in range(PROJ_B):
        for path in range(2):
            load(path, k).start()
    v = vec_ref[...].astype(F32)
    silu = (v * (1.0 / (1.0 + jnp.exp(-v)))).astype(BF16)
    pl.semaphore_wait(barrier, n_dev - 1)

    def compute(k, path):
        load(path, k).wait()
        acc = jnp.dot(silu, wbuf[path, k], preferred_element_type=F32)
        return (acc + (bt_ref, bi_ref)[path][k:k + 1, :].astype(F32)).astype(BF16)

    def send(part, buf, d):
        return pltpu.make_async_remote_copy(src_ref=buf.at[me], dst_ref=buf.at[me], send_sem=ssem.at[part, d], recv_sem=rsem.at[part, d], device_id={'tp': (me + d) % n_dev}, device_id_type=MESH)

    def receive(part, buf, d):
        ref = buf.at[(me + n_dev - d) % n_dev]
        return pltpu.make_async_remote_copy(src_ref=ref, dst_ref=ref, send_sem=ssem.at[part, d], recv_sem=rsem.at[part, d], device_id={'tp': (me + d) % n_dev}, device_id_type=MESH)

    early_kinds, late_kinds = (SHIFT1, SCALE1), (GATE1, SHIFT2, SCALE2, GATE2)
    early[me] = jnp.concatenate([compute(k, path) for k in early_kinds for path in range(2)], axis=0)
    for d in range(1, n_dev):
        send(0, early, d).start()
    late[me] = jnp.concatenate([compute(k, path) for k in late_kinds for path in range(2)], axis=0)
    for d in range(1, n_dev):
        send(1, late, d).start()

    def row(ref):
        return ref[...].astype(F32)

    for path, (pb, fb) in enumerate(((pt_ref, ft_ref), (pi_ref, fi_ref))):
        for b in range(batch):
            out_ref[path * batch + b, PROJ_B:FC2_B, :] = row(pb)
            out_ref[path * batch + b, FC2_B:, :] = row(fb)
    for part, buf, ks in ((0, early, early_kinds), (1, late, late_kinds)):
        for d in range(1, n_dev):
            send(part, buf, d).wait_send()
            receive(part, buf, d).wait_recv()
        for j in range(n_dev):
            for n, k in enumerate(ks):
                for path in range(2):
                    at = (n * 2 + path) * batch
                    block = buf[j, at:at + batch, :].astype(F32)
                    for b in range(batch):
                        out_ref[path * batch + b, k:k + 1, j * width:(j + 1) * width] = block[b:b + 1, :]


def mods_call(vec, wt, wi, bt, bi, pt, pi, ft, fi, n_dev):
    batch, dim = vec.shape
    width = wt.shape[2]
    vmem = pl.BlockSpec(memory_space=pltpu.VMEM)
    anywhere = pl.BlockSpec(memory_space=pl.ANY)
    return pl.pallas_call(
        mods_kernel,
        in_specs=[vmem] * 7 + [anywhere] * 2,
        out_specs=vmem,
        out_shape=jax.ShapeDtypeStruct((2 * batch, 8, dim), F32),
        scratch_shapes=[
            pltpu.VMEM((2, 6, dim, width), BF16),
            pltpu.VMEM((n_dev, 4 * batch, width), BF16),
            pltpu.VMEM((n_dev, 8 * batch, width), BF16),
            pltpu.SemaphoreType.DMA((2, 6)),
            pltpu.SemaphoreType.DMA((2, n_dev)),
            pltpu.SemaphoreType.DMA((2, n_dev)),
        ],
        compiler_params=pltpu.CompilerParams(collective_id=1, has_side_effects=True, vmem_limit_bytes=VMEM_BYTES),
        cost_estimate=pl.CostEstimate(flops=2 * batch * dim * 12 * width, bytes_accessed=24 * dim * width, transcendentals=0),
        name="mods",
    )(vec, bt, bi, pt[None, :], pi[None, :], ft[None, :], fi[None, :], wt, wi)

LOG2E = 1.4426950408889634
(W_FIRST, W_SECOND, W_RELAY, W_CORE, W_CORE_FIRST, W_CORE_SECOND, W_CORE_RELAY) = range(7)
(T_CORE, T_FIRST, T_SECOND, T_OUT_FIRST, T_OUT_SECOND, T_OUT_RELAY, T_CORE_OWN, T_CORE_FIRST, T_CORE_SECOND, T_CORE_RELAY) = range(10)
PIECES = 4
HEADS_HERE = 3


class Place:
    def __init__(self):
        me = lax.axis_index('tp')
        core = me % 2
        xi = (me // 2) % 2
        yi = me // 4
        x_next = me + 2 - 4 * xi
        y_next = me + 4 - 8 * yi
        self.me, self.core = me, core
        self.partner = me + 1 - 2 * core
        self.first = x_next * (1 - core) + y_next * core
        self.second = x_next * core + y_next * (1 - core)
        self.diagonal = x_next + y_next - me
        self.bit1 = xi * (1 - core) + yi * core
        self.bit2 = xi * core + yi * (1 - core)

    def enter(self):
        barrier = pltpu.get_barrier_semaphore()
        for dev in (self.partner, self.first, self.second):
            pl.semaphore_signal(barrier, inc=1, device_id={'tp': dev}, device_id_type=MESH)
        pl.semaphore_wait(barrier, 3)


def rows_at(start, size):
    return pl.ds(pl.multiple_of(start, size), size)


def front_kernel(cfg, txt_hbm, img_hbm, wt_hbm, wi_hbm, pw_hbm, tw_hbm, vec_ref, bias_ref, gain_ref, ids_ref, tab_ref,
                 o_hbm, wp_hbm, ut_hbm, x1_ref,
                 w, xs, ua, ub, qkv, s0, s1, s2, o_all, tw, t_send, t_recv, t_own, t_sum, t_rs1, t_rs2_out, t_rs2_in, t_keep, t_x, t_u,
                 wsem, xsem, osem, tsem, psend, precv, tsend, trecv):
    batch, txt_len, img_len, rows = cfg
    half, quarter, eighth = rows // 2, rows // 4, rows // 8
    total = txt_len + img_len
    per_img = img_len // rows
    blocks = batch * (per_img + 1)
    dim = w.shape[1]
    width = o_all.shape[1]
    heads = width // HEAD
    place = Place()
    me, core, partner, first, second, diagonal, bit1, bit2 = place.me, place.core, place.partner, place.first, place.second, place.diagonal, place.bit1, place.bit2
    piece = width // PIECES

    def position(n):
        n = jnp.int32(n)
        img = (n >= batch).astype(jnp.int32)
        m = n - batch
        b = (1 - img) * n + img * (m // per_img)
        r = img * (1 + m % per_img)
        return b, r * rows

    def x_copy(n, source):
        b, r0 = position(n)
        ref = txt_hbm.at[b] if source == 0 else img_hbm.at[b, rows_at(r0 - rows, rows), :]
        return pltpu.make_async_copy(ref, xs.at[n % 4], xsem.at[n % 4])

    def x_start(n):
        @pl.when(n < batch)
        def _():
            x_copy(n, 0).start()

        @pl.when((n >= batch) & (n < blocks))
        def _():
            x_copy(n, 1).start()

    def x_wait(n):
        @pl.when(n < blocks)
        def _():
            pltpu.make_async_copy(txt_hbm.at[0], xs.at[n % 4], xsem.at[n % 4]).wait()

    def w_load(path, j):
        return pltpu.make_async_copy((wt_hbm, wi_hbm)[path].at[j], w.at[path, :, j * width:(j + 1) * width], wsem.at[path, j])

    for path in range(2):
        for j in range(3):
            w_load(path, j).start()
            if path == 0 and j == 0:
                for n in range(3):
                    x_copy(n, 0 if n < batch else 1).start()
    tw_load = pltpu.make_async_copy(tw_hbm, tw, tsem.at[0])
    tw_load.start()
    place.enter()

    def piece_at(j):
        return rows_at(j * piece, piece)

    def remote(sends, recvs, kind, j, src, dst, dev):
        return pltpu.make_async_remote_copy(src_ref=src, dst_ref=dst, send_sem=sends.at[kind, j], recv_sem=recvs.at[kind, j], device_id={'tp': dev}, device_id_type=MESH)

    def p_copy(kind, j, owner, dev):
        dst = wp_hbm.at[owner, piece_at(j), :]
        src = pw_hbm.at[piece_at(j), :] if kind in (W_FIRST, W_SECOND, W_CORE) else dst
        return remote(psend, precv, kind, j, src, dst, dev)

    def w_relay(j):
        p_copy(W_FIRST, j, first, first).wait_recv()
        p_copy(W_RELAY, j, first, second).start()
        p_copy(W_CORE_FIRST, j, first, partner).start()

    def w_second(j):
        p_copy(W_SECOND, j, second, second).wait_recv()
        p_copy(W_CORE_SECOND, j, second, partner).start()

    def w_last(j):
        p_copy(W_RELAY, j, diagonal, second).wait_recv()
        p_copy(W_CORE_RELAY, j, diagonal, partner).start()

    for j in range(PIECES):
        p_copy(W_FIRST, j, me, first).start()
        p_copy(W_SECOND, j, me, second).start()
    for j in range(PIECES):
        p_copy(W_CORE, j, me, partner).start()

    even = lax.broadcasted_iota(jnp.int32, (rows, HEAD), 1) % 2 == 0
    code = lax.broadcasted_iota(jnp.int32, (N_IDS, rows), 0)

    def select(n):
        n = jnp.int32(n)
        img = (n >= batch).astype(jnp.int32)
        return (1 - img) * n + img * (batch + (n - batch) // per_img)

    def norm(n, u):
        u[...] = modulated(xs[n % 4].astype(F32), vec_ref, select(n), SHIFT1, SCALE1)

    def heads_of(n, u):
        b, r0 = position(n)
        path = (jnp.int32(n) >= batch).astype(jnp.int32)
        hot = jnp.concatenate([(ids_ref[b, axis:axis + 1, rows_at(r0, rows)] == code).astype(F32).astype(BF16) for axis in range(3)], axis=0)
        parts = lax.dot_general(hot, tab_ref[...], (((0,), (0,)), ((), ())), preferred_element_type=F32)
        cos_t, sin_t = (sum(parts[:, (3 * i + j) * HEAD:(3 * i + j + 1) * HEAD] for j in range(3)) for i in range(2))
        at = rows_at(b * total + r0, rows)
        for c0 in range(0, 3 * heads, 4):
            c1 = min(c0 + 4, 3 * heads)
            a = jnp.dot(u[...], w[path, :, c0 * HEAD:c1 * HEAD], preferred_element_type=F32) + bias_ref[path, 0:1, c0 * HEAD:c1 * HEAD]
            for c in range(c0, c1):
                t = a[:, (c - c0) * HEAD:(c - c0 + 1) * HEAD]
                kind = c // heads
                if kind < 2:
                    mean_sq = jnp.mean(t * t, axis=-1, keepdims=True)
                    t = t * lax.rsqrt(mean_sq + NORM_EPS) * gain_ref[path, kind:kind + 1, :]
                    swapped = jnp.where(even, pltpu.roll(t, HEAD - 1, 1), pltpu.roll(t, 1, 1))
                    t = t * cos_t + swapped * sin_t
                qkv[c, at, :] = t.astype(BF16)

    x_wait(0)
    norm(0, ua)
    for path in range(2):
        for j in range(3):
            w_load(path, j).wait()

    def qkv_step(t):
        x_start(2 * t + 3)
        x_start(2 * t + 4)
        x_wait(2 * t + 1)
        x_wait(2 * t + 2)
        for j, when in enumerate(QKV_RELAY):
            @pl.when(t == when)
            def _():
                w_relay(j)
        norm(2 * t + 1, ub)
        heads_of(2 * t, ua)
        norm(jnp.minimum(2 * t + 2, blocks - 1), ua)
        heads_of(2 * t + 1, ub)

    loop(blocks // 2, qkv_step)

    factor = HEAD ** -0.5 * LOG2E

    def scores(n, h, s):
        b, r0 = position(n)
        q = qkv[h, rows_at(b * total + r0, rows), :]
        k = qkv[heads + h, pl.ds(pl.multiple_of(b * total, rows), total), :]
        s[...] = lax.dot_general(q, k, (((1,), (1,)), ((), ())), preferred_element_type=F32)

    def weigh(n, h, s):
        b, r0 = position(n)
        v = qkv[2 * heads + h, pl.ds(pl.multiple_of(b * total, rows), total), :]
        top = jnp.max(s[...], axis=-1, keepdims=True)
        p = jnp.exp2((s[...] - top) * factor)
        denom = jnp.sum(p, axis=-1, keepdims=True)
        o = jnp.dot(p.astype(BF16), v, preferred_element_type=F32)
        o_all[rows_at(b * total + r0, rows), h * HEAD:(h + 1) * HEAD] = (o * (1.0 / denom)).astype(BF16)

    def t_copy(kind, src, dst, dev):
        return remote(tsend, trecv, kind, 0, src, dst, dev)

    def t_core():
        return t_copy(T_CORE, t_send, t_recv, partner)

    def t_first():
        return t_copy(T_FIRST, t_sum.at[:, rows_at((1 - bit1) * quarter, quarter), :], t_rs1, first)

    def t_second():
        return t_copy(T_SECOND, t_rs2_out, t_rs2_in, second)

    def own_rows(b1, b2):
        return rows_at(core * half + b1 * quarter + b2 * eighth, eighth)

    def t_out(kind, b1, b2, dev):
        ref = ut_hbm.at[:, own_rows(b1, b2), :]
        return t_copy(kind, t_u if kind in (T_OUT_FIRST, T_OUT_SECOND, T_CORE_OWN) else ref, ref, dev)

    def t_local():
        return pltpu.make_async_copy(t_u, ut_hbm.at[:, own_rows(bit1, bit2), :], tsem.at[1])

    def t_load(b):
        return pltpu.make_async_copy(txt_hbm.at[b, own_rows(bit1, bit2), :], t_x.at[b], tsem.at[2 + b])

    tile = min(512, dim)

    def text_partial():
        tw_load.wait()
        for b in range(batch):
            t_load(b).start()

            def theirs(n):
                at = rows_at(n * tile, tile)
                t_send[b, :, at] = jnp.dot(o_all[rows_at(b * total + (1 - core) * half, half), :], tw[:, at], preferred_element_type=F32).astype(BF16)

            loop(dim // tile, theirs)
        t_core().start()
        for b in range(batch):
            def mine(n):
                at = rows_at(n * tile, tile)
                t_own[b, :, at] = jnp.dot(o_all[rows_at(b * total + core * half, half), :], tw[:, at], preferred_element_type=F32)

            loop(dim // tile, mine)

    def text_sum():
        t_core().wait()
        for b in range(batch):
            def add(n):
                at = rows_at(n * 16, 16)
                t_sum[b, at, :] = (t_own[b, at, :] + t_recv[b, at, :].astype(F32)).astype(BF16)

            loop(half // 16, add)
        t_first().start()

    def text_quarter():
        t_first().wait()
        for b in range(batch):
            t_rs2_out[b] = (t_sum[b, rows_at(bit1 * quarter + (1 - bit2) * eighth, eighth), :].astype(F32) + t_rs1[b, rows_at((1 - bit2) * eighth, eighth), :].astype(F32)).astype(BF16)
            t_keep[b] = t_sum[b, rows_at(bit1 * quarter + bit2 * eighth, eighth), :].astype(F32) + t_rs1[b, rows_at(bit2 * eighth, eighth), :].astype(F32)
        t_second().start()

    def text_finish():
        t_second().wait()
        for b in range(batch):
            t_load(b).wait()
            branch = t_keep[b] + t_rs2_in[b].astype(F32) + row_of(vec_ref, b, PROJ_B)
            x1 = (t_x[b].astype(F32) + row_of(vec_ref, b, GATE1) * branch).astype(BF16)
            x1_ref[b] = x1
            t_u[b] = modulated(x1.astype(F32), vec_ref, b, SHIFT2, SCALE2)
        t_out(T_OUT_FIRST, bit1, bit2, first).start()
        t_out(T_OUT_SECOND, bit1, bit2, second).start()
        t_out(T_CORE_OWN, bit1, bit2, partner).start()
        t_local().start()

    def text_relay():
        t_out(T_OUT_FIRST, 1 - bit1, bit2, first).wait_recv()
        t_out(T_OUT_RELAY, 1 - bit1, bit2, second).start()
        t_out(T_CORE_FIRST, 1 - bit1, bit2, partner).start()
        t_out(T_OUT_SECOND, bit1, 1 - bit2, second).wait_recv()
        t_out(T_CORE_SECOND, bit1, 1 - bit2, partner).start()

    def text_last():
        t_out(T_OUT_RELAY, 1 - bit1, 1 - bit2, second).wait_recv()
        t_out(T_CORE_RELAY, 1 - bit1, 1 - bit2, partner).start()

    hooks = {
        1: [functools.partial(w_relay, 2)],
        2: [text_partial],
        3: [text_sum, functools.partial(w_relay, 3)],
        6: [text_quarter, functools.partial(w_second, 0), functools.partial(w_second, 1)],
        8: [text_finish, functools.partial(w_second, 2), functools.partial(w_second, 3)],
        11: [text_relay, functools.partial(w_last, 0)],
        14: [text_last, functools.partial(w_last, 1)],
        15: [functools.partial(w_last, 2)],
    }

    def o_store(n):
        b, r0 = position(n)
        return pltpu.make_async_copy(o_all.at[rows_at(b * total + r0, rows), :], o_hbm.at[b, rows_at(r0, rows), :], osem.at[n % 4])

    scores(0, 0, s0)

    def attention_step(n):
        for when, calls in hooks.items():
            @pl.when(n == min(when, blocks - 1))
            def _():
                for call in calls:
                    call()

        @pl.when(n >= 4)
        def _():
            o_store(n - 4).wait()

        scores(n, 1, s1)
        weigh(n, 0, s0)
        scores(n, 2, s2)
        weigh(n, 1, s1)
        scores(jnp.minimum(n + 1, blocks - 1), 0, s0)
        weigh(n, 2, s2)
        o_store(n).start()

    loop(blocks, attention_step)

    w_last(3)
    for n in range(blocks - 4, blocks):
        o_store(n).wait()
    t_local().wait()
    for kind, b1, b2, dev in ((T_OUT_FIRST, bit1, bit2, first), (T_OUT_SECOND, bit1, bit2, second), (T_OUT_RELAY, 1 - bit1, bit2, second)):
        t_out(kind, b1, b2, dev).wait_send()
    for kind, b1, b2 in ((T_CORE_OWN, bit1, bit2), (T_CORE_FIRST, 1 - bit1, bit2), (T_CORE_SECOND, bit1, 1 - bit2), (T_CORE_RELAY, 1 - bit1, 1 - bit2)):
        t_out(kind, b1, b2, partner).wait()
    for j in range(PIECES):
        for kind, owner, dev in ((W_FIRST, me, first), (W_SECOND, me, second), (W_RELAY, first, second)):
            p_copy(kind, j, owner, dev).wait_send()
        for kind, owner in ((W_CORE, me), (W_CORE_FIRST, first), (W_CORE_SECOND, second), (W_CORE_RELAY, diagonal)):
            p_copy(kind, j, owner, partner).wait()


QKV_RELAY = (4, 7)


def front_call(txt, img, wt, wi, pw, tw, vecs, bias, gains, ids_t, table, n_dev, rows):
    batch, txt_len, dim = txt.shape
    img_len = img.shape[1]
    total = txt_len + img_len
    width = pw.shape[0]
    heads = width // HEAD
    half, quarter, eighth = rows // 2, rows // 4, rows // 8
    assert heads == HEADS_HERE or heads == 1
    cfg = (batch, txt_len, img_len, rows)
    vmem = pl.BlockSpec(memory_space=pltpu.VMEM)
    anywhere = pl.BlockSpec(memory_space=pl.ANY)
    flops = 2 * batch * total * dim * 3 * width + 8 * batch * heads * total * total * HEAD
    return pl.pallas_call(
        functools.partial(front_kernel, cfg),
        in_specs=[anywhere] * 6 + [vmem] * 5,
        out_specs=[anywhere, anywhere, anywhere, vmem],
        out_shape=[
            jax.ShapeDtypeStruct((batch, total, width), BF16),
            jax.ShapeDtypeStruct((n_dev, width, dim), BF16),
            jax.ShapeDtypeStruct((batch, txt_len, dim), BF16),
            jax.ShapeDtypeStruct((batch, eighth, dim), BF16),
        ],
        scratch_shapes=[
            pltpu.VMEM((2, dim, 3 * width), BF16),
            pltpu.VMEM((4, rows, dim), BF16),
            pltpu.VMEM((rows, dim), BF16),
            pltpu.VMEM((rows, dim), BF16),
            pltpu.VMEM((3 * heads, batch * total, HEAD), BF16),
            pltpu.VMEM((rows, total), F32),
            pltpu.VMEM((rows, total), F32),
            pltpu.VMEM((rows, total), F32),
            pltpu.VMEM((batch * total, width), BF16),
            pltpu.VMEM((width, dim), BF16),
            pltpu.VMEM((batch, half, dim), BF16),
            pltpu.VMEM((batch, half, dim), BF16),
            pltpu.VMEM((batch, half, dim), F32),
            pltpu.VMEM((batch, half, dim), BF16),
            pltpu.VMEM((batch, quarter, dim), BF16),
            pltpu.VMEM((batch, eighth, dim), BF16),
            pltpu.VMEM((batch, eighth, dim), BF16),
            pltpu.VMEM((batch, eighth, dim), F32),
            pltpu.VMEM((batch, eighth, dim), BF16),
            pltpu.VMEM((batch, eighth, dim), BF16),
            pltpu.SemaphoreType.DMA((2, 3)),
            pltpu.SemaphoreType.DMA((4,)),
            pltpu.SemaphoreType.DMA((4,)),
            pltpu.SemaphoreType.DMA((4,)),
            pltpu.SemaphoreType.DMA((7, PIECES)),
            pltpu.SemaphoreType.DMA((7, PIECES)),
            pltpu.SemaphoreType.DMA((10, 1)),
            pltpu.SemaphoreType.DMA((10, 1)),
        ],
        compiler_params=pltpu.CompilerParams(collective_id=2, has_side_effects=True, vmem_limit_bytes=VMEM_BYTES),
        cost_estimate=pl.CostEstimate(flops=flops, bytes_accessed=2 * batch * total * (dim + width), transcendentals=batch * heads * total * total),
        name="front",
    )(txt, img, wt, wi, pw, tw, vecs, bias, gains, ids_t, table)


(O_CORE, O_FIRST, O_SECOND, O_RELAY, U_CORE, PART_CORE, RS_FIRST, RS_SECOND, OUT_FIRST, OUT_SECOND, OUT_RELAY, CORE_OWN, CORE_FIRST, CORE_SECOND, CORE_RELAY) = range(15)
(L_O, L_X, L_OUT) = range(3)
SLOTS = 4
SEMS = 8


def block_kernel(cfg, o_hbm, x_hbm, ut_hbm, x1t_hbm, wp_hbm, pw_hbm, w1t_hbm, w2t_hbm, w1i_hbm, w2i_hbm, vec_ref, fb_ref, out_hbm,
                 wp, w1, w2, obuf, xbuf, x1buf, x1keep, u2, hid, psend, precv, own, chip_sum, rs1, keep2, rs2_out, rs2_in, outb,
                 wsem, lsem, tsem, ssem, rsem):
    batch, txt_chunks, img_chunks, per_img, rows, tile = cfg
    half, quarter, eighth = rows // 2, rows // 4, rows // 8
    dim = wp.shape[0]
    ff = w1.shape[1]
    cols = o_hbm.shape[2]
    total = txt_chunks + img_chunks
    per_txt = txt_chunks // batch

    place = Place()
    me, core, partner, first, second, bit1, bit2 = place.me, place.core, place.partner, place.first, place.second, place.bit1, place.bit2
    txt_len = ut_hbm.shape[1]
    place.enter()

    def remote(kind, g, src, dst, dev):
        return pltpu.make_async_remote_copy(src_ref=src, dst_ref=dst, send_sem=ssem.at[kind, g % SEMS], recv_sem=rsem.at[kind, g % SEMS], device_id={'tp': dev}, device_id_type=MESH)

    def img_pos(g):
        k = g - txt_chunks
        return k // per_img, (k % per_img) * rows

    def chip_cols(dev):
        return rows_at((dev // 2) * (2 * cols), 2 * cols)

    def own_rows(b1, b2):
        return core * half + b1 * quarter + b2 * eighth

    def o_local(g):
        b, r0 = img_pos(g)
        return pltpu.make_async_copy(o_hbm.at[b, rows_at(txt_len + r0 + core * half, half), :], obuf.at[g % SLOTS, :, rows_at(me * cols, cols)], lsem.at[L_O, g % SEMS])

    def o_core(g):
        b, r0 = img_pos(g)
        return remote(O_CORE, g, o_hbm.at[b, rows_at(txt_len + r0 + (1 - core) * half, half), :], obuf.at[g % SLOTS, :, rows_at(me * cols, cols)], partner)

    def o_send(kind, g, owner, dev):
        ref = obuf.at[g % SLOTS, :, chip_cols(owner)]
        return remote(kind, g, ref, ref, dev)

    def x_load(g):
        b, r0 = img_pos(g)
        return pltpu.make_async_copy(x_hbm.at[b, rows_at(r0 + core * half, half), :], xbuf.at[g % 2], lsem.at[L_X, g % SEMS])

    def u_core(g):
        ref = u2.at[g % 2, rows_at(core * half, half), :]
        return remote(U_CORE, g, ref, ref, partner)

    def part_core(g):
        return remote(PART_CORE, g, psend, precv.at[g % 2], partner)

    def rs_first(g):
        return remote(RS_FIRST, g, chip_sum.at[rows_at((1 - bit1) * quarter, quarter), :], rs1.at[g % 2], first)

    def rs_second(g):
        return remote(RS_SECOND, g, rs2_out.at[g % 2], rs2_in.at[g % SLOTS], second)

    def out_ref(g, b1, b2):
        return out_hbm.at[rows_at(g * rows + own_rows(b1, b2), eighth), :]

    def out_send(kind, g, b1, b2, dev):
        ref = out_ref(g, b1, b2)
        mine = kind in (OUT_FIRST, OUT_SECOND, CORE_OWN)
        return remote(kind, g, outb.at[g % SLOTS] if mine else ref, ref, dev)

    def out_local(g):
        return pltpu.make_async_copy(outb.at[g % SLOTS], out_ref(g, bit1, bit2), lsem.at[L_OUT, g % SEMS])

    def txt_load(g):
        b, r0 = g // per_txt, (g % per_txt) * rows
        return (pltpu.make_async_copy(ut_hbm.at[b, rows_at(r0, rows), :], u2.at[g % 2], tsem.at[0, g % 2]),
                pltpu.make_async_copy(x1t_hbm.at[g], x1keep.at[g % SLOTS], tsem.at[1, g % 2]))

    def w_load(k, src, dst):
        return pltpu.make_async_copy(src, dst, wsem.at[k])

    def wp_load(j, src):
        return pltpu.make_async_copy(src, wp.at[j * cols:(j + 1) * cols, :], wsem.at[2 + j])

    def select(g):
        txt = (g < txt_chunks).astype(jnp.int32)
        return txt * (g // per_txt) + (1 - txt) * (batch + (g - txt_chunks) // per_img)

    def start_o(g):
        o_local(g).start()
        o_core(g).start()

    def send_o(g):
        o_local(g).wait()
        o_core(g).wait()
        o_send(O_FIRST, g, me, first).start()
        o_send(O_SECOND, g, me, second).start()

    def relay_o(g):
        o_send(O_FIRST, g, first, first).wait_recv()
        o_send(O_RELAY, g, first, second).start()
        x_load(g).start()

    def project(g):
        o_send(O_FIRST, g, me, first).wait_send()
        o_send(O_SECOND, g, me, second).wait_send()
        o_send(O_RELAY, g, first, second).wait_send()
        o_send(O_SECOND, g, second, second).wait_recv()
        o_send(O_RELAY, g, second, second).wait_recv()
        x_load(g).wait()

        @pl.when(g == txt_chunks)
        def _():
            for j in range(wp_hbm.shape[0]):
                wp_load(j, wp_hbm.at[j]).wait()

        sel = select(g)
        slot = g % SLOTS

        def columns(n):
            at = rows_at(n * tile, tile)
            acc = jnp.dot(obuf[slot], wp[:, at], preferred_element_type=F32)
            branch = acc + row_of(vec_ref, sel, PROJ_B, at)
            x1buf[:, at] = (xbuf[g % 2, :, at].astype(F32) + row_of(vec_ref, sel, GATE1, at) * branch).astype(BF16)

        loop(dim // tile, columns)

        def norm(n):
            at = rows_at(n * 16, 16)
            u2[g % 2, rows_at(core * half + n * 16, 16), :] = modulated(x1buf[at, :].astype(F32), vec_ref, sel, SHIFT2, SCALE2)

        loop(half // 16, norm)
        u_core(g).start()
        x1keep[slot] = x1buf[rows_at(bit1 * quarter + bit2 * eighth, eighth), :]

    def mlp(g):
        @pl.when(g < txt_chunks)
        def _():
            for copy in txt_load(g):
                copy.wait()

        @pl.when(g >= txt_chunks)
        def _():
            u_core(g).wait()

        @pl.when(g == 0)
        def _():
            w_load(0, w1t_hbm, w1).wait()
            w_load(1, w2t_hbm, w2).wait()

        @pl.when(g == txt_chunks)
        def _():
            w_load(0, w1i_hbm, w1).wait()
            w_load(1, w2i_hbm, w2).wait()

        path = (g >= txt_chunks).astype(jnp.int32)

        def hidden(n):
            at = rows_at(n * tile, tile)
            acc = jnp.dot(u2[g % 2], w1[:, at], preferred_element_type=F32)
            pre = acc + fb_ref[path, 0:1, at]
            hid[:, at] = jax.nn.gelu(pre, approximate=True).astype(BF16)

        loop(ff // tile, hidden)

        def theirs(n):
            at = rows_at(n * tile, tile)
            psend[:, at] = jnp.dot(hid[rows_at((1 - core) * half, half), :], w2[:, at], preferred_element_type=F32).astype(BF16)

        loop(dim // tile, theirs)
        part_core(g).start()

        def mine(n):
            at = rows_at(n * tile, tile)
            own[:, at] = jnp.dot(hid[rows_at(core * half, half), :], w2[:, at], preferred_element_type=F32)

        loop(dim // tile, mine)

        @pl.when(g == txt_chunks - 1)
        def _():
            w_load(0, w1i_hbm, w1).start()
            w_load(1, w2i_hbm, w2).start()

        part_core(g).wait()

        def add(n):
            at = rows_at(n * 16, 16)
            chip_sum[at, :] = (own[at, :] + precv[g % 2, at, :].astype(F32)).astype(BF16)

        loop(half // 16, add)
        rs_first(g).start()

    def add_first(g):
        rs_first(g).wait()
        rs2_out[g % 2] = (chip_sum[rows_at(bit1 * quarter + (1 - bit2) * eighth, eighth), :].astype(F32) + rs1[g % 2, rows_at((1 - bit2) * eighth, eighth), :].astype(F32)).astype(BF16)
        rs_second(g).start()
        keep2[g % 2] = chip_sum[rows_at(bit1 * quarter + bit2 * eighth, eighth), :].astype(F32) + rs1[g % 2, rows_at(bit2 * eighth, eighth), :].astype(F32)

    def finish(g):
        rs_second(g).wait()
        sel = select(g)
        branch = keep2[g % 2] + rs2_in[g % SLOTS].astype(F32) + row_of(vec_ref, sel, FC2_B)
        outb[g % SLOTS] = (x1keep[g % SLOTS].astype(F32) + row_of(vec_ref, sel, GATE2) * branch).astype(BF16)
        out_send(OUT_FIRST, g, bit1, bit2, first).start()
        out_send(OUT_SECOND, g, bit1, bit2, second).start()
        out_send(CORE_OWN, g, bit1, bit2, partner).start()
        out_local(g).start()

    def relay_out(g):
        out_send(OUT_FIRST, g, 1 - bit1, bit2, first).wait_recv()
        out_send(OUT_RELAY, g, 1 - bit1, bit2, second).start()
        out_send(CORE_FIRST, g, 1 - bit1, bit2, partner).start()
        out_send(OUT_SECOND, g, bit1, 1 - bit2, second).wait_recv()
        out_send(CORE_SECOND, g, bit1, 1 - bit2, partner).start()

    def relay_core(g):
        out_send(OUT_RELAY, g, 1 - bit1, 1 - bit2, second).wait_recv()
        out_send(CORE_RELAY, g, 1 - bit1, 1 - bit2, partner).start()

    def drain(g):
        out_local(g).wait()
        out_send(OUT_FIRST, g, bit1, bit2, first).wait_send()
        out_send(OUT_SECOND, g, bit1, bit2, second).wait_send()
        out_send(OUT_RELAY, g, 1 - bit1, bit2, second).wait_send()
        out_send(CORE_OWN, g, bit1, bit2, partner).wait()
        out_send(CORE_FIRST, g, 1 - bit1, bit2, partner).wait()
        out_send(CORE_SECOND, g, bit1, 1 - bit2, partner).wait()
        out_send(CORE_RELAY, g, 1 - bit1, 1 - bit2, partner).wait()

    w_load(0, w1t_hbm, w1).start()
    w_load(1, w2t_hbm, w2).start()
    for g in range(txt_chunks):
        for copy in txt_load(g):
            copy.start()
    for j in range(wp_hbm.shape[0]):
        @pl.when(j != me)
        def _():
            wp_load(j, wp_hbm.at[j]).start()

        @pl.when(j == me)
        def _():
            wp_load(j, pw_hbm).start()

    stages = ((start_o, 4, txt_chunks), (send_o, 3, txt_chunks), (relay_o, 2, txt_chunks), (relay_out, -3, 0), (relay_core, -4, 0), (drain, -5, 0),
              (project, 1, txt_chunks), (add_first, -1, 0), (finish, -2, 0), (mlp, 0, 0))
    lead = 4 - txt_chunks

    def step(i):
        for stage, ahead, lowest in stages:
            g = i - lead + ahead

            @pl.when((g >= lowest) & (g < total))
            def _():
                stage(g)

    loop(total + lead + 5, step)


def block_call(img_o, x, u_txt, x1_txt, wp, pw, w1t, w2t, w1i, w2i, vecs, fb, rows):
    batch, img_len, dim = x.shape
    txt_len = u_txt.shape[1]
    ff = w1t.shape[1]
    txt_chunks = batch * (txt_len // rows)
    per_img = img_len // rows
    img_chunks = batch * per_img
    assert txt_chunks == 2
    half, quarter, eighth = rows // 2, rows // 4, rows // 8
    cfg = (batch, txt_chunks, img_chunks, per_img, rows, 512)
    total = txt_chunks + img_chunks
    anywhere = pl.BlockSpec(memory_space=pl.ANY)
    flops = 2 * total * rows * 2 * dim * ff + 2 * img_chunks * half * dim * dim
    return pl.pallas_call(
        functools.partial(block_kernel, cfg),
        in_specs=[anywhere] * 10 + [pl.BlockSpec(memory_space=pltpu.VMEM)] * 2,
        out_specs=anywhere,
        out_shape=jax.ShapeDtypeStruct((total * rows, dim), BF16),
        scratch_shapes=[
            pltpu.VMEM((dim, dim), BF16),
            pltpu.VMEM((dim, ff), BF16),
            pltpu.VMEM((ff, dim), BF16),
            pltpu.VMEM((SLOTS, half, dim), BF16),
            pltpu.VMEM((2, half, dim), BF16),
            pltpu.VMEM((half, dim), BF16),
            pltpu.VMEM((SLOTS, eighth, dim), BF16),
            pltpu.VMEM((2, rows, dim), BF16),
            pltpu.VMEM((rows, ff), BF16),
            pltpu.VMEM((half, dim), BF16),
            pltpu.VMEM((2, half, dim), BF16),
            pltpu.VMEM((half, dim), F32),
            pltpu.VMEM((half, dim), BF16),
            pltpu.VMEM((2, quarter, dim), BF16),
            pltpu.VMEM((2, eighth, dim), F32),
            pltpu.VMEM((2, eighth, dim), BF16),
            pltpu.VMEM((SLOTS, eighth, dim), BF16),
            pltpu.VMEM((SLOTS, eighth, dim), BF16),
            pltpu.SemaphoreType.DMA((10,)),
            pltpu.SemaphoreType.DMA((3, SEMS)),
            pltpu.SemaphoreType.DMA((2, 2)),
            pltpu.SemaphoreType.DMA((15, SEMS)),
            pltpu.SemaphoreType.DMA((15, SEMS)),
        ],
        compiler_params=pltpu.CompilerParams(collective_id=0, has_side_effects=True, vmem_limit_bytes=VMEM_BYTES),
        cost_estimate=pl.CostEstimate(flops=flops, bytes_accessed=4 * dim * dim + 8 * dim * ff + 4 * total * rows * dim, transcendentals=0),
        name="block",
    )(img_o, x, u_txt, x1_txt, wp, pw, w1t, w2t, w1i, w2i, vecs, fb)


def copy_kernel(pieces, flat_hbm, *rest):
    outs, (buf, isem, osem) = rest[:-3], rest[-3:]
    rows = buf.shape[1]
    loads = []
    for n, (which, b, r) in enumerate(pieces):
        load = pltpu.make_async_copy(flat_hbm.at[n * rows:(n + 1) * rows, :], buf.at[n], isem.at[n])
        load.start()
        loads.append(load)
    stores = []
    for n, (which, b, r) in enumerate(pieces):
        loads[n].wait()
        store = pltpu.make_async_copy(buf.at[n], outs[which].at[b, r:r + rows, :], osem.at[n])
        store.start()
        stores.append(store)
    for store in stores:
        store.wait()


def copy_call(flat, shapes, rows):
    pieces = [(which, b, r) for which, shape in enumerate(shapes) for b in range(shape[0]) for r in range(0, shape[1], rows)]
    anywhere = pl.BlockSpec(memory_space=pl.ANY)
    dim = flat.shape[1]
    return pl.pallas_call(
        functools.partial(copy_kernel, pieces),
        in_specs=[anywhere],
        out_specs=[anywhere] * len(shapes),
        out_shape=[jax.ShapeDtypeStruct(shape, flat.dtype) for shape in shapes],
        scratch_shapes=[
            pltpu.VMEM((len(pieces), rows, dim), flat.dtype),
            pltpu.SemaphoreType.DMA((len(pieces),)),
            pltpu.SemaphoreType.DMA((len(pieces),)),
        ],
        compiler_params=pltpu.CompilerParams(vmem_limit_bytes=VMEM_BYTES),
        cost_estimate=pl.CostEstimate(flops=0, bytes_accessed=4 * flat.shape[0] * dim, transcendentals=0),
        name="copy_out",
    )(flat)


def local_block(img, txt, vec, ids, img_w, txt_w):
    n_dev = 8
    batch, txt_len = txt.shape[:2]
    rows = txt_len

    def by_kind(weight):
        return jnp.transpose(weight, (1, 0, 2))

    def both(pick):
        return jnp.stack([pick(txt_w), pick(img_w)]).astype(F32)

    vecs = mods_call(vec, by_kind(txt_w[0]), by_kind(img_w[0]), txt_w[1], img_w[1], txt_w[7], img_w[7], txt_w[11], img_w[11], n_dev)
    bias = both(lambda w: w[3].reshape(1, -1))
    gains = both(lambda w: jnp.stack([w[4], w[5]]))
    fb = both(lambda w: w[9][None, :])
    table = jnp.asarray(rope_table())
    ids_t = jnp.swapaxes(ids, 1, 2)
    o, proj_w, txt_u, txt_x1 = front_call(txt, img, by_kind(txt_w[2]), by_kind(img_w[2]), img_w[6], txt_w[6], vecs, bias, gains, ids_t, table, n_dev, rows)
    flat = block_call(o, img, txt_u, txt_x1, proj_w, img_w[6], txt_w[8], txt_w[10], img_w[8], img_w[10], vecs, fb, rows)
    txt_out, img_out = copy_call(flat, (txt.shape, img.shape), rows)
    return img_out, txt_out


def solution(mesh):
    act_spec = P('dp', WHOLE, WHOLE)
    mapped = jax.shard_map(local_block, mesh=mesh, in_specs=(act_spec, act_spec, P('dp', WHOLE), act_spec, PATH_SPECS, PATH_SPECS), out_specs=(act_spec, act_spec), check_vma=False)

    def forward(img, txt, vec, ids, *weights):
        return mapped(img, txt, vec, ids, weights[:12], weights[12:])

    return forward
```

```python
import functools

import jax
import jax.numpy as jnp
import numpy as np
from jax import lax
from jax.experimental import pallas as pl
from jax.experimental.pallas import tpu as pltpu
from jax.sharding import PartitionSpec as P

HEAD = 128
NORM_EPS = 1e-6
ROPE_THETA = 10000.0
AXES_DIM = (16, 56, 56)
N_IDS = 64
WHOLE = None
PATH_SPECS = (P(WHOLE, WHOLE, 'tp'), P(WHOLE, 'tp'), P(WHOLE, WHOLE, 'tp'), P(WHOLE, 'tp'), P(WHOLE), P(WHOLE), P('tp', WHOLE), P(WHOLE), P(WHOLE, 'tp'), P('tp'), P('tp', WHOLE), P(WHOLE))
F32 = jnp.float32
BF16 = jnp.bfloat16


def rope_table():
    cos = np.zeros((3 * N_IDS, HEAD), np.float32)
    sin = np.zeros((3 * N_IDS, HEAD), np.float32)
    lane = 0
    for axis, dim in enumerate(AXES_DIM):
        inv_freq = np.float32(ROPE_THETA) ** (-np.arange(0, dim, 2, dtype=np.float32) / np.float32(dim))
        angles = np.arange(N_IDS, dtype=np.float32)[:, None] * inv_freq.astype(np.float32)
        rows = slice(axis * N_IDS, (axis + 1) * N_IDS)
        c = np.cos(angles.astype(np.float64)).astype(np.float32)
        s = np.sin(angles.astype(np.float64)).astype(np.float32)
        cos[rows, lane:lane + dim:2] = c
        cos[rows, lane + 1:lane + dim:2] = c
        sin[rows, lane:lane + dim:2] = -s
        sin[rows, lane + 1:lane + dim:2] = s
        lane += dim
    parts = []
    for table in (cos, sin):
        rest = table
        for _ in range(3):
            part = rest.astype(jnp.bfloat16)
            parts.append(np.asarray(part))
            rest = rest - np.asarray(part).astype(np.float32)
    return np.concatenate(parts, axis=1)


MESH = pl.DeviceIdType.MESH


SHIFT1, SCALE1, GATE1, SHIFT2, SCALE2, GATE2, PROJ_B, FC2_B = range(8)
QKV_B, Q_GAIN, K_GAIN, FC1_B = range(4)
VMEM_BYTES = 67043328


def row_of(ref, sel, row, at=slice(None)):
    return ref[sel, pl.ds(row, 1), at]


def loop(count, body):
    lax.fori_loop(0, count, lambda i, carry: (body(i), carry)[-1], 0)


def normalize(x):
    centered = x - jnp.mean(x, axis=-1, keepdims=True)
    variance = jnp.mean(centered * centered, axis=-1, keepdims=True)
    return centered * lax.rsqrt(variance + NORM_EPS)


def modulated(x, vec_ref, sel, shift, scale):
    return ((1.0 + row_of(vec_ref, sel, scale)) * normalize(x) + row_of(vec_ref, sel, shift)).astype(BF16)


def mods_kernel(vec_ref, small_t, small_i, wt_hbm, wi_hbm, vecs_ref, small_ref, wbuf, early, late, wsem, ssem, rsem):
    me = lax.axis_index('tp')
    batch = vec_ref.shape[0]
    width = wbuf.shape[-1]
    n_dev = early.shape[0]
    barrier = pltpu.get_barrier_semaphore()
    for d in range(1, n_dev):
        pl.semaphore_signal(barrier, inc=1, device_id={'tp': (me + d) % n_dev}, device_id_type=MESH)

    def load(path, k):
        return pltpu.make_async_copy((wt_hbm, wi_hbm)[path].at[k], wbuf.at[path, k], wsem.at[path, k])

    for k in range(PROJ_B):
        for path in range(2):
            load(path, k).start()
    v = vec_ref[...].astype(F32)
    silu = (v * (1.0 / (1.0 + jnp.exp(-v)))).astype(BF16)
    for path, (mod_b, qkv_b, q_gain, k_gain, proj_b, fc1_b, fc2_b) in enumerate((small_t, small_i)):
        for row, ref in ((PROJ_B, proj_b), (FC2_B, fc2_b)):
            vector = ref[...].astype(F32)[None, :]
            for b in range(batch):
                vecs_ref[path * batch + b, row:row + 1, :] = vector
        for row, ref in ((Q_GAIN, q_gain), (K_GAIN, k_gain), (FC1_B, fc1_b)):
            vector = ref[...].astype(F32)[None, :]
            small_ref[path, row:row + 1, :vector.shape[1]] = vector
        for j in range(qkv_b.shape[0]):
            small_ref[path, QKV_B:Q_GAIN, j * width:(j + 1) * width] = qkv_b[j:j + 1, :].astype(F32)
    pl.semaphore_wait(barrier, n_dev - 1)

    def compute(k, path):
        load(path, k).wait()
        acc = jnp.dot(silu, wbuf[path, k], preferred_element_type=F32)
        return (acc + (small_t, small_i)[path][0][k:k + 1, :].astype(F32)).astype(BF16)

    def send(part, buf, d):
        return pltpu.make_async_remote_copy(src_ref=buf.at[me], dst_ref=buf.at[me], send_sem=ssem.at[part, d], recv_sem=rsem.at[part, d], device_id={'tp': (me + d) % n_dev}, device_id_type=MESH)

    def receive(part, buf, d):
        ref = buf.at[(me + n_dev - d) % n_dev]
        return pltpu.make_async_remote_copy(src_ref=ref, dst_ref=ref, send_sem=ssem.at[part, d], recv_sem=rsem.at[part, d], device_id={'tp': (me + d) % n_dev}, device_id_type=MESH)

    parts = ((early, (SHIFT1, SCALE1)), (late, (GATE1, SHIFT2, SCALE2, GATE2)))
    for part, (buf, kinds) in enumerate(parts):
        buf[me] = jnp.concatenate([compute(k, path) for k in kinds for path in range(2)], axis=0)
        for d in range(1, n_dev):
            send(part, buf, d).start()
    for part, (buf, kinds) in enumerate(parts):
        for d in range(1, n_dev):
            send(part, buf, d).wait_send()
            receive(part, buf, d).wait_recv()
        for j in range(n_dev):
            for n, k in enumerate(kinds):
                for path in range(2):
                    at = (n * 2 + path) * batch
                    block = buf[j, at:at + batch, :].astype(F32)
                    for b in range(batch):
                        vecs_ref[path * batch + b, k:k + 1, j * width:(j + 1) * width] = block[b:b + 1, :]


def mods_call(vec, small_t, small_i, wt, wi, n_dev):
    batch, dim = vec.shape
    width = wt.shape[-1]
    vmem = pl.BlockSpec(memory_space=pltpu.VMEM)
    anywhere = pl.BlockSpec(memory_space=pl.ANY)
    return pl.pallas_call(
        mods_kernel,
        in_specs=[vmem, (vmem,) * len(small_t), (vmem,) * len(small_i), anywhere, anywhere],
        out_specs=[vmem, vmem],
        out_shape=[jax.ShapeDtypeStruct((2 * batch, FC2_B + 1, dim), F32), jax.ShapeDtypeStruct((2, FC1_B + 1, dim), F32)],
        scratch_shapes=[
            pltpu.VMEM((2, PROJ_B, dim, width), BF16),
            pltpu.VMEM((n_dev, 4 * batch, width), BF16),
            pltpu.VMEM((n_dev, 8 * batch, width), BF16),
            pltpu.SemaphoreType.DMA((2, PROJ_B)),
            pltpu.SemaphoreType.DMA((2, n_dev)),
            pltpu.SemaphoreType.DMA((2, n_dev)),
        ],
        compiler_params=pltpu.CompilerParams(collective_id=1, has_side_effects=True, vmem_limit_bytes=VMEM_BYTES),
        cost_estimate=pl.CostEstimate(flops=2 * batch * dim * 12 * width, bytes_accessed=24 * dim * width, transcendentals=0),
        name="mods",
    )(vec, small_t, small_i, wt, wi)


LOG2E = 1.4426950408889634
(W_FIRST, W_SECOND, W_RELAY, W_CORE, W_CORE_FIRST, W_CORE_SECOND, W_CORE_RELAY) = range(7)
(T_CORE, T_FIRST, T_SECOND, T_OUT_FIRST, T_OUT_SECOND, T_OUT_RELAY, T_CORE_OWN, T_CORE_FIRST, T_CORE_SECOND, T_CORE_RELAY) = range(10)
PIECES = 4
HEADS_HERE = 3


class Place:
    def __init__(self):
        me = lax.axis_index('tp')
        core = me % 2
        xi = (me // 2) % 2
        yi = me // 4
        x_next = me + 2 - 4 * xi
        y_next = me + 4 - 8 * yi
        self.me, self.core = me, core
        self.partner = me + 1 - 2 * core
        self.first = x_next * (1 - core) + y_next * core
        self.second = x_next * core + y_next * (1 - core)
        self.diagonal = x_next + y_next - me
        self.bit1 = xi * (1 - core) + yi * core
        self.bit2 = xi * core + yi * (1 - core)

    def enter(self):
        barrier = pltpu.get_barrier_semaphore()
        for dev in (self.partner, self.first, self.second):
            pl.semaphore_signal(barrier, inc=1, device_id={'tp': dev}, device_id_type=MESH)
        pl.semaphore_wait(barrier, 3)


def rows_at(start, size):
    return pl.ds(pl.multiple_of(start, size), size)


def front_kernel(cfg, txt_hbm, img_hbm, wt_hbm, wi_hbm, pw_hbm, tw_hbm, vec_ref, small_ref, ids_ref, tab_ref,
                 o_hbm, wp_hbm, ut_hbm, x1_ref,
                 w, xs, ua, ub, qkv, s0, s1, s2, o_all, tw, t_send, t_recv, t_own, t_sum, t_rs1, t_rs2_out, t_rs2_in, t_keep, t_x, t_u,
                 wsem, xsem, osem, tsem, psend, precv, tsend, trecv):
    batch, txt_len, img_len, rows = cfg
    half, quarter, eighth = rows // 2, rows // 4, rows // 8
    total = txt_len + img_len
    per_img = img_len // rows
    blocks = batch * (per_img + 1)
    dim = w.shape[1]
    width = o_all.shape[1]
    heads = width // HEAD
    place = Place()
    me, core, partner, first, second, diagonal, bit1, bit2 = place.me, place.core, place.partner, place.first, place.second, place.diagonal, place.bit1, place.bit2
    piece = width // PIECES

    def position(n):
        n = jnp.int32(n)
        img = (n >= batch).astype(jnp.int32)
        m = n - batch
        b = (1 - img) * n + img * (m // per_img)
        r = img * (1 + m % per_img)
        return b, r * rows

    def x_copy(n, source):
        b, r0 = position(n)
        ref = txt_hbm.at[b] if source == 0 else img_hbm.at[b, rows_at(r0 - rows, rows), :]
        return pltpu.make_async_copy(ref, xs.at[n % 4], xsem.at[n % 4])

    def x_start(n):
        @pl.when(n < batch)
        def _():
            x_copy(n, 0).start()

        @pl.when((n >= batch) & (n < blocks))
        def _():
            x_copy(n, 1).start()

    def x_wait(n):
        @pl.when(n < blocks)
        def _():
            pltpu.make_async_copy(txt_hbm.at[0], xs.at[n % 4], xsem.at[n % 4]).wait()

    def w_load(path, j):
        return pltpu.make_async_copy((wt_hbm, wi_hbm)[path].at[j], w.at[path, :, j * width:(j + 1) * width], wsem.at[path, j])

    for path in range(2):
        for j in range(3):
            w_load(path, j).start()
            if path == 0 and j == 0:
                for n in range(3):
                    x_copy(n, 0 if n < batch else 1).start()
    tw_load = pltpu.make_async_copy(tw_hbm, tw, tsem.at[0])
    tw_load.start()
    place.enter()

    def piece_at(j):
        return rows_at(j * piece, piece)

    def remote(sends, recvs, kind, j, src, dst, dev):
        return pltpu.make_async_remote_copy(src_ref=src, dst_ref=dst, send_sem=sends.at[kind, j], recv_sem=recvs.at[kind, j], device_id={'tp': dev}, device_id_type=MESH)

    def p_copy(kind, j, owner, dev):
        dst = wp_hbm.at[owner, piece_at(j), :]
        src = pw_hbm.at[piece_at(j), :] if kind in (W_FIRST, W_SECOND, W_CORE) else dst
        return remote(psend, precv, kind, j, src, dst, dev)

    def w_relay(j):
        p_copy(W_FIRST, j, first, first).wait_recv()
        p_copy(W_RELAY, j, first, second).start()
        p_copy(W_CORE_FIRST, j, first, partner).start()

    def w_second(j):
        p_copy(W_SECOND, j, second, second).wait_recv()
        p_copy(W_CORE_SECOND, j, second, partner).start()

    def w_last(j):
        p_copy(W_RELAY, j, diagonal, second).wait_recv()
        p_copy(W_CORE_RELAY, j, diagonal, partner).start()

    for j in range(PIECES):
        p_copy(W_FIRST, j, me, first).start()
        p_copy(W_SECOND, j, me, second).start()
    for j in range(PIECES):
        p_copy(W_CORE, j, me, partner).start()

    even = lax.broadcasted_iota(jnp.int32, (rows, HEAD), 1) % 2 == 0
    code = lax.broadcasted_iota(jnp.int32, (N_IDS, rows), 0)

    def select(n):
        n = jnp.int32(n)
        img = (n >= batch).astype(jnp.int32)
        return (1 - img) * n + img * (batch + (n - batch) // per_img)

    def norm(n, u):
        u[...] = modulated(xs[n % 4].astype(F32), vec_ref, select(n), SHIFT1, SCALE1)

    def heads_of(n, u):
        b, r0 = position(n)
        path = (jnp.int32(n) >= batch).astype(jnp.int32)
        hot = jnp.concatenate([(ids_ref[axis, pl.ds(b, 1), rows_at(r0, rows)] == code).astype(F32).astype(BF16) for axis in range(3)], axis=0)
        parts = lax.dot_general(hot, tab_ref[...], (((0,), (0,)), ((), ())), preferred_element_type=F32)
        cos_t, sin_t = (sum(parts[:, (3 * i + j) * HEAD:(3 * i + j + 1) * HEAD] for j in range(3)) for i in range(2))
        at = rows_at(b * total + r0, rows)
        for c0 in range(0, 3 * heads, 4):
            c1 = min(c0 + 4, 3 * heads)
            a = jnp.dot(u[...], w[path, :, c0 * HEAD:c1 * HEAD], preferred_element_type=F32) + row_of(small_ref, path, QKV_B, slice(c0 * HEAD, c1 * HEAD))
            for c in range(c0, c1):
                t = a[:, (c - c0) * HEAD:(c - c0 + 1) * HEAD]
                kind = c // heads
                if kind < 2:
                    mean_sq = jnp.mean(t * t, axis=-1, keepdims=True)
                    t = t * lax.rsqrt(mean_sq + NORM_EPS) * row_of(small_ref, path, Q_GAIN + kind, slice(HEAD))
                    swapped = jnp.where(even, pltpu.roll(t, HEAD - 1, 1), pltpu.roll(t, 1, 1))
                    t = t * cos_t + swapped * sin_t
                qkv[c, at, :] = t.astype(BF16)

    x_wait(0)
    norm(0, ua)
    for path in range(2):
        for j in range(3):
            w_load(path, j).wait()

    def qkv_step(t):
        x_start(2 * t + 3)
        x_start(2 * t + 4)
        x_wait(2 * t + 1)
        x_wait(2 * t + 2)
        norm(2 * t + 1, ub)
        heads_of(2 * t, ua)
        norm(jnp.minimum(2 * t + 2, blocks - 1), ua)
        heads_of(2 * t + 1, ub)

    loop(blocks // 2, qkv_step)

    factor = HEAD ** -0.5 * LOG2E

    def scores(n, h, s):
        b, r0 = position(n)
        q = qkv[h, rows_at(b * total + r0, rows), :]
        k = qkv[heads + h, pl.ds(pl.multiple_of(b * total, rows), total), :]
        s[...] = lax.dot_general(q, k, (((1,), (1,)), ((), ())), preferred_element_type=F32)

    def weigh(n, h, s):
        b, r0 = position(n)
        v = qkv[2 * heads + h, pl.ds(pl.multiple_of(b * total, rows), total), :]
        top = jnp.max(s[...], axis=-1, keepdims=True)
        p = jnp.exp2((s[...] - top) * factor)
        denom = jnp.sum(p, axis=-1, keepdims=True)
        o = jnp.dot(p.astype(BF16), v, preferred_element_type=F32)
        o_all[rows_at(b * total + r0, rows), h * HEAD:(h + 1) * HEAD] = (o * (1.0 / denom)).astype(BF16)

    def t_copy(kind, src, dst, dev):
        return remote(tsend, trecv, kind, 0, src, dst, dev)

    def t_core():
        return t_copy(T_CORE, t_send, t_recv, partner)

    def t_first():
        return t_copy(T_FIRST, t_sum.at[:, rows_at((1 - bit1) * quarter, quarter), :], t_rs1, first)

    def t_second():
        return t_copy(T_SECOND, t_rs2_out, t_rs2_in, second)

    def own_rows(b1, b2):
        return rows_at(core * half + b1 * quarter + b2 * eighth, eighth)

    def t_out(kind, b1, b2, dev):
        ref = ut_hbm.at[:, own_rows(b1, b2), :]
        return t_copy(kind, t_u if kind in (T_OUT_FIRST, T_OUT_SECOND, T_CORE_OWN) else ref, ref, dev)

    def t_local():
        return pltpu.make_async_copy(t_u, ut_hbm.at[:, own_rows(bit1, bit2), :], tsem.at[1])

    def t_load(b):
        return pltpu.make_async_copy(txt_hbm.at[b, own_rows(bit1, bit2), :], t_x.at[b], tsem.at[2 + b])

    tile = min(512, dim)

    def text_partial():
        tw_load.wait()
        for b in range(batch):
            t_load(b).start()

            def theirs(n):
                at = rows_at(n * tile, tile)
                t_send[b, :, at] = jnp.dot(o_all[rows_at(b * total + (1 - core) * half, half), :], tw[:, at], preferred_element_type=F32).astype(BF16)

            loop(dim // tile, theirs)
        t_core().start()
        for b in range(batch):
            def mine(n):
                at = rows_at(n * tile, tile)
                t_own[b, :, at] = jnp.dot(o_all[rows_at(b * total + core * half, half), :], tw[:, at], preferred_element_type=F32)

            loop(dim // tile, mine)

    def text_sum():
        t_core().wait()
        for b in range(batch):
            def add(n):
                at = rows_at(n * 16, 16)
                t_sum[b, at, :] = (t_own[b, at, :] + t_recv[b, at, :].astype(F32)).astype(BF16)

            loop(half // 16, add)
        t_first().start()

    def text_quarter():
        t_first().wait()
        for b in range(batch):
            t_rs2_out[b] = (t_sum[b, rows_at(bit1 * quarter + (1 - bit2) * eighth, eighth), :].astype(F32) + t_rs1[b, rows_at((1 - bit2) * eighth, eighth), :].astype(F32)).astype(BF16)
            t_keep[b] = t_sum[b, rows_at(bit1 * quarter + bit2 * eighth, eighth), :].astype(F32) + t_rs1[b, rows_at(bit2 * eighth, eighth), :].astype(F32)
        t_second().start()

    def text_finish():
        t_second().wait()
        for b in range(batch):
            t_load(b).wait()
            branch = t_keep[b] + t_rs2_in[b].astype(F32) + row_of(vec_ref, b, PROJ_B)
            x1 = (t_x[b].astype(F32) + row_of(vec_ref, b, GATE1) * branch).astype(BF16)
            x1_ref[b] = x1
            t_u[b] = modulated(x1.astype(F32), vec_ref, b, SHIFT2, SCALE2)
        t_out(T_OUT_FIRST, bit1, bit2, first).start()
        t_out(T_OUT_SECOND, bit1, bit2, second).start()
        t_out(T_CORE_OWN, bit1, bit2, partner).start()
        t_local().start()

    def text_relay():
        t_out(T_OUT_FIRST, 1 - bit1, bit2, first).wait_recv()
        t_out(T_OUT_RELAY, 1 - bit1, bit2, second).start()
        t_out(T_CORE_FIRST, 1 - bit1, bit2, partner).start()
        t_out(T_OUT_SECOND, bit1, 1 - bit2, second).wait_recv()
        t_out(T_CORE_SECOND, bit1, 1 - bit2, partner).start()

    def text_last():
        t_out(T_OUT_RELAY, 1 - bit1, 1 - bit2, second).wait_recv()
        t_out(T_CORE_RELAY, 1 - bit1, 1 - bit2, partner).start()

    hooks = {
        0: [functools.partial(w_relay, j) for j in range(PIECES)],
        2: [text_partial],
        3: [text_sum],
        4: [functools.partial(w_second, j) for j in range(PIECES)],
        10: [text_quarter],
        12: [text_finish],
        15: [text_relay, functools.partial(w_last, 0), functools.partial(w_last, 1)],
        17: [text_last, functools.partial(w_last, 2)],
    }

    def o_store(n):
        b, r0 = position(n)
        return pltpu.make_async_copy(o_all.at[rows_at(b * total + r0, rows), :], o_hbm.at[b, rows_at(r0, rows), :], osem.at[n % 4])

    scores(0, 0, s0)

    def attention_step(n):
        for when, calls in hooks.items():
            @pl.when(n == min(when, blocks - 1))
            def _():
                for call in calls:
                    call()

        @pl.when(n >= 4)
        def _():
            o_store(n - 4).wait()

        scores(n, 1, s1)
        weigh(n, 0, s0)
        scores(n, 2, s2)
        weigh(n, 1, s1)
        scores(jnp.minimum(n + 1, blocks - 1), 0, s0)
        weigh(n, 2, s2)
        o_store(n).start()

    loop(blocks, attention_step)

    w_last(3)
    for n in range(blocks - 4, blocks):
        o_store(n).wait()
    t_local().wait()
    for kind, b1, b2, dev in ((T_OUT_FIRST, bit1, bit2, first), (T_OUT_SECOND, bit1, bit2, second), (T_OUT_RELAY, 1 - bit1, bit2, second)):
        t_out(kind, b1, b2, dev).wait_send()
    for kind, b1, b2 in ((T_CORE_OWN, bit1, bit2), (T_CORE_FIRST, 1 - bit1, bit2), (T_CORE_SECOND, bit1, 1 - bit2), (T_CORE_RELAY, 1 - bit1, 1 - bit2)):
        t_out(kind, b1, b2, partner).wait()
    for j in range(PIECES):
        for kind, owner, dev in ((W_FIRST, me, first), (W_SECOND, me, second), (W_RELAY, first, second)):
            p_copy(kind, j, owner, dev).wait_send()
        for kind, owner in ((W_CORE, me), (W_CORE_FIRST, first), (W_CORE_SECOND, second), (W_CORE_RELAY, diagonal)):
            p_copy(kind, j, owner, partner).wait()


def front_call(txt, img, wt, wi, pw, tw, vecs, small, ids_t, table, n_dev, rows):
    batch, txt_len, dim = txt.shape
    img_len = img.shape[1]
    total = txt_len + img_len
    width = pw.shape[0]
    heads = width // HEAD
    half, quarter, eighth = rows // 2, rows // 4, rows // 8
    assert heads == HEADS_HERE or heads == 1
    cfg = (batch, txt_len, img_len, rows)
    vmem = pl.BlockSpec(memory_space=pltpu.VMEM)
    anywhere = pl.BlockSpec(memory_space=pl.ANY)
    flops = 2 * batch * total * dim * 3 * width + 8 * batch * heads * total * total * HEAD
    return pl.pallas_call(
        functools.partial(front_kernel, cfg),
        in_specs=[anywhere] * 6 + [vmem] * 4,
        out_specs=[anywhere, anywhere, anywhere, vmem],
        out_shape=[
            jax.ShapeDtypeStruct((batch, total, width), BF16),
            jax.ShapeDtypeStruct((n_dev, width, dim), BF16),
            jax.ShapeDtypeStruct((batch, txt_len, dim), BF16),
            jax.ShapeDtypeStruct((batch, eighth, dim), BF16),
        ],
        scratch_shapes=[
            pltpu.VMEM((2, dim, 3 * width), BF16),
            pltpu.VMEM((4, rows, dim), BF16),
            pltpu.VMEM((rows, dim), BF16),
            pltpu.VMEM((rows, dim), BF16),
            pltpu.VMEM((3 * heads, batch * total, HEAD), BF16),
            pltpu.VMEM((rows, total), F32),
            pltpu.VMEM((rows, total), F32),
            pltpu.VMEM((rows, total), F32),
            pltpu.VMEM((batch * total, width), BF16),
            pltpu.VMEM((width, dim), BF16),
            pltpu.VMEM((batch, half, dim), BF16),
            pltpu.VMEM((batch, half, dim), BF16),
            pltpu.VMEM((batch, half, dim), F32),
            pltpu.VMEM((batch, half, dim), BF16),
            pltpu.VMEM((batch, quarter, dim), BF16),
            pltpu.VMEM((batch, eighth, dim), BF16),
            pltpu.VMEM((batch, eighth, dim), BF16),
            pltpu.VMEM((batch, eighth, dim), F32),
            pltpu.VMEM((batch, eighth, dim), BF16),
            pltpu.VMEM((batch, eighth, dim), BF16),
            pltpu.SemaphoreType.DMA((2, 3)),
            pltpu.SemaphoreType.DMA((4,)),
            pltpu.SemaphoreType.DMA((4,)),
            pltpu.SemaphoreType.DMA((4,)),
            pltpu.SemaphoreType.DMA((7, PIECES)),
            pltpu.SemaphoreType.DMA((7, PIECES)),
            pltpu.SemaphoreType.DMA((10, 1)),
            pltpu.SemaphoreType.DMA((10, 1)),
        ],
        compiler_params=pltpu.CompilerParams(collective_id=2, has_side_effects=True, vmem_limit_bytes=VMEM_BYTES),
        cost_estimate=pl.CostEstimate(flops=flops, bytes_accessed=2 * batch * total * (dim + width), transcendentals=batch * heads * total * total),
        name="front",
    )(txt, img, wt, wi, pw, tw, vecs, small, ids_t, table)


(O_CORE, O_FIRST, O_SECOND, O_RELAY, U_CORE, PART_CORE, RS_FIRST, RS_SECOND, OUT_FIRST, OUT_SECOND, OUT_RELAY, CORE_OWN, CORE_FIRST, CORE_SECOND, CORE_RELAY) = range(15)
(L_O, L_X, L_OUT) = range(3)
SLOTS = 4
O_SLOTS = 6
SEMS = 8


def block_kernel(cfg, o_hbm, x_hbm, ut_hbm, x1t_hbm, wp_hbm, pw_hbm, w1t_hbm, w2t_hbm, w1i_hbm, w2i_hbm, vec_ref, fb_ref, out_hbm,
                 wp, w1, w2, obuf, xbuf, x1buf, x1keep, u2, hid, psend, precv, own, chip_sum, rs1, keep2, rs2_out, rs2_in, outb,
                 wsem, lsem, tsem, ssem, rsem):
    batch, txt_chunks, img_chunks, per_img, rows, tile = cfg
    half, quarter, eighth = rows // 2, rows // 4, rows // 8
    dim = wp.shape[0]
    ff = w1.shape[1]
    cols = o_hbm.shape[2]
    total = txt_chunks + img_chunks
    per_txt = txt_chunks // batch

    place = Place()
    me, core, partner, first, second, bit1, bit2 = place.me, place.core, place.partner, place.first, place.second, place.bit1, place.bit2
    txt_len = ut_hbm.shape[1]
    place.enter()

    def remote(kind, g, src, dst, dev):
        return pltpu.make_async_remote_copy(src_ref=src, dst_ref=dst, send_sem=ssem.at[kind, g % SEMS], recv_sem=rsem.at[kind, g % SEMS], device_id={'tp': dev}, device_id_type=MESH)

    def img_pos(g):
        k = g - txt_chunks
        return k // per_img, (k % per_img) * rows

    def chip_cols(dev):
        return rows_at((dev // 2) * (2 * cols), 2 * cols)

    def own_rows(b1, b2):
        return core * half + b1 * quarter + b2 * eighth

    def o_local(g):
        b, r0 = img_pos(g)
        return pltpu.make_async_copy(o_hbm.at[b, rows_at(txt_len + r0 + core * half, half), :], obuf.at[g % O_SLOTS, :, rows_at(me * cols, cols)], lsem.at[L_O, g % SEMS])

    def o_core(g):
        b, r0 = img_pos(g)
        return remote(O_CORE, g, o_hbm.at[b, rows_at(txt_len + r0 + (1 - core) * half, half), :], obuf.at[g % O_SLOTS, :, rows_at(me * cols, cols)], partner)

    def o_send(kind, g, owner, dev):
        ref = obuf.at[g % O_SLOTS, :, chip_cols(owner)]
        return remote(kind, g, ref, ref, dev)

    def x_load(g):
        b, r0 = img_pos(g)
        return pltpu.make_async_copy(x_hbm.at[b, rows_at(r0 + core * half, half), :], xbuf.at[g % 2], lsem.at[L_X, g % SEMS])

    def u_core(g):
        ref = u2.at[g % 2, rows_at(core * half, half), :]
        return remote(U_CORE, g, ref, ref, partner)

    def part_core(g):
        return remote(PART_CORE, g, psend, precv.at[g % 2], partner)

    def rs_first(g):
        return remote(RS_FIRST, g, chip_sum.at[rows_at((1 - bit1) * quarter, quarter), :], rs1.at[g % 2], first)

    def rs_second(g):
        return remote(RS_SECOND, g, rs2_out.at[g % 2], rs2_in.at[g % SLOTS], second)

    def out_ref(g, b1, b2):
        return out_hbm.at[rows_at(g * rows + own_rows(b1, b2), eighth), :]

    def out_send(kind, g, b1, b2, dev):
        ref = out_ref(g, b1, b2)
        mine = kind in (OUT_FIRST, OUT_SECOND, CORE_OWN)
        return remote(kind, g, outb.at[g % SLOTS] if mine else ref, ref, dev)

    def out_local(g):
        return pltpu.make_async_copy(outb.at[g % SLOTS], out_ref(g, bit1, bit2), lsem.at[L_OUT, g % SEMS])

    def txt_load(g):
        b, r0 = g // per_txt, (g % per_txt) * rows
        return (pltpu.make_async_copy(ut_hbm.at[b, rows_at(r0, rows), :], u2.at[g % 2], tsem.at[0, g % 2]),
                pltpu.make_async_copy(x1t_hbm.at[g], x1keep.at[g % SLOTS], tsem.at[1, g % 2]))

    def w_load(k, src, dst):
        return pltpu.make_async_copy(src, dst, wsem.at[k])

    def wp_load(j, src):
        return pltpu.make_async_copy(src, wp.at[j * cols:(j + 1) * cols, :], wsem.at[2 + j])

    def select(g):
        txt = (g < txt_chunks).astype(jnp.int32)
        return txt * (g // per_txt) + (1 - txt) * (batch + (g - txt_chunks) // per_img)

    def start_o(g):
        o_local(g).start()
        o_core(g).start()

    def send_o(g):
        o_local(g).wait()
        o_core(g).wait()
        o_send(O_FIRST, g, me, first).start()
        o_send(O_SECOND, g, me, second).start()

    def relay_o(g):
        o_send(O_FIRST, g, first, first).wait_recv()
        o_send(O_RELAY, g, first, second).start()
        x_load(g).start()

    def project(g):
        o_send(O_FIRST, g, me, first).wait_send()
        o_send(O_SECOND, g, me, second).wait_send()
        o_send(O_RELAY, g, first, second).wait_send()
        o_send(O_SECOND, g, second, second).wait_recv()
        o_send(O_RELAY, g, second, second).wait_recv()
        x_load(g).wait()

        @pl.when(g == txt_chunks)
        def _():
            for j in range(wp_hbm.shape[0]):
                wp_load(j, wp_hbm.at[j]).wait()

        sel = select(g)
        slot = g % SLOTS

        def columns(n):
            at = rows_at(n * tile, tile)
            acc = jnp.dot(obuf[g % O_SLOTS], wp[:, at], preferred_element_type=F32)
            branch = acc + row_of(vec_ref, sel, PROJ_B, at)
            x1buf[:, at] = (xbuf[g % 2, :, at].astype(F32) + row_of(vec_ref, sel, GATE1, at) * branch).astype(BF16)

        loop(dim // tile, columns)

        def norm(n):
            at = rows_at(n * 16, 16)
            u2[g % 2, rows_at(core * half + n * 16, 16), :] = modulated(x1buf[at, :].astype(F32), vec_ref, sel, SHIFT2, SCALE2)

        loop(half // 16, norm)
        u_core(g).start()
        x1keep[slot] = x1buf[rows_at(bit1 * quarter + bit2 * eighth, eighth), :]

    def mlp_hidden(g):
        @pl.when(g < txt_chunks)
        def _():
            for copy in txt_load(g):
                copy.wait()

        @pl.when(g >= txt_chunks)
        def _():
            u_core(g).wait()

        @pl.when(g == 0)
        def _():
            w_load(0, w1t_hbm, w1).wait()
            w_load(1, w2t_hbm, w2).wait()
            for j in range(wp_hbm.shape[0]):
                @pl.when(j != me)
                def _():
                    wp_load(j, wp_hbm.at[j]).start()

                @pl.when(j == me)
                def _():
                    wp_load(j, pw_hbm).start()

        @pl.when(g == txt_chunks)
        def _():
            w_load(0, w1i_hbm, w1).wait()
            w_load(1, w2i_hbm, w2).wait()

        path = (g >= txt_chunks).astype(jnp.int32)

        def hidden(n):
            at = rows_at(n * tile, tile)
            acc = jnp.dot(u2[g % 2], w1[:, at], preferred_element_type=F32)
            pre = acc + row_of(fb_ref, path, FC1_B, at)
            hid[:, at] = jax.nn.gelu(pre, approximate=True).astype(BF16)

        loop(ff // tile, hidden)

    def mlp_theirs(g):
        def theirs(n):
            at = rows_at(n * tile, tile)
            psend[:, at] = jnp.dot(hid[rows_at((1 - core) * half, half), :], w2[:, at], preferred_element_type=F32).astype(BF16)

        loop(dim // tile, theirs)
        part_core(g).start()

    def mlp_mine(g):
        def mine(n):
            at = rows_at(n * tile, tile)
            own[:, at] = jnp.dot(hid[rows_at(core * half, half), :], w2[:, at], preferred_element_type=F32)

        loop(dim // tile, mine)

        @pl.when(g == txt_chunks - 1)
        def _():
            w_load(0, w1i_hbm, w1).start()
            w_load(1, w2i_hbm, w2).start()

        part_core(g).wait()

        def add(n):
            at = rows_at(n * 16, 16)
            chip_sum[at, :] = (own[at, :] + precv[g % 2, at, :].astype(F32)).astype(BF16)

        loop(half // 16, add)
        rs_first(g).start()

    def add_first(g):
        rs_first(g).wait()
        rs2_out[g % 2] = (chip_sum[rows_at(bit1 * quarter + (1 - bit2) * eighth, eighth), :].astype(F32) + rs1[g % 2, rows_at((1 - bit2) * eighth, eighth), :].astype(F32)).astype(BF16)
        rs_second(g).start()
        keep2[g % 2] = chip_sum[rows_at(bit1 * quarter + bit2 * eighth, eighth), :].astype(F32) + rs1[g % 2, rows_at(bit2 * eighth, eighth), :].astype(F32)

    def finish(g):
        rs_second(g).wait()
        sel = select(g)
        branch = keep2[g % 2] + rs2_in[g % SLOTS].astype(F32) + row_of(vec_ref, sel, FC2_B)
        outb[g % SLOTS] = (x1keep[g % SLOTS].astype(F32) + row_of(vec_ref, sel, GATE2) * branch).astype(BF16)
        out_send(OUT_FIRST, g, bit1, bit2, first).start()
        out_send(OUT_SECOND, g, bit1, bit2, second).start()
        out_send(CORE_OWN, g, bit1, bit2, partner).start()
        out_local(g).start()

    def relay_out(g):
        out_send(OUT_FIRST, g, 1 - bit1, bit2, first).wait_recv()
        out_send(OUT_RELAY, g, 1 - bit1, bit2, second).start()
        out_send(CORE_FIRST, g, 1 - bit1, bit2, partner).start()

    def second_out(g):
        out_send(OUT_SECOND, g, bit1, 1 - bit2, second).wait_recv()
        out_send(CORE_SECOND, g, bit1, 1 - bit2, partner).start()

    def relay_core(g):
        out_send(OUT_RELAY, g, 1 - bit1, 1 - bit2, second).wait_recv()
        out_send(CORE_RELAY, g, 1 - bit1, 1 - bit2, partner).start()

    def drain(g):
        out_local(g).wait()
        out_send(OUT_FIRST, g, bit1, bit2, first).wait_send()
        out_send(OUT_SECOND, g, bit1, bit2, second).wait_send()
        out_send(OUT_RELAY, g, 1 - bit1, bit2, second).wait_send()
        out_send(CORE_OWN, g, bit1, bit2, partner).wait()
        out_send(CORE_FIRST, g, 1 - bit1, bit2, partner).wait()
        out_send(CORE_SECOND, g, bit1, 1 - bit2, partner).wait()
        out_send(CORE_RELAY, g, 1 - bit1, 1 - bit2, partner).wait()

    w_load(0, w1t_hbm, w1).start()
    w_load(1, w2t_hbm, w2).start()
    for g in range(txt_chunks):
        for copy in txt_load(g):
            copy.start()

    stages = ((mlp_hidden, 0, 0), (relay_o, 2, 1), (finish, -3, 0), (start_o, 5, 1), (relay_out, -4, 0), (mlp_theirs, 0, 0), (second_out, -5, 0),
              (send_o, 5, 1), (relay_core, -6, 0), (project, 1, 1), (add_first, -1, 0), (mlp_mine, 0, 0), (drain, -6, 0))
    most = max(ahead for _, ahead, _ in stages)
    least = min(ahead for _, ahead, _ in stages)

    def step(i):
        for stage, ahead, img_only in stages:
            g = i + txt_chunks - most + ahead

            @pl.when((g >= img_only * txt_chunks) & (g < total))
            def _():
                stage(g)

    loop(total - txt_chunks + most - least, step)


def block_call(img_o, x, u_txt, x1_txt, wp, pw, w1t, w2t, w1i, w2i, vecs, fb, rows):
    batch, img_len, dim = x.shape
    txt_len = u_txt.shape[1]
    ff = w1t.shape[1]
    txt_chunks = batch * (txt_len // rows)
    per_img = img_len // rows
    img_chunks = batch * per_img
    assert txt_chunks == 2
    half, quarter, eighth = rows // 2, rows // 4, rows // 8
    cfg = (batch, txt_chunks, img_chunks, per_img, rows, 512)
    total = txt_chunks + img_chunks
    anywhere = pl.BlockSpec(memory_space=pl.ANY)
    flops = 2 * total * rows * 2 * dim * ff + 2 * img_chunks * half * dim * dim
    return pl.pallas_call(
        functools.partial(block_kernel, cfg),
        in_specs=[anywhere] * 10 + [pl.BlockSpec(memory_space=pltpu.VMEM)] * 2,
        out_specs=anywhere,
        out_shape=jax.ShapeDtypeStruct((total * rows, dim), BF16),
        scratch_shapes=[
            pltpu.VMEM((dim, dim), BF16),
            pltpu.VMEM((dim, ff), BF16),
            pltpu.VMEM((ff, dim), BF16),
            pltpu.VMEM((O_SLOTS, half, dim), BF16),
            pltpu.VMEM((2, half, dim), BF16),
            pltpu.VMEM((half, dim), BF16),
            pltpu.VMEM((SLOTS, eighth, dim), BF16),
            pltpu.VMEM((2, rows, dim), BF16),
            pltpu.VMEM((rows, ff), BF16),
            pltpu.VMEM((half, dim), BF16),
            pltpu.VMEM((2, half, dim), BF16),
            pltpu.VMEM((half, dim), F32),
            pltpu.VMEM((half, dim), BF16),
            pltpu.VMEM((2, quarter, dim), BF16),
            pltpu.VMEM((2, eighth, dim), F32),
            pltpu.VMEM((2, eighth, dim), BF16),
            pltpu.VMEM((SLOTS, eighth, dim), BF16),
            pltpu.VMEM((SLOTS, eighth, dim), BF16),
            pltpu.SemaphoreType.DMA((10,)),
            pltpu.SemaphoreType.DMA((3, SEMS)),
            pltpu.SemaphoreType.DMA((2, 2)),
            pltpu.SemaphoreType.DMA((15, SEMS)),
            pltpu.SemaphoreType.DMA((15, SEMS)),
        ],
        compiler_params=pltpu.CompilerParams(collective_id=0, has_side_effects=True, vmem_limit_bytes=VMEM_BYTES),
        cost_estimate=pl.CostEstimate(flops=flops, bytes_accessed=4 * dim * dim + 8 * dim * ff + 4 * total * rows * dim, transcendentals=0),
        name="block",
    )(img_o, x, u_txt, x1_txt, wp, pw, w1t, w2t, w1i, w2i, vecs, fb)


def copy_kernel(pieces, flat_hbm, *rest):
    outs, (buf, isem, osem) = rest[:-3], rest[-3:]
    rows = buf.shape[1]
    loads = []
    for n, (which, b, r) in enumerate(pieces):
        load = pltpu.make_async_copy(flat_hbm.at[n * rows:(n + 1) * rows, :], buf.at[n], isem.at[n])
        load.start()
        loads.append(load)
    stores = []
    for n, (which, b, r) in enumerate(pieces):
        loads[n].wait()
        store = pltpu.make_async_copy(buf.at[n], outs[which].at[b, r:r + rows, :], osem.at[n])
        store.start()
        stores.append(store)
    for store in stores:
        store.wait()


def copy_call(flat, shapes, rows):
    pieces = [(which, b, r) for which, shape in enumerate(shapes) for b in range(shape[0]) for r in range(0, shape[1], rows)]
    anywhere = pl.BlockSpec(memory_space=pl.ANY)
    dim = flat.shape[1]
    return pl.pallas_call(
        functools.partial(copy_kernel, pieces),
        in_specs=[anywhere],
        out_specs=[anywhere] * len(shapes),
        out_shape=[jax.ShapeDtypeStruct(shape, flat.dtype) for shape in shapes],
        scratch_shapes=[
            pltpu.VMEM((len(pieces), rows, dim), flat.dtype),
            pltpu.SemaphoreType.DMA((len(pieces),)),
            pltpu.SemaphoreType.DMA((len(pieces),)),
        ],
        compiler_params=pltpu.CompilerParams(vmem_limit_bytes=VMEM_BYTES),
        cost_estimate=pl.CostEstimate(flops=0, bytes_accessed=4 * flat.shape[0] * dim, transcendentals=0),
        name="copy_out",
    )(flat)


def local_block(img, txt, vec, ids, img_w, txt_w):
    n_dev = 8
    batch, txt_len = txt.shape[:2]
    rows = txt_len

    def by_kind(weight):
        return jnp.transpose(weight, (1, 0, 2))

    def small_of(w):
        return w[1], w[3], w[4], w[5], w[7], w[9], w[11]

    vecs, small = mods_call(vec, small_of(txt_w), small_of(img_w), by_kind(txt_w[0]), by_kind(img_w[0]), n_dev)
    table = jnp.asarray(rope_table())
    ids_t = jnp.transpose(ids, (2, 0, 1))
    o, proj_w, txt_u, txt_x1 = front_call(txt, img, by_kind(txt_w[2]), by_kind(img_w[2]), img_w[6], txt_w[6], vecs, small, ids_t, table, n_dev, rows)
    flat = block_call(o, img, txt_u, txt_x1, proj_w, img_w[6], txt_w[8], txt_w[10], img_w[8], img_w[10], vecs, small, rows)
    txt_out, img_out = copy_call(flat, (txt.shape, img.shape), rows)
    return img_out, txt_out


def solution(mesh):
    act_spec = P('dp', WHOLE, WHOLE)
    mapped = jax.shard_map(local_block, mesh=mesh, in_specs=(act_spec, act_spec, P('dp', WHOLE), act_spec, PATH_SPECS, PATH_SPECS), out_specs=(act_spec, act_spec), check_vma=False)

    def forward(img, txt, vec, ids, *weights):
        return mapped(img, txt, vec, ids, weights[:12], weights[12:])

    return forward
```

```python
import functools

import jax
import jax.numpy as jnp
import numpy as np
from jax import lax
from jax.experimental import pallas as pl
from jax.experimental.pallas import tpu as pltpu
from jax.sharding import PartitionSpec as P

HEAD = 128
NORM_EPS = 1e-6
ROPE_THETA = 10000.0
AXES_DIM = (16, 56, 56)
N_IDS = 64
WHOLE = None
PATH_SPECS = (P(WHOLE, WHOLE, 'tp'), P(WHOLE, 'tp'), P(WHOLE, WHOLE, 'tp'), P(WHOLE, 'tp'), P(WHOLE), P(WHOLE), P('tp', WHOLE), P(WHOLE), P(WHOLE, 'tp'), P('tp'), P('tp', WHOLE), P(WHOLE))
F32 = jnp.float32
BF16 = jnp.bfloat16


def rope_table():
    cos = np.zeros((3 * N_IDS, HEAD), np.float32)
    sin = np.zeros((3 * N_IDS, HEAD), np.float32)
    lane = 0
    for axis, dim in enumerate(AXES_DIM):
        inv_freq = np.float32(ROPE_THETA) ** (-np.arange(0, dim, 2, dtype=np.float32) / np.float32(dim))
        angles = np.arange(N_IDS, dtype=np.float32)[:, None] * inv_freq.astype(np.float32)
        rows = slice(axis * N_IDS, (axis + 1) * N_IDS)
        c = np.cos(angles.astype(np.float64)).astype(np.float32)
        s = np.sin(angles.astype(np.float64)).astype(np.float32)
        cos[rows, lane:lane + dim:2] = c
        cos[rows, lane + 1:lane + dim:2] = c
        sin[rows, lane:lane + dim:2] = -s
        sin[rows, lane + 1:lane + dim:2] = s
        lane += dim
    parts = []
    for table in (cos, sin):
        rest = table
        for _ in range(3):
            part = rest.astype(jnp.bfloat16)
            parts.append(np.asarray(part))
            rest = rest - np.asarray(part).astype(np.float32)
    return np.concatenate(parts, axis=1)


MESH = pl.DeviceIdType.MESH


SHIFT1, SCALE1, GATE1, SHIFT2, SCALE2, GATE2, PROJ_B, FC2_B = range(8)
QKV_B, Q_GAIN, K_GAIN, FC1_B = range(4)
VMEM_BYTES = 67043328


def row_of(ref, sel, row, at=slice(None)):
    return ref[sel, pl.ds(row, 1), at]


STRIP = 16
PATHS = range(2)


def loop(count, body):
    lax.fori_loop(0, count, lambda i, carry: (body(i), carry)[-1], 0)


def row_mean(x):
    return jnp.mean(x, axis=-1, keepdims=True)


def normalize(x):
    centered = x - row_mean(x)
    return centered * lax.rsqrt(row_mean(centered * centered) + NORM_EPS)


def weighted(s, v):
    top = jnp.max(s, axis=-1, keepdims=True)
    p = jnp.exp2((s - top) * (HEAD ** -0.5 * LOG2E))
    total = jnp.sum(p, axis=-1, keepdims=True)
    o = jnp.dot(p.astype(BF16), v, preferred_element_type=F32)
    return (o * (1.0 / total)).astype(BF16)


def scores_of(q, k):
    return lax.dot_general(q, k, (((1,), (1,)), ((), ())), preferred_element_type=F32)


def modulated(x, vec_ref, sel, shift, scale):
    return ((1.0 + row_of(vec_ref, sel, scale)) * normalize(x) + row_of(vec_ref, sel, shift)).astype(BF16)


LOG2E = 1.4426950408889634
(W_FIRST, W_SECOND, W_RELAY, W_CORE, W_CORE_FIRST, W_CORE_SECOND, W_CORE_RELAY, Z_FIRST, Z_SECOND, Z_RELAY) = range(10)
(G_CORE, G_FIRST, G_SECOND, G_RELAY) = range(4)
(T_CORE, T_FIRST, T_SECOND, T_OUT_FIRST, T_OUT_SECOND, T_OUT_RELAY, T_CORE_OWN, T_CORE_FIRST, T_CORE_SECOND, T_CORE_RELAY) = range(10)
SHARED, COMMON, MISSING = range(3)
PIECES = 3
READY = 3
EARLY = 2
HEADS_HERE = 3


def ident(dev):
    return dev if isinstance(dev, dict) else {'tp': dev}


class Place:
    def __init__(self):
        me = lax.axis_index('tp')
        core = me % 2
        xi = (me // 2) % 2
        yi = me // 4
        x_next = me + 2 - 4 * xi
        y_next = me + 4 - 8 * yi
        self.me, self.core = me, core
        self.partner = me + 1 - 2 * core
        self.first = x_next * (1 - core) + y_next * core
        self.second = x_next * core + y_next * (1 - core)
        self.diagonal = x_next + y_next - me
        self.bit1 = xi * (1 - core) + yi * core
        self.bit2 = xi * core + yi * (1 - core)
        self.not1, self.not2, self.far = 1 - self.bit1, 1 - self.bit2, 1 - core

    def enter(self, others):
        barrier = pltpu.get_barrier_semaphore()
        for dev in others:
            pl.semaphore_signal(barrier, inc=1, device_id=ident(dev), device_id_type=MESH)
        pl.semaphore_wait(barrier, len(others))


def rows_at(start, size):
    return pl.ds(pl.multiple_of(start, size), size)


def front_kernel(cfg, txt_hbm, img_hbm, wt_hbm, wi_hbm, mt_hbm, mi_hbm, pw_hbm, tw_hbm, cond_ref, small_t, small_i, ids_ref, tab_ref,
                 o_hbm, kv_hbm, wp_hbm, ut_hbm, og_hbm, x1_ref, vec_ref, small_ref,
                 w, m_w, m_b, m_early, m_late, xs, ua, ub, qkv, s0, s1, s2, o_all, tw, t_send, t_recv, t_own, t_sum, t_rs1, t_rs2_out, t_rs2_in, t_keep, t_x, t_u,
                 wsem, msem, xsem, osem, tsem, gsem, psend, precv, tsend, trecv, gsend, grecv, msend, mrecv):
    batch, txt_len, img_len, rows = cfg
    half, quarter, eighth = rows // 2, rows // 4, rows // 8
    total = txt_len + img_len
    per_img = img_len // rows
    blocks = batch * (per_img + 1)
    n_dev = m_early.shape[0]
    others = range(1, n_dev)
    dim = w.shape[1]
    width = o_all.shape[1]
    heads = width // HEAD
    place = Place()
    me, core, partner, first, second, diagonal, bit1, bit2 = place.me, place.core, place.partner, place.first, place.second, place.diagonal, place.bit1, place.bit2
    not1, not2, far = place.not1, place.not2, place.far
    piece = width // PIECES
    plane = lax.axis_index('dp')
    odd = plane % 2
    beside = {'dp': plane + 1 - 2 * odd}

    def position(n):
        n = jnp.int32(n)
        img = (n >= batch).astype(jnp.int32)
        m = n - batch
        b = (1 - img) * n + img * (m // per_img)
        r = img * (1 + m % per_img)
        return b, r * rows

    def x_copy(n, source):
        b, r0 = position(n)
        ref = txt_hbm.at[b] if source == 0 else img_hbm.at[b, rows_at(r0 - rows, rows), :]
        return pltpu.make_async_copy(ref, xs.at[n % 4], xsem.at[n % 4])

    def x_start(n):
        @pl.when(n < batch)
        def _():
            x_copy(n, 0).start()

        @pl.when((n >= batch) & (n < blocks))
        def _():
            x_copy(n, 1).start()

    def x_wait(n):
        @pl.when(n < blocks)
        def _():
            pltpu.make_async_copy(txt_hbm.at[0], xs.at[n % 4], xsem.at[n % 4]).wait()

    def w_columns(path, j):
        return w.at[path, :, j * width:(j + 1) * width]

    def w_load(path, j):
        return pltpu.make_async_copy((wt_hbm, wi_hbm)[path].at[j], w_columns(path, j), wsem.at[path, j])

    def early_load(path, k):
        return pltpu.make_async_copy((mt_hbm, mi_hbm)[path].at[k], w_columns(path, k), wsem.at[path, k])

    def late_load(c, path):
        return pltpu.make_async_copy((mt_hbm, mi_hbm)[path].at[GATE1 + c // 2], m_w.at[c % 2], msem.at[c % 2])

    def late_start(c):
        for path in PATHS:
            @pl.when(c % 2 == path)
            def _():
                late_load(c, path).start()

    def m_copy(part, d, send):
        buf = (m_early, m_late)[part]
        ref = buf.at[me if send else (me + n_dev - d) % n_dev, :8]
        return pltpu.make_async_remote_copy(src_ref=ref, dst_ref=ref, send_sem=msend.at[part, d], recv_sem=mrecv.at[part, d], device_id={'tp': (me + d) % n_dev}, device_id_type=MESH)

    def m_send(part):
        for d in others:
            m_copy(part, d, True).start()

    def m_wait(part):
        for d in others:
            m_copy(part, d, True).wait_send()
            m_copy(part, d, False).wait_recv()

    for k in (SHIFT1, SCALE1):
        for path in PATHS:
            early_load(path, k).start()
    for n in range(3):
        x_copy(n, 0 if n < batch else 1).start()
    v = cond_ref[...].astype(F32)
    silu = (v * (1.0 / (1.0 + jnp.exp(-v)))).astype(BF16)
    for path, (mod_b, qkv_b, q_gain, k_gain, proj_b, fc1_b, fc2_b) in enumerate((small_t, small_i)):
        m_b[path] = mod_b[...].astype(F32)
        for row, ref in ((PROJ_B, proj_b), (FC2_B, fc2_b)):
            vector = ref[...].astype(F32)[None, :]
            for b in range(batch):
                vec_ref[path * batch + b, row:row + 1, :] = vector
        for row, ref in ((Q_GAIN, q_gain), (K_GAIN, k_gain), (FC1_B, fc1_b)):
            vector = ref[...].astype(F32)[None, :]
            small_ref[path, row:row + 1, :vector.shape[1]] = vector
        for j in range(qkv_b.shape[0]):
            small_ref[path, QKV_B:Q_GAIN, j * width:(j + 1) * width] = qkv_b[j:j + 1, :].astype(F32)
    place.enter([(me + d) % n_dev for d in others] + [beside])

    def early_chunk(k, path):
        early_load(path, k).wait()
        acc = jnp.dot(silu, w_columns(path, k)[...], preferred_element_type=F32)
        return (acc + m_b[path, k:k + 1, :]).astype(BF16)

    m_early[me] = jnp.concatenate([early_chunk(k, path) for k in (SHIFT1, SCALE1) for path in PATHS], axis=0)
    m_send(0)
    for path in PATHS:
        for j in range(3):
            w_load(path, j).start()
    for c in range(2):
        late_load(c, c).start()
    tw_load = pltpu.make_async_copy(tw_hbm, tw, tsem.at[1])
    tw_load.start()

    def late_chunk(t):
        c = jnp.minimum(t, 7)
        path, k = c % 2, GATE1 + c // 2
        acc = jnp.dot(silu, m_w[c % 2], preferred_element_type=F32) + m_b[path, pl.ds(k, 1), :]
        m_late[me, t] = acc.astype(BF16).astype(F32)

    def late_rows():
        m_wait(1)
        for j in range(n_dev):
            for c in range(8):
                for b in range(batch):
                    vec_ref[c % 2 * batch + b, pl.ds(GATE1 + c // 2, 1), j * width:(j + 1) * width] = m_late[j, c, b:b + 1, :]

    def piece_at(j):
        return rows_at(((1 - j) * (2 * odd - 1) + 1) * piece, piece)

    def remote(sends, recvs, kind, j, src, dst, dev):
        return pltpu.make_async_remote_copy(src_ref=src, dst_ref=dst, send_sem=sends.at[kind, j], recv_sem=recvs.at[kind, j], device_id=ident(dev), device_id_type=MESH)

    def p_copy(kind, j, owner, dev):
        dst = wp_hbm.at[owner, piece_at(j), :]
        src = pw_hbm.at[piece_at(j), :] if kind in (W_FIRST, W_SECOND) else dst
        return remote(psend, precv, kind, j, src, dst, dev)

    def w_own():
        return remote(psend, precv, W_CORE, SHARED, pw_hbm, wp_hbm.at[me], partner)

    def z_copy(kind, owner, j=SHARED):
        ref = wp_hbm.at[owner, piece_at(j), :]
        return remote(psend, precv, kind, SHARED, ref, ref, beside)

    def w_relay(j):
        p_copy(W_FIRST, j, first, first).wait_recv()
        p_copy(W_RELAY, j, first, second).start()
        p_copy(W_CORE_FIRST, j, first, partner).start()
        if j == SHARED:
            p_copy(W_SECOND, COMMON, me, second).start()
            z_copy(Z_FIRST, first).start()

    def w_second(j):
        p_copy(W_SECOND, j, second, second).wait_recv()
        p_copy(W_CORE_SECOND, j, second, partner).start()
        if j == SHARED:
            z_copy(Z_SECOND, second).start()

    def w_last(j):
        p_copy(W_RELAY, j, diagonal, second).wait_recv()
        p_copy(W_CORE_RELAY, j, diagonal, partner).start()
        if j == SHARED:
            z_copy(Z_RELAY, diagonal).start()

    from_beside = ((Z_FIRST, first, W_CORE_FIRST), (Z_SECOND, second, W_CORE_SECOND), (Z_RELAY, diagonal, W_CORE_RELAY))

    def w_beside(n):
        kind, owner, core_kind = from_beside[n]
        z_copy(kind, owner, MISSING).wait_recv()
        p_copy(core_kind, MISSING, owner, partner).start()

    p_copy(W_FIRST, SHARED, me, first).start()
    p_copy(W_SECOND, SHARED, me, second).start()
    p_copy(W_FIRST, COMMON, me, first).start()
    w_own().start()

    even = lax.broadcasted_iota(jnp.int32, (rows, HEAD), 1) % 2 == 0
    code = lax.broadcasted_iota(jnp.int32, (N_IDS, rows), 0)

    def select(n):
        n = jnp.int32(n)
        img = (n >= batch).astype(jnp.int32)
        return (1 - img) * n + img * (batch + (n - batch) // per_img)

    def norm(n, u):
        u[...] = modulated(xs[n % 4].astype(F32), vec_ref, select(n), SHIFT1, SCALE1).reshape(u.shape)

    def heads_of(n, u):
        b, r0 = position(n)
        path = (jnp.int32(n) >= batch).astype(jnp.int32)
        hot = jnp.concatenate([(ids_ref[axis, pl.ds(b, 1), rows_at(r0, rows)] == code).astype(F32).astype(BF16) for axis in range(3)], axis=0)
        parts = lax.dot_general(hot, tab_ref[...], (((0,), (0,)), ((), ())), preferred_element_type=F32)
        cos_t, sin_t = (sum(parts[:, (3 * i + j) * HEAD:(3 * i + j + 1) * HEAD] for j in range(3)) for i in range(2))
        at = rows_at(b * total + r0, rows)
        for c0 in range(0, 3 * heads, 4):
            c1 = min(c0 + 4, 3 * heads)
            a = jnp.dot(u[...].reshape(rows, dim), w[path, :, c0 * HEAD:c1 * HEAD], preferred_element_type=F32) + row_of(small_ref, path, QKV_B, slice(c0 * HEAD, c1 * HEAD))
            for c in range(c0, c1):
                t = a[:, (c - c0) * HEAD:(c - c0 + 1) * HEAD]
                kind = c // heads
                if kind < 2:
                    t = t * lax.rsqrt(row_mean(t * t) + NORM_EPS) * row_of(small_ref, path, Q_GAIN + kind, slice(HEAD))
                    swapped = jnp.where(even, pltpu.roll(t, HEAD - 1, 1), pltpu.roll(t, 1, 1))
                    t = t * cos_t + swapped * sin_t
                qkv[c, at, :] = t.astype(BF16)

    m_wait(0)
    for j in range(n_dev):
        rows_here = m_early[j].astype(F32)
        for n in range(2 * 2 * batch):
            k, sel = n // (2 * batch), n % (2 * batch)
            vec_ref[sel, k:k + 1, j * width:(j + 1) * width] = rows_here[n:n + 1, :]
    x_wait(0)
    norm(0, ua)
    for path in PATHS:
        for j in range(3):
            w_load(path, j).wait()

    def qkv_step(t):
        x_start(2 * t + 3)
        x_start(2 * t + 4)
        x_wait(2 * t + 1)
        x_wait(2 * t + 2)
        @pl.when(t < 8)
        def _():
            late_load(t, 0).wait()

        late_chunk(t)
        norm(2 * t + 1, ub)
        heads_of(2 * t, ua)
        norm(jnp.minimum(2 * t + 2, blocks - 1), ua)
        heads_of(2 * t + 1, ub)

        @pl.when(t < 6)
        def _():
            late_start(t + 2)

    kv_store = pltpu.make_async_copy(qkv.at[:, total:, :], kv_hbm, tsem.at[0])

    def late_send():
        m_send(1)

    def kv_send():
        kv_store.start()

    done_here = batch + per_img

    def rows_of(n, c, size, r0):
        return qkv[c, rows_at(position(n)[0] * total + r0, size), :]

    def scores(n, h, s):
        s[...] = scores_of(rows_of(n, h, rows, position(n)[1]), rows_of(n, heads + h, total, 0))

    def weigh(n, h, s):
        o_all[rows_at(n * rows, rows), h * HEAD:(h + 1) * HEAD] = weighted(s[...], rows_of(n, 2 * heads + h, total, 0))

    def t_copy(kind, b, src, dst, dev):
        return remote(tsend, trecv, kind, b, src, dst, dev)

    def t_core(b):
        return t_copy(T_CORE, b, t_send, t_recv.at[b], partner)

    def t_first(b):
        return t_copy(T_FIRST, b, t_sum.at[b, rows_at(not1 * quarter, quarter), :], t_rs1.at[b], first)

    def t_second(b):
        return t_copy(T_SECOND, b, t_rs2_out.at[b], t_rs2_in.at[b], second)

    def own_rows(b1, b2):
        return rows_at(core * half + b1 * quarter + b2 * eighth, eighth)

    def t_out(kind, b, b1, b2, dev):
        ref = ut_hbm.at[b, own_rows(b1, b2), :]
        return t_copy(kind, b, t_u.at[b] if kind in (T_OUT_FIRST, T_OUT_SECOND, T_CORE_OWN) else ref, ref, dev)

    def t_local(b):
        return pltpu.make_async_copy(t_u.at[b], ut_hbm.at[b, own_rows(bit1, bit2), :], tsem.at[2 + b])

    def t_load(b):
        return pltpu.make_async_copy(txt_hbm.at[b, own_rows(bit1, bit2), :], t_x.at[b], tsem.at[2 + batch + b])

    tile = min(512, dim)

    def text_product(b, who, store):
        def columns(n):
            at = rows_at(n * tile, tile)
            store(at, jnp.dot(o_all[rows_at(b * rows + who * half, half), :], tw[:, at], preferred_element_type=F32))

        loop(dim // tile, columns)

    def text_partial(b):
        if b == 0:
            tw_load.wait()
        t_load(b).start()

        def to_send(at, value):
            t_send[:, at] = value.astype(BF16)

        def to_own(at, value):
            t_own[:, at] = value

        text_product(b, far, to_send)
        t_core(b).start()
        text_product(b, core, to_own)

    def text_sum(b):
        t_core(b).wait()

        def add(n):
            at = rows_at(n * STRIP, STRIP)
            t_sum[b, at, :] = (t_own[at, :] + t_recv[b, at, :].astype(F32)).astype(BF16)

        loop(half // STRIP, add)
        t_first(b).start()

    def text_quarter(b):
        t_first(b).wait()
        t_rs2_out[b] = (t_sum[b, rows_at(bit1 * quarter + not2 * eighth, eighth), :].astype(F32) + t_rs1[b, rows_at(not2 * eighth, eighth), :].astype(F32)).astype(BF16)
        t_keep[b] = t_sum[b, rows_at(bit1 * quarter + bit2 * eighth, eighth), :].astype(F32) + t_rs1[b, rows_at(bit2 * eighth, eighth), :].astype(F32)
        t_second(b).start()

    def text_finish(b):
        t_second(b).wait()
        t_load(b).wait()
        branch = t_keep[b] + t_rs2_in[b].astype(F32) + row_of(vec_ref, b, PROJ_B)
        x1 = (t_x[b].astype(F32) + row_of(vec_ref, b, GATE1) * branch).astype(BF16)
        x1_ref[b] = x1
        t_u[b] = modulated(x1.astype(F32), vec_ref, b, SHIFT2, SCALE2)
        t_out(T_OUT_FIRST, b, bit1, bit2, first).start()
        t_out(T_OUT_SECOND, b, bit1, bit2, second).start()
        t_out(T_CORE_OWN, b, bit1, bit2, partner).start()
        t_local(b).start()

    def text_relay(b):
        t_out(T_OUT_FIRST, b, not1, bit2, first).wait_recv()
        t_out(T_OUT_RELAY, b, not1, bit2, second).start()
        t_out(T_CORE_FIRST, b, not1, bit2, partner).start()
        t_out(T_OUT_SECOND, b, bit1, not2, second).wait_recv()
        t_out(T_CORE_SECOND, b, bit1, not2, partner).start()

    def text_last(b):
        t_out(T_OUT_RELAY, b, not1, not2, second).wait_recv()
        t_out(T_CORE_RELAY, b, not1, not2, partner).start()

    def g_rows(m, who):
        return o_all.at[rows_at((batch + m) * rows + who * half, half), :]

    def g_mine(m):
        return og_hbm.at[m, :, rows_at(me * width, width)]

    def g_local(m):
        return pltpu.make_async_copy(g_rows(m, core), g_mine(m), gsem.at[m])

    def g_core(m):
        return remote(gsend, grecv, G_CORE, m, g_rows(m, far), g_mine(m), partner)

    def g_copy(kind, m, owner, dev):
        ref = og_hbm.at[m, :, rows_at(owner // 2 * (2 * width), 2 * width)]
        return remote(gsend, grecv, kind, m, ref, ref, dev)

    def gather_start(m):
        g_local(m).start()
        g_core(m).start()

    def gather_send(m):
        g_local(m).wait()
        g_core(m).wait()
        g_copy(G_FIRST, m, me, first).start()
        g_copy(G_SECOND, m, me, second).start()

    def gather_relay(m):
        g_copy(G_FIRST, m, first, first).wait_recv()
        g_copy(G_RELAY, m, first, second).start()

    qkv_first, attend_first = (batch + per_img) // 2, 1 + EARLY
    resume = blocks // 2 + attend_first
    steps = blocks // 2 + done_here
    known = dict(locals())

    def run(calls):
        for call in calls:
            name, *args = call.split()
            known[name](*map(int, args))

    def attended(a):
        early = ((a >= 1) & (a <= EARLY)).astype(jnp.int32)
        return a + early - EARLY * (a == attend_first).astype(jnp.int32)

    def attention_step(a, begins):
        n = attended(a)

        @pl.when(begins)
        def _():
            scores(n, 0, s0)

        scores(n, 1, s1)
        weigh(n, 0, s0)
        scores(n, 2, s2)
        weigh(n, 1, s1)
        scores(attended(jnp.minimum(a + 1, done_here - 1)), 0, s0)
        weigh(n, 2, s2)

    def step(i):
        for when, calls in enumerate(HOOKS[:steps]):
            if calls:
                @pl.when(i == when)
                def _():
                    run(calls)

        in_first = i < qkv_first
        in_second = (i >= qkv_first + attend_first) & (i < resume)

        @pl.when(in_first | in_second)
        def _():
            qkv_step(i - attend_first * in_second.astype(jnp.int32))

        @pl.when(jnp.logical_not(in_first | in_second))
        def _():
            late = (i >= resume).astype(jnp.int32)
            attention_step(i - late * (blocks // 2) - (1 - late) * qkv_first, (i == qkv_first) | (i == resume))

    loop(steps, step)

    o_out = pltpu.make_async_copy(o_all.at[batch * rows:, :], o_hbm, osem)
    o_out.start()
    run(HOOKS[steps])
    o_out.wait()
    kv_store.wait()
    for b in range(batch):
        t_local(b).wait()
        for kind, b1, b2, dev in ((T_OUT_FIRST, bit1, bit2, first), (T_OUT_SECOND, bit1, bit2, second), (T_OUT_RELAY, not1, bit2, second)):
            t_out(kind, b, b1, b2, dev).wait_send()
        for kind, b1, b2 in ((T_CORE_OWN, bit1, bit2), (T_CORE_FIRST, not1, bit2), (T_CORE_SECOND, bit1, not2), (T_CORE_RELAY, not1, not2)):
            t_out(kind, b, b1, b2, partner).wait()
    for j in (SHARED, COMMON):
        for kind, owner, dev in ((W_FIRST, me, first), (W_SECOND, me, second), (W_RELAY, first, second)):
            p_copy(kind, j, owner, dev).wait_send()
    w_own().wait()
    for kind, owner, core_kind in from_beside:
        z_copy(kind, owner).wait_send()
        for j in range(PIECES):
            p_copy(core_kind, j, owner, partner).wait()
    for m in range(READY):
        g_copy(G_FIRST, m, me, first).wait_send()
        g_copy(G_SECOND, m, me, second).wait_send()
        g_copy(G_RELAY, m, first, second).wait_send()
        g_copy(G_SECOND, m, second, second).wait_recv()
        g_copy(G_RELAY, m, diagonal, second).wait_recv()


HOOKS = (
    (),
    (),
    (),
    (),
    ('w_relay 0', 'w_second 0'),
    ('w_relay 1',),
    ('text_partial 0',),
    ('text_sum 0',),
    ('gather_start 0',),
    (),
    ('gather_send 0',),
    ('late_send', 'text_quarter 0', 'gather_start 1'),
    ('kv_send', 'w_last 1', 'gather_send 1'),
    ('late_rows', 'text_finish 0', 'text_partial 1', 'w_beside 0', 'w_last 0', 'text_sum 1'),
    (),
    ('gather_relay 1', 'text_quarter 1', 'gather_start 2', 'gather_send 2', 'text_relay 0'),
    ('w_beside 1', 'text_finish 1'),
    ('w_beside 2', 'w_second 1', 'gather_relay 0'),
    ('text_relay 1', 'gather_relay 2'),
    ('text_last 1', 'text_last 0'),
)


def front_call(txt, img, wt, wi, mt, mi, pw, tw, cond, small_t, small_i, ids_t, table, n_dev, rows):
    batch, txt_len, dim = txt.shape
    img_len = img.shape[1]
    total = txt_len + img_len
    width = pw.shape[0]
    heads = width // HEAD
    half, quarter, eighth = rows // 2, rows // 4, rows // 8
    assert heads == HEADS_HERE and batch == 2
    cfg = (batch, txt_len, img_len, rows)
    blocks = batch * (1 + img_len // rows)
    vmem = pl.BlockSpec(memory_space=pltpu.VMEM)
    anywhere = pl.BlockSpec(memory_space=pl.ANY)
    tall = [pltpu.VMEM((half, dim), BF16), pltpu.VMEM((batch, half, dim), BF16), pltpu.VMEM((half, dim), F32), pltpu.VMEM((batch, half, dim), BF16), pltpu.VMEM((batch, quarter, dim), BF16)]
    short = [pltpu.VMEM((batch, eighth, dim), dtype) for dtype in (BF16, BF16, F32, BF16, BF16)]
    return pl.pallas_call(
        functools.partial(front_kernel, cfg),
        in_specs=[anywhere] * 8 + [vmem, (vmem,) * len(small_t), (vmem,) * len(small_i), vmem, vmem],
        out_specs=[anywhere] * 5 + [vmem] * 3,
        out_shape=[
            jax.ShapeDtypeStruct((img_len, width), BF16),
            jax.ShapeDtypeStruct((3 * heads, total, HEAD), BF16),
            jax.ShapeDtypeStruct((n_dev, width, dim), BF16),
            jax.ShapeDtypeStruct((batch, txt_len, dim), BF16),
            jax.ShapeDtypeStruct((READY, half, dim), BF16),
            jax.ShapeDtypeStruct((batch, eighth, dim), BF16),
            jax.ShapeDtypeStruct((2 * batch, FC2_B + 1, dim), F32),
            jax.ShapeDtypeStruct((2, FC1_B + 1, dim), F32),
        ],
        scratch_shapes=[
            pltpu.VMEM((2, dim, 3 * width), BF16),
            pltpu.VMEM((2, dim, width), BF16),
            pltpu.VMEM((2, PROJ_B, width), F32),
            pltpu.VMEM((n_dev, 4 * batch, width), BF16),
            pltpu.VMEM((n_dev, blocks // 2, batch, width), F32),
            pltpu.VMEM((4, rows, dim), BF16),
            pltpu.VMEM((batch, half, dim), BF16),
            pltpu.VMEM((batch, half, dim), BF16),
            pltpu.VMEM((3 * heads, batch * total, HEAD), BF16),
            pltpu.VMEM((rows, total), F32),
            pltpu.VMEM((rows, total), F32),
            pltpu.VMEM((rows, total), F32),
            pltpu.VMEM((batch * txt_len + img_len, width), BF16),
            pltpu.VMEM((width, dim), BF16),
            *tall,
            *short,
            pltpu.SemaphoreType.DMA((2, 3)),
            pltpu.SemaphoreType.DMA((2,)),
            pltpu.SemaphoreType.DMA((4,)),
            pltpu.SemaphoreType.DMA,
            pltpu.SemaphoreType.DMA((6,)),
            pltpu.SemaphoreType.DMA((READY,)),
            *[pltpu.SemaphoreType.DMA((10, PIECES))] * 2,
            *[pltpu.SemaphoreType.DMA((10, batch))] * 2,
            *[pltpu.SemaphoreType.DMA((4, READY))] * 2,
            pltpu.SemaphoreType.DMA((2, n_dev)),
            pltpu.SemaphoreType.DMA((2, n_dev)),
        ],
        compiler_params=pltpu.CompilerParams(collective_id=2, has_side_effects=True, vmem_limit_bytes=VMEM_BYTES),
        name="front",
    )(txt, img, wt, wi, mt, mi, pw, tw, cond, small_t, small_i, ids_t, table)


(O_CORE, O_FIRST, O_SECOND, O_RELAY, U_CORE, PART_CORE, RS_FIRST, RS_SECOND, OUT_FIRST, OUT_SECOND, OUT_RELAY, CORE_OWN, CORE_FIRST, CORE_SECOND, CORE_RELAY) = range(15)
(L_O, L_X, L_OUT) = range(3)
SLOTS = 4
O_SLOTS = 6
SEMS = 8


def two(n):
    return n % 2


def block_kernel(cfg, o_hbm, og_hbm, kv_hbm, x_hbm, ut_hbm, x1t_hbm, wp_hbm, pw_hbm, w1t_hbm, w2t_hbm, w1i_hbm, w2i_hbm, vec_ref, fb_ref, out_hbm, o2_hbm,
                 kv, qs, os, wp, w1, w2, obuf, xbuf, x1buf, x1keep, u2, hid, psend, precv, own, chip_sum, rs1, keep2, rs2_out, rs2_in, outb,
                 asem, wsem, lsem, tsem, ssem, rsem):
    batch, txt_chunks, img_chunks, per_img, rows, tile = cfg
    half, quarter, eighth = rows // 2, rows // 4, rows // 8
    dim = wp.shape[0]
    ff = w1.shape[1]
    cols = o_hbm.shape[1]
    heads = cols // HEAD
    total = txt_chunks + img_chunks
    per_txt = txt_chunks // batch

    place = Place()
    me, core, partner, first, second, bit1, bit2 = place.me, place.core, place.partner, place.first, place.second, place.bit1, place.bit2
    not1, not2, far = place.not1, place.not2, place.far
    txt_len = ut_hbm.shape[1]
    place.enter([partner, first, second])

    def remote(kind, g, src, dst, dev):
        return pltpu.make_async_remote_copy(src_ref=src, dst_ref=dst, send_sem=ssem.at[kind, g % SEMS], recv_sem=rsem.at[kind, g % SEMS], device_id={'tp': dev}, device_id_type=MESH)

    def img_pos(g):
        k = g - txt_chunks
        return k // per_img, (k % per_img) * rows

    def chip_cols(dev):
        return rows_at((dev // 2) * (2 * cols), 2 * cols)

    def own_rows(b1, b2):
        return core * half + b1 * quarter + b2 * eighth

    def o_from(b):
        return (o_hbm, o2_hbm)[b]

    first_open = txt_chunks + og_hbm.shape[0]

    def o_ready(g):
        return pltpu.make_async_copy(og_hbm.at[g - txt_chunks], obuf.at[g % O_SLOTS], lsem.at[L_O, g % SEMS])

    def o_local(g, b):
        r0 = img_pos(g)[1]
        return pltpu.make_async_copy(o_from(b).at[rows_at(r0 + core * half, half), :], obuf.at[g % O_SLOTS, :, rows_at(me * cols, cols)], lsem.at[L_O, g % SEMS])

    def o_core(g, b):
        r0 = img_pos(g)[1]
        return remote(O_CORE, g, o_from(b).at[rows_at(r0 + far * half, half), :], obuf.at[g % O_SLOTS, :, rows_at(me * cols, cols)], partner)

    units = per_img * heads

    def q_load(u):
        r0 = txt_len + u // heads * rows
        return pltpu.make_async_copy(kv_hbm.at[u % heads, rows_at(r0, rows), :], qs.at[two(u)], asem.at[two(u)])

    def o_store(u):
        return pltpu.make_async_copy(os.at[two(u)], o2_hbm.at[rows_at(u // heads * rows, rows), rows_at(u % heads * HEAD, HEAD)], asem.at[2 + two(u)])

    def kv_load():
        return pltpu.make_async_copy(kv_hbm.at[heads:], kv, asem.at[4])

    def attend(u):
        q_load(u).wait()

        @pl.when(u + 1 < units)
        def _():
            q_load(u + 1).start()

        @pl.when(u >= 2)
        def _():
            o_store(u - 2).wait()

        k = kv[u % heads]
        v = kv[heads + u % heads]
        for r in range(0, rows, half):
            os[two(u), r:r + half, :] = weighted(scores_of(qs[two(u), r:r + half, :], k), v)
        o_store(u).start()

    def attend_pair(i):
        @pl.when(i == 0)
        def _():
            kv_load().wait()

        attend(2 * i)
        attend(2 * i + 1)

        @pl.when(i == units // 2 - 1)
        def _():
            o_store(units - 2).wait()
            o_store(units - 1).wait()

    def o_send(kind, g, owner, dev):
        ref = obuf.at[g % O_SLOTS, :, chip_cols(owner)]
        return remote(kind, g, ref, ref, dev)

    def x_load(g):
        b, r0 = img_pos(g)
        return pltpu.make_async_copy(x_hbm.at[b, rows_at(r0 + core * half, half), :], xbuf.at[two(g)], lsem.at[L_X, g % SEMS])

    def u_core(g):
        ref = u2.at[two(g), rows_at(core * half, half), :]
        return remote(U_CORE, g, ref, ref, partner)

    def part_core(g):
        return remote(PART_CORE, g, psend, precv.at[two(g)], partner)

    def rs_first(g):
        return remote(RS_FIRST, g, chip_sum.at[rows_at(not1 * quarter, quarter), :], rs1.at[two(g)], first)

    def rs_second(g):
        return remote(RS_SECOND, g, rs2_out.at[two(g)], rs2_in.at[g % SLOTS], second)

    def out_ref(g, b1, b2):
        return out_hbm.at[rows_at(g * rows + own_rows(b1, b2), eighth), :]

    def out_send(kind, g, b1, b2, dev):
        ref = out_ref(g, b1, b2)
        mine = kind in (OUT_FIRST, OUT_SECOND, CORE_OWN)
        return remote(kind, g, outb.at[g % SLOTS] if mine else ref, ref, dev)

    def out_local(g):
        return pltpu.make_async_copy(outb.at[g % SLOTS], out_ref(g, bit1, bit2), lsem.at[L_OUT, g % SEMS])

    def txt_load(g):
        b, r0 = g // per_txt, (g % per_txt) * rows
        return (pltpu.make_async_copy(ut_hbm.at[b, rows_at(r0, rows), :], u2.at[two(g)], tsem.at[0, two(g)]),
                pltpu.make_async_copy(x1t_hbm.at[g], x1keep.at[g % SLOTS], tsem.at[1, two(g)]))

    def w_load(k, src, dst):
        return pltpu.make_async_copy(src, dst, wsem.at[k])

    def wp_load(j, src):
        return pltpu.make_async_copy(src, wp.at[j * cols:(j + 1) * cols, :], wsem.at[2 + j])

    def select(g):
        txt = (g < txt_chunks).astype(jnp.int32)
        return txt * (g // per_txt) + (1 - txt) * (batch + (g - txt_chunks) // per_img)

    def start_o(g):
        @pl.when(g < first_open)
        def _():
            o_ready(g).start()

        for b in range(batch):
            @pl.when((g >= first_open) & (img_pos(g)[0] == b))
            def _():
                o_local(g, b).start()
                o_core(g, b).start()

    def send_o(g):
        o_local(g, 0).wait()
        o_core(g, 0).wait()
        o_send(O_FIRST, g, me, first).start()
        o_send(O_SECOND, g, me, second).start()

    def relay_o(g):
        o_send(O_FIRST, g, first, first).wait_recv()
        o_send(O_RELAY, g, first, second).start()

    def start_x(g):
        x_load(g).start()

    def project(g):
        @pl.when(g < first_open)
        def _():
            o_ready(g).wait()

        @pl.when(g >= first_open)
        def _():
            o_send(O_FIRST, g, me, first).wait_send()
            o_send(O_SECOND, g, me, second).wait_send()
            o_send(O_RELAY, g, first, second).wait_send()
            o_send(O_SECOND, g, second, second).wait_recv()
            o_send(O_RELAY, g, second, second).wait_recv()

        x_load(g).wait()

        @pl.when(g == txt_chunks)
        def _():
            for j in range(wp_hbm.shape[0]):
                wp_load(j, wp_hbm.at[j]).wait()

        sel = select(g)
        slot = g % SLOTS

        def columns(n):
            at = rows_at(n * tile, tile)
            acc = jnp.dot(obuf[g % O_SLOTS], wp[:, at], preferred_element_type=F32)
            branch = acc + row_of(vec_ref, sel, PROJ_B, at)
            x1buf[:, at] = (xbuf[two(g), :, at].astype(F32) + row_of(vec_ref, sel, GATE1, at) * branch).astype(BF16)

        loop(dim // tile, columns)

        def norm(n):
            at = rows_at(n * STRIP, STRIP)
            u2[two(g), rows_at(core * half + n * STRIP, STRIP), :] = modulated(x1buf[at, :].astype(F32), vec_ref, sel, SHIFT2, SCALE2)

        loop(half // STRIP, norm)
        u_core(g).start()
        x1keep[slot] = x1buf[rows_at(bit1 * quarter + bit2 * eighth, eighth), :]

    def mlp_hidden(g):
        @pl.when(g < txt_chunks)
        def _():
            for copy in txt_load(g):
                copy.wait()

        @pl.when(g >= txt_chunks)
        def _():
            u_core(g).wait()

        @pl.when(g == 0)
        def _():
            w_load(0, w1t_hbm, w1).wait()
            w_load(1, w2t_hbm, w2).wait()
            for j in range(wp_hbm.shape[0]):
                @pl.when(j != me)
                def _():
                    wp_load(j, wp_hbm.at[j]).start()

                @pl.when(j == me)
                def _():
                    wp_load(j, pw_hbm).start()

        @pl.when(g == txt_chunks)
        def _():
            w_load(0, w1i_hbm, w1).wait()
            w_load(1, w2i_hbm, w2).wait()

        path = (g >= txt_chunks).astype(jnp.int32)

        def hidden(n):
            at = rows_at(n * tile, tile)
            acc = jnp.dot(u2[two(g)], w1[:, at], preferred_element_type=F32)
            pre = acc + row_of(fb_ref, path, FC1_B, at)
            hid[:, at] = jax.nn.gelu(pre, approximate=True).astype(BF16)

        loop(ff // tile, hidden)

    def mlp_theirs(g):
        def theirs(n):
            at = rows_at(n * tile, tile)
            psend[:, at] = jnp.dot(hid[rows_at(far * half, half), :], w2[:, at], preferred_element_type=F32).astype(BF16)

        loop(dim // tile, theirs)
        part_core(g).start()

    def mlp_mine(g):
        def mine(n):
            at = rows_at(n * tile, tile)
            own[:, at] = jnp.dot(hid[rows_at(core * half, half), :], w2[:, at], preferred_element_type=F32)

        loop(dim // tile, mine)

        @pl.when(g == txt_chunks - 1)
        def _():
            w_load(0, w1i_hbm, w1).start()
            w_load(1, w2i_hbm, w2).start()

        part_core(g).wait()

        def add(n):
            at = rows_at(n * STRIP, STRIP)
            chip_sum[at, :] = (own[at, :] + precv[two(g), at, :].astype(F32)).astype(BF16)

        loop(half // STRIP, add)
        rs_first(g).start()

    def add_first(g):
        rs_first(g).wait()
        rs2_out[two(g)] = (chip_sum[rows_at(bit1 * quarter + not2 * eighth, eighth), :].astype(F32) + rs1[two(g), rows_at(not2 * eighth, eighth), :].astype(F32)).astype(BF16)
        rs_second(g).start()
        keep2[two(g)] = chip_sum[rows_at(bit1 * quarter + bit2 * eighth, eighth), :].astype(F32) + rs1[two(g), rows_at(bit2 * eighth, eighth), :].astype(F32)

    def finish(g):
        rs_second(g).wait()
        sel = select(g)
        branch = keep2[two(g)] + rs2_in[g % SLOTS].astype(F32) + row_of(vec_ref, sel, FC2_B)
        outb[g % SLOTS] = (x1keep[g % SLOTS].astype(F32) + row_of(vec_ref, sel, GATE2) * branch).astype(BF16)
        out_send(OUT_FIRST, g, bit1, bit2, first).start()
        out_send(OUT_SECOND, g, bit1, bit2, second).start()
        out_send(CORE_OWN, g, bit1, bit2, partner).start()
        out_local(g).start()

    def relay_out(g):
        out_send(OUT_FIRST, g, not1, bit2, first).wait_recv()
        out_send(OUT_RELAY, g, not1, bit2, second).start()
        out_send(CORE_FIRST, g, not1, bit2, partner).start()

    def second_out(g):
        out_send(OUT_SECOND, g, bit1, not2, second).wait_recv()
        out_send(CORE_SECOND, g, bit1, not2, partner).start()

    def relay_core(g):
        out_send(OUT_RELAY, g, not1, not2, second).wait_recv()
        out_send(CORE_RELAY, g, not1, not2, partner).start()

    def drain(g):
        out_local(g).wait()
        out_send(OUT_FIRST, g, bit1, bit2, first).wait_send()
        out_send(OUT_SECOND, g, bit1, bit2, second).wait_send()
        out_send(OUT_RELAY, g, not1, bit2, second).wait_send()
        out_send(CORE_OWN, g, bit1, bit2, partner).wait()
        out_send(CORE_FIRST, g, not1, bit2, partner).wait()
        out_send(CORE_SECOND, g, bit1, not2, partner).wait()
        out_send(CORE_RELAY, g, not1, not2, partner).wait()

    kv_load().start()
    q_load(0).start()
    w_load(0, w1t_hbm, w1).start()
    w_load(1, w2t_hbm, w2).start()
    for g in range(txt_chunks):
        for copy in txt_load(g):
            copy.start()

    stages = ((mlp_hidden, 0, 0), (relay_o, 2, first_open), (start_x, 2, txt_chunks), (finish, -3, 0), (start_o, 5, txt_chunks), (relay_out, -4, 0), (mlp_theirs, 0, 0), (second_out, -5, 0),
              (send_o, 5, first_open), (relay_core, -6, 0), (project, 1, txt_chunks), (add_first, -1, 0), (mlp_mine, 0, 0), (drain, -6, 0))
    most = max(ahead for _, ahead, _ in stages)
    least = min(ahead for _, ahead, _ in stages)

    def step(i):
        for stage, ahead, lowest in stages:
            g = i + txt_chunks - most + ahead

            @pl.when((g >= lowest) & (g < total))
            def _():
                stage(g)

        @pl.when((i >= ATTEND_FROM) & (i < ATTEND_FROM + units // 2))
        def _():
            attend_pair(i - ATTEND_FROM)

    loop(total - txt_chunks + most - least, step)


ATTEND_FROM = 1


def block_call(img_o, og, kv, x, u_txt, x1_txt, wp, pw, w1t, w2t, w1i, w2i, vecs, fb, rows):
    batch, img_len, dim = x.shape
    txt_len = u_txt.shape[1]
    ff = w1t.shape[1]
    txt_chunks = batch * (txt_len // rows)
    per_img = img_len // rows
    img_chunks = batch * per_img
    assert txt_chunks == 2
    half, quarter, eighth = rows // 2, rows // 4, rows // 8
    cfg = (batch, txt_chunks, img_chunks, per_img, rows, 512)
    total = txt_chunks + img_chunks
    anywhere = pl.BlockSpec(memory_space=pl.ANY)
    return pl.pallas_call(
        functools.partial(block_kernel, cfg),
        in_specs=[anywhere] * 12 + [pl.BlockSpec(memory_space=pltpu.VMEM)] * 2,
        out_specs=[anywhere, anywhere],
        out_shape=[jax.ShapeDtypeStruct((total * rows, dim), BF16), jax.ShapeDtypeStruct(img_o.shape, BF16)],
        scratch_shapes=[
            pltpu.VMEM((kv.shape[0] // 3 * 2,) + kv.shape[1:], BF16),
            pltpu.VMEM((2, rows, HEAD), BF16),
            pltpu.VMEM((2, rows, HEAD), BF16),
            pltpu.VMEM((dim, dim), BF16),
            pltpu.VMEM((dim, ff), BF16),
            pltpu.VMEM((ff, dim), BF16),
            pltpu.VMEM((O_SLOTS, half, dim), BF16),
            pltpu.VMEM((2, half, dim), BF16),
            pltpu.VMEM((half, dim), BF16),
            pltpu.VMEM((SLOTS, eighth, dim), BF16),
            pltpu.VMEM((2, rows, dim), BF16),
            pltpu.VMEM((rows, ff), BF16),
            pltpu.VMEM((half, dim), BF16),
            pltpu.VMEM((2, half, dim), BF16),
            pltpu.VMEM((half, dim), F32),
            pltpu.VMEM((half, dim), BF16),
            pltpu.VMEM((2, quarter, dim), BF16),
            pltpu.VMEM((2, eighth, dim), F32),
            pltpu.VMEM((2, eighth, dim), BF16),
            pltpu.VMEM((SLOTS, eighth, dim), BF16),
            pltpu.VMEM((SLOTS, eighth, dim), BF16),
            pltpu.SemaphoreType.DMA((5,)),
            pltpu.SemaphoreType.DMA((10,)),
            pltpu.SemaphoreType.DMA((3, SEMS)),
            pltpu.SemaphoreType.DMA((2, 2)),
            pltpu.SemaphoreType.DMA((15, SEMS)),
            pltpu.SemaphoreType.DMA((15, SEMS)),
        ],
        compiler_params=pltpu.CompilerParams(collective_id=0, has_side_effects=True, vmem_limit_bytes=VMEM_BYTES),
        name="block",
    )(img_o, og, kv, x, u_txt, x1_txt, wp, pw, w1t, w2t, w1i, w2i, vecs, fb)


def copy_kernel(pieces, flat_hbm, *rest):
    outs, (buf, isem, osem) = rest[:-3], rest[-3:]
    rows = buf.shape[1]
    loads = []
    for n, (which, b, r) in enumerate(pieces):
        load = pltpu.make_async_copy(flat_hbm.at[n * rows:(n + 1) * rows, :], buf.at[n], isem.at[n])
        load.start()
        loads.append(load)
    stores = []
    for n, (which, b, r) in enumerate(pieces):
        loads[n].wait()
        store = pltpu.make_async_copy(buf.at[n], outs[which].at[b, r:r + rows, :], osem.at[n])
        store.start()
        stores.append(store)
    for store in stores:
        store.wait()


def copy_call(flat, shapes, rows):
    pieces = [(which, b, r) for which, shape in enumerate(shapes) for b in range(shape[0]) for r in range(0, shape[1], rows)]
    anywhere = pl.BlockSpec(memory_space=pl.ANY)
    dim = flat.shape[1]
    return pl.pallas_call(
        functools.partial(copy_kernel, pieces),
        in_specs=[anywhere],
        out_specs=[anywhere] * len(shapes),
        out_shape=[jax.ShapeDtypeStruct(shape, flat.dtype) for shape in shapes],
        scratch_shapes=[
            pltpu.VMEM((len(pieces), rows, dim), flat.dtype),
            pltpu.SemaphoreType.DMA((len(pieces),)),
            pltpu.SemaphoreType.DMA((len(pieces),)),
        ],
        compiler_params=pltpu.CompilerParams(vmem_limit_bytes=VMEM_BYTES),
        name="copy_out",
    )(flat)


def local_block(img, txt, vec, ids, img_w, txt_w):
    n_dev = 8
    batch, txt_len = txt.shape[:2]
    rows = txt_len

    def by_kind(weight):
        return jnp.transpose(weight, (1, 0, 2))

    def small_of(w):
        return w[1], w[3], w[4], w[5], w[7], w[9], w[11]

    table = jnp.asarray(rope_table())
    ids_t = jnp.transpose(ids, (2, 0, 1))
    o, kv, proj_w, txt_u, og, txt_x1, vecs, small = front_call(txt, img, by_kind(txt_w[2]), by_kind(img_w[2]), by_kind(txt_w[0]), by_kind(img_w[0]), img_w[6], txt_w[6], vec, small_of(txt_w), small_of(img_w), ids_t, table, n_dev, rows)
    flat, _ = block_call(o, og, kv, img, txt_u, txt_x1, proj_w, img_w[6], txt_w[8], txt_w[10], img_w[8], img_w[10], vecs, small, rows)
    txt_out, img_out = copy_call(flat, (txt.shape, img.shape), rows)
    return img_out, txt_out


def solution(mesh):
    act_spec = P('dp', WHOLE, WHOLE)
    mapped = jax.shard_map(local_block, mesh=mesh, in_specs=(act_spec, act_spec, P('dp', WHOLE), act_spec, PATH_SPECS, PATH_SPECS), out_specs=(act_spec, act_spec), check_vma=False)

    def forward(img, txt, vec, ids, *weights):
        return mapped(img, txt, vec, ids, weights[:12], weights[12:])

    return forward
```

```python
import functools

import jax
import jax.numpy as jnp
import numpy as np
from jax import lax
from jax.experimental import pallas as pl
from jax.experimental.pallas import tpu as pltpu
from jax.sharding import PartitionSpec as P

HEAD = 128
NORM_EPS = 1e-6
ROPE_THETA = 10000.0
AXES_DIM = (16, 56, 56)
N_IDS = 64
WHOLE = None
PATH_SPECS = (P(WHOLE, WHOLE, 'tp'), P(WHOLE, 'tp'), P(WHOLE, WHOLE, 'tp'), P(WHOLE, 'tp'), P(WHOLE), P(WHOLE), P('tp', WHOLE), P(WHOLE), P(WHOLE, 'tp'), P('tp'), P('tp', WHOLE), P(WHOLE))
F32 = jnp.float32
BF16 = jnp.bfloat16


def rope_table():
    cos = np.zeros((3 * N_IDS, HEAD), np.float32)
    sin = np.zeros((3 * N_IDS, HEAD), np.float32)
    lane = 0
    for axis, dim in enumerate(AXES_DIM):
        inv_freq = np.float32(ROPE_THETA) ** (-np.arange(0, dim, 2, dtype=np.float32) / np.float32(dim))
        angles = np.arange(N_IDS, dtype=np.float32)[:, None] * inv_freq.astype(np.float32)
        rows = slice(axis * N_IDS, (axis + 1) * N_IDS)
        c = np.cos(angles.astype(np.float64)).astype(np.float32)
        s = np.sin(angles.astype(np.float64)).astype(np.float32)
        cos[rows, lane:lane + dim:2] = c
        cos[rows, lane + 1:lane + dim:2] = c
        sin[rows, lane:lane + dim:2] = -s
        sin[rows, lane + 1:lane + dim:2] = s
        lane += dim
    parts = []
    for table in (cos, sin):
        rest = table
        for _ in range(3):
            part = rest.astype(jnp.bfloat16)
            parts.append(np.asarray(part))
            rest = rest - np.asarray(part).astype(np.float32)
    return np.concatenate(parts, axis=1)


MESH = pl.DeviceIdType.MESH


SHIFT1, SCALE1, GATE1, SHIFT2, SCALE2, GATE2, PROJ_B, FC2_B = range(8)
QKV_B, Q_GAIN, K_GAIN, FC1_B = range(4)
VMEM_BYTES = 67043328


def row_of(ref, sel, row, at=slice(None)):
    return ref[sel, pl.ds(row, 1), at]


STRIP = 16
PATHS = range(2)


def loop(count, body):
    lax.fori_loop(0, count, lambda i, carry: (body(i), carry)[-1], 0)


def row_mean(x):
    return jnp.mean(x, axis=-1, keepdims=True)


def normalize(x):
    centered = x - row_mean(x)
    return centered * lax.rsqrt(row_mean(centered * centered) + NORM_EPS)


def weighted(s, v):
    top = jnp.max(s, axis=-1, keepdims=True)
    p = jnp.exp2((s - top) * (HEAD ** -0.5 * LOG2E))
    total = jnp.sum(p, axis=-1, keepdims=True)
    o = jnp.dot(p.astype(BF16), v, preferred_element_type=F32)
    return (o * (1.0 / total)).astype(BF16)


def scores_of(q, k):
    return lax.dot_general(q, k, (((1,), (1,)), ((), ())), preferred_element_type=F32)


def modulated(x, vec_ref, sel, shift, scale):
    return ((1.0 + row_of(vec_ref, sel, scale)) * normalize(x) + row_of(vec_ref, sel, shift)).astype(BF16)


LOG2E = 1.4426950408889634
(W_FIRST, W_SECOND, W_RELAY, W_CORE, W_CORE_FIRST, W_CORE_SECOND, W_CORE_RELAY, Z_FIRST, Z_SECOND, Z_RELAY) = range(10)
(G_CORE, G_FIRST, G_SECOND, G_RELAY) = range(4)
(T_CORE, T_FIRST, T_SECOND, T_OUT_FIRST, T_OUT_SECOND, T_OUT_RELAY, T_CORE_OWN, T_CORE_FIRST, T_CORE_SECOND, T_CORE_RELAY) = range(10)
SHARED, COMMON, MISSING = range(3)
PIECES = 3
READY = 3
EARLY = 2
HEADS_HERE = 3


def ident(dev):
    return dev if isinstance(dev, dict) else {'tp': dev}


class Place:
    def __init__(self):
        me = lax.axis_index('tp')
        core = me % 2
        xi = (me // 2) % 2
        yi = me // 4
        x_next = me + 2 - 4 * xi
        y_next = me + 4 - 8 * yi
        self.me, self.core = me, core
        self.partner = me + 1 - 2 * core
        self.first = x_next * (1 - core) + y_next * core
        self.second = x_next * core + y_next * (1 - core)
        self.diagonal = x_next + y_next - me
        self.bit1 = xi * (1 - core) + yi * core
        self.bit2 = xi * core + yi * (1 - core)
        self.not1, self.not2, self.far = 1 - self.bit1, 1 - self.bit2, 1 - core

    def enter(self, others):
        barrier = pltpu.get_barrier_semaphore()
        for dev in others:
            pl.semaphore_signal(barrier, inc=1, device_id=ident(dev), device_id_type=MESH)
        pl.semaphore_wait(barrier, len(others))


def rows_at(start, size):
    return pl.ds(pl.multiple_of(start, size), size)


def front_kernel(cfg, txt_hbm, img_hbm, wt_hbm, wi_hbm, mt_hbm, mi_hbm, pw_hbm, tw_hbm, cond_ref, small_t, small_i, ids_ref, tab_ref,
                 o_hbm, kv_hbm, wp_hbm, ut_hbm, og_hbm, x1_ref, vec_ref, small_ref,
                 w, m_w, m_b, m_early, m_late, xs, ua, ub, qkv, s0, s1, s2, o_all, tw, t_send, t_recv, t_own, t_sum, t_rs1, t_rs2_out, t_rs2_in, t_keep, t_x, t_u,
                 wsem, msem, xsem, osem, tsem, gsem, psend, precv, tsend, trecv, gsend, grecv, msend, mrecv):
    batch, txt_len, img_len, rows = cfg
    half, quarter, eighth = rows // 2, rows // 4, rows // 8
    total = txt_len + img_len
    per_img = img_len // rows
    blocks = batch * (per_img + 1)
    n_dev = m_early.shape[0]
    others = range(1, n_dev)
    dim = w.shape[1]
    width = o_all.shape[1]
    heads = width // HEAD
    place = Place()
    me, core, partner, first, second, diagonal, bit1, bit2 = place.me, place.core, place.partner, place.first, place.second, place.diagonal, place.bit1, place.bit2
    not1, not2, far = place.not1, place.not2, place.far
    piece = width // PIECES
    plane = lax.axis_index('dp')
    odd = plane % 2
    beside = {'dp': plane + 1 - 2 * odd}

    def position(n):
        n = jnp.int32(n)
        img = (n >= batch).astype(jnp.int32)
        m = n - batch
        b = (1 - img) * n + img * (m // per_img)
        r = img * (1 + m % per_img)
        return b, r * rows

    def x_copy(n, source):
        b, r0 = position(n)
        ref = txt_hbm.at[b] if source == 0 else img_hbm.at[b, rows_at(r0 - rows, rows), :]
        return pltpu.make_async_copy(ref, xs.at[n % 4], xsem.at[n % 4])

    def x_start(n):
        @pl.when(n < batch)
        def _():
            x_copy(n, 0).start()

        @pl.when((n >= batch) & (n < blocks))
        def _():
            x_copy(n, 1).start()

    def x_wait(n):
        @pl.when(n < blocks)
        def _():
            pltpu.make_async_copy(txt_hbm.at[0], xs.at[n % 4], xsem.at[n % 4]).wait()

    def w_columns(path, j):
        return w.at[path, :, j * width:(j + 1) * width]

    def w_load(path, j):
        return pltpu.make_async_copy((wt_hbm, wi_hbm)[path].at[j], w_columns(path, j), wsem.at[path, j])

    def early_load(path, k):
        return pltpu.make_async_copy((mt_hbm, mi_hbm)[path].at[k], w_columns(path, k), wsem.at[path, k])

    def late_load(c, path):
        return pltpu.make_async_copy((mt_hbm, mi_hbm)[path].at[GATE1 + c // 2], m_w.at[c % 2], msem.at[c % 2])

    def late_start(c):
        for path in PATHS:
            @pl.when(c % 2 == path)
            def _():
                late_load(c, path).start()

    def m_copy(part, d, send):
        buf = (m_early, m_late)[part]
        ref = buf.at[me if send else (me + n_dev - d) % n_dev, :8]
        return pltpu.make_async_remote_copy(src_ref=ref, dst_ref=ref, send_sem=msend.at[part, d], recv_sem=mrecv.at[part, d], device_id={'tp': (me + d) % n_dev}, device_id_type=MESH)

    def m_send(part):
        for d in others:
            m_copy(part, d, True).start()

    def m_wait(part):
        for d in others:
            m_copy(part, d, True).wait_send()
            m_copy(part, d, False).wait_recv()

    for k in (SHIFT1, SCALE1):
        for path in PATHS:
            early_load(path, k).start()
    for n in range(3):
        x_copy(n, 0 if n < batch else 1).start()
    v = cond_ref[...].astype(F32)
    silu = (v * (1.0 / (1.0 + jnp.exp(-v)))).astype(BF16)
    for path, (mod_b, qkv_b, q_gain, k_gain, proj_b, fc1_b, fc2_b) in enumerate((small_t, small_i)):
        m_b[path] = mod_b[...].astype(F32)
        for row, ref in ((PROJ_B, proj_b), (FC2_B, fc2_b)):
            vector = ref[...].astype(F32)[None, :]
            for b in range(batch):
                vec_ref[path * batch + b, row:row + 1, :] = vector
        for row, ref in ((Q_GAIN, q_gain), (K_GAIN, k_gain), (FC1_B, fc1_b)):
            vector = ref[...].astype(F32)[None, :]
            small_ref[path, row:row + 1, :vector.shape[1]] = vector
        for j in range(qkv_b.shape[0]):
            small_ref[path, QKV_B:Q_GAIN, j * width:(j + 1) * width] = qkv_b[j:j + 1, :].astype(F32)
    place.enter([(me + d) % n_dev for d in others] + [beside])

    def early_chunk(k, path):
        early_load(path, k).wait()
        acc = jnp.dot(silu, w_columns(path, k)[...], preferred_element_type=F32)
        return (acc + m_b[path, k:k + 1, :]).astype(BF16)

    m_early[me] = jnp.concatenate([early_chunk(k, path) for k in (SHIFT1, SCALE1) for path in PATHS], axis=0)
    m_send(0)
    for j in range(3):
        w_load(0, j).start()
    tw_load = pltpu.make_async_copy(tw_hbm, tw, tsem.at[1])

    def late_chunk(t):
        c = jnp.minimum(t, 7)
        path, k = c % 2, GATE1 + c // 2
        acc = jnp.dot(silu, m_w[c % 2], preferred_element_type=F32) + m_b[path, pl.ds(k, 1), :]
        m_late[me, t] = acc.astype(BF16).astype(F32)

    def late_rows():
        m_wait(1)
        for j in range(n_dev):
            for c in range(8):
                for b in range(batch):
                    vec_ref[c % 2 * batch + b, pl.ds(GATE1 + c // 2, 1), j * width:(j + 1) * width] = m_late[j, c, b:b + 1, :]

    def piece_at(j):
        return rows_at(((1 - j) * (2 * odd - 1) + 1) * piece, piece)

    def remote(sends, recvs, kind, j, src, dst, dev):
        return pltpu.make_async_remote_copy(src_ref=src, dst_ref=dst, send_sem=sends.at[kind, j], recv_sem=recvs.at[kind, j], device_id=ident(dev), device_id_type=MESH)

    def p_copy(kind, j, owner, dev):
        dst = wp_hbm.at[owner, piece_at(j), :]
        src = pw_hbm.at[piece_at(j), :] if kind in (W_FIRST, W_SECOND) else dst
        return remote(psend, precv, kind, j, src, dst, dev)

    def w_own():
        return remote(psend, precv, W_CORE, SHARED, pw_hbm, wp_hbm.at[me], partner)

    def z_copy(kind, owner, j=SHARED):
        ref = wp_hbm.at[owner, piece_at(j), :]
        return remote(psend, precv, kind, SHARED, ref, ref, beside)

    def w_relay(j):
        p_copy(W_FIRST, j, first, first).wait_recv()
        p_copy(W_RELAY, j, first, second).start()
        p_copy(W_CORE_FIRST, j, first, partner).start()
        if j == SHARED:
            p_copy(W_SECOND, COMMON, me, second).start()
            z_copy(Z_FIRST, first).start()

    def w_second(j):
        p_copy(W_SECOND, j, second, second).wait_recv()
        p_copy(W_CORE_SECOND, j, second, partner).start()
        if j == SHARED:
            z_copy(Z_SECOND, second).start()

    def w_last(j):
        p_copy(W_RELAY, j, diagonal, second).wait_recv()
        p_copy(W_CORE_RELAY, j, diagonal, partner).start()
        if j == SHARED:
            z_copy(Z_RELAY, diagonal).start()

    from_beside = ((Z_FIRST, first, W_CORE_FIRST), (Z_SECOND, second, W_CORE_SECOND), (Z_RELAY, diagonal, W_CORE_RELAY))

    def w_beside(n):
        kind, owner, core_kind = from_beside[n]
        z_copy(kind, owner, MISSING).wait_recv()
        p_copy(core_kind, MISSING, owner, partner).start()

    p_copy(W_FIRST, SHARED, me, first).start()
    p_copy(W_SECOND, SHARED, me, second).start()
    p_copy(W_FIRST, COMMON, me, first).start()
    w_own().start()

    even = lax.broadcasted_iota(jnp.int32, (rows, HEAD), 1) % 2 == 0
    code = lax.broadcasted_iota(jnp.int32, (N_IDS, rows), 0)

    def select(n):
        n = jnp.int32(n)
        img = (n >= batch).astype(jnp.int32)
        return (1 - img) * n + img * (batch + (n - batch) // per_img)

    def norm(n, u):
        u[...] = modulated(xs[n % 4].astype(F32), vec_ref, select(n), SHIFT1, SCALE1).reshape(u.shape)

    def heads_of(n, u):
        b, r0 = position(n)
        path = (jnp.int32(n) >= batch).astype(jnp.int32)
        hot = jnp.concatenate([(ids_ref[axis, pl.ds(b, 1), rows_at(r0, rows)] == code).astype(F32).astype(BF16) for axis in range(3)], axis=0)
        parts = lax.dot_general(hot, tab_ref[...], (((0,), (0,)), ((), ())), preferred_element_type=F32)
        cos_t, sin_t = (sum(parts[:, (3 * i + j) * HEAD:(3 * i + j + 1) * HEAD] for j in range(3)) for i in range(2))
        at = rows_at(b * total + r0, rows)
        for c0 in range(0, 3 * heads, 4):
            c1 = min(c0 + 4, 3 * heads)
            a = jnp.dot(u[...].reshape(rows, dim), w[path, :, c0 * HEAD:c1 * HEAD], preferred_element_type=F32) + row_of(small_ref, path, QKV_B, slice(c0 * HEAD, c1 * HEAD))
            for c in range(c0, c1):
                t = a[:, (c - c0) * HEAD:(c - c0 + 1) * HEAD]
                kind = c // heads
                if kind < 2:
                    t = t * lax.rsqrt(row_mean(t * t) + NORM_EPS) * row_of(small_ref, path, Q_GAIN + kind, slice(HEAD))
                    swapped = jnp.where(even, pltpu.roll(t, HEAD - 1, 1), pltpu.roll(t, 1, 1))
                    t = t * cos_t + swapped * sin_t
                qkv[c, at, :] = t.astype(BF16)

    m_wait(0)
    for j in range(n_dev):
        rows_here = m_early[j].astype(F32)
        for n in range(2 * 2 * batch):
            k, sel = n // (2 * batch), n % (2 * batch)
            vec_ref[sel, k:k + 1, j * width:(j + 1) * width] = rows_here[n:n + 1, :]
    x_wait(0)
    norm(0, ua)
    for j in range(3):
        w_load(0, j).wait()
    for c in range(2):
        late_load(c, c).start()
    for j in range(3):
        w_load(1, j).start()
    tw_load.start()

    def qkv_step(t):
        x_start(2 * t + 3)
        x_start(2 * t + 4)
        x_wait(2 * t + 1)
        x_wait(2 * t + 2)
        @pl.when(t == 1)
        def _():
            for j in range(3):
                w_load(1, j).wait()

        @pl.when(t < 8)
        def _():
            late_load(t, 0).wait()

        late_chunk(t)
        norm(2 * t + 1, ub)
        heads_of(2 * t, ua)
        norm(jnp.minimum(2 * t + 2, blocks - 1), ua)
        heads_of(2 * t + 1, ub)

        @pl.when(t < 6)
        def _():
            late_start(t + 2)

    kv_store = pltpu.make_async_copy(qkv.at[:, total:, :], kv_hbm, tsem.at[0])

    def late_send():
        m_send(1)

    def kv_send():
        kv_store.start()

    done_here = batch + per_img

    def rows_of(n, c, size, r0):
        return qkv[c, rows_at(position(n)[0] * total + r0, size), :]

    def scores(n, h, s):
        s[...] = scores_of(rows_of(n, h, rows, position(n)[1]), rows_of(n, heads + h, total, 0))

    def weigh(n, h, s):
        o_all[rows_at(n * rows, rows), h * HEAD:(h + 1) * HEAD] = weighted(s[...], rows_of(n, 2 * heads + h, total, 0))

    def t_copy(kind, b, src, dst, dev):
        return remote(tsend, trecv, kind, b, src, dst, dev)

    def t_core(b):
        return t_copy(T_CORE, b, t_send, t_recv.at[b], partner)

    def t_first(b):
        return t_copy(T_FIRST, b, t_sum.at[b, rows_at(not1 * quarter, quarter), :], t_rs1.at[b], first)

    def t_second(b):
        return t_copy(T_SECOND, b, t_rs2_out.at[b], t_rs2_in.at[b], second)

    def own_rows(b1, b2):
        return rows_at(core * half + b1 * quarter + b2 * eighth, eighth)

    def t_out(kind, b, b1, b2, dev):
        ref = ut_hbm.at[b, own_rows(b1, b2), :]
        return t_copy(kind, b, t_u.at[b] if kind in (T_OUT_FIRST, T_OUT_SECOND, T_CORE_OWN) else ref, ref, dev)

    def t_local(b):
        return pltpu.make_async_copy(t_u.at[b], ut_hbm.at[b, own_rows(bit1, bit2), :], tsem.at[2 + b])

    def t_load(b):
        return pltpu.make_async_copy(txt_hbm.at[b, own_rows(bit1, bit2), :], t_x.at[b], tsem.at[2 + batch + b])

    tile = min(512, dim)

    def text_product(b, who, store):
        def columns(n):
            at = rows_at(n * tile, tile)
            store(at, jnp.dot(o_all[rows_at(b * rows + who * half, half), :], tw[:, at], preferred_element_type=F32))

        loop(dim // tile, columns)

    def text_partial(b):
        if b == 0:
            tw_load.wait()
        t_load(b).start()

        def to_send(at, value):
            t_send[:, at] = value.astype(BF16)

        def to_own(at, value):
            t_own[:, at] = value

        text_product(b, far, to_send)
        t_core(b).start()
        text_product(b, core, to_own)

    def text_sum(b):
        t_core(b).wait()

        def add(n):
            at = rows_at(n * STRIP, STRIP)
            t_sum[b, at, :] = (t_own[at, :] + t_recv[b, at, :].astype(F32)).astype(BF16)

        loop(half // STRIP, add)
        t_first(b).start()

    def text_quarter(b):
        t_first(b).wait()
        t_rs2_out[b] = (t_sum[b, rows_at(bit1 * quarter + not2 * eighth, eighth), :].astype(F32) + t_rs1[b, rows_at(not2 * eighth, eighth), :].astype(F32)).astype(BF16)
        t_keep[b] = t_sum[b, rows_at(bit1 * quarter + bit2 * eighth, eighth), :].astype(F32) + t_rs1[b, rows_at(bit2 * eighth, eighth), :].astype(F32)
        t_second(b).start()

    def text_finish(b):
        t_second(b).wait()
        t_load(b).wait()
        branch = t_keep[b] + t_rs2_in[b].astype(F32) + row_of(vec_ref, b, PROJ_B)
        x1 = (t_x[b].astype(F32) + row_of(vec_ref, b, GATE1) * branch).astype(BF16)
        x1_ref[b] = x1
        t_u[b] = modulated(x1.astype(F32), vec_ref, b, SHIFT2, SCALE2)
        t_out(T_OUT_FIRST, b, bit1, bit2, first).start()
        t_out(T_OUT_SECOND, b, bit1, bit2, second).start()
        t_out(T_CORE_OWN, b, bit1, bit2, partner).start()
        t_local(b).start()

    def text_relay(b):
        t_out(T_OUT_FIRST, b, not1, bit2, first).wait_recv()
        t_out(T_OUT_RELAY, b, not1, bit2, second).start()
        t_out(T_CORE_FIRST, b, not1, bit2, partner).start()
        t_out(T_OUT_SECOND, b, bit1, not2, second).wait_recv()
        t_out(T_CORE_SECOND, b, bit1, not2, partner).start()

    def text_last(b):
        t_out(T_OUT_RELAY, b, not1, not2, second).wait_recv()
        t_out(T_CORE_RELAY, b, not1, not2, partner).start()

    def g_rows(m, who):
        return o_all.at[rows_at((batch + m) * rows + who * half, half), :]

    def g_mine(m):
        return og_hbm.at[m, :, rows_at(me * width, width)]

    def g_local(m):
        return pltpu.make_async_copy(g_rows(m, core), g_mine(m), gsem.at[m])

    def g_core(m):
        return remote(gsend, grecv, G_CORE, m, g_rows(m, far), g_mine(m), partner)

    def g_copy(kind, m, owner, dev):
        ref = og_hbm.at[m, :, rows_at(owner // 2 * (2 * width), 2 * width)]
        return remote(gsend, grecv, kind, m, ref, ref, dev)

    def gather_start(m):
        g_local(m).start()
        g_core(m).start()

    def gather_send(m):
        g_local(m).wait()
        g_core(m).wait()
        g_copy(G_FIRST, m, me, first).start()
        g_copy(G_SECOND, m, me, second).start()

    def gather_relay(m):
        g_copy(G_FIRST, m, first, first).wait_recv()
        g_copy(G_RELAY, m, first, second).start()

    qkv_first, attend_first = (batch + per_img) // 2, 1 + EARLY
    resume = blocks // 2 + attend_first
    steps = blocks // 2 + done_here
    known = dict(locals())

    def run(calls):
        for call in calls:
            name, *args = call.split()
            known[name](*map(int, args))

    def attended(a):
        early = ((a >= 1) & (a <= EARLY)).astype(jnp.int32)
        return a + early - EARLY * (a == attend_first).astype(jnp.int32)

    def attention_step(a, begins):
        n = attended(a)

        @pl.when(begins)
        def _():
            scores(n, 0, s0)

        scores(n, 1, s1)
        weigh(n, 0, s0)
        scores(n, 2, s2)
        weigh(n, 1, s1)
        scores(attended(jnp.minimum(a + 1, done_here - 1)), 0, s0)
        weigh(n, 2, s2)

    def step(i):
        for when, calls in enumerate(HOOKS[:steps]):
            if calls:
                @pl.when(i == when)
                def _():
                    run(calls)

        in_first = i < qkv_first
        in_second = (i >= qkv_first + attend_first) & (i < resume)

        @pl.when(in_first | in_second)
        def _():
            qkv_step(i - attend_first * in_second.astype(jnp.int32))

        @pl.when(jnp.logical_not(in_first | in_second))
        def _():
            late = (i >= resume).astype(jnp.int32)
            attention_step(i - late * (blocks // 2) - (1 - late) * qkv_first, (i == qkv_first) | (i == resume))

    loop(steps, step)

    o_out = pltpu.make_async_copy(o_all.at[batch * rows:, :], o_hbm, osem)
    o_out.start()
    run(HOOKS[steps])
    o_out.wait()
    kv_store.wait()
    for b in range(batch):
        t_local(b).wait()
        for kind, b1, b2, dev in ((T_OUT_FIRST, bit1, bit2, first), (T_OUT_SECOND, bit1, bit2, second), (T_OUT_RELAY, not1, bit2, second)):
            t_out(kind, b, b1, b2, dev).wait_send()
        for kind, b1, b2 in ((T_CORE_OWN, bit1, bit2), (T_CORE_FIRST, not1, bit2), (T_CORE_SECOND, bit1, not2), (T_CORE_RELAY, not1, not2)):
            t_out(kind, b, b1, b2, partner).wait()
    for j in (SHARED, COMMON):
        for kind, owner, dev in ((W_FIRST, me, first), (W_SECOND, me, second), (W_RELAY, first, second)):
            p_copy(kind, j, owner, dev).wait_send()
    w_own().wait()
    for kind, owner, core_kind in from_beside:
        z_copy(kind, owner).wait_send()
        for j in range(PIECES):
            p_copy(core_kind, j, owner, partner).wait()
    for m in range(READY):
        g_copy(G_FIRST, m, me, first).wait_send()
        g_copy(G_SECOND, m, me, second).wait_send()
        g_copy(G_RELAY, m, first, second).wait_send()
        g_copy(G_SECOND, m, second, second).wait_recv()
        g_copy(G_RELAY, m, diagonal, second).wait_recv()


HOOKS = (
    (),
    (),
    (),
    (),
    ('w_relay 0', 'w_second 0'),
    ('w_relay 1',),
    ('text_partial 0',),
    ('text_sum 0',),
    ('gather_start 0',),
    (),
    ('gather_send 0',),
    ('late_send', 'text_quarter 0', 'gather_start 1'),
    ('kv_send', 'w_last 1', 'gather_send 1'),
    ('late_rows', 'text_finish 0', 'text_partial 1', 'w_beside 0', 'w_last 0', 'text_sum 1'),
    (),
    ('gather_relay 1', 'text_quarter 1', 'gather_start 2', 'gather_send 2', 'text_relay 0'),
    ('w_beside 1', 'text_finish 1'),
    ('w_beside 2', 'w_second 1', 'gather_relay 0'),
    ('text_relay 1', 'gather_relay 2'),
    ('text_last 1', 'text_last 0'),
)


def front_call(txt, img, wt, wi, mt, mi, pw, tw, cond, small_t, small_i, ids_t, table, n_dev, rows):
    batch, txt_len, dim = txt.shape
    img_len = img.shape[1]
    total = txt_len + img_len
    width = pw.shape[0]
    heads = width // HEAD
    half, quarter, eighth = rows // 2, rows // 4, rows // 8
    assert heads == HEADS_HERE and batch == 2
    cfg = (batch, txt_len, img_len, rows)
    blocks = batch * (1 + img_len // rows)
    vmem = pl.BlockSpec(memory_space=pltpu.VMEM)
    anywhere = pl.BlockSpec(memory_space=pl.ANY)
    tall = [pltpu.VMEM((half, dim), BF16), pltpu.VMEM((batch, half, dim), BF16), pltpu.VMEM((half, dim), F32), pltpu.VMEM((batch, half, dim), BF16), pltpu.VMEM((batch, quarter, dim), BF16)]
    short = [pltpu.VMEM((batch, eighth, dim), dtype) for dtype in (BF16, BF16, F32, BF16, BF16)]
    return pl.pallas_call(
        functools.partial(front_kernel, cfg),
        in_specs=[anywhere] * 8 + [vmem, (vmem,) * len(small_t), (vmem,) * len(small_i), vmem, vmem],
        out_specs=[anywhere] * 5 + [vmem] * 3,
        out_shape=[
            jax.ShapeDtypeStruct((img_len, width), BF16),
            jax.ShapeDtypeStruct((3 * heads, total, HEAD), BF16),
            jax.ShapeDtypeStruct((n_dev, width, dim), BF16),
            jax.ShapeDtypeStruct((batch, txt_len, dim), BF16),
            jax.ShapeDtypeStruct((READY, half, dim), BF16),
            jax.ShapeDtypeStruct((batch, eighth, dim), BF16),
            jax.ShapeDtypeStruct((2 * batch, FC2_B + 1, dim), F32),
            jax.ShapeDtypeStruct((2, FC1_B + 1, dim), F32),
        ],
        scratch_shapes=[
            pltpu.VMEM((2, dim, 3 * width), BF16),
            pltpu.VMEM((2, dim, width), BF16),
            pltpu.VMEM((2, PROJ_B, width), F32),
            pltpu.VMEM((n_dev, 4 * batch, width), BF16),
            pltpu.VMEM((n_dev, blocks // 2, batch, width), F32),
            pltpu.VMEM((4, rows, dim), BF16),
            pltpu.VMEM((batch, half, dim), BF16),
            pltpu.VMEM((batch, half, dim), BF16),
            pltpu.VMEM((3 * heads, batch * total, HEAD), BF16),
            pltpu.VMEM((rows, total), F32),
            pltpu.VMEM((rows, total), F32),
            pltpu.VMEM((rows, total), F32),
            pltpu.VMEM((batch * txt_len + img_len, width), BF16),
            pltpu.VMEM((width, dim), BF16),
            *tall,
            *short,
            pltpu.SemaphoreType.DMA((2, 3)),
            pltpu.SemaphoreType.DMA((2,)),
            pltpu.SemaphoreType.DMA((4,)),
            pltpu.SemaphoreType.DMA,
            pltpu.SemaphoreType.DMA((6,)),
            pltpu.SemaphoreType.DMA((READY,)),
            *[pltpu.SemaphoreType.DMA((10, PIECES))] * 2,
            *[pltpu.SemaphoreType.DMA((10, batch))] * 2,
            *[pltpu.SemaphoreType.DMA((4, READY))] * 2,
            pltpu.SemaphoreType.DMA((2, n_dev)),
            pltpu.SemaphoreType.DMA((2, n_dev)),
        ],
        compiler_params=pltpu.CompilerParams(collective_id=2, has_side_effects=True, vmem_limit_bytes=VMEM_BYTES),
        name="front",
    )(txt, img, wt, wi, mt, mi, pw, tw, cond, small_t, small_i, ids_t, table)


(O_CORE, O_FIRST, O_SECOND, O_RELAY, U_CORE, PART_CORE, RS_FIRST, RS_SECOND, OUT_FIRST, OUT_SECOND, OUT_RELAY, CORE_OWN, CORE_FIRST, CORE_SECOND, CORE_RELAY) = range(15)
(L_O, L_X, L_OUT) = range(3)
SLOTS = 4
O_SLOTS = 7
SEMS = 8


def two(n):
    return n % 2


def block_kernel(cfg, o_hbm, og_hbm, kv_hbm, x_hbm, ut_hbm, x1t_hbm, wp_hbm, pw_hbm, w1t_hbm, w2t_hbm, w1i_hbm, w2i_hbm, vec_ref, fb_ref, out_hbm, o2_hbm,
                 kv, qs, os, wp, w1, w2, obuf, xbuf, x1buf, x1keep, u2, hid, psend, precv, own, chip_sum, rs1, keep2, rs2_out, rs2_in, outb,
                 asem, wsem, lsem, tsem, ssem, rsem):
    batch, txt_chunks, img_chunks, per_img, rows, tile = cfg
    half, quarter, eighth = rows // 2, rows // 4, rows // 8
    dim = wp.shape[0]
    ff = w1.shape[1]
    cols = o_hbm.shape[1]
    heads = cols // HEAD
    total = txt_chunks + img_chunks
    per_txt = txt_chunks // batch

    place = Place()
    me, core, partner, first, second, bit1, bit2 = place.me, place.core, place.partner, place.first, place.second, place.bit1, place.bit2
    not1, not2, far = place.not1, place.not2, place.far
    txt_len = ut_hbm.shape[1]
    place.enter([partner, first, second])

    def remote(kind, g, src, dst, dev):
        return pltpu.make_async_remote_copy(src_ref=src, dst_ref=dst, send_sem=ssem.at[kind, g % SEMS], recv_sem=rsem.at[kind, g % SEMS], device_id={'tp': dev}, device_id_type=MESH)

    def img_pos(g):
        k = g - txt_chunks
        return k // per_img, (k % per_img) * rows

    def chip_cols(dev):
        return rows_at((dev // 2) * (2 * cols), 2 * cols)

    def own_rows(b1, b2):
        return core * half + b1 * quarter + b2 * eighth

    def o_from(b):
        return (o_hbm, o2_hbm)[b]

    first_open = txt_chunks + og_hbm.shape[0]

    def o_ready(g):
        return pltpu.make_async_copy(og_hbm.at[g - txt_chunks], obuf.at[g % O_SLOTS], lsem.at[L_O, g % SEMS])

    def o_local(g, b):
        r0 = img_pos(g)[1]
        return pltpu.make_async_copy(o_from(b).at[rows_at(r0 + core * half, half), :], obuf.at[g % O_SLOTS, :, rows_at(me * cols, cols)], lsem.at[L_O, g % SEMS])

    def o_core(g, b):
        r0 = img_pos(g)[1]
        return remote(O_CORE, g, o_from(b).at[rows_at(r0 + far * half, half), :], obuf.at[g % O_SLOTS, :, rows_at(me * cols, cols)], partner)

    units = per_img * heads

    def q_load(u):
        r0 = txt_len + u // heads * rows
        return pltpu.make_async_copy(kv_hbm.at[u % heads, rows_at(r0, rows), :], qs.at[two(u)], asem.at[two(u)])

    def o_store(u):
        return pltpu.make_async_copy(os.at[two(u)], o2_hbm.at[rows_at(u // heads * rows, rows), rows_at(u % heads * HEAD, HEAD)], asem.at[2 + two(u)])

    def kv_load():
        return pltpu.make_async_copy(kv_hbm.at[heads:], kv, asem.at[4])

    def attend(u):
        q_load(u).wait()

        @pl.when(u + 1 < units)
        def _():
            q_load(u + 1).start()

        @pl.when(u >= 2)
        def _():
            o_store(u - 2).wait()

        k = kv[u % heads]
        v = kv[heads + u % heads]
        for r in range(0, rows, half):
            os[two(u), r:r + half, :] = weighted(scores_of(qs[two(u), r:r + half, :], k), v)
        o_store(u).start()

    def attend_pair(i):
        @pl.when(i == 0)
        def _():
            kv_load().wait()

        attend(2 * i)
        attend(2 * i + 1)

        @pl.when(i == units // 2 - 1)
        def _():
            o_store(units - 2).wait()
            o_store(units - 1).wait()

    def o_send(kind, g, owner, dev):
        ref = obuf.at[g % O_SLOTS, :, chip_cols(owner)]
        return remote(kind, g, ref, ref, dev)

    def x_load(g):
        b, r0 = img_pos(g)
        return pltpu.make_async_copy(x_hbm.at[b, rows_at(r0 + core * half, half), :], xbuf.at[two(g)], lsem.at[L_X, g % SEMS])

    def u_core(g):
        ref = u2.at[two(g), rows_at(core * half, half), :]
        return remote(U_CORE, g, ref, ref, partner)

    def part_core(g):
        return remote(PART_CORE, g, psend, precv.at[two(g)], partner)

    def rs_first(g):
        return remote(RS_FIRST, g, chip_sum.at[rows_at(not1 * quarter, quarter), :], rs1.at[two(g)], first)

    def rs_second(g):
        return remote(RS_SECOND, g, rs2_out.at[two(g)], rs2_in.at[g % SLOTS], second)

    def out_ref(g, b1, b2):
        return out_hbm.at[rows_at(g * rows + own_rows(b1, b2), eighth), :]

    def out_send(kind, g, b1, b2, dev):
        ref = out_ref(g, b1, b2)
        mine = kind in (OUT_FIRST, OUT_SECOND, CORE_OWN)
        return remote(kind, g, outb.at[g % SLOTS] if mine else ref, ref, dev)

    def out_local(g):
        return pltpu.make_async_copy(outb.at[g % SLOTS], out_ref(g, bit1, bit2), lsem.at[L_OUT, g % SEMS])

    def txt_load(g):
        b, r0 = g // per_txt, (g % per_txt) * rows
        return (pltpu.make_async_copy(ut_hbm.at[b, rows_at(r0, rows), :], u2.at[two(g)], tsem.at[0, two(g)]),
                pltpu.make_async_copy(x1t_hbm.at[g], x1keep.at[g % SLOTS], tsem.at[1, two(g)]))

    def w_load(k, src, dst):
        return pltpu.make_async_copy(src, dst, wsem.at[k])

    def wp_load(j, src):
        return pltpu.make_async_copy(src, wp.at[j * cols:(j + 1) * cols, :], wsem.at[2 + j])

    def select(g):
        txt = (g < txt_chunks).astype(jnp.int32)
        return txt * (g // per_txt) + (1 - txt) * (batch + (g - txt_chunks) // per_img)

    def start_o(g):
        @pl.when(g < first_open)
        def _():
            o_ready(g).start()

        for b in range(batch):
            @pl.when((g >= first_open) & (img_pos(g)[0] == b))
            def _():
                o_local(g, b).start()
                o_core(g, b).start()

    def send_o(g):
        o_local(g, 0).wait()
        o_core(g, 0).wait()
        o_send(O_FIRST, g, me, first).start()
        o_send(O_SECOND, g, me, second).start()

    def relay_o(g):
        o_send(O_FIRST, g, first, first).wait_recv()
        o_send(O_RELAY, g, first, second).start()

    def start_x(g):
        x_load(g).start()

    def project(g):
        @pl.when(g < first_open)
        def _():
            o_ready(g).wait()

        @pl.when(g >= first_open)
        def _():
            o_send(O_FIRST, g, me, first).wait_send()
            o_send(O_SECOND, g, me, second).wait_send()
            o_send(O_RELAY, g, first, second).wait_send()
            o_send(O_SECOND, g, second, second).wait_recv()
            o_send(O_RELAY, g, second, second).wait_recv()

        x_load(g).wait()

        @pl.when(g == txt_chunks)
        def _():
            for j in range(wp_hbm.shape[0]):
                wp_load(j, wp_hbm.at[j]).wait()

        sel = select(g)
        slot = g % SLOTS

        def columns(n):
            at = rows_at(n * tile, tile)
            acc = jnp.dot(obuf[g % O_SLOTS], wp[:, at], preferred_element_type=F32)
            branch = acc + row_of(vec_ref, sel, PROJ_B, at)
            x1buf[:, at] = (xbuf[two(g), :, at].astype(F32) + row_of(vec_ref, sel, GATE1, at) * branch).astype(BF16)

        loop(dim // tile, columns)

        def norm(n):
            at = rows_at(n * STRIP, STRIP)
            u2[two(g), rows_at(core * half + n * STRIP, STRIP), :] = modulated(x1buf[at, :].astype(F32), vec_ref, sel, SHIFT2, SCALE2)

        loop(half // STRIP, norm)
        u_core(g).start()
        x1keep[slot] = x1buf[rows_at(bit1 * quarter + bit2 * eighth, eighth), :]

    def mlp_hidden(g):
        @pl.when(g < txt_chunks)
        def _():
            for copy in txt_load(g):
                copy.wait()

        @pl.when(g >= txt_chunks)
        def _():
            u_core(g).wait()

        @pl.when(g == 0)
        def _():
            w_load(0, w1t_hbm, w1).wait()
            w_load(1, w2t_hbm, w2).wait()
            for j in range(wp_hbm.shape[0]):
                @pl.when(j != me)
                def _():
                    wp_load(j, wp_hbm.at[j]).start()

                @pl.when(j == me)
                def _():
                    wp_load(j, pw_hbm).start()

        @pl.when(g == txt_chunks)
        def _():
            w_load(0, w1i_hbm, w1).wait()
            w_load(1, w2i_hbm, w2).wait()

        path = (g >= txt_chunks).astype(jnp.int32)

        def hidden(n):
            at = rows_at(n * tile, tile)
            acc = jnp.dot(u2[two(g)], w1[:, at], preferred_element_type=F32)
            pre = acc + row_of(fb_ref, path, FC1_B, at)
            hid[:, at] = jax.nn.gelu(pre, approximate=True).astype(BF16)

        loop(ff // tile, hidden)

    def mlp_theirs(g):
        def theirs(n):
            at = rows_at(n * tile, tile)
            psend[:, at] = jnp.dot(hid[rows_at(far * half, half), :], w2[:, at], preferred_element_type=F32).astype(BF16)

        loop(dim // tile, theirs)
        part_core(g).start()

    def mlp_mine(g):
        def mine(n):
            at = rows_at(n * tile, tile)
            own[:, at] = jnp.dot(hid[rows_at(core * half, half), :], w2[:, at], preferred_element_type=F32)

        loop(dim // tile, mine)

        @pl.when(g == txt_chunks - 1)
        def _():
            w_load(0, w1i_hbm, w1).start()
            w_load(1, w2i_hbm, w2).start()

        part_core(g).wait()

        def add(n):
            at = rows_at(n * STRIP, STRIP)
            chip_sum[at, :] = (own[at, :] + precv[two(g), at, :].astype(F32)).astype(BF16)

        loop(half // STRIP, add)
        rs_first(g).start()

    def add_first(g):
        rs_first(g).wait()
        rs2_out[two(g)] = (chip_sum[rows_at(bit1 * quarter + not2 * eighth, eighth), :].astype(F32) + rs1[two(g), rows_at(not2 * eighth, eighth), :].astype(F32)).astype(BF16)
        rs_second(g).start()
        keep2[two(g)] = chip_sum[rows_at(bit1 * quarter + bit2 * eighth, eighth), :].astype(F32) + rs1[two(g), rows_at(bit2 * eighth, eighth), :].astype(F32)

    def finish(g):
        rs_second(g).wait()
        sel = select(g)
        branch = keep2[two(g)] + rs2_in[g % SLOTS].astype(F32) + row_of(vec_ref, sel, FC2_B)
        outb[g % SLOTS] = (x1keep[g % SLOTS].astype(F32) + row_of(vec_ref, sel, GATE2) * branch).astype(BF16)
        out_send(OUT_FIRST, g, bit1, bit2, first).start()
        out_send(OUT_SECOND, g, bit1, bit2, second).start()
        out_send(CORE_OWN, g, bit1, bit2, partner).start()
        out_local(g).start()

    def relay_out(g):
        out_send(OUT_FIRST, g, not1, bit2, first).wait_recv()
        out_send(OUT_RELAY, g, not1, bit2, second).start()
        out_send(CORE_FIRST, g, not1, bit2, partner).start()

    def second_out(g):
        out_send(OUT_SECOND, g, bit1, not2, second).wait_recv()
        out_send(CORE_SECOND, g, bit1, not2, partner).start()

    def relay_core(g):
        out_send(OUT_RELAY, g, not1, not2, second).wait_recv()
        out_send(CORE_RELAY, g, not1, not2, partner).start()

    def drain(g):
        out_local(g).wait()
        out_send(OUT_FIRST, g, bit1, bit2, first).wait_send()
        out_send(OUT_SECOND, g, bit1, bit2, second).wait_send()
        out_send(OUT_RELAY, g, not1, bit2, second).wait_send()
        out_send(CORE_OWN, g, bit1, bit2, partner).wait()
        out_send(CORE_FIRST, g, not1, bit2, partner).wait()
        out_send(CORE_SECOND, g, bit1, not2, partner).wait()
        out_send(CORE_RELAY, g, not1, not2, partner).wait()

    opened = txt_chunks + O_SLOTS - 1
    for g in range(txt_chunks, opened):
        start_o(jnp.int32(g))
    w_load(0, w1t_hbm, w1).start()
    w_load(1, w2t_hbm, w2).start()
    for g in range(txt_chunks):
        for copy in txt_load(g):
            copy.start()

    kv_load().start()
    q_load(0).start()
    for g in range(first_open, opened):
        send_o(jnp.int32(g))

    stages = ((second_out, -5, 0), (attend_pair, 0, 0), (mlp_hidden, 0, 0), (start_o, 5, opened), (relay_o, 4, first_open), (start_x, 2, txt_chunks), (relay_out, -4, 0), (mlp_theirs, 0, 0),
              (send_o, 5, opened), (add_first, -1, 0), (mlp_mine, 0, 0), (relay_core, -6, 0), (project, 1, txt_chunks), (drain, -6, 0), (finish, -2, 0))
    most = max(ahead for _, ahead, _ in stages)
    least = min(ahead for _, ahead, _ in stages)

    def step(i):
        for stage, ahead, lowest in stages:
            if stage is attend_pair:
                g, lowest, highest = i - ATTEND_FROM, 0, units // 2
            else:
                g, highest = i + txt_chunks - most + ahead, total

            @pl.when((g >= lowest) & (g < highest))
            def _():
                stage(g)

    loop(total - txt_chunks + most - least, step)


ATTEND_FROM = 3


def block_call(img_o, og, kv, x, u_txt, x1_txt, wp, pw, w1t, w2t, w1i, w2i, vecs, fb, rows):
    batch, img_len, dim = x.shape
    txt_len = u_txt.shape[1]
    ff = w1t.shape[1]
    txt_chunks = batch * (txt_len // rows)
    per_img = img_len // rows
    img_chunks = batch * per_img
    assert txt_chunks == 2
    half, quarter, eighth = rows // 2, rows // 4, rows // 8
    cfg = (batch, txt_chunks, img_chunks, per_img, rows, 512)
    total = txt_chunks + img_chunks
    anywhere = pl.BlockSpec(memory_space=pl.ANY)
    return pl.pallas_call(
        functools.partial(block_kernel, cfg),
        in_specs=[anywhere] * 12 + [pl.BlockSpec(memory_space=pltpu.VMEM)] * 2,
        out_specs=[anywhere, anywhere],
        out_shape=[jax.ShapeDtypeStruct((total * rows, dim), BF16), jax.ShapeDtypeStruct(img_o.shape, BF16)],
        scratch_shapes=[
            pltpu.VMEM((kv.shape[0] // 3 * 2,) + kv.shape[1:], BF16),
            pltpu.VMEM((2, rows, HEAD), BF16),
            pltpu.VMEM((2, rows, HEAD), BF16),
            pltpu.VMEM((dim, dim), BF16),
            pltpu.VMEM((dim, ff), BF16),
            pltpu.VMEM((ff, dim), BF16),
            pltpu.VMEM((O_SLOTS, half, dim), BF16),
            pltpu.VMEM((2, half, dim), BF16),
            pltpu.VMEM((half, dim), BF16),
            pltpu.VMEM((SLOTS, eighth, dim), BF16),
            pltpu.VMEM((2, rows, dim), BF16),
            pltpu.VMEM((rows, ff), BF16),
            pltpu.VMEM((half, dim), BF16),
            pltpu.VMEM((2, half, dim), BF16),
            pltpu.VMEM((half, dim), F32),
            pltpu.VMEM((half, dim), BF16),
            pltpu.VMEM((2, quarter, dim), BF16),
            pltpu.VMEM((2, eighth, dim), F32),
            pltpu.VMEM((2, eighth, dim), BF16),
            pltpu.VMEM((SLOTS, eighth, dim), BF16),
            pltpu.VMEM((SLOTS, eighth, dim), BF16),
            pltpu.SemaphoreType.DMA((5,)),
            pltpu.SemaphoreType.DMA((10,)),
            pltpu.SemaphoreType.DMA((3, SEMS)),
            pltpu.SemaphoreType.DMA((2, 2)),
            pltpu.SemaphoreType.DMA((15, SEMS)),
            pltpu.SemaphoreType.DMA((15, SEMS)),
        ],
        compiler_params=pltpu.CompilerParams(collective_id=0, has_side_effects=True, vmem_limit_bytes=VMEM_BYTES),
        name="block",
    )(img_o, og, kv, x, u_txt, x1_txt, wp, pw, w1t, w2t, w1i, w2i, vecs, fb)


def copy_kernel(pieces, flat_hbm, *rest):
    outs, (buf, isem, osem) = rest[:-3], rest[-3:]
    rows = buf.shape[1]
    loads = []
    for n, (which, b, r) in enumerate(pieces):
        load = pltpu.make_async_copy(flat_hbm.at[n * rows:(n + 1) * rows, :], buf.at[n], isem.at[n])
        load.start()
        loads.append(load)
    stores = []
    for n, (which, b, r) in enumerate(pieces):
        loads[n].wait()
        store = pltpu.make_async_copy(buf.at[n], outs[which].at[b, r:r + rows, :], osem.at[n])
        store.start()
        stores.append(store)
    for store in stores:
        store.wait()


def copy_call(flat, shapes, rows):
    pieces = [(which, b, r) for which, shape in enumerate(shapes) for b in range(shape[0]) for r in range(0, shape[1], rows)]
    anywhere = pl.BlockSpec(memory_space=pl.ANY)
    dim = flat.shape[1]
    return pl.pallas_call(
        functools.partial(copy_kernel, pieces),
        in_specs=[anywhere],
        out_specs=[anywhere] * len(shapes),
        out_shape=[jax.ShapeDtypeStruct(shape, flat.dtype) for shape in shapes],
        scratch_shapes=[
            pltpu.VMEM((len(pieces), rows, dim), flat.dtype),
            pltpu.SemaphoreType.DMA((len(pieces),)),
            pltpu.SemaphoreType.DMA((len(pieces),)),
        ],
        compiler_params=pltpu.CompilerParams(vmem_limit_bytes=VMEM_BYTES),
        name="copy_out",
    )(flat)


def local_block(img, txt, vec, ids, img_w, txt_w):
    n_dev = 8
    batch, txt_len = txt.shape[:2]
    rows = txt_len

    def by_kind(weight):
        return jnp.transpose(weight, (1, 0, 2))

    def small_of(w):
        return w[1], w[3], w[4], w[5], w[7], w[9], w[11]

    table = jnp.asarray(rope_table())
    ids_t = jnp.transpose(ids, (2, 0, 1))
    o, kv, proj_w, txt_u, og, txt_x1, vecs, small = front_call(txt, img, by_kind(txt_w[2]), by_kind(img_w[2]), by_kind(txt_w[0]), by_kind(img_w[0]), img_w[6], txt_w[6], vec, small_of(txt_w), small_of(img_w), ids_t, table, n_dev, rows)
    flat, _ = block_call(o, og, kv, img, txt_u, txt_x1, proj_w, img_w[6], txt_w[8], txt_w[10], img_w[8], img_w[10], vecs, small, rows)
    txt_out, img_out = copy_call(flat, (txt.shape, img.shape), rows)
    return img_out, txt_out


def solution(mesh):
    act_spec = P('dp', WHOLE, WHOLE)
    mapped = jax.shard_map(local_block, mesh=mesh, in_specs=(act_spec, act_spec, P('dp', WHOLE), act_spec, PATH_SPECS, PATH_SPECS), out_specs=(act_spec, act_spec), check_vma=False)

    def forward(img, txt, vec, ids, *weights):
        return mapped(img, txt, vec, ids, weights[:12], weights[12:])

    return forward
```

```python
import functools

import jax
import jax.numpy as jnp
import numpy as np
from jax import lax
from jax.experimental import pallas as pl
from jax.experimental.pallas import tpu as pltpu
from jax.sharding import PartitionSpec as P

HEAD = 128
NORM_EPS = 1e-6
ROPE_THETA = 10000.0
AXES_DIM = (16, 56, 56)
N_IDS = 64
WHOLE = None
PATH_SPECS = (P(WHOLE, WHOLE, 'tp'), P(WHOLE, 'tp'), P(WHOLE, WHOLE, 'tp'), P(WHOLE, 'tp'), P(WHOLE), P(WHOLE), P('tp', WHOLE), P(WHOLE), P(WHOLE, 'tp'), P('tp'), P('tp', WHOLE), P(WHOLE))
F32 = jnp.float32
BF16 = jnp.bfloat16


def rope_table():
    cos = np.zeros((3 * N_IDS, HEAD), np.float32)
    sin = np.zeros((3 * N_IDS, HEAD), np.float32)
    lane = 0
    for axis, dim in enumerate(AXES_DIM):
        inv_freq = np.float32(ROPE_THETA) ** (-np.arange(0, dim, 2, dtype=np.float32) / np.float32(dim))
        angles = np.arange(N_IDS, dtype=np.float32)[:, None] * inv_freq.astype(np.float32)
        rows = slice(axis * N_IDS, (axis + 1) * N_IDS)
        c = np.cos(angles.astype(np.float64)).astype(np.float32)
        s = np.sin(angles.astype(np.float64)).astype(np.float32)
        cos[rows, lane:lane + dim:2] = c
        cos[rows, lane + 1:lane + dim:2] = c
        sin[rows, lane:lane + dim:2] = -s
        sin[rows, lane + 1:lane + dim:2] = s
        lane += dim
    parts = []
    for table in (cos, sin):
        rest = table
        for _ in range(3):
            part = rest.astype(jnp.bfloat16)
            parts.append(np.asarray(part))
            rest = rest - np.asarray(part).astype(np.float32)
    return np.concatenate(parts, axis=1)


MESH = pl.DeviceIdType.MESH


SHIFT1, SCALE1, GATE1, SHIFT2, SCALE2, GATE2, PROJ_B, FC2_B = range(8)
QKV_B, Q_GAIN, K_GAIN, FC1_B = range(4)
VMEM_BYTES = 67043328


def row_of(ref, sel, row, at=slice(None)):
    return ref[sel, pl.ds(row, 1), at]


STRIP = 16
PATHS = range(2)


def loop(count, body):
    lax.fori_loop(0, count, lambda i, carry: (body(i), carry)[-1], 0)


def row_mean(x):
    return jnp.mean(x, axis=-1, keepdims=True)


def normalize(x):
    centered = x - row_mean(x)
    return centered * lax.rsqrt(row_mean(centered * centered) + NORM_EPS)


def softened(s):
    top = jnp.max(s, axis=-1, keepdims=True)
    p = jnp.exp2((s - top) * (HEAD ** -0.5 * LOG2E))
    return p.astype(BF16), jnp.sum(p, axis=-1, keepdims=True)


def weighted(s, v):
    p, total = softened(s)
    return (jnp.dot(p, v, preferred_element_type=F32) * (1.0 / total)).astype(BF16)


def scores_of(q, k):
    return lax.dot_general(q, k, (((1,), (1,)), ((), ())), preferred_element_type=F32)


def modulated(x, vec_ref, sel, shift, scale):
    return ((1.0 + row_of(vec_ref, sel, scale)) * normalize(x) + row_of(vec_ref, sel, shift)).astype(BF16)


LOG2E = 1.4426950408889634
(W_FIRST, W_SECOND, W_RELAY, W_CORE, W_CORE_FIRST, W_CORE_SECOND, W_CORE_RELAY, Z_FIRST, Z_SECOND, Z_RELAY) = range(10)
(G_CORE, G_FIRST, G_SECOND, G_RELAY) = range(4)
(T_CORE, T_FIRST, T_SECOND, T_OUT_FIRST, T_OUT_SECOND, T_OUT_RELAY, T_CORE_OWN, T_CORE_FIRST, T_CORE_SECOND, T_CORE_RELAY) = range(10)
SHARED, COMMON, MISSING = range(3)
PIECES = 3
READY = 4
EARLY = 4
FIRST_LATE = 5
HEADS_HERE = 3


def ident(dev):
    return dev if isinstance(dev, dict) else {'tp': dev}


class Place:
    def __init__(self):
        me = lax.axis_index('tp')
        core = me % 2
        xi = (me // 2) % 2
        yi = me // 4
        x_next = me + 2 - 4 * xi
        y_next = me + 4 - 8 * yi
        self.me, self.core = me, core
        self.partner = me + 1 - 2 * core
        self.first = x_next * (1 - core) + y_next * core
        self.second = x_next * core + y_next * (1 - core)
        self.diagonal = x_next + y_next - me
        self.bit1 = xi * (1 - core) + yi * core
        self.bit2 = xi * core + yi * (1 - core)
        self.not1, self.not2, self.far = 1 - self.bit1, 1 - self.bit2, 1 - core

    def enter(self, others):
        barrier = pltpu.get_barrier_semaphore()
        for dev in others:
            pl.semaphore_signal(barrier, inc=1, device_id=ident(dev), device_id_type=MESH)
        pl.semaphore_wait(barrier, len(others))


def rows_at(start, size):
    return pl.ds(pl.multiple_of(start, size), size)


def front_kernel(cfg, txt_hbm, img_hbm, wt_hbm, wi_hbm, mt_hbm, mi_hbm, pw_hbm, tw_hbm, cond_ref, small_t, small_i, ids_ref, tab_ref,
                 o_hbm, kv_hbm, wp_hbm, ut_hbm, og_hbm, x1_ref, tu_ref, vec_ref, small_ref,
                 w, m_w, m_b, m_early, m_late, xs, ua, ub, qkv, s0, s1, s2, probs, o_all, tw, t_send, t_recv, t_own, t_sum, t_rs1, t_rs2_out, t_rs2_in, t_keep, t_x, t_u,
                 wsem, msem, xsem, osem, tsem, gsem, psend, precv, tsend, trecv, gsend, grecv, msend, mrecv):
    batch, txt_len, img_len, rows = cfg
    half, quarter, eighth = rows // 2, rows // 4, rows // 8
    total = txt_len + img_len
    per_img = img_len // rows
    blocks = batch * (per_img + 1)
    n_dev = m_early.shape[0]
    others = range(1, n_dev)
    dim = w.shape[1]
    width = o_all.shape[1]
    heads = width // HEAD
    place = Place()
    me, core, partner, first, second, diagonal, bit1, bit2 = place.me, place.core, place.partner, place.first, place.second, place.diagonal, place.bit1, place.bit2
    not1, not2, far = place.not1, place.not2, place.far
    piece = width // PIECES
    plane = lax.axis_index('dp')
    odd = plane % 2
    beside = {'dp': plane + 1 - 2 * odd}

    def position(n):
        n = jnp.int32(n)
        img = (n >= batch).astype(jnp.int32)
        m = n - batch
        b = (1 - img) * n + img * (m // per_img)
        r = img * (1 + m % per_img)
        return b, r * rows

    def x_copy(n, source):
        b, r0 = position(n)
        ref = txt_hbm.at[b] if source == 0 else img_hbm.at[b, rows_at(r0 - rows, rows), :]
        return pltpu.make_async_copy(ref, xs.at[n % 4], xsem.at[n % 4])

    def x_start(n):
        @pl.when(n < batch)
        def _():
            x_copy(n, 0).start()

        @pl.when((n >= batch) & (n < blocks))
        def _():
            x_copy(n, 1).start()

    def x_wait(n):
        @pl.when(n < blocks)
        def _():
            pltpu.make_async_copy(txt_hbm.at[0], xs.at[n % 4], xsem.at[n % 4]).wait()

    def w_columns(path, j):
        return w.at[path, :, j * width:(j + 1) * width]

    def w_load(path, j):
        return pltpu.make_async_copy((wt_hbm, wi_hbm)[path].at[j], w_columns(path, j), wsem.at[path, j])

    def early_load(path, k):
        return pltpu.make_async_copy((mt_hbm, mi_hbm)[path].at[k], w_columns(path, k), wsem.at[path, k])

    def late_load(c, path):
        return pltpu.make_async_copy((mt_hbm, mi_hbm)[path].at[GATE1 + c // 2], m_w.at[c % 2], msem.at[c % 2])

    def late_start(c):
        for path in PATHS:
            @pl.when(c % 2 == path)
            def _():
                late_load(c, path).start()

    def m_copy(part, d, send):
        buf, at = ((m_early, slice(None)), (m_late, slice(FIRST_LATE)), (m_late, slice(FIRST_LATE, 8)))[part]
        ref = buf.at[me if send else (me + n_dev - d) % n_dev, at]
        return pltpu.make_async_remote_copy(src_ref=ref, dst_ref=ref, send_sem=msend.at[part, d], recv_sem=mrecv.at[part, d], device_id={'tp': (me + d) % n_dev}, device_id_type=MESH)

    def m_send(part):
        for d in others:
            m_copy(part, d, True).start()

    def m_wait(part):
        for d in others:
            m_copy(part, d, True).wait_send()
            m_copy(part, d, False).wait_recv()

    for k in (SHIFT1, SCALE1):
        for path in PATHS:
            early_load(path, k).start()
    for n in range(3):
        x_copy(n, 0 if n < batch else 1).start()
    v = cond_ref[...].astype(F32)
    silu = (v * (1.0 / (1.0 + jnp.exp(-v)))).astype(BF16)
    for path, (mod_b, qkv_b, q_gain, k_gain, proj_b, fc1_b, fc2_b) in enumerate((small_t, small_i)):
        m_b[path] = mod_b[...].astype(F32)
        for row, ref in ((PROJ_B, proj_b), (FC2_B, fc2_b)):
            vector = ref[...].astype(F32)[None, :]
            for b in range(batch):
                vec_ref[path * batch + b, row:row + 1, :] = vector
        for row, ref in ((Q_GAIN, q_gain), (K_GAIN, k_gain), (FC1_B, fc1_b)):
            vector = ref[...].astype(F32)[None, :]
            small_ref[path, row:row + 1, :vector.shape[1]] = vector
        for j in range(qkv_b.shape[0]):
            small_ref[path, QKV_B:Q_GAIN, j * width:(j + 1) * width] = qkv_b[j:j + 1, :].astype(F32)
    place.enter([(me + d) % n_dev for d in others] + [beside])

    def early_chunk(k, path):
        early_load(path, k).wait()
        acc = jnp.dot(silu, w_columns(path, k)[...], preferred_element_type=F32)
        return (acc + m_b[path, k:k + 1, :]).astype(BF16)

    m_early[me] = jnp.concatenate([early_chunk(k, path) for k in (SHIFT1, SCALE1) for path in PATHS], axis=0)
    m_send(0)
    for j in range(3):
        w_load(0, j).start()
    tw_load = pltpu.make_async_copy(tw_hbm, tw, tsem.at[1])

    def late_chunk(t):
        c = jnp.minimum(t, 7)
        path, k = c % 2, GATE1 + c // 2
        acc = jnp.dot(silu, m_w[c % 2], preferred_element_type=F32) + m_b[path, pl.ds(k, 1), :]
        m_late[me, t] = acc.astype(BF16).astype(F32)

    def late_rows(part):
        m_wait(1 + part)
        for j in range(n_dev):
            for c in range(8)[slice(FIRST_LATE) if part == 0 else slice(FIRST_LATE, 8)]:
                for b in range(batch):
                    vec_ref[c % 2 * batch + b, pl.ds(GATE1 + c // 2, 1), j * width:(j + 1) * width] = m_late[j, c, b:b + 1, :]

    def piece_at(j):
        return rows_at(((1 - j) * (2 * odd - 1) + 1) * piece, piece)

    def remote(sends, recvs, kind, j, src, dst, dev):
        return pltpu.make_async_remote_copy(src_ref=src, dst_ref=dst, send_sem=sends.at[kind, j], recv_sem=recvs.at[kind, j], device_id=ident(dev), device_id_type=MESH)

    def p_copy(kind, j, owner, dev):
        dst = wp_hbm.at[owner, piece_at(j), :]
        src = pw_hbm.at[piece_at(j), :] if kind in (W_FIRST, W_SECOND) else dst
        return remote(psend, precv, kind, j, src, dst, dev)

    def w_own():
        return remote(psend, precv, W_CORE, SHARED, pw_hbm, wp_hbm.at[me], partner)

    def w_core():
        w_own().start()

    def z_copy(kind, owner, j=SHARED):
        ref = wp_hbm.at[owner, piece_at(j), :]
        return remote(psend, precv, kind, SHARED, ref, ref, beside)

    def w_relay(j):
        p_copy(W_FIRST, j, first, first).wait_recv()
        p_copy(W_RELAY, j, first, second).start()
        p_copy(W_CORE_FIRST, j, first, partner).start()
        if j == SHARED:
            p_copy(W_SECOND, COMMON, me, second).start()
            z_copy(Z_FIRST, first).start()

    def w_second(j):
        p_copy(W_SECOND, j, second, second).wait_recv()
        p_copy(W_CORE_SECOND, j, second, partner).start()
        if j == SHARED:
            z_copy(Z_SECOND, second).start()

    def w_last(j):
        p_copy(W_RELAY, j, diagonal, second).wait_recv()
        p_copy(W_CORE_RELAY, j, diagonal, partner).start()
        if j == SHARED:
            z_copy(Z_RELAY, diagonal).start()

    from_beside = ((Z_FIRST, first, W_CORE_FIRST), (Z_SECOND, second, W_CORE_SECOND), (Z_RELAY, diagonal, W_CORE_RELAY))

    def w_beside(n):
        kind, owner, core_kind = from_beside[n]
        z_copy(kind, owner, MISSING).wait_recv()
        p_copy(core_kind, MISSING, owner, partner).start()

    p_copy(W_FIRST, SHARED, me, first).start()
    p_copy(W_SECOND, SHARED, me, second).start()
    p_copy(W_FIRST, COMMON, me, first).start()

    even = lax.broadcasted_iota(jnp.int32, (rows, HEAD), 1) % 2 == 0
    code = lax.broadcasted_iota(jnp.int32, (N_IDS, rows), 0)

    def select(n):
        n = jnp.int32(n)
        img = (n >= batch).astype(jnp.int32)
        return (1 - img) * n + img * (batch + (n - batch) // per_img)

    def norm(n, u):
        sel = select(n)
        for r in range(0, rows, STRIP):
            u[r // half, r % half:r % half + STRIP, :] = modulated(xs[n % 4, r:r + STRIP, :].astype(F32), vec_ref, sel, SHIFT1, SCALE1)

    def heads_of(n, u):
        b, r0 = position(n)
        path = (jnp.int32(n) >= batch).astype(jnp.int32)
        hot = jnp.concatenate([(ids_ref[axis, pl.ds(b, 1), rows_at(r0, rows)] == code).astype(F32).astype(BF16) for axis in range(3)], axis=0)
        parts = lax.dot_general(hot, tab_ref[...], (((0,), (0,)), ((), ())), preferred_element_type=F32)
        cos_t, sin_t = (sum(parts[:, (3 * i + j) * HEAD:(3 * i + j + 1) * HEAD] for j in range(3)) for i in range(2))
        at = rows_at(b * total + r0, rows)
        for c0 in range(0, 3 * heads, 4):
            c1 = min(c0 + 4, 3 * heads)
            a = jnp.dot(u[...].reshape(rows, dim), w[path, :, c0 * HEAD:c1 * HEAD], preferred_element_type=F32) + row_of(small_ref, path, QKV_B, slice(c0 * HEAD, c1 * HEAD))
            for c in range(c0, c1):
                t = a[:, (c - c0) * HEAD:(c - c0 + 1) * HEAD]
                kind = c // heads
                if kind < 2:
                    t = t * lax.rsqrt(row_mean(t * t) + NORM_EPS) * row_of(small_ref, path, Q_GAIN + kind, slice(HEAD))
                    swapped = jnp.where(even, pltpu.roll(t, HEAD - 1, 1), pltpu.roll(t, 1, 1))
                    t = t * cos_t + swapped * sin_t
                qkv[c, at, :] = t.astype(BF16)

    m_wait(0)
    for j in range(n_dev):
        rows_here = m_early[j].astype(F32)
        for n in range(2 * 2 * batch):
            k, sel = n // (2 * batch), n % (2 * batch)
            vec_ref[sel, k:k + 1, j * width:(j + 1) * width] = rows_here[n:n + 1, :]
    x_wait(0)
    norm(0, ua)
    for j in range(3):
        w_load(0, j).wait()
    for c in range(2):
        late_load(c, c).start()
    for j in range(3):
        w_load(1, j).start()
    tw_load.start()

    def qkv_step(t):
        x_start(2 * t + 3)
        x_start(2 * t + 4)
        x_wait(2 * t + 1)
        x_wait(2 * t + 2)
        @pl.when(t == 1)
        def _():
            for j in range(3):
                w_load(1, j).wait()

        @pl.when(t < 8)
        def _():
            late_load(t, 0).wait()

        late_chunk(t)
        norm(2 * t + 1, ub)
        heads_of(2 * t, ua)
        norm(jnp.minimum(2 * t + 2, blocks - 1), ua)
        heads_of(2 * t + 1, ub)

        @pl.when(t < 6)
        def _():
            late_start(t + 2)

    kv_store = pltpu.make_async_copy(qkv.at[:, total:, :], kv_hbm, tsem.at[0])

    def late_send(part):
        m_send(1 + part)

    def kv_send():
        kv_store.start()

    done_here = batch + per_img

    def rows_of(n, c, size, r0):
        return qkv[c, rows_at(position(n)[0] * total + r0, size), :]

    def scores(n, h, s):
        s[...] = scores_of(rows_of(n, h, rows, position(n)[1]), rows_of(n, heads + h, total, 0))

    def weigh(n, h, s):
        sums = []
        for r in range(0, rows, STRIP):
            p, total_p = softened(s[r:r + STRIP, :])
            sums.append(total_p)
            probs[r:r + STRIP, :] = p
        o = jnp.dot(probs[...], rows_of(n, 2 * heads + h, total, 0), preferred_element_type=F32)
        o_all[rows_at(n * rows, rows), h * HEAD:(h + 1) * HEAD] = (o * (1.0 / jnp.concatenate(sums, axis=0))).astype(BF16)

    def t_copy(kind, b, src, dst, dev):
        return remote(tsend, trecv, kind, b, src, dst, dev)

    def t_core(b):
        return t_copy(T_CORE, b, t_send, t_recv.at[b], partner)

    def t_first(b):
        return t_copy(T_FIRST, b, t_sum.at[b, rows_at(not1 * quarter, quarter), :], t_rs1.at[b], first)

    def t_second(b):
        return t_copy(T_SECOND, b, t_rs2_out.at[b], t_rs2_in.at[b], second)

    def own_rows(b1, b2):
        return rows_at(core * half + b1 * quarter + b2 * eighth, eighth)

    def t_out(kind, b, b1, b2, dev):
        ref = ut_hbm.at[b, own_rows(b1, b2), :]
        return t_copy(kind, b, t_u.at[b] if kind in (T_OUT_FIRST, T_OUT_SECOND, T_CORE_OWN) else ref, ref, dev)

    def t_local(b):
        return pltpu.make_async_copy(t_u.at[b], ut_hbm.at[b, own_rows(bit1, bit2), :], tsem.at[2 + b])

    def t_load(b):
        return pltpu.make_async_copy(txt_hbm.at[b, own_rows(bit1, bit2), :], t_x.at[b], tsem.at[2 + batch + b])

    tile = min(512, dim)

    def text_product(b, who, store):
        def columns(n):
            at = rows_at(n * tile, tile)
            store(at, jnp.dot(o_all[rows_at(b * rows + who * half, half), :], tw[:, at], preferred_element_type=F32))

        loop(dim // tile, columns)

    def text_partial(b):
        if b == 0:
            tw_load.wait()
        t_load(b).start()

        def to_send(at, value):
            t_send[:, at] = value.astype(BF16)

        def to_own(at, value):
            t_own[:, at] = value

        text_product(b, far, to_send)
        t_core(b).start()
        text_product(b, core, to_own)

    def text_sum(b):
        t_core(b).wait()

        def add(n):
            at = rows_at(n * STRIP, STRIP)
            t_sum[b, at, :] = (t_own[at, :] + t_recv[b, at, :].astype(F32)).astype(BF16)

        loop(half // STRIP, add)
        t_first(b).start()

    def text_quarter(b):
        t_first(b).wait()
        t_rs2_out[b] = (t_sum[b, rows_at(bit1 * quarter + not2 * eighth, eighth), :].astype(F32) + t_rs1[b, rows_at(not2 * eighth, eighth), :].astype(F32)).astype(BF16)
        t_keep[b] = t_sum[b, rows_at(bit1 * quarter + bit2 * eighth, eighth), :].astype(F32) + t_rs1[b, rows_at(bit2 * eighth, eighth), :].astype(F32)
        t_second(b).start()

    def text_finish(b):
        t_second(b).wait()
        t_load(b).wait()
        branch = t_keep[b] + t_rs2_in[b].astype(F32) + row_of(vec_ref, b, PROJ_B)
        x1 = (t_x[b].astype(F32) + row_of(vec_ref, b, GATE1) * branch).astype(BF16)
        x1_ref[b] = x1
        u = modulated(x1.astype(F32), vec_ref, b, SHIFT2, SCALE2)
        if b == batch - 1:
            tu_ref[...] = u
            return
        t_u[b] = u
        t_out(T_OUT_FIRST, b, bit1, bit2, first).start()
        t_out(T_OUT_SECOND, b, bit1, bit2, second).start()
        t_out(T_CORE_OWN, b, bit1, bit2, partner).start()
        t_local(b).start()

    def text_relay(b):
        t_out(T_OUT_FIRST, b, not1, bit2, first).wait_recv()
        t_out(T_OUT_RELAY, b, not1, bit2, second).start()
        t_out(T_CORE_FIRST, b, not1, bit2, partner).start()
        t_out(T_OUT_SECOND, b, bit1, not2, second).wait_recv()
        t_out(T_CORE_SECOND, b, bit1, not2, partner).start()

    def text_last(b):
        t_out(T_OUT_RELAY, b, not1, not2, second).wait_recv()
        t_out(T_CORE_RELAY, b, not1, not2, partner).start()

    def g_rows(m, who):
        return o_all.at[rows_at((batch + m) * rows + who * half, half), :]

    def g_mine(m):
        return og_hbm.at[m, :, rows_at(me * width, width)]

    def g_local(m):
        return pltpu.make_async_copy(g_rows(m, core), g_mine(m), gsem.at[m])

    def g_core(m):
        return remote(gsend, grecv, G_CORE, m, g_rows(m, far), g_mine(m), partner)

    def g_copy(kind, m, owner, dev):
        ref = og_hbm.at[m, :, rows_at(owner // 2 * (2 * width), 2 * width)]
        return remote(gsend, grecv, kind, m, ref, ref, dev)

    def gather_start(m):
        g_local(m).start()
        g_core(m).start()

    def gather_send(m):
        g_local(m).wait()
        g_core(m).wait()
        g_copy(G_FIRST, m, me, first).start()
        g_copy(G_SECOND, m, me, second).start()

    def gather_relay(m):
        g_copy(G_FIRST, m, first, first).wait_recv()
        g_copy(G_RELAY, m, first, second).start()

    qkv_first, attend_first = (batch + per_img) // 2, 1 + EARLY
    resume = blocks // 2 + attend_first
    steps = blocks // 2 + done_here
    known = dict(locals())

    def run(calls):
        for call in calls:
            name, *args = call.split()
            known[name](*map(int, args))

    def attended(a):
        early = ((a >= 1) & (a <= EARLY)).astype(jnp.int32)
        return a + early - EARLY * (a == attend_first).astype(jnp.int32)

    def attention_step(a, begins):
        n = attended(a)

        @pl.when(begins)
        def _():
            scores(n, 0, s0)

        scores(n, 1, s1)
        weigh(n, 0, s0)
        scores(n, 2, s2)
        weigh(n, 1, s1)
        scores(attended(jnp.minimum(a + 1, done_here - 1)), 0, s0)
        weigh(n, 2, s2)

    def step(i):
        for when, calls in enumerate(HOOKS[:steps]):
            if calls:
                @pl.when(i == when)
                def _():
                    run(calls)

        in_first = i < qkv_first
        in_second = (i >= qkv_first + attend_first) & (i < resume)

        @pl.when(in_first | in_second)
        def _():
            qkv_step(i - attend_first * in_second.astype(jnp.int32))

        @pl.when(jnp.logical_not(in_first | in_second))
        def _():
            late = (i >= resume).astype(jnp.int32)
            attention_step(i - late * (blocks // 2) - (1 - late) * qkv_first, (i == qkv_first) | (i == resume))

    loop(steps, step)

    o_out = pltpu.make_async_copy(o_all.at[batch * rows:, :], o_hbm, osem)
    o_out.start()
    run(HOOKS[steps])
    o_out.wait()
    kv_store.wait()
    t_local(0).wait()
    for kind, b1, b2, dev in ((T_OUT_FIRST, bit1, bit2, first), (T_OUT_SECOND, bit1, bit2, second), (T_OUT_RELAY, not1, bit2, second)):
        t_out(kind, 0, b1, b2, dev).wait_send()
    for kind, b1, b2 in ((T_CORE_OWN, bit1, bit2), (T_CORE_FIRST, not1, bit2), (T_CORE_SECOND, bit1, not2), (T_CORE_RELAY, not1, not2)):
        t_out(kind, 0, b1, b2, partner).wait()
    for j in (SHARED, COMMON):
        for kind, owner, dev in ((W_FIRST, me, first), (W_SECOND, me, second), (W_RELAY, first, second)):
            p_copy(kind, j, owner, dev).wait_send()
    w_own().wait()
    for kind, owner, core_kind in from_beside:
        z_copy(kind, owner).wait_send()
        for j in range(PIECES):
            p_copy(core_kind, j, owner, partner).wait()
    for m in range(READY):
        g_copy(G_FIRST, m, me, first).wait_send()
        g_copy(G_SECOND, m, me, second).wait_send()
        g_copy(G_RELAY, m, first, second).wait_send()
        g_copy(G_SECOND, m, second, second).wait_recv()
        g_copy(G_RELAY, m, diagonal, second).wait_recv()


HOOKS = (
    (),
    (),
    (),
    ('w_relay 0',),
    (),
    ('late_send 0', 'w_relay 1'),
    ('w_core', 'text_partial 0'),
    ('w_second 0',),
    (),
    ('text_sum 0', 'gather_start 1', 'gather_start 0'),
    ('gather_start 3', 'gather_send 1'),
    ('gather_send 0', 'gather_start 2'),
    ('gather_send 3', 'text_quarter 0'),
    ('late_send 1', 'gather_send 2', 'w_last 0'),
    ('kv_send', 'late_rows 0', 'gather_relay 3', 'text_finish 0', 'w_second 1', 'gather_relay 1'),
    ('text_partial 1', 'w_last 1'),
    ('w_beside 0', 'w_beside 1', 'text_sum 1'),
    ('text_relay 0',),
    ('gather_relay 0', 'text_quarter 1', 'gather_relay 2'),
    ('late_rows 1', 'w_beside 2', 'text_last 0', 'text_finish 1'),
)


def front_call(txt, img, wt, wi, mt, mi, pw, tw, cond, small_t, small_i, ids_t, table, n_dev, rows):
    batch, txt_len, dim = txt.shape
    img_len = img.shape[1]
    total = txt_len + img_len
    width = pw.shape[0]
    heads = width // HEAD
    half, quarter, eighth = rows // 2, rows // 4, rows // 8
    assert heads == HEADS_HERE and batch == 2
    cfg = (batch, txt_len, img_len, rows)
    blocks = batch * (1 + img_len // rows)
    vmem = pl.BlockSpec(memory_space=pltpu.VMEM)
    anywhere = pl.BlockSpec(memory_space=pl.ANY)
    tall = [pltpu.VMEM((half, dim), BF16), pltpu.VMEM((batch, half, dim), BF16), pltpu.VMEM((half, dim), F32), pltpu.VMEM((batch, half, dim), BF16), pltpu.VMEM((batch, quarter, dim), BF16)]
    short = [pltpu.VMEM((batch, eighth, dim), dtype) for dtype in (BF16, BF16, F32, BF16, BF16)]
    return pl.pallas_call(
        functools.partial(front_kernel, cfg),
        in_specs=[anywhere] * 8 + [vmem, (vmem,) * len(small_t), (vmem,) * len(small_i), vmem, vmem],
        out_specs=[anywhere] * 5 + [vmem] * 4,
        out_shape=[
            jax.ShapeDtypeStruct((img_len, width), BF16),
            jax.ShapeDtypeStruct((3 * heads, total, HEAD), BF16),
            jax.ShapeDtypeStruct((n_dev, width, dim), BF16),
            jax.ShapeDtypeStruct((batch, txt_len, dim), BF16),
            jax.ShapeDtypeStruct((READY, half, dim), BF16),
            jax.ShapeDtypeStruct((batch, eighth, dim), BF16),
            jax.ShapeDtypeStruct((eighth, dim), BF16),
            jax.ShapeDtypeStruct((2 * batch, FC2_B + 1, dim), F32),
            jax.ShapeDtypeStruct((2, FC1_B + 1, dim), F32),
        ],
        scratch_shapes=[
            pltpu.VMEM((2, dim, 3 * width), BF16),
            pltpu.VMEM((2, dim, width), BF16),
            pltpu.VMEM((2, PROJ_B, width), F32),
            pltpu.VMEM((n_dev, 4 * batch, width), BF16),
            pltpu.VMEM((n_dev, blocks // 2, batch, width), F32),
            pltpu.VMEM((4, rows, dim), BF16),
            pltpu.VMEM((batch, half, dim), BF16),
            pltpu.VMEM((batch, half, dim), BF16),
            pltpu.VMEM((3 * heads, batch * total, HEAD), BF16),
            pltpu.VMEM((rows, total), F32),
            pltpu.VMEM((rows, total), F32),
            pltpu.VMEM((rows, total), F32),
            pltpu.VMEM((rows, total), BF16),
            pltpu.VMEM((batch * txt_len + img_len, width), BF16),
            pltpu.VMEM((width, dim), BF16),
            *tall,
            *short,
            pltpu.SemaphoreType.DMA((2, 3)),
            pltpu.SemaphoreType.DMA((2,)),
            pltpu.SemaphoreType.DMA((4,)),
            pltpu.SemaphoreType.DMA,
            pltpu.SemaphoreType.DMA((6,)),
            pltpu.SemaphoreType.DMA((READY,)),
            *[pltpu.SemaphoreType.DMA((10, PIECES))] * 2,
            *[pltpu.SemaphoreType.DMA((10, batch))] * 2,
            *[pltpu.SemaphoreType.DMA((4, READY))] * 2,
            *[pltpu.SemaphoreType.DMA((3, n_dev))] * 2,
        ],
        compiler_params=pltpu.CompilerParams(collective_id=2, has_side_effects=True, vmem_limit_bytes=VMEM_BYTES),
        name="front",
    )(txt, img, wt, wi, mt, mi, pw, tw, cond, small_t, small_i, ids_t, table)


(O_CORE, O_FIRST, O_SECOND, O_RELAY, U_CORE, PART_CORE, RS_FIRST, RS_SECOND, OUT_FIRST, OUT_SECOND, OUT_RELAY, CORE_OWN, CORE_FIRST, CORE_SECOND, CORE_RELAY,
 U_FIRST, U_SECOND, U_RELAY, U_OWN, U_CORE_FIRST, U_CORE_SECOND, U_CORE_RELAY) = range(22)
(L_O, L_X, L_OUT) = range(3)
SLOTS = 4
O_SLOTS = 7
SEMS = 8


def two(n):
    return n % 2


def block_kernel(cfg, o_hbm, og_hbm, kv_hbm, x_hbm, ut_hbm, x1t_hbm, tu_hbm, wp_hbm, pw_hbm, w1t_hbm, w2t_hbm, w1i_hbm, w2i_hbm, vec_ref, fb_ref, out_hbm, o2_hbm,
                 kv, qs, os, wp, w1, w2, obuf, xbuf, x1buf, x1keep, u2, hid, psend, precv, own, chip_sum, rs1, keep2, rs2_out, rs2_in, outb,
                 asem, wsem, lsem, tsem, ssem, rsem):
    batch, txt_chunks, img_chunks, per_img, rows, tile = cfg
    half, quarter, eighth = rows // 2, rows // 4, rows // 8
    dim = wp.shape[0]
    ff = w1.shape[1]
    cols = o_hbm.shape[1]
    heads = cols // HEAD
    total = txt_chunks + img_chunks
    per_txt = txt_chunks // batch

    place = Place()
    me, core, partner, first, second, bit1, bit2 = place.me, place.core, place.partner, place.first, place.second, place.bit1, place.bit2
    not1, not2, far = place.not1, place.not2, place.far
    txt_len = ut_hbm.shape[1]
    place.enter([partner, first, second])

    def remote(kind, g, src, dst, dev):
        return pltpu.make_async_remote_copy(src_ref=src, dst_ref=dst, send_sem=ssem.at[kind, g % SEMS], recv_sem=rsem.at[kind, g % SEMS], device_id={'tp': dev}, device_id_type=MESH)

    def img_pos(g):
        k = g - txt_chunks
        return k // per_img, (k % per_img) * rows

    def chip_cols(dev):
        return rows_at((dev // 2) * (2 * cols), 2 * cols)

    def own_rows(b1, b2):
        return core * half + b1 * quarter + b2 * eighth

    def o_from(b):
        return (o_hbm, o2_hbm)[b]

    first_open = txt_chunks + og_hbm.shape[0]

    def o_ready(g):
        return pltpu.make_async_copy(og_hbm.at[g - txt_chunks], obuf.at[g % O_SLOTS], lsem.at[L_O, g % SEMS])

    def o_local(g, b):
        r0 = img_pos(g)[1]
        return pltpu.make_async_copy(o_from(b).at[rows_at(r0 + core * half, half), :], obuf.at[g % O_SLOTS, :, rows_at(me * cols, cols)], lsem.at[L_O, g % SEMS])

    def o_core(g, b):
        r0 = img_pos(g)[1]
        return remote(O_CORE, g, o_from(b).at[rows_at(r0 + far * half, half), :], obuf.at[g % O_SLOTS, :, rows_at(me * cols, cols)], partner)

    units = per_img * heads

    def q_load(u):
        r0 = txt_len + u // heads * rows
        return pltpu.make_async_copy(kv_hbm.at[u % heads, rows_at(r0, rows), :], qs.at[two(u)], asem.at[two(u)])

    def o_store(u):
        return pltpu.make_async_copy(os.at[two(u)], o2_hbm.at[rows_at(u // heads * rows, rows), rows_at(u % heads * HEAD, HEAD)], asem.at[2 + two(u)])

    def kv_load():
        return pltpu.make_async_copy(kv_hbm.at[heads:], kv, asem.at[4])

    def attend(u):
        q_load(u).wait()

        @pl.when(u + 1 < units)
        def _():
            q_load(u + 1).start()

        @pl.when(u >= 2)
        def _():
            o_store(u - 2).wait()

        k = kv[u % heads]
        v = kv[heads + u % heads]
        for r in range(0, rows, half):
            os[two(u), r:r + half, :] = weighted(scores_of(qs[two(u), r:r + half, :], k), v)
        o_store(u).start()

    def attend_pair(i):
        @pl.when(i == 0)
        def _():
            kv_load().wait()

        attend(2 * i)
        attend(2 * i + 1)

        @pl.when(i == units // 2 - 1)
        def _():
            o_store(units - 2).wait()
            o_store(units - 1).wait()

    def o_send(kind, g, owner, dev):
        ref = obuf.at[g % O_SLOTS, :, chip_cols(owner)]
        return remote(kind, g, ref, ref, dev)

    def x_load(g):
        b, r0 = img_pos(g)
        return pltpu.make_async_copy(x_hbm.at[b, rows_at(r0 + core * half, half), :], xbuf.at[two(g)], lsem.at[L_X, g % SEMS])

    def u_core(g):
        ref = u2.at[two(g), rows_at(core * half, half), :]
        return remote(U_CORE, g, ref, ref, partner)

    def part_core(g):
        return remote(PART_CORE, g, psend, precv.at[two(g)], partner)

    def rs_first(g):
        return remote(RS_FIRST, g, chip_sum.at[rows_at(not1 * quarter, quarter), :], rs1.at[two(g)], first)

    def rs_second(g):
        return remote(RS_SECOND, g, rs2_out.at[two(g)], rs2_in.at[g % SLOTS], second)

    def out_ref(g, b1, b2):
        return out_hbm.at[rows_at(g * rows + own_rows(b1, b2), eighth), :]

    def out_send(kind, g, b1, b2, dev):
        ref = out_ref(g, b1, b2)
        mine = kind in (OUT_FIRST, OUT_SECOND, CORE_OWN)
        return remote(kind, g, outb.at[g % SLOTS] if mine else ref, ref, dev)

    def out_local(g):
        return pltpu.make_async_copy(outb.at[g % SLOTS], out_ref(g, bit1, bit2), lsem.at[L_OUT, g % SEMS])

    last_txt = txt_chunks - 1

    def txt_load(g):
        return pltpu.make_async_copy(ut_hbm.at[g], u2.at[two(g)], tsem.at[0, g])

    def x1_load(g):
        return pltpu.make_async_copy(x1t_hbm.at[g], x1keep.at[g], tsem.at[1, g])

    def u_rows(b1, b2):
        return u2.at[two(last_txt), pl.ds(own_rows(b1, b2), eighth), :]

    def u_local():
        return pltpu.make_async_copy(tu_hbm, u_rows(bit1, bit2), tsem.at[0, last_txt])

    def u_send(kind, b1, b2, dev):
        ref = u_rows(b1, b2)
        return remote(kind, last_txt, tu_hbm if kind in (U_FIRST, U_SECOND, U_OWN) else ref, ref, dev)

    def u_start():
        u_local().start()
        u_send(U_FIRST, bit1, bit2, first).start()
        u_send(U_SECOND, bit1, bit2, second).start()
        u_send(U_OWN, bit1, bit2, partner).start()

    def u_relay():
        u_send(U_FIRST, not1, bit2, first).wait_recv()
        u_send(U_RELAY, not1, bit2, second).start()
        u_send(U_CORE_FIRST, not1, bit2, partner).start()
        u_send(U_SECOND, bit1, not2, second).wait_recv()
        u_send(U_CORE_SECOND, bit1, not2, partner).start()

    def u_last():
        u_send(U_RELAY, not1, not2, second).wait_recv()
        u_send(U_CORE_RELAY, not1, not2, partner).start()

    def u_wait():
        u_local().wait()
        u_send(U_FIRST, bit1, bit2, first).wait_send()
        u_send(U_SECOND, bit1, bit2, second).wait_send()
        u_send(U_RELAY, not1, bit2, second).wait_send()
        for kind, b1, b2 in ((U_OWN, bit1, bit2), (U_CORE_FIRST, not1, bit2), (U_CORE_SECOND, bit1, not2), (U_CORE_RELAY, not1, not2)):
            u_send(kind, b1, b2, partner).wait()

    def w_load(k, src, dst):
        return pltpu.make_async_copy(src, dst, wsem.at[k])

    def wp_load(j, src):
        return pltpu.make_async_copy(src, wp.at[j * cols:(j + 1) * cols, :], wsem.at[2 + j])

    def select(g):
        txt = (g < txt_chunks).astype(jnp.int32)
        return txt * (g // per_txt) + (1 - txt) * (batch + (g - txt_chunks) // per_img)

    def start_o(g):
        @pl.when(g < first_open)
        def _():
            o_ready(g).start()

        for b in range(batch):
            @pl.when((g >= first_open) & (img_pos(g)[0] == b))
            def _():
                o_local(g, b).start()
                o_core(g, b).start()

    def send_o(g):
        o_local(g, 0).wait()
        o_core(g, 0).wait()
        o_send(O_FIRST, g, me, first).start()
        o_send(O_SECOND, g, me, second).start()

    def relay_o(g):
        o_send(O_FIRST, g, first, first).wait_recv()
        o_send(O_RELAY, g, first, second).start()

    def start_x(g):
        x_load(g).start()

    def project(g):
        @pl.when(g < first_open)
        def _():
            o_ready(g).wait()

        @pl.when(g >= first_open)
        def _():
            o_send(O_FIRST, g, me, first).wait_send()
            o_send(O_SECOND, g, me, second).wait_send()
            o_send(O_RELAY, g, first, second).wait_send()
            o_send(O_SECOND, g, second, second).wait_recv()
            o_send(O_RELAY, g, second, second).wait_recv()

        x_load(g).wait()

        @pl.when(g == txt_chunks)
        def _():
            for j in range(wp_hbm.shape[0]):
                wp_load(j, wp_hbm.at[j]).wait()

        sel = select(g)
        slot = g % SLOTS

        def columns(n):
            at = rows_at(n * tile, tile)
            acc = jnp.dot(obuf[g % O_SLOTS], wp[:, at], preferred_element_type=F32)
            branch = acc + row_of(vec_ref, sel, PROJ_B, at)
            x1buf[:, at] = (xbuf[two(g), :, at].astype(F32) + row_of(vec_ref, sel, GATE1, at) * branch).astype(BF16)

        loop(dim // tile, columns)

        def norm(n):
            at = rows_at(n * STRIP, STRIP)
            u2[two(g), rows_at(core * half + n * STRIP, STRIP), :] = modulated(x1buf[at, :].astype(F32), vec_ref, sel, SHIFT2, SCALE2)

        loop(half // STRIP, norm)
        u_core(g).start()
        x1keep[slot] = x1buf[rows_at(bit1 * quarter + bit2 * eighth, eighth), :]

    def mlp_hidden(g):
        @pl.when(g < last_txt)
        def _():
            txt_load(g).wait()

        @pl.when(g == last_txt)
        def _():
            u_wait()

        @pl.when(g < txt_chunks)
        def _():
            x1_load(g).wait()

        @pl.when(g >= txt_chunks)
        def _():
            u_core(g).wait()

        @pl.when(g == 0)
        def _():
            w_load(0, w1t_hbm, w1).wait()
            w_load(1, w2t_hbm, w2).wait()
            for j in range(wp_hbm.shape[0]):
                @pl.when(j != me)
                def _():
                    wp_load(j, wp_hbm.at[j]).start()

                @pl.when(j == me)
                def _():
                    wp_load(j, pw_hbm).start()

        @pl.when(g == txt_chunks)
        def _():
            w_load(0, w1i_hbm, w1).wait()
            w_load(1, w2i_hbm, w2).wait()

        path = (g >= txt_chunks).astype(jnp.int32)

        def hidden(n):
            at = rows_at(n * tile, tile)
            acc = jnp.dot(u2[two(g)], w1[:, at], preferred_element_type=F32)
            pre = acc + row_of(fb_ref, path, FC1_B, at)
            hid[:, at] = jax.nn.gelu(pre, approximate=True).astype(BF16)

        loop(ff // tile, hidden)

    def mlp_theirs(g):
        def theirs(n):
            at = rows_at(n * tile, tile)
            psend[:, at] = jnp.dot(hid[rows_at(far * half, half), :], w2[:, at], preferred_element_type=F32).astype(BF16)

        loop(dim // tile, theirs)
        part_core(g).start()

    def mlp_mine(g):
        def mine(n):
            at = rows_at(n * tile, tile)
            own[:, at] = jnp.dot(hid[rows_at(core * half, half), :], w2[:, at], preferred_element_type=F32)

        loop(dim // tile, mine)

        @pl.when(g == txt_chunks - 1)
        def _():
            w_load(0, w1i_hbm, w1).start()
            w_load(1, w2i_hbm, w2).start()

        part_core(g).wait()

        def add(n):
            at = rows_at(n * STRIP, STRIP)
            chip_sum[at, :] = (own[at, :] + precv[two(g), at, :].astype(F32)).astype(BF16)

        loop(half // STRIP, add)
        rs_first(g).start()

    def add_first(g):
        rs_first(g).wait()
        rs2_out[two(g)] = (chip_sum[rows_at(bit1 * quarter + not2 * eighth, eighth), :].astype(F32) + rs1[two(g), rows_at(not2 * eighth, eighth), :].astype(F32)).astype(BF16)
        rs_second(g).start()
        keep2[two(g)] = chip_sum[rows_at(bit1 * quarter + bit2 * eighth, eighth), :].astype(F32) + rs1[two(g), rows_at(bit2 * eighth, eighth), :].astype(F32)

    def finish(g):
        rs_second(g).wait()
        sel = select(g)
        branch = keep2[two(g)] + rs2_in[g % SLOTS].astype(F32) + row_of(vec_ref, sel, FC2_B)
        outb[g % SLOTS] = (x1keep[g % SLOTS].astype(F32) + row_of(vec_ref, sel, GATE2) * branch).astype(BF16)
        out_send(OUT_FIRST, g, bit1, bit2, first).start()
        out_send(OUT_SECOND, g, bit1, bit2, second).start()
        out_send(CORE_OWN, g, bit1, bit2, partner).start()
        out_local(g).start()

    def relay_out(g):
        out_send(OUT_FIRST, g, not1, bit2, first).wait_recv()
        out_send(OUT_RELAY, g, not1, bit2, second).start()
        out_send(CORE_FIRST, g, not1, bit2, partner).start()

    def second_out(g):
        out_send(OUT_SECOND, g, bit1, not2, second).wait_recv()
        out_send(CORE_SECOND, g, bit1, not2, partner).start()

    def relay_core(g):
        out_send(OUT_RELAY, g, not1, not2, second).wait_recv()
        out_send(CORE_RELAY, g, not1, not2, partner).start()

    def drain(g):
        out_local(g).wait()
        out_send(OUT_FIRST, g, bit1, bit2, first).wait_send()
        out_send(OUT_SECOND, g, bit1, bit2, second).wait_send()
        out_send(OUT_RELAY, g, not1, bit2, second).wait_send()
        out_send(CORE_OWN, g, bit1, bit2, partner).wait()
        out_send(CORE_FIRST, g, not1, bit2, partner).wait()
        out_send(CORE_SECOND, g, bit1, not2, partner).wait()
        out_send(CORE_RELAY, g, not1, not2, partner).wait()

    u_start()
    opened = txt_chunks + O_SLOTS - 1
    for g in range(txt_chunks, opened):
        start_o(jnp.int32(g))
    w_load(0, w1t_hbm, w1).start()
    w_load(1, w2t_hbm, w2).start()
    for g in range(txt_chunks):
        x1_load(g).start()
        if g < last_txt:
            txt_load(g).start()
    kv_load().start()
    q_load(0).start()
    for g in range(first_open, opened):
        send_o(jnp.int32(g))

    stages = ((second_out, -5, 0), (attend_pair, 0, 0), (mlp_hidden, 0, 0), (start_o, 5, opened), (relay_o, 4, first_open), (start_x, 2, txt_chunks), (relay_out, -4, 0), (mlp_theirs, 0, 0),
              (send_o, 5, opened), (add_first, -1, 0), (mlp_mine, 0, 0), (relay_core, -6, 0), (project, 1, txt_chunks), (drain, -6, 0), (finish, -2, 0))
    most = max(ahead for _, ahead, _ in stages)
    least = min(ahead for _, ahead, _ in stages)

    def step(i):
        @pl.when(i == U_RELAY_STEP)
        def _():
            u_relay()

        for stage, ahead, lowest in stages:
            if stage is attend_pair:
                g, lowest, highest = i - ATTEND_FROM, 0, units // 2
            else:
                g, highest = i + txt_chunks - most + ahead, total

            @pl.when((g >= lowest) & (g < highest))
            def _():
                stage(g)

        @pl.when(i == U_RELAY_STEP + 1)
        def _():
            u_last()

    loop(total - txt_chunks + most - least, step)


ATTEND_FROM = 3
U_RELAY_STEP = 2


def block_call(img_o, og, kv, x, u_txt, x1_txt, tu, wp, pw, w1t, w2t, w1i, w2i, vecs, fb, rows):
    batch, img_len, dim = x.shape
    txt_len = u_txt.shape[1]
    ff = w1t.shape[1]
    txt_chunks = batch * (txt_len // rows)
    per_img = img_len // rows
    img_chunks = batch * per_img
    assert txt_chunks == 2
    half, quarter, eighth = rows // 2, rows // 4, rows // 8
    cfg = (batch, txt_chunks, img_chunks, per_img, rows, 512)
    total = txt_chunks + img_chunks
    anywhere = pl.BlockSpec(memory_space=pl.ANY)
    return pl.pallas_call(
        functools.partial(block_kernel, cfg),
        in_specs=[anywhere] * 13 + [pl.BlockSpec(memory_space=pltpu.VMEM)] * 2,
        out_specs=[anywhere, anywhere],
        out_shape=[jax.ShapeDtypeStruct((total * rows, dim), BF16), jax.ShapeDtypeStruct(img_o.shape, BF16)],
        scratch_shapes=[
            pltpu.VMEM((kv.shape[0] // 3 * 2,) + kv.shape[1:], BF16),
            pltpu.VMEM((2, rows, HEAD), BF16),
            pltpu.VMEM((2, rows, HEAD), BF16),
            pltpu.VMEM((dim, dim), BF16),
            pltpu.VMEM((dim, ff), BF16),
            pltpu.VMEM((ff, dim), BF16),
            pltpu.VMEM((O_SLOTS, half, dim), BF16),
            pltpu.VMEM((2, half, dim), BF16),
            pltpu.VMEM((half, dim), BF16),
            pltpu.VMEM((SLOTS, eighth, dim), BF16),
            pltpu.VMEM((2, rows, dim), BF16),
            pltpu.VMEM((rows, ff), BF16),
            pltpu.VMEM((half, dim), BF16),
            pltpu.VMEM((2, half, dim), BF16),
            pltpu.VMEM((half, dim), F32),
            pltpu.VMEM((half, dim), BF16),
            pltpu.VMEM((2, quarter, dim), BF16),
            pltpu.VMEM((2, eighth, dim), F32),
            pltpu.VMEM((2, eighth, dim), BF16),
            pltpu.VMEM((SLOTS, eighth, dim), BF16),
            pltpu.VMEM((SLOTS, eighth, dim), BF16),
            pltpu.SemaphoreType.DMA((5,)),
            pltpu.SemaphoreType.DMA((10,)),
            pltpu.SemaphoreType.DMA((3, SEMS)),
            pltpu.SemaphoreType.DMA((2, 2)),
            *[pltpu.SemaphoreType.DMA((22, SEMS))] * 2,
        ],
        compiler_params=pltpu.CompilerParams(collective_id=0, has_side_effects=True, vmem_limit_bytes=VMEM_BYTES),
        name="block",
    )(img_o, og, kv, x, u_txt, x1_txt, tu, wp, pw, w1t, w2t, w1i, w2i, vecs, fb)


def copy_kernel(pieces, flat_hbm, *rest):
    outs, (buf, isem, osem) = rest[:-3], rest[-3:]
    rows = buf.shape[1]
    loads = []
    for n, (which, b, r) in enumerate(pieces):
        load = pltpu.make_async_copy(flat_hbm.at[n * rows:(n + 1) * rows, :], buf.at[n], isem.at[n])
        load.start()
        loads.append(load)
    stores = []
    for n, (which, b, r) in enumerate(pieces):
        loads[n].wait()
        store = pltpu.make_async_copy(buf.at[n], outs[which].at[b, r:r + rows, :], osem.at[n])
        store.start()
        stores.append(store)
    for store in stores:
        store.wait()


def copy_call(flat, shapes, rows):
    pieces = [(which, b, r) for which, shape in enumerate(shapes) for b in range(shape[0]) for r in range(0, shape[1], rows)]
    anywhere = pl.BlockSpec(memory_space=pl.ANY)
    dim = flat.shape[1]
    return pl.pallas_call(
        functools.partial(copy_kernel, pieces),
        in_specs=[anywhere],
        out_specs=[anywhere] * len(shapes),
        out_shape=[jax.ShapeDtypeStruct(shape, flat.dtype) for shape in shapes],
        scratch_shapes=[
            pltpu.VMEM((len(pieces), rows, dim), flat.dtype),
            pltpu.SemaphoreType.DMA((len(pieces),)),
            pltpu.SemaphoreType.DMA((len(pieces),)),
        ],
        compiler_params=pltpu.CompilerParams(vmem_limit_bytes=VMEM_BYTES),
        name="copy_out",
    )(flat)


def local_block(img, txt, vec, ids, img_w, txt_w):
    n_dev = 8
    batch, txt_len = txt.shape[:2]
    rows = txt_len

    def by_kind(weight):
        return jnp.transpose(weight, (1, 0, 2))

    def small_of(w):
        return w[1], w[3], w[4], w[5], w[7], w[9], w[11]

    table = jnp.asarray(rope_table())
    ids_t = jnp.transpose(ids, (2, 0, 1))
    o, kv, proj_w, txt_u, og, txt_x1, txt_tu, vecs, small = front_call(txt, img, by_kind(txt_w[2]), by_kind(img_w[2]), by_kind(txt_w[0]), by_kind(img_w[0]), img_w[6], txt_w[6], vec, small_of(txt_w), small_of(img_w), ids_t, table, n_dev, rows)
    flat, _ = block_call(o, og, kv, img, txt_u, txt_x1, txt_tu, proj_w, img_w[6], txt_w[8], txt_w[10], img_w[8], img_w[10], vecs, small, rows)
    txt_out, img_out = copy_call(flat, (txt.shape, img.shape), rows)
    return img_out, txt_out


def solution(mesh):
    act_spec = P('dp', WHOLE, WHOLE)
    mapped = jax.shard_map(local_block, mesh=mesh, in_specs=(act_spec, act_spec, P('dp', WHOLE), act_spec, PATH_SPECS, PATH_SPECS), out_specs=(act_spec, act_spec), check_vma=False)

    def forward(img, txt, vec, ids, *weights):
        return mapped(img, txt, vec, ids, weights[:12], weights[12:])

    return forward
```

```python
import functools

import jax
import jax.numpy as jnp
import numpy as np
from jax import lax
from jax.experimental import pallas as pl
from jax.experimental.pallas import tpu as pltpu
from jax.sharding import PartitionSpec as P

HEAD = 128
NORM_EPS = 1e-6
ROPE_THETA = 10000.0
AXES_DIM = (16, 56, 56)
N_IDS = 64
WHOLE = None
PATH_SPECS = (P(WHOLE, WHOLE, 'tp'), P(WHOLE, 'tp'), P(WHOLE, WHOLE, 'tp'), P(WHOLE, 'tp'), P(WHOLE), P(WHOLE), P('tp', WHOLE), P(WHOLE), P(WHOLE, 'tp'), P('tp'), P('tp', WHOLE), P(WHOLE))
F32 = jnp.float32
BF16 = jnp.bfloat16


def rope_table():
    cos = np.zeros((3 * N_IDS, HEAD), np.float32)
    sin = np.zeros((3 * N_IDS, HEAD), np.float32)
    lane = 0
    for axis, dim in enumerate(AXES_DIM):
        inv_freq = np.float32(ROPE_THETA) ** (-np.arange(0, dim, 2, dtype=np.float32) / np.float32(dim))
        angles = np.arange(N_IDS, dtype=np.float32)[:, None] * inv_freq.astype(np.float32)
        rows = slice(axis * N_IDS, (axis + 1) * N_IDS)
        c = np.cos(angles.astype(np.float64)).astype(np.float32)
        s = np.sin(angles.astype(np.float64)).astype(np.float32)
        cos[rows, lane:lane + dim:2] = c
        cos[rows, lane + 1:lane + dim:2] = c
        sin[rows, lane:lane + dim:2] = -s
        sin[rows, lane + 1:lane + dim:2] = s
        lane += dim
    parts = []
    for table in (cos, sin):
        rest = table
        for _ in range(3):
            part = rest.astype(jnp.bfloat16)
            parts.append(np.asarray(part))
            rest = rest - np.asarray(part).astype(np.float32)
    return np.concatenate(parts, axis=1)


MESH = pl.DeviceIdType.MESH


SHIFT1, SCALE1, GATE1, SHIFT2, SCALE2, GATE2, PROJ_B, FC2_B = range(8)
QKV_B, Q_GAIN, K_GAIN, FC1_B = range(4)
VMEM_BYTES = 67043328


def row_of(ref, sel, row, at=slice(None)):
    return ref[sel, pl.ds(row, 1), at]


STRIP = 16
PATHS = range(2)


def loop(count, body):
    lax.fori_loop(0, count, lambda i, carry: (body(i), carry)[-1], 0)


def row_mean(x):
    return jnp.mean(x, axis=-1, keepdims=True)


def normalize(x):
    centered = x - row_mean(x)
    return centered * lax.rsqrt(row_mean(centered * centered) + NORM_EPS)


def softened(s):
    top = jnp.max(s, axis=-1, keepdims=True)
    p = jnp.exp2((s - top) * (HEAD ** -0.5 * LOG2E))
    return p.astype(BF16), jnp.sum(p, axis=-1, keepdims=True)


def weighted(s, v):
    p, total = softened(s)
    return (jnp.dot(p, v, preferred_element_type=F32) * (1.0 / total)).astype(BF16)


def scores_of(q, k):
    return lax.dot_general(q, k, (((1,), (1,)), ((), ())), preferred_element_type=F32)


def modulated(x, vec_ref, sel, shift, scale):
    return ((1.0 + row_of(vec_ref, sel, scale)) * normalize(x) + row_of(vec_ref, sel, shift)).astype(BF16)


LOG2E = 1.4426950408889634
(W_FIRST, W_SECOND, W_RELAY, W_CORE, W_CORE_FIRST, W_CORE_SECOND, W_CORE_RELAY, Z_FIRST, Z_SECOND, Z_RELAY) = range(10)
(G_CORE, G_FIRST, G_SECOND, G_RELAY) = range(4)
(T_CORE, T_FIRST, T_SECOND, T_OUT_FIRST, T_OUT_SECOND, T_OUT_RELAY, T_CORE_OWN, T_CORE_FIRST, T_CORE_SECOND, T_CORE_RELAY) = range(10)
SHARED, COMMON, MISSING = range(3)
PIECES = 3
READY = 4
EARLY = 4
FIRST_LATE = 5
HEADS_HERE = 3


def ident(dev):
    return dev if isinstance(dev, dict) else {'tp': dev}


class Place:
    def __init__(self):
        me = lax.axis_index('tp')
        core = me % 2
        xi = (me // 2) % 2
        yi = me // 4
        x_next = me + 2 - 4 * xi
        y_next = me + 4 - 8 * yi
        self.me, self.core = me, core
        self.partner = me + 1 - 2 * core
        self.first = x_next * (1 - core) + y_next * core
        self.second = x_next * core + y_next * (1 - core)
        self.diagonal = x_next + y_next - me
        self.bit1 = xi * (1 - core) + yi * core
        self.bit2 = xi * core + yi * (1 - core)
        self.not1, self.not2, self.far = 1 - self.bit1, 1 - self.bit2, 1 - core

    def enter(self, others):
        barrier = pltpu.get_barrier_semaphore()
        for dev in others:
            pl.semaphore_signal(barrier, inc=1, device_id=ident(dev), device_id_type=MESH)
        pl.semaphore_wait(barrier, len(others))


def rows_at(start, size):
    return pl.ds(pl.multiple_of(start, size), size)


def front_kernel(cfg, txt_hbm, img_hbm, wt_hbm, wi_hbm, mt_hbm, mi_hbm, pw_hbm, tw_hbm, cond_ref, small_t, small_i, ids_ref, tab_ref,
                 o_hbm, kv_hbm, wp_hbm, ut_hbm, og_hbm, x1_ref, tu_ref, vec_ref, small_ref,
                 w, m_w, m_b, m_early, m_late, xs, ua, ub, qkv, s0, s1, s2, probs, o_all, tw, t_send, t_recv, t_own, t_sum, t_rs1, t_rs2_out, t_rs2_in, t_keep, t_x, t_u,
                 wsem, msem, xsem, osem, tsem, gsem, psend, precv, tsend, trecv, gsend, grecv, msend, mrecv):
    batch, txt_len, img_len, rows = cfg
    half, quarter, eighth = rows // 2, rows // 4, rows // 8
    total = txt_len + img_len
    per_img = img_len // rows
    blocks = batch * (per_img + 1)
    n_dev = m_early.shape[0]
    others = range(1, n_dev)
    dim = w.shape[1]
    width = o_all.shape[1]
    heads = width // HEAD
    place = Place()
    me, core, partner, first, second, diagonal, bit1, bit2 = place.me, place.core, place.partner, place.first, place.second, place.diagonal, place.bit1, place.bit2
    not1, not2, far = place.not1, place.not2, place.far
    piece = width // PIECES
    plane = lax.axis_index('dp')
    odd = plane % 2
    beside = {'dp': plane + 1 - 2 * odd}

    def position(n):
        n = jnp.int32(n)
        img = (n >= batch).astype(jnp.int32)
        m = n - batch
        b = (1 - img) * n + img * (m // per_img)
        r = img * (1 + m % per_img)
        return b, r * rows

    def x_copy(n, source):
        b, r0 = position(n)
        ref = txt_hbm.at[b] if source == 0 else img_hbm.at[b, rows_at(r0 - rows, rows), :]
        return pltpu.make_async_copy(ref, xs.at[n % 4], xsem.at[n % 4])

    def x_start(n):
        @pl.when(n < batch)
        def _():
            x_copy(n, 0).start()

        @pl.when((n >= batch) & (n < blocks))
        def _():
            x_copy(n, 1).start()

    def x_wait(n):
        @pl.when(n < blocks)
        def _():
            pltpu.make_async_copy(txt_hbm.at[0], xs.at[n % 4], xsem.at[n % 4]).wait()

    def w_columns(path, j):
        return w.at[path, :, j * width:(j + 1) * width]

    def w_load(path, j):
        return pltpu.make_async_copy((wt_hbm, wi_hbm)[path].at[j], w_columns(path, j), wsem.at[path, j])

    def early_load(path, k):
        return pltpu.make_async_copy((mt_hbm, mi_hbm)[path].at[k], w_columns(path, k), wsem.at[path, k])

    def late_load(c, path):
        return pltpu.make_async_copy((mt_hbm, mi_hbm)[path].at[GATE1 + c // 2], m_w.at[c % 2], msem.at[c % 2])

    def late_start(c):
        for path in PATHS:
            @pl.when(c % 2 == path)
            def _():
                late_load(c, path).start()

    def m_copy(part, d, send):
        buf, at = ((m_early, slice(None)), (m_late, slice(FIRST_LATE)), (m_late, slice(FIRST_LATE, 8)))[part]
        ref = buf.at[me if send else (me + n_dev - d) % n_dev, at]
        return pltpu.make_async_remote_copy(src_ref=ref, dst_ref=ref, send_sem=msend.at[part, d], recv_sem=mrecv.at[part, d], device_id={'tp': (me + d) % n_dev}, device_id_type=MESH)

    def m_send(part):
        for d in others:
            m_copy(part, d, True).start()

    def m_wait(part):
        for d in others:
            m_copy(part, d, True).wait_send()
            m_copy(part, d, False).wait_recv()

    for k in (SHIFT1, SCALE1):
        for path in PATHS:
            early_load(path, k).start()
    for n in range(3):
        x_copy(n, 0 if n < batch else 1).start()
    v = cond_ref[...].astype(F32)
    silu = (v * (1.0 / (1.0 + jnp.exp(-v)))).astype(BF16)
    for path, (mod_b, qkv_b, q_gain, k_gain, proj_b, fc1_b, fc2_b) in enumerate((small_t, small_i)):
        m_b[path] = mod_b[...].astype(F32)
        for row, ref in ((PROJ_B, proj_b), (FC2_B, fc2_b)):
            vector = ref[...].astype(F32)[None, :]
            for b in range(batch):
                vec_ref[path * batch + b, row:row + 1, :] = vector
        for row, ref in ((Q_GAIN, q_gain), (K_GAIN, k_gain), (FC1_B, fc1_b)):
            vector = ref[...].astype(F32)[None, :]
            small_ref[path, row:row + 1, :vector.shape[1]] = vector
        for j in range(qkv_b.shape[0]):
            small_ref[path, QKV_B:Q_GAIN, j * width:(j + 1) * width] = qkv_b[j:j + 1, :].astype(F32)
    place.enter([(me + d) % n_dev for d in others] + [beside])

    def early_chunk(k, path):
        early_load(path, k).wait()
        acc = jnp.dot(silu, w_columns(path, k)[...], preferred_element_type=F32)
        return (acc + m_b[path, k:k + 1, :]).astype(BF16)

    m_early[me] = jnp.concatenate([early_chunk(k, path) for k in (SHIFT1, SCALE1) for path in PATHS], axis=0)
    m_send(0)
    for j in range(3):
        w_load(0, j).start()
    tw_load = pltpu.make_async_copy(tw_hbm, tw, tsem.at[1])

    def late_chunk(t):
        c = jnp.minimum(t, 7)
        path, k = c % 2, GATE1 + c // 2
        acc = jnp.dot(silu, m_w[c % 2], preferred_element_type=F32) + m_b[path, pl.ds(k, 1), :]
        m_late[me, t] = acc.astype(BF16).astype(F32)

    def late_rows(part):
        m_wait(1 + part)
        for j in range(n_dev):
            for c in range(8)[slice(FIRST_LATE) if part == 0 else slice(FIRST_LATE, 8)]:
                for b in range(batch):
                    vec_ref[c % 2 * batch + b, pl.ds(GATE1 + c // 2, 1), j * width:(j + 1) * width] = m_late[j, c, b:b + 1, :]

    def piece_at(j):
        return rows_at(((1 - j) * (2 * odd - 1) + 1) * piece, piece)

    def remote(sends, recvs, kind, j, src, dst, dev):
        return pltpu.make_async_remote_copy(src_ref=src, dst_ref=dst, send_sem=sends.at[kind, j], recv_sem=recvs.at[kind, j], device_id=ident(dev), device_id_type=MESH)

    def p_copy(kind, j, owner, dev):
        dst = wp_hbm.at[owner, piece_at(j), :]
        src = pw_hbm.at[piece_at(j), :] if kind in (W_FIRST, W_SECOND) else dst
        return remote(psend, precv, kind, j, src, dst, dev)

    def w_own():
        return remote(psend, precv, W_CORE, SHARED, pw_hbm, wp_hbm.at[me], partner)

    def w_core():
        w_own().start()

    def z_copy(kind, owner, j=SHARED):
        ref = wp_hbm.at[owner, piece_at(j), :]
        return remote(psend, precv, kind, SHARED, ref, ref, beside)

    def w_relay(j):
        p_copy(W_FIRST, j, first, first).wait_recv()
        p_copy(W_RELAY, j, first, second).start()
        p_copy(W_CORE_FIRST, j, first, partner).start()
        if j == SHARED:
            p_copy(W_SECOND, COMMON, me, second).start()
            z_copy(Z_FIRST, first).start()

    def w_second(j):
        p_copy(W_SECOND, j, second, second).wait_recv()
        p_copy(W_CORE_SECOND, j, second, partner).start()
        if j == SHARED:
            z_copy(Z_SECOND, second).start()

    def w_last(j):
        p_copy(W_RELAY, j, diagonal, second).wait_recv()
        p_copy(W_CORE_RELAY, j, diagonal, partner).start()
        if j == SHARED:
            z_copy(Z_RELAY, diagonal).start()

    from_beside = ((Z_FIRST, first, W_CORE_FIRST), (Z_SECOND, second, W_CORE_SECOND), (Z_RELAY, diagonal, W_CORE_RELAY))

    def w_beside(n):
        kind, owner, core_kind = from_beside[n]
        z_copy(kind, owner, MISSING).wait_recv()
        p_copy(core_kind, MISSING, owner, partner).start()

    p_copy(W_FIRST, SHARED, me, first).start()
    p_copy(W_SECOND, SHARED, me, second).start()
    p_copy(W_FIRST, COMMON, me, first).start()

    even = lax.broadcasted_iota(jnp.int32, (rows, HEAD), 1) % 2 == 0
    code = lax.broadcasted_iota(jnp.int32, (N_IDS, rows), 0)

    def select(n):
        n = jnp.int32(n)
        img = (n >= batch).astype(jnp.int32)
        return (1 - img) * n + img * (batch + (n - batch) // per_img)

    def norm(n, u):
        sel = select(n)
        for r in range(0, rows, STRIP):
            u[r // half, r % half:r % half + STRIP, :] = modulated(xs[n % 4, r:r + STRIP, :].astype(F32), vec_ref, sel, SHIFT1, SCALE1)

    def heads_of(n, u):
        b, r0 = position(n)
        path = (jnp.int32(n) >= batch).astype(jnp.int32)
        hot = jnp.concatenate([(ids_ref[axis, pl.ds(b, 1), rows_at(r0, rows)] == code).astype(F32).astype(BF16) for axis in range(3)], axis=0)
        parts = lax.dot_general(hot, tab_ref[...], (((0,), (0,)), ((), ())), preferred_element_type=F32)
        cos_t, sin_t = (sum(parts[:, (3 * i + j) * HEAD:(3 * i + j + 1) * HEAD] for j in range(3)) for i in range(2))
        at = rows_at(b * total + r0, rows)
        for c0 in range(0, 3 * heads, 4):
            c1 = min(c0 + 4, 3 * heads)
            a = jnp.dot(u[...].reshape(rows, dim), w[path, :, c0 * HEAD:c1 * HEAD], preferred_element_type=F32) + row_of(small_ref, path, QKV_B, slice(c0 * HEAD, c1 * HEAD))
            for c in range(c0, c1):
                t = a[:, (c - c0) * HEAD:(c - c0 + 1) * HEAD]
                kind = c // heads
                if kind < 2:
                    t = t * lax.rsqrt(row_mean(t * t) + NORM_EPS) * row_of(small_ref, path, Q_GAIN + kind, slice(HEAD))
                    swapped = jnp.where(even, pltpu.roll(t, HEAD - 1, 1), pltpu.roll(t, 1, 1))
                    t = t * cos_t + swapped * sin_t
                qkv[c, at, :] = t.astype(BF16)

    m_wait(0)
    for j in range(n_dev):
        rows_here = m_early[j].astype(F32)
        for n in range(2 * 2 * batch):
            k, sel = n // (2 * batch), n % (2 * batch)
            vec_ref[sel, k:k + 1, j * width:(j + 1) * width] = rows_here[n:n + 1, :]
    x_wait(0)
    norm(0, ua)
    for j in range(3):
        w_load(0, j).wait()
    for c in range(2):
        late_load(c, c).start()
    for j in range(3):
        w_load(1, j).start()
    tw_load.start()

    def qkv_step(t):
        x_start(2 * t + 3)
        x_start(2 * t + 4)
        x_wait(2 * t + 1)
        x_wait(2 * t + 2)
        @pl.when(t == 1)
        def _():
            for j in range(3):
                w_load(1, j).wait()

        @pl.when(t < 8)
        def _():
            late_load(t, 0).wait()

        late_chunk(t)
        norm(2 * t + 1, ub)
        heads_of(2 * t, ua)
        norm(jnp.minimum(2 * t + 2, blocks - 1), ua)
        heads_of(2 * t + 1, ub)

        @pl.when(t < 6)
        def _():
            late_start(t + 2)

    kv_store = pltpu.make_async_copy(qkv.at[:, total:, :], kv_hbm, tsem.at[0])

    def late_send(part):
        m_send(1 + part)

    def kv_send():
        kv_store.start()

    done_here = batch + per_img

    def rows_of(n, c, size, r0):
        return qkv[c, rows_at(position(n)[0] * total + r0, size), :]

    def scores(n, h, s):
        s[...] = scores_of(rows_of(n, h, rows, position(n)[1]), rows_of(n, heads + h, total, 0))

    def weigh(n, h, s):
        sums = []
        for r in range(0, rows, STRIP):
            p, total_p = softened(s[r:r + STRIP, :])
            sums.append(total_p)
            probs[r:r + STRIP, :] = p
        o = jnp.dot(probs[...], rows_of(n, 2 * heads + h, total, 0), preferred_element_type=F32)
        o_all[rows_at(n * rows, rows), h * HEAD:(h + 1) * HEAD] = (o * (1.0 / jnp.concatenate(sums, axis=0))).astype(BF16)

    def t_copy(kind, b, src, dst, dev):
        return remote(tsend, trecv, kind, b, src, dst, dev)

    def t_core(b):
        return t_copy(T_CORE, b, t_send, t_recv.at[b], partner)

    def t_first(b):
        return t_copy(T_FIRST, b, t_sum.at[b, rows_at(not1 * quarter, quarter), :], t_rs1.at[b], first)

    def t_second(b):
        return t_copy(T_SECOND, b, t_rs2_out.at[b], t_rs2_in.at[b], second)

    def own_rows(b1, b2):
        return rows_at(core * half + b1 * quarter + b2 * eighth, eighth)

    def t_out(kind, b, b1, b2, dev):
        ref = ut_hbm.at[b, own_rows(b1, b2), :]
        return t_copy(kind, b, t_u.at[b] if kind in (T_OUT_FIRST, T_OUT_SECOND, T_CORE_OWN) else ref, ref, dev)

    def t_local(b):
        return pltpu.make_async_copy(t_u.at[b], ut_hbm.at[b, own_rows(bit1, bit2), :], tsem.at[2 + b])

    def t_load(b):
        return pltpu.make_async_copy(txt_hbm.at[b, own_rows(bit1, bit2), :], t_x.at[b], tsem.at[2 + batch + b])

    tile = min(512, dim)

    def text_product(b, who, store):
        def columns(n):
            at = rows_at(n * tile, tile)
            store(at, jnp.dot(o_all[rows_at(b * rows + who * half, half), :], tw[:, at], preferred_element_type=F32))

        loop(dim // tile, columns)

    def text_partial(b):
        if b == 0:
            tw_load.wait()
        t_load(b).start()

        def to_send(at, value):
            t_send[:, at] = value.astype(BF16)

        def to_own(at, value):
            t_own[:, at] = value

        text_product(b, far, to_send)
        t_core(b).start()
        text_product(b, core, to_own)

    def text_sum(b):
        t_core(b).wait()

        def add(n):
            at = rows_at(n * STRIP, STRIP)
            t_sum[b, at, :] = (t_own[at, :] + t_recv[b, at, :].astype(F32)).astype(BF16)

        loop(half // STRIP, add)
        t_first(b).start()

    def text_quarter(b):
        t_first(b).wait()
        t_rs2_out[b] = (t_sum[b, rows_at(bit1 * quarter + not2 * eighth, eighth), :].astype(F32) + t_rs1[b, rows_at(not2 * eighth, eighth), :].astype(F32)).astype(BF16)
        t_keep[b] = t_sum[b, rows_at(bit1 * quarter + bit2 * eighth, eighth), :].astype(F32) + t_rs1[b, rows_at(bit2 * eighth, eighth), :].astype(F32)
        t_second(b).start()

    def text_finish(b):
        t_second(b).wait()
        t_load(b).wait()
        branch = t_keep[b] + t_rs2_in[b].astype(F32) + row_of(vec_ref, b, PROJ_B)
        x1 = (t_x[b].astype(F32) + row_of(vec_ref, b, GATE1) * branch).astype(BF16)
        x1_ref[b] = x1
        u = modulated(x1.astype(F32), vec_ref, b, SHIFT2, SCALE2)
        if b == batch - 1:
            tu_ref[...] = u
            return
        t_u[b] = u
        t_out(T_OUT_FIRST, b, bit1, bit2, first).start()
        t_out(T_OUT_SECOND, b, bit1, bit2, second).start()
        t_out(T_CORE_OWN, b, bit1, bit2, partner).start()
        t_local(b).start()

    def text_relay(b):
        t_out(T_OUT_FIRST, b, not1, bit2, first).wait_recv()
        t_out(T_OUT_RELAY, b, not1, bit2, second).start()
        t_out(T_CORE_FIRST, b, not1, bit2, partner).start()
        t_out(T_OUT_SECOND, b, bit1, not2, second).wait_recv()
        t_out(T_CORE_SECOND, b, bit1, not2, partner).start()

    def text_last(b):
        t_out(T_OUT_RELAY, b, not1, not2, second).wait_recv()
        t_out(T_CORE_RELAY, b, not1, not2, partner).start()

    def g_rows(m, who):
        return o_all.at[rows_at((batch + m) * rows + who * half, half), :]

    def g_mine(m):
        return og_hbm.at[m, :, rows_at(me * width, width)]

    def g_local(m):
        return pltpu.make_async_copy(g_rows(m, core), g_mine(m), gsem.at[m])

    def g_core(m):
        return remote(gsend, grecv, G_CORE, m, g_rows(m, far), g_mine(m), partner)

    def g_copy(kind, m, owner, dev):
        ref = og_hbm.at[m, :, rows_at(owner // 2 * (2 * width), 2 * width)]
        return remote(gsend, grecv, kind, m, ref, ref, dev)

    def gather_start(m):
        g_local(m).start()
        g_core(m).start()

    def gather_send(m):
        g_local(m).wait()
        g_core(m).wait()
        g_copy(G_FIRST, m, me, first).start()
        g_copy(G_SECOND, m, me, second).start()

    def gather_relay(m):
        g_copy(G_FIRST, m, first, first).wait_recv()
        g_copy(G_RELAY, m, first, second).start()

    qkv_first, attend_first = (batch + per_img) // 2, 1 + EARLY
    resume = blocks // 2 + attend_first
    steps = blocks // 2 + done_here
    known = dict(locals())

    def run(calls):
        for call in calls:
            name, *args = call.split()
            known[name](*map(int, args))

    def attended(a):
        early = ((a >= 1) & (a <= EARLY)).astype(jnp.int32)
        return a + early - EARLY * (a == attend_first).astype(jnp.int32)

    def attention_step(a, begins):
        n = attended(a)

        @pl.when(begins)
        def _():
            scores(n, 0, s0)

        scores(n, 1, s1)
        weigh(n, 0, s0)
        scores(n, 2, s2)
        weigh(n, 1, s1)
        scores(attended(jnp.minimum(a + 1, done_here - 1)), 0, s0)
        weigh(n, 2, s2)

    def step(i):
        for when, calls in enumerate(HOOKS[:steps]):
            if calls:
                @pl.when(i == when)
                def _():
                    run(calls)

        in_first = i < qkv_first
        in_second = (i >= qkv_first + attend_first) & (i < resume)

        @pl.when(in_first | in_second)
        def _():
            qkv_step(i - attend_first * in_second.astype(jnp.int32))

        @pl.when(jnp.logical_not(in_first | in_second))
        def _():
            late = (i >= resume).astype(jnp.int32)
            attention_step(i - late * (blocks // 2) - (1 - late) * qkv_first, (i == qkv_first) | (i == resume))

    loop(steps, step)

    o_out = pltpu.make_async_copy(o_all.at[batch * rows:, :], o_hbm, osem)
    o_out.start()
    run(HOOKS[steps])
    o_out.wait()
    kv_store.wait()
    t_local(0).wait()
    for kind, b1, b2, dev in ((T_OUT_FIRST, bit1, bit2, first), (T_OUT_SECOND, bit1, bit2, second), (T_OUT_RELAY, not1, bit2, second)):
        t_out(kind, 0, b1, b2, dev).wait_send()
    for kind, b1, b2 in ((T_CORE_OWN, bit1, bit2), (T_CORE_FIRST, not1, bit2), (T_CORE_SECOND, bit1, not2), (T_CORE_RELAY, not1, not2)):
        t_out(kind, 0, b1, b2, partner).wait()
    for j in (SHARED, COMMON):
        for kind, owner, dev in ((W_FIRST, me, first), (W_SECOND, me, second), (W_RELAY, first, second)):
            p_copy(kind, j, owner, dev).wait_send()
    w_own().wait()
    for kind, owner, core_kind in from_beside:
        z_copy(kind, owner).wait_send()
        for j in range(PIECES):
            p_copy(core_kind, j, owner, partner).wait()
    for m in range(READY):
        g_copy(G_FIRST, m, me, first).wait_send()
        g_copy(G_SECOND, m, me, second).wait_send()
        g_copy(G_RELAY, m, first, second).wait_send()
        g_copy(G_SECOND, m, second, second).wait_recv()
        g_copy(G_RELAY, m, diagonal, second).wait_recv()


HOOKS = (
    (),
    (),
    (),
    ('w_relay 0',),
    (),
    ('late_send 0', 'w_relay 1'),
    ('w_core', 'text_partial 0'),
    ('w_second 0',),
    (),
    ('text_sum 0', 'gather_start 1', 'gather_start 0'),
    ('gather_start 3', 'gather_send 1'),
    ('gather_send 0', 'gather_start 2'),
    ('gather_send 3', 'text_quarter 0'),
    ('late_send 1', 'gather_send 2', 'w_last 0'),
    ('kv_send', 'late_rows 0', 'gather_relay 3', 'text_finish 0', 'w_second 1', 'gather_relay 1'),
    ('text_partial 1', 'w_last 1'),
    ('w_beside 0', 'w_beside 1', 'text_sum 1'),
    ('text_relay 0',),
    ('gather_relay 0', 'text_quarter 1', 'gather_relay 2'),
    ('late_rows 1', 'w_beside 2', 'text_last 0', 'text_finish 1'),
)


def front_call(txt, img, wt, wi, mt, mi, pw, tw, cond, small_t, small_i, ids_t, table, n_dev, rows):
    batch, txt_len, dim = txt.shape
    img_len = img.shape[1]
    total = txt_len + img_len
    width = pw.shape[0]
    heads = width // HEAD
    half, quarter, eighth = rows // 2, rows // 4, rows // 8
    assert heads == HEADS_HERE and batch == 2
    cfg = (batch, txt_len, img_len, rows)
    blocks = batch * (1 + img_len // rows)
    vmem = pl.BlockSpec(memory_space=pltpu.VMEM)
    anywhere = pl.BlockSpec(memory_space=pl.ANY)
    tall = [pltpu.VMEM((half, dim), BF16), pltpu.VMEM((batch, half, dim), BF16), pltpu.VMEM((half, dim), F32), pltpu.VMEM((batch, half, dim), BF16), pltpu.VMEM((batch, quarter, dim), BF16)]
    short = [pltpu.VMEM((batch, eighth, dim), dtype) for dtype in (BF16, BF16, F32, BF16, BF16)]
    return pl.pallas_call(
        functools.partial(front_kernel, cfg),
        in_specs=[anywhere] * 8 + [vmem, (vmem,) * len(small_t), (vmem,) * len(small_i), vmem, vmem],
        out_specs=[anywhere] * 5 + [vmem] * 4,
        out_shape=[
            jax.ShapeDtypeStruct((img_len, width), BF16),
            jax.ShapeDtypeStruct((3 * heads, total, HEAD), BF16),
            jax.ShapeDtypeStruct((n_dev, width, dim), BF16),
            jax.ShapeDtypeStruct((batch, txt_len, dim), BF16),
            jax.ShapeDtypeStruct((READY, half, dim), BF16),
            jax.ShapeDtypeStruct((batch, eighth, dim), BF16),
            jax.ShapeDtypeStruct((eighth, dim), BF16),
            jax.ShapeDtypeStruct((2 * batch, FC2_B + 1, dim), F32),
            jax.ShapeDtypeStruct((2, FC1_B + 1, dim), F32),
        ],
        scratch_shapes=[
            pltpu.VMEM((2, dim, 3 * width), BF16),
            pltpu.VMEM((2, dim, width), BF16),
            pltpu.VMEM((2, PROJ_B, width), F32),
            pltpu.VMEM((n_dev, 4 * batch, width), BF16),
            pltpu.VMEM((n_dev, blocks // 2, batch, width), F32),
            pltpu.VMEM((4, rows, dim), BF16),
            pltpu.VMEM((batch, half, dim), BF16),
            pltpu.VMEM((batch, half, dim), BF16),
            pltpu.VMEM((3 * heads, batch * total, HEAD), BF16),
            pltpu.VMEM((rows, total), F32),
            pltpu.VMEM((rows, total), F32),
            pltpu.VMEM((rows, total), F32),
            pltpu.VMEM((rows, total), BF16),
            pltpu.VMEM((batch * txt_len + img_len, width), BF16),
            pltpu.VMEM((width, dim), BF16),
            *tall,
            *short,
            pltpu.SemaphoreType.DMA((2, 3)),
            pltpu.SemaphoreType.DMA((2,)),
            pltpu.SemaphoreType.DMA((4,)),
            pltpu.SemaphoreType.DMA,
            pltpu.SemaphoreType.DMA((6,)),
            pltpu.SemaphoreType.DMA((READY,)),
            *[pltpu.SemaphoreType.DMA((10, PIECES))] * 2,
            *[pltpu.SemaphoreType.DMA((10, batch))] * 2,
            *[pltpu.SemaphoreType.DMA((4, READY))] * 2,
            *[pltpu.SemaphoreType.DMA((3, n_dev))] * 2,
        ],
        compiler_params=pltpu.CompilerParams(collective_id=2, has_side_effects=True, vmem_limit_bytes=VMEM_BYTES),
        name="front",
    )(txt, img, wt, wi, mt, mi, pw, tw, cond, small_t, small_i, ids_t, table)


(O_CORE, O_FIRST, O_SECOND, O_RELAY, U_CORE, PART_CORE, RS_FIRST, RS_SECOND, OUT_FIRST, OUT_SECOND, OUT_RELAY, CORE_OWN, CORE_FIRST, CORE_SECOND, CORE_RELAY,
 U_FIRST, U_SECOND, U_RELAY, U_OWN, U_CORE_FIRST, U_CORE_SECOND, U_CORE_RELAY) = range(22)
(L_O, L_X, L_OUT) = range(3)
SLOTS = 4
O_SLOTS = 10
OPENED = 1
SEMS = 12


def two(n):
    return n % 2


def block_kernel(cfg, o_hbm, og_hbm, kv_hbm, x_hbm, ut_hbm, x1t_hbm, tu_hbm, wp_hbm, pw_hbm, w1t_hbm, w2t_hbm, w1i_hbm, w2i_hbm, vec_ref, fb_ref, out_hbm, o2_hbm,
                 kv, qs, os, wp, w1, w2, obuf, xbuf, x1keep, u2, hid, psend, precv, own, chip_sum, rs1, keep2, rs2_out, rs2_in, outb,
                 asem, wsem, lsem, tsem, ssem, rsem):
    batch, txt_chunks, img_chunks, per_img, rows, tile = cfg
    half, quarter, eighth = rows // 2, rows // 4, rows // 8
    dim = wp.shape[0]
    ff = w1.shape[1]
    cols = o_hbm.shape[1]
    heads = cols // HEAD
    total = txt_chunks + img_chunks
    per_txt = txt_chunks // batch

    place = Place()
    me, core, partner, first, second, bit1, bit2 = place.me, place.core, place.partner, place.first, place.second, place.bit1, place.bit2
    not1, not2, far = place.not1, place.not2, place.far
    txt_len = ut_hbm.shape[1]
    place.enter([partner, first, second])

    def remote(kind, g, src, dst, dev):
        return pltpu.make_async_remote_copy(src_ref=src, dst_ref=dst, send_sem=ssem.at[kind, g % SEMS], recv_sem=rsem.at[kind, g % SEMS], device_id={'tp': dev}, device_id_type=MESH)

    def img_pos(g):
        k = g - txt_chunks
        return k // per_img, (k % per_img) * rows

    def chip_cols(dev):
        return rows_at((dev // 2) * (2 * cols), 2 * cols)

    def own_rows(b1, b2):
        return core * half + b1 * quarter + b2 * eighth

    def o_from(b):
        return (o_hbm, o2_hbm)[b]

    first_open = txt_chunks + og_hbm.shape[0]

    def o_ready(g):
        return pltpu.make_async_copy(og_hbm.at[g - txt_chunks], obuf.at[g % O_SLOTS], lsem.at[L_O, g % SEMS])

    def o_local(g, b):
        r0 = img_pos(g)[1]
        return pltpu.make_async_copy(o_from(b).at[rows_at(r0 + core * half, half), :], obuf.at[g % O_SLOTS, :, rows_at(me * cols, cols)], lsem.at[L_O, g % SEMS])

    def o_core(g, b):
        r0 = img_pos(g)[1]
        return remote(O_CORE, g, o_from(b).at[rows_at(r0 + far * half, half), :], obuf.at[g % O_SLOTS, :, rows_at(me * cols, cols)], partner)

    units = per_img * heads

    def q_load(u):
        r0 = txt_len + u // heads * rows
        return pltpu.make_async_copy(kv_hbm.at[u % heads, rows_at(r0, rows), :], qs.at[two(u)], asem.at[two(u)])

    def o_store(u):
        return pltpu.make_async_copy(os.at[two(u)], o2_hbm.at[rows_at(u // heads * rows, rows), rows_at(u % heads * HEAD, HEAD)], asem.at[2 + two(u)])

    def kv_load():
        return pltpu.make_async_copy(kv_hbm.at[heads:], kv, asem.at[4])

    def attend(u, carry):
        @pl.when(u == 0)
        def _():
            kv_load().wait()

        q_load(u).wait()

        @pl.when(u + 1 < units)
        def _():
            q_load(u + 1).start()

        @pl.when(u >= 2)
        def _():
            o_store(u - 2).wait()

        k = kv[u % heads]
        v = kv[heads + u % heads]
        for r in range(0, rows, half):
            os[two(u), r:r + half, :] = weighted(scores_of(qs[two(u), r:r + half, :], k), v)
        o_store(u).start()

        @pl.when(u == units - 1)
        def _():
            o_store(u - 1).wait()
            o_store(u).wait()
        return carry

    def attended(i):
        return sum(count * (i > n).astype(jnp.int32) for n, count in enumerate(ATTEND) if count)

    def o_send(kind, g, owner, dev):
        ref = obuf.at[g % O_SLOTS, :, chip_cols(owner)]
        return remote(kind, g, ref, ref, dev)

    def x_load(g):
        b, r0 = img_pos(g)
        return pltpu.make_async_copy(x_hbm.at[b, rows_at(r0 + core * half, half), :], xbuf.at[two(g)], lsem.at[L_X, g % SEMS])

    def u_core(g):
        return remote(U_CORE, g, u2.at[two(g), :half, :], u2.at[two(g), half:, :], partner)

    def part_core(g):
        return remote(PART_CORE, g, psend, precv.at[two(g)], partner)

    def rs_first(g):
        return remote(RS_FIRST, g, chip_sum.at[rows_at(not1 * quarter, quarter), :], rs1.at[two(g)], first)

    def rs_second(g):
        return remote(RS_SECOND, g, rs2_out.at[two(g)], rs2_in.at[g % SLOTS], second)

    def out_ref(g, b1, b2):
        return out_hbm.at[rows_at(g * rows + own_rows(b1, b2), eighth), :]

    def out_send(kind, g, b1, b2, dev):
        ref = out_ref(g, b1, b2)
        mine = kind in (OUT_FIRST, OUT_SECOND, CORE_OWN)
        return remote(kind, g, outb.at[g % SLOTS] if mine else ref, ref, dev)

    def out_local(g):
        return pltpu.make_async_copy(outb.at[g % SLOTS], out_ref(g, bit1, bit2), lsem.at[L_OUT, g % SEMS])

    last_txt = txt_chunks - 1

    def txt_load(g, who):
        mine = who is core
        return pltpu.make_async_copy(ut_hbm.at[g, rows_at(who * half, half), :], u2.at[two(g), slice(half) if mine else slice(half, rows), :], tsem.at[0 if mine else 2, g])

    def x1_load(g):
        return pltpu.make_async_copy(x1t_hbm.at[g], x1keep.at[g], tsem.at[1, g])

    def u_rows(b1, b2, base=0):
        return u2.at[two(last_txt), rows_at(base + b1 * quarter + b2 * eighth, eighth), :]

    def u_local():
        return pltpu.make_async_copy(tu_hbm, u_rows(bit1, bit2), tsem.at[0, last_txt])

    def u_send(kind, b1, b2, dev):
        src = tu_hbm if kind in (U_FIRST, U_SECOND, U_OWN) else u_rows(b1, b2)
        return remote(kind, last_txt, src, u_rows(b1, b2, 0 if dev is not partner else half), dev)

    def u_start():
        u_local().start()
        u_send(U_FIRST, bit1, bit2, first).start()
        u_send(U_SECOND, bit1, bit2, second).start()
        u_send(U_OWN, bit1, bit2, partner).start()

    def u_relay():
        u_send(U_FIRST, not1, bit2, first).wait_recv()
        u_send(U_RELAY, not1, bit2, second).start()
        u_send(U_CORE_FIRST, not1, bit2, partner).start()
        u_send(U_SECOND, bit1, not2, second).wait_recv()
        u_send(U_CORE_SECOND, bit1, not2, partner).start()

    def u_last():
        u_send(U_RELAY, not1, not2, second).wait_recv()
        u_send(U_CORE_RELAY, not1, not2, partner).start()

    def u_wait():
        u_local().wait()
        u_send(U_FIRST, bit1, bit2, first).wait_send()
        u_send(U_SECOND, bit1, bit2, second).wait_send()
        u_send(U_RELAY, not1, bit2, second).wait_send()
        for kind, b1, b2 in ((U_OWN, bit1, bit2), (U_CORE_FIRST, not1, bit2), (U_CORE_SECOND, bit1, not2), (U_CORE_RELAY, not1, not2)):
            u_send(kind, b1, b2, partner).wait()

    def w_load(k, src, dst):
        return pltpu.make_async_copy(src, dst, wsem.at[k])

    def wp_load(j, src):
        return pltpu.make_async_copy(src, wp.at[j * cols:(j + 1) * cols, :], wsem.at[2 + j])

    def select(g):
        txt = (g < txt_chunks).astype(jnp.int32)
        return txt * (g // per_txt) + (1 - txt) * (batch + (g - txt_chunks) // per_img)

    def start_o(g):
        @pl.when(g < first_open)
        def _():
            o_ready(g).start()

        for b in range(batch):
            @pl.when((g >= first_open) & (img_pos(g)[0] == b))
            def _():
                o_local(g, b).start()
                o_core(g, b).start()

    def send_o(g):
        o_local(g, 0).wait()
        o_core(g, 0).wait()
        o_send(O_FIRST, g, me, first).start()
        o_send(O_SECOND, g, me, second).start()

    def relay_o(g):
        o_send(O_FIRST, g, first, first).wait_recv()
        o_send(O_RELAY, g, first, second).start()

    def start_x(g):
        x_load(g).start()

    wide = 2 * tile

    def project(g):
        @pl.when(g < first_open)
        def _():
            o_ready(g).wait()

        @pl.when(g >= first_open)
        def _():
            o_send(O_FIRST, g, me, first).wait_send()
            o_send(O_SECOND, g, me, second).wait_send()
            o_send(O_RELAY, g, first, second).wait_send()
            o_send(O_SECOND, g, second, second).wait_recv()
            o_send(O_RELAY, g, second, second).wait_recv()

        x_load(g).wait()

        @pl.when(g == txt_chunks)
        def _():
            for j in range(wp_hbm.shape[0]):
                wp_load(j, wp_hbm.at[j]).wait()

        sel = select(g)
        slot = g % SLOTS

        def columns(n):
            at = rows_at(n * wide, wide)
            acc = jnp.dot(obuf[g % O_SLOTS], wp[:, at], preferred_element_type=F32)
            branch = acc + row_of(vec_ref, sel, PROJ_B, at)
            xbuf[two(g), :, at] = (xbuf[two(g), :, at].astype(F32) + row_of(vec_ref, sel, GATE1, at) * branch).astype(BF16)

        loop(dim // wide, columns)

        def norm(n):
            at = rows_at(n * STRIP, STRIP)
            u2[two(g), at, :] = modulated(xbuf[two(g), at, :].astype(F32), vec_ref, sel, SHIFT2, SCALE2)

        loop(half // STRIP, norm)
        u_core(g).start()
        x1keep[slot] = xbuf[two(g), rows_at(bit1 * quarter + bit2 * eighth, eighth), :]

    def mlp_hidden(g):
        @pl.when(g < last_txt)
        def _():
            for who in (core, far):
                txt_load(g, who).wait()

        @pl.when(g == last_txt)
        def _():
            u_wait()

        @pl.when(g < txt_chunks)
        def _():
            x1_load(g).wait()

        @pl.when(g >= txt_chunks)
        def _():
            u_core(g).wait()

        @pl.when(g == 0)
        def _():
            w_load(0, w1t_hbm, w1).wait()
            w_load(1, w2t_hbm, w2).wait()
            for j in range(wp_hbm.shape[0]):
                @pl.when(j != me)
                def _():
                    wp_load(j, wp_hbm.at[j]).start()

                @pl.when(j == me)
                def _():
                    wp_load(j, pw_hbm).start()

        @pl.when(g == txt_chunks)
        def _():
            w_load(0, w1i_hbm, w1).wait()
            w_load(1, w2i_hbm, w2).wait()

        path = (g >= txt_chunks).astype(jnp.int32)

        def hidden(n):
            at = rows_at(n * tile, tile)
            acc = jnp.dot(u2[two(g)], w1[:, at], preferred_element_type=F32)
            pre = acc + row_of(fb_ref, path, FC1_B, at)
            hid[:, at] = jax.nn.gelu(pre, approximate=True).astype(BF16)

        loop(ff // tile, hidden)

    def mlp_out(g):
        def columns(n):
            at = rows_at(n * tile, tile)
            acc = jnp.dot(hid[...], w2[:, at], preferred_element_type=F32)
            own[:, at] = acc[:half]
            psend[:, at] = acc[half:].astype(BF16)

        loop(dim // tile, columns)
        part_core(g).start()

        @pl.when(g == txt_chunks - 1)
        def _():
            w_load(0, w1i_hbm, w1).start()
            w_load(1, w2i_hbm, w2).start()

    def mlp_sum(g):
        part_core(g).wait()

        def add(n):
            at = rows_at(n * STRIP, STRIP)
            chip_sum[at, :] = (own[at, :] + precv[two(g), at, :].astype(F32)).astype(BF16)

        loop(half // STRIP, add)
        rs_first(g).start()

    def add_first(g):
        rs_first(g).wait()
        rs2_out[two(g)] = (chip_sum[rows_at(bit1 * quarter + not2 * eighth, eighth), :].astype(F32) + rs1[two(g), rows_at(not2 * eighth, eighth), :].astype(F32)).astype(BF16)
        rs_second(g).start()
        keep2[two(g)] = chip_sum[rows_at(bit1 * quarter + bit2 * eighth, eighth), :].astype(F32) + rs1[two(g), rows_at(bit2 * eighth, eighth), :].astype(F32)

    def finish(g):
        rs_second(g).wait()
        sel = select(g)
        branch = keep2[two(g)] + rs2_in[g % SLOTS].astype(F32) + row_of(vec_ref, sel, FC2_B)
        outb[g % SLOTS] = (x1keep[g % SLOTS].astype(F32) + row_of(vec_ref, sel, GATE2) * branch).astype(BF16)
        out_send(OUT_FIRST, g, bit1, bit2, first).start()
        out_send(OUT_SECOND, g, bit1, bit2, second).start()
        out_send(CORE_OWN, g, bit1, bit2, partner).start()
        out_local(g).start()

    def relay_out(g):
        out_send(OUT_FIRST, g, not1, bit2, first).wait_recv()
        out_send(OUT_RELAY, g, not1, bit2, second).start()
        out_send(CORE_FIRST, g, not1, bit2, partner).start()

    def second_out(g):
        out_send(OUT_SECOND, g, bit1, not2, second).wait_recv()
        out_send(CORE_SECOND, g, bit1, not2, partner).start()

    def relay_core(g):
        out_send(OUT_RELAY, g, not1, not2, second).wait_recv()
        out_send(CORE_RELAY, g, not1, not2, partner).start()

    def drain(g):
        out_local(g).wait()
        out_send(OUT_FIRST, g, bit1, bit2, first).wait_send()
        out_send(OUT_SECOND, g, bit1, bit2, second).wait_send()
        out_send(OUT_RELAY, g, not1, bit2, second).wait_send()
        out_send(CORE_OWN, g, bit1, bit2, partner).wait()
        out_send(CORE_FIRST, g, not1, bit2, partner).wait()
        out_send(CORE_SECOND, g, bit1, not2, partner).wait()
        out_send(CORE_RELAY, g, not1, not2, partner).wait()

    u_start()
    opened = first_open + OPENED
    for g in range(txt_chunks, opened):
        start_o(jnp.int32(g))
    w_load(0, w1t_hbm, w1).start()
    w_load(1, w2t_hbm, w2).start()
    for g in range(txt_chunks):
        x1_load(g).start()
        if g < last_txt:
            for who in (core, far):
                txt_load(g, who).start()
    kv_load().start()
    q_load(0).start()
    for g in range(first_open, opened):
        send_o(jnp.int32(g))

    stages = ((finish, -3, 0), (start_o, 8, opened), (relay_out, -4, 0), (mlp_hidden, 0, 0), (send_o, 8, opened), (relay_core, -6, 0), (mlp_out, 0, 0), (relay_o, 7, first_open),
              (start_x, 2, txt_chunks), (project, 1, txt_chunks), (second_out, -4, 0), (add_first, -1, 0), (mlp_sum, 0, 0), (drain, -6, 0), (attend, 0, 0))
    most = max(ahead for _, ahead, _ in stages)
    least = min(ahead for _, ahead, _ in stages)

    def step(i):
        @pl.when(i == U_RELAY_STEP)
        def _():
            u_relay()

        for stage, ahead, lowest in stages:
            if stage is attend:
                lax.fori_loop(attended(i), attended(i + 1), attend, 0)
                continue
            g = i + txt_chunks - most + ahead

            @pl.when((g >= lowest) & (g < total))
            def _():
                stage(g)

        @pl.when(i == U_RELAY_STEP + 1)
        def _():
            u_last()

    loop(total - txt_chunks + most - least, step)


ATTEND = (2, 2, 2, 0, 0, 0, 0, 1, 2, 2, 3, 3, 3, 3, 1)
U_RELAY_STEP = 2


def block_call(img_o, og, kv, x, u_txt, x1_txt, tu, wp, pw, w1t, w2t, w1i, w2i, vecs, fb, rows):
    batch, img_len, dim = x.shape
    txt_len = u_txt.shape[1]
    ff = w1t.shape[1]
    txt_chunks = batch * (txt_len // rows)
    per_img = img_len // rows
    img_chunks = batch * per_img
    assert txt_chunks == 2
    half, quarter, eighth = rows // 2, rows // 4, rows // 8
    cfg = (batch, txt_chunks, img_chunks, per_img, rows, 512)
    total = txt_chunks + img_chunks
    anywhere = pl.BlockSpec(memory_space=pl.ANY)
    return pl.pallas_call(
        functools.partial(block_kernel, cfg),
        in_specs=[anywhere] * 13 + [pl.BlockSpec(memory_space=pltpu.VMEM)] * 2,
        out_specs=[anywhere, anywhere],
        out_shape=[jax.ShapeDtypeStruct((total * rows, dim), BF16), jax.ShapeDtypeStruct(img_o.shape, BF16)],
        scratch_shapes=[
            pltpu.VMEM((kv.shape[0] // 3 * 2,) + kv.shape[1:], BF16),
            pltpu.VMEM((2, rows, HEAD), BF16),
            pltpu.VMEM((2, rows, HEAD), BF16),
            pltpu.VMEM((dim, dim), BF16),
            pltpu.VMEM((dim, ff), BF16),
            pltpu.VMEM((ff, dim), BF16),
            pltpu.VMEM((O_SLOTS, half, dim), BF16),
            pltpu.VMEM((2, half, dim), BF16),
            pltpu.VMEM((SLOTS, eighth, dim), BF16),
            pltpu.VMEM((2, rows, dim), BF16),
            pltpu.VMEM((rows, ff), BF16),
            pltpu.VMEM((half, dim), BF16),
            pltpu.VMEM((2, half, dim), BF16),
            pltpu.VMEM((half, dim), F32),
            pltpu.VMEM((half, dim), BF16),
            pltpu.VMEM((2, quarter, dim), BF16),
            pltpu.VMEM((2, eighth, dim), F32),
            pltpu.VMEM((2, eighth, dim), BF16),
            pltpu.VMEM((SLOTS, eighth, dim), BF16),
            pltpu.VMEM((SLOTS, eighth, dim), BF16),
            pltpu.SemaphoreType.DMA((5,)),
            pltpu.SemaphoreType.DMA((10,)),
            pltpu.SemaphoreType.DMA((3, SEMS)),
            pltpu.SemaphoreType.DMA((3, 2)),
            *[pltpu.SemaphoreType.DMA((22, SEMS))] * 2,
        ],
        compiler_params=pltpu.CompilerParams(collective_id=0, has_side_effects=True, vmem_limit_bytes=VMEM_BYTES),
        name="block",
    )(img_o, og, kv, x, u_txt, x1_txt, tu, wp, pw, w1t, w2t, w1i, w2i, vecs, fb)


def copy_kernel(pieces, flat_hbm, *rest):
    outs, (buf, isem, osem) = rest[:-3], rest[-3:]
    rows = buf.shape[1]
    loads = []
    for n, (which, b, r) in enumerate(pieces):
        load = pltpu.make_async_copy(flat_hbm.at[n * rows:(n + 1) * rows, :], buf.at[n], isem.at[n])
        load.start()
        loads.append(load)
    stores = []
    for n, (which, b, r) in enumerate(pieces):
        loads[n].wait()
        store = pltpu.make_async_copy(buf.at[n], outs[which].at[b, r:r + rows, :], osem.at[n])
        store.start()
        stores.append(store)
    for store in stores:
        store.wait()


def copy_call(flat, shapes, rows):
    pieces = [(which, b, r) for which, shape in enumerate(shapes) for b in range(shape[0]) for r in range(0, shape[1], rows)]
    anywhere = pl.BlockSpec(memory_space=pl.ANY)
    dim = flat.shape[1]
    return pl.pallas_call(
        functools.partial(copy_kernel, pieces),
        in_specs=[anywhere],
        out_specs=[anywhere] * len(shapes),
        out_shape=[jax.ShapeDtypeStruct(shape, flat.dtype) for shape in shapes],
        scratch_shapes=[
            pltpu.VMEM((len(pieces), rows, dim), flat.dtype),
            pltpu.SemaphoreType.DMA((len(pieces),)),
            pltpu.SemaphoreType.DMA((len(pieces),)),
        ],
        compiler_params=pltpu.CompilerParams(vmem_limit_bytes=VMEM_BYTES),
        name="copy_out",
    )(flat)


def local_block(img, txt, vec, ids, img_w, txt_w):
    n_dev = 8
    batch, txt_len = txt.shape[:2]
    rows = txt_len

    def by_kind(weight):
        return jnp.transpose(weight, (1, 0, 2))

    def small_of(w):
        return w[1], w[3], w[4], w[5], w[7], w[9], w[11]

    table = jnp.asarray(rope_table())
    ids_t = jnp.transpose(ids, (2, 0, 1))
    o, kv, proj_w, txt_u, og, txt_x1, txt_tu, vecs, small = front_call(txt, img, by_kind(txt_w[2]), by_kind(img_w[2]), by_kind(txt_w[0]), by_kind(img_w[0]), img_w[6], txt_w[6], vec, small_of(txt_w), small_of(img_w), ids_t, table, n_dev, rows)
    flat, _ = block_call(o, og, kv, img, txt_u, txt_x1, txt_tu, proj_w, img_w[6], txt_w[8], txt_w[10], img_w[8], img_w[10], vecs, small, rows)
    txt_out, img_out = copy_call(flat, (txt.shape, img.shape), rows)
    return img_out, txt_out


def solution(mesh):
    act_spec = P('dp', WHOLE, WHOLE)
    mapped = jax.shard_map(local_block, mesh=mesh, in_specs=(act_spec, act_spec, P('dp', WHOLE), act_spec, PATH_SPECS, PATH_SPECS), out_specs=(act_spec, act_spec), check_vma=False)

    def forward(img, txt, vec, ids, *weights):
        return mapped(img, txt, vec, ids, weights[:12], weights[12:])

    return forward
```

```python
import functools

import jax
import jax.numpy as jnp
import numpy as np
from jax import lax
from jax.experimental import pallas as pl
from jax.experimental.pallas import tpu as pltpu
from jax.sharding import PartitionSpec as P

HEAD = 128
NORM_EPS = 1e-6
ROPE_THETA = 10000.0
AXES_DIM = (16, 56, 56)
N_IDS = 64
WHOLE = None
PATH_SPECS = (P(WHOLE, WHOLE, 'tp'), P(WHOLE, 'tp'), P(WHOLE, WHOLE, 'tp'), P(WHOLE, 'tp'), P(WHOLE), P(WHOLE), P('tp', WHOLE), P(WHOLE), P(WHOLE, 'tp'), P('tp'), P('tp', WHOLE), P(WHOLE))
F32 = jnp.float32
BF16 = jnp.bfloat16


def rope_table():
    cos = np.zeros((3 * N_IDS, HEAD), np.float32)
    sin = np.zeros((3 * N_IDS, HEAD), np.float32)
    lane = 0
    for axis, dim in enumerate(AXES_DIM):
        inv_freq = np.float32(ROPE_THETA) ** (-np.arange(0, dim, 2, dtype=np.float32) / np.float32(dim))
        angles = np.arange(N_IDS, dtype=np.float32)[:, None] * inv_freq.astype(np.float32)
        rows = slice(axis * N_IDS, (axis + 1) * N_IDS)
        c = np.cos(angles.astype(np.float64)).astype(np.float32)
        s = np.sin(angles.astype(np.float64)).astype(np.float32)
        cos[rows, lane:lane + dim:2] = c
        cos[rows, lane + 1:lane + dim:2] = c
        sin[rows, lane:lane + dim:2] = -s
        sin[rows, lane + 1:lane + dim:2] = s
        lane += dim
    parts = []
    for table in (cos, sin):
        rest = table
        for _ in range(3):
            part = rest.astype(jnp.bfloat16)
            parts.append(np.asarray(part))
            rest = rest - np.asarray(part).astype(np.float32)
    return np.concatenate(parts, axis=1)


MESH = pl.DeviceIdType.MESH


SHIFT1, SCALE1, GATE1, SHIFT2, SCALE2, GATE2, PROJ_B, FC2_B = range(8)
QKV_B, Q_GAIN, K_GAIN, FC1_B = range(4)
VMEM_BYTES = 67043328


def row_of(ref, sel, row, at=slice(None)):
    return ref[sel, pl.ds(row, 1), at]


STRIP = 16
PATHS = range(2)


def loop(count, body):
    lax.fori_loop(0, count, lambda i, carry: (body(i), carry)[-1], 0)


def row_mean(x):
    return jnp.mean(x, axis=-1, keepdims=True)


def normalize(x):
    centered = x - row_mean(x)
    return centered * lax.rsqrt(row_mean(centered * centered) + NORM_EPS)


def softened(s):
    top = jnp.max(s, axis=-1, keepdims=True)
    p = jnp.exp2((s - top) * (HEAD ** -0.5 * LOG2E))
    return p.astype(BF16), jnp.sum(p, axis=-1, keepdims=True)


def weighted(s, v):
    p, total = softened(s)
    return (jnp.dot(p, v, preferred_element_type=F32) * (1.0 / total)).astype(BF16)


def scores_of(q, k):
    return lax.dot_general(q, k, (((1,), (1,)), ((), ())), preferred_element_type=F32)


def modulated(x, vec_ref, sel, shift, scale):
    return ((1.0 + row_of(vec_ref, sel, scale)) * normalize(x) + row_of(vec_ref, sel, shift)).astype(BF16)


LOG2E = 1.4426950408889634
(W_FIRST, W_SECOND, W_RELAY, W_CORE, W_CORE_FIRST, W_CORE_SECOND, W_CORE_RELAY, Z_FIRST, Z_SECOND, Z_RELAY) = range(10)
(G_CORE, G_FIRST, G_SECOND, G_RELAY) = range(4)
(T_CORE, T_FIRST, T_SECOND, T_OUT_FIRST, T_OUT_SECOND, T_OUT_RELAY, T_CORE_OWN, T_CORE_FIRST, T_CORE_SECOND, T_CORE_RELAY) = range(10)
PIECES = 4
SHARED = range(2)
READY = 5
EARLY = 5
FIRST_LATE = 5
HEADS_HERE = 3


def ident(dev):
    return dev if isinstance(dev, dict) else {'tp': dev}


class Place:
    def __init__(self):
        me = lax.axis_index('tp')
        core = me % 2
        xi = (me // 2) % 2
        yi = me // 4
        x_next = me + 2 - 4 * xi
        y_next = me + 4 - 8 * yi
        self.me, self.core = me, core
        self.partner = me + 1 - 2 * core
        self.first = x_next * (1 - core) + y_next * core
        self.second = x_next * core + y_next * (1 - core)
        self.diagonal = x_next + y_next - me
        self.bit1 = xi * (1 - core) + yi * core
        self.bit2 = xi * core + yi * (1 - core)
        self.not1, self.not2, self.far = 1 - self.bit1, 1 - self.bit2, 1 - core

    def enter(self, others):
        barrier = pltpu.get_barrier_semaphore()
        for dev in others:
            pl.semaphore_signal(barrier, inc=1, device_id=ident(dev), device_id_type=MESH)
        pl.semaphore_wait(barrier, len(others))


def rows_at(start, size):
    return pl.ds(pl.multiple_of(start, size), size)


def front_kernel(cfg, txt_hbm, img_hbm, wt_hbm, wi_hbm, mt_hbm, mi_hbm, pw_hbm, tw_hbm, cond_ref, small_t, small_i, ids_ref, tab_ref,
                 o_hbm, kv_hbm, wp_hbm, ut_hbm, og_hbm, x1_ref, tu_ref, vec_ref, small_ref,
                 w, m_w, m_b, m_early, m_late, xs, ua, ub, qkv, s0, s1, s2, probs, o_all, tw, t_send, t_recv, t_own, t_sum, t_rs1, t_rs2_out, t_rs2_in, t_keep, t_x, t_u,
                 wsem, msem, xsem, osem, tsem, gsem, psend, precv, tsend, trecv, gsend, grecv, msend, mrecv):
    batch, txt_len, img_len, rows = cfg
    half, quarter, eighth = rows // 2, rows // 4, rows // 8
    total = txt_len + img_len
    per_img = img_len // rows
    blocks = batch * (per_img + 1)
    n_dev = m_early.shape[0]
    others = range(1, n_dev)
    dim = w.shape[1]
    width = o_all.shape[1]
    heads = width // HEAD
    place = Place()
    me, core, partner, first, second, diagonal, bit1, bit2 = place.me, place.core, place.partner, place.first, place.second, place.diagonal, place.bit1, place.bit2
    not1, not2, far = place.not1, place.not2, place.far
    piece = width // PIECES
    plane = lax.axis_index('dp')
    odd = plane % 2
    beside = {'dp': plane + 1 - 2 * odd}

    def position(n):
        n = jnp.int32(n)
        img = (n >= batch).astype(jnp.int32)
        m = n - batch
        b = (1 - img) * n + img * (m // per_img)
        r = img * (1 + m % per_img)
        return b, r * rows

    def x_copy(n, source):
        b, r0 = position(n)
        ref = txt_hbm.at[b] if source == 0 else img_hbm.at[b, rows_at(r0 - rows, rows), :]
        return pltpu.make_async_copy(ref, xs.at[n % 4], xsem.at[n % 4])

    def x_start(n):
        @pl.when(n < batch)
        def _():
            x_copy(n, 0).start()

        @pl.when((n >= batch) & (n < blocks))
        def _():
            x_copy(n, 1).start()

    def x_wait(n):
        @pl.when(n < blocks)
        def _():
            pltpu.make_async_copy(txt_hbm.at[0], xs.at[n % 4], xsem.at[n % 4]).wait()

    def w_columns(path, j):
        return w.at[path, :, j * width:(j + 1) * width]

    def w_load(path, j):
        return pltpu.make_async_copy((wt_hbm, wi_hbm)[path].at[j], w_columns(path, j), wsem.at[path, j])

    def early_place(path, k):
        return m_w.at[k] if path == 0 else w_columns(path, k)

    def early_load(path, k):
        return pltpu.make_async_copy((mt_hbm, mi_hbm)[path].at[k], early_place(path, k), (msem if path == 0 else wsem.at[path]).at[k])

    def late_load(c, path):
        return pltpu.make_async_copy((mt_hbm, mi_hbm)[path].at[GATE1 + c // 2], m_w.at[c % 2], msem.at[c % 2])

    def late_start(c):
        for path in PATHS:
            @pl.when(c % 2 == path)
            def _():
                late_load(c, path).start()

    def m_copy(part, d, send):
        buf, at = ((m_early, slice(None)), (m_late, slice(FIRST_LATE)), (m_late, slice(FIRST_LATE, 8)))[part]
        ref = buf.at[me if send else (me + n_dev - d) % n_dev, at]
        return pltpu.make_async_remote_copy(src_ref=ref, dst_ref=ref, send_sem=msend.at[part, d], recv_sem=mrecv.at[part, d], device_id={'tp': (me + d) % n_dev}, device_id_type=MESH)

    def m_send(part):
        for d in others:
            m_copy(part, d, True).start()

    def m_wait(part):
        for d in others:
            m_copy(part, d, True).wait_send()
            m_copy(part, d, False).wait_recv()

    for k in (SHIFT1, SCALE1):
        for path in PATHS:
            early_load(path, k).start()
    for n in range(3):
        x_copy(n, 0 if n < batch else 1).start()
    for j in range(3):
        w_load(0, j).start()
    v = cond_ref[...].astype(F32)
    silu = (v * (1.0 / (1.0 + jnp.exp(-v)))).astype(BF16)
    for path, (mod_b, qkv_b, q_gain, k_gain, proj_b, fc1_b, fc2_b) in enumerate((small_t, small_i)):
        m_b[path] = mod_b[...].astype(F32)
        for row, ref in ((PROJ_B, proj_b), (FC2_B, fc2_b)):
            vector = ref[...].astype(F32)[None, :]
            for b in range(batch):
                vec_ref[path * batch + b, row:row + 1, :] = vector
        for row, ref in ((Q_GAIN, q_gain), (K_GAIN, k_gain), (FC1_B, fc1_b)):
            vector = ref[...].astype(F32)[None, :]
            small_ref[path, row:row + 1, :vector.shape[1]] = vector
        for j in range(qkv_b.shape[0]):
            small_ref[path, QKV_B:Q_GAIN, j * width:(j + 1) * width] = qkv_b[j:j + 1, :].astype(F32)
    place.enter([(me + d) % n_dev for d in others] + [beside])

    def early_chunk(k, path):
        early_load(path, k).wait()
        acc = jnp.dot(silu, early_place(path, k)[...], preferred_element_type=F32)
        return (acc + m_b[path, k:k + 1, :]).astype(BF16)

    m_early[me] = jnp.concatenate([early_chunk(k, path) for k in (SHIFT1, SCALE1) for path in PATHS], axis=0)
    m_send(0)
    tw_load = pltpu.make_async_copy(tw_hbm, tw, tsem.at[1])

    def late_chunk(t):
        c = jnp.minimum(t, 7)
        path, k = c % 2, GATE1 + c // 2
        acc = jnp.dot(silu, m_w[c % 2], preferred_element_type=F32) + m_b[path, pl.ds(k, 1), :]
        m_late[me, t] = acc.astype(BF16).astype(F32)

    def late_rows(part):
        m_wait(1 + part)
        for j in range(n_dev):
            for c in range(8)[slice(FIRST_LATE) if part == 0 else slice(FIRST_LATE, 8)]:
                for b in range(batch):
                    vec_ref[c % 2 * batch + b, pl.ds(GATE1 + c // 2, 1), j * width:(j + 1) * width] = m_late[j, c, b:b + 1, :]

    def piece_at(j):
        return rows_at((j + 2 * odd) % PIECES * piece, piece)

    def remote(sends, recvs, kind, j, src, dst, dev):
        return pltpu.make_async_remote_copy(src_ref=src, dst_ref=dst, send_sem=sends.at[kind, j], recv_sem=recvs.at[kind, j], device_id=ident(dev), device_id_type=MESH)

    def p_copy(kind, j, owner, dev):
        dst = wp_hbm.at[owner, piece_at(j), :]
        src = pw_hbm.at[piece_at(j), :] if kind in (W_FIRST, W_SECOND) else dst
        return remote(psend, precv, kind, j, src, dst, dev)

    def w_own():
        return remote(psend, precv, W_CORE, 0, pw_hbm, wp_hbm.at[me], partner)

    def w_core():
        w_own().start()

    def z_copy(kind, owner, j, at):
        ref = wp_hbm.at[owner, piece_at(at), :]
        return remote(psend, precv, kind, j, ref, ref, beside)

    def w_relay(j):
        p_copy(W_FIRST, j, first, first).wait_recv()
        p_copy(W_RELAY, j, first, second).start()
        p_copy(W_CORE_FIRST, j, first, partner).start()
        z_copy(Z_FIRST, first, j, j).start()
        if j == 0:
            p_copy(W_SECOND, 1, me, second).start()

    def w_second(j):
        p_copy(W_SECOND, j, second, second).wait_recv()
        p_copy(W_CORE_SECOND, j, second, partner).start()
        z_copy(Z_SECOND, second, j, j).start()

    def w_last(j):
        p_copy(W_RELAY, j, diagonal, second).wait_recv()
        p_copy(W_CORE_RELAY, j, diagonal, partner).start()
        z_copy(Z_RELAY, diagonal, j, j).start()

    from_beside = ((Z_FIRST, first, W_CORE_FIRST), (Z_SECOND, second, W_CORE_SECOND), (Z_RELAY, diagonal, W_CORE_RELAY))

    def w_beside(n):
        kind, owner, core_kind = from_beside[n % 3]
        j = n // 3
        z_copy(kind, owner, j, j + 2).wait_recv()
        p_copy(core_kind, j + 2, owner, partner).start()

    p_copy(W_FIRST, 0, me, first).start()
    p_copy(W_SECOND, 0, me, second).start()
    p_copy(W_FIRST, 1, me, first).start()

    even = lax.broadcasted_iota(jnp.int32, (rows, HEAD), 1) % 2 == 0
    code = lax.broadcasted_iota(jnp.int32, (N_IDS, rows), 0)

    def select(n):
        n = jnp.int32(n)
        img = (n >= batch).astype(jnp.int32)
        return (1 - img) * n + img * (batch + (n - batch) // per_img)

    def norm(n, u):
        sel = select(n)
        for r in range(0, rows, STRIP):
            u[r // half, r % half:r % half + STRIP, :] = modulated(xs[n % 4, r:r + STRIP, :].astype(F32), vec_ref, sel, SHIFT1, SCALE1)

    def heads_of(n, u):
        b, r0 = position(n)
        path = (jnp.int32(n) >= batch).astype(jnp.int32)
        hot = jnp.concatenate([(ids_ref[axis, pl.ds(b, 1), rows_at(r0, rows)] == code).astype(F32).astype(BF16) for axis in range(3)], axis=0)
        parts = lax.dot_general(hot, tab_ref[...], (((0,), (0,)), ((), ())), preferred_element_type=F32)
        cos_t, sin_t = (sum(parts[:, (3 * i + j) * HEAD:(3 * i + j + 1) * HEAD] for j in range(3)) for i in range(2))
        at = rows_at(b * total + r0, rows)
        for c0 in range(0, 3 * heads, 4):
            c1 = min(c0 + 4, 3 * heads)
            a = jnp.dot(u[...].reshape(rows, dim), w[path, :, c0 * HEAD:c1 * HEAD], preferred_element_type=F32) + row_of(small_ref, path, QKV_B, slice(c0 * HEAD, c1 * HEAD))
            for c in range(c0, c1):
                t = a[:, (c - c0) * HEAD:(c - c0 + 1) * HEAD]
                kind = c // heads
                if kind < 2:
                    t = t * lax.rsqrt(row_mean(t * t) + NORM_EPS) * row_of(small_ref, path, Q_GAIN + kind, slice(HEAD))
                    swapped = jnp.where(even, pltpu.roll(t, HEAD - 1, 1), pltpu.roll(t, 1, 1))
                    t = t * cos_t + swapped * sin_t
                qkv[c, at, :] = t.astype(BF16)

    m_wait(0)
    for j in range(n_dev):
        rows_here = m_early[j].astype(F32)
        for n in range(2 * 2 * batch):
            k, sel = n // (2 * batch), n % (2 * batch)
            vec_ref[sel, k:k + 1, j * width:(j + 1) * width] = rows_here[n:n + 1, :]
    x_wait(0)
    norm(0, ua)
    for j in range(3):
        w_load(0, j).wait()
    for c in range(2):
        late_load(c, c).start()
    for j in range(3):
        w_load(1, j).start()
    tw_load.start()

    def qkv_step(t):
        x_start(2 * t + 3)
        x_start(2 * t + 4)
        x_wait(2 * t + 1)
        x_wait(2 * t + 2)
        @pl.when(t == 1)
        def _():
            for j in range(3):
                w_load(1, j).wait()

        @pl.when(t < 8)
        def _():
            late_load(t, 0).wait()

        late_chunk(t)
        norm(2 * t + 1, ub)
        heads_of(2 * t, ua)
        norm(jnp.minimum(2 * t + 2, blocks - 1), ua)
        heads_of(2 * t + 1, ub)

        @pl.when(t < 6)
        def _():
            late_start(t + 2)

    kv_store = pltpu.make_async_copy(qkv.at[:, total:, :], kv_hbm, tsem.at[0])

    def late_send(part):
        m_send(1 + part)

    def kv_send():
        kv_store.start()

    done_here = batch + per_img

    def rows_of(n, c, size, r0):
        return qkv[c, rows_at(position(n)[0] * total + r0, size), :]

    def scores(n, h, s):
        s[...] = scores_of(rows_of(n, heads + h, total, 0), rows_of(n, h, rows, position(n)[1]))

    def weigh(n, h, s):
        top = jnp.max(s[...], axis=0, keepdims=True)
        keys = total // 9
        sums = 0.0
        for r in range(0, total, keys):
            p = jnp.exp2((s[r:r + keys, :] - top) * (HEAD ** -0.5 * LOG2E))
            sums += jnp.sum(p, axis=0, keepdims=True)
            probs[r:r + keys, :] = p.astype(BF16)
        o = lax.dot_general(rows_of(n, 2 * heads + h, total, 0), probs[...], (((0,), (0,)), ((), ())), preferred_element_type=F32)
        o_all[rows_at(n * rows, rows), h * HEAD:(h + 1) * HEAD] = (o * (1.0 / sums)).T.astype(BF16)

    def t_copy(kind, b, src, dst, dev):
        return remote(tsend, trecv, kind, b, src, dst, dev)

    def t_core(b):
        return t_copy(T_CORE, b, t_send, t_recv.at[b], partner)

    def t_first(b):
        return t_copy(T_FIRST, b, t_sum.at[b, rows_at(not1 * quarter, quarter), :], t_rs1.at[b], first)

    def t_second(b):
        return t_copy(T_SECOND, b, t_rs2_out.at[b], t_rs2_in.at[b], second)

    def own_rows(b1, b2):
        return rows_at(core * half + b1 * quarter + b2 * eighth, eighth)

    def t_out(kind, b, b1, b2, dev):
        ref = ut_hbm.at[b, own_rows(b1, b2), :]
        return t_copy(kind, b, t_u.at[b] if kind in (T_OUT_FIRST, T_OUT_SECOND, T_CORE_OWN) else ref, ref, dev)

    def t_local(b):
        return pltpu.make_async_copy(t_u.at[b], ut_hbm.at[b, own_rows(bit1, bit2), :], tsem.at[2 + b])

    def t_load(b):
        return pltpu.make_async_copy(txt_hbm.at[b, own_rows(bit1, bit2), :], t_x.at[b], tsem.at[2 + batch + b])

    tile = min(512, dim)

    def text_product(b, who, store):
        def columns(n):
            at = rows_at(n * tile, tile)
            store(at, jnp.dot(o_all[rows_at(b * rows + who * half, half), :], tw[:, at], preferred_element_type=F32))

        loop(dim // tile, columns)

    def text_partial(b):
        if b == 0:
            tw_load.wait()
        t_load(b).start()

        def to_send(at, value):
            t_send[:, at] = value.astype(BF16)

        def to_own(at, value):
            t_own[:, at] = value

        text_product(b, far, to_send)
        t_core(b).start()
        text_product(b, core, to_own)

    def text_sum(b):
        t_core(b).wait()

        def add(n):
            at = rows_at(n * STRIP, STRIP)
            t_sum[b, at, :] = (t_own[at, :] + t_recv[b, at, :].astype(F32)).astype(BF16)

        loop(half // STRIP, add)
        t_first(b).start()

    def text_quarter(b):
        t_first(b).wait()
        t_rs2_out[b] = (t_sum[b, rows_at(bit1 * quarter + not2 * eighth, eighth), :].astype(F32) + t_rs1[b, rows_at(not2 * eighth, eighth), :].astype(F32)).astype(BF16)
        t_keep[b] = t_sum[b, rows_at(bit1 * quarter + bit2 * eighth, eighth), :].astype(F32) + t_rs1[b, rows_at(bit2 * eighth, eighth), :].astype(F32)
        t_second(b).start()

    def text_finish(b):
        t_second(b).wait()
        t_load(b).wait()
        branch = t_keep[b] + t_rs2_in[b].astype(F32) + row_of(vec_ref, b, PROJ_B)
        x1 = (t_x[b].astype(F32) + row_of(vec_ref, b, GATE1) * branch).astype(BF16)
        x1_ref[b] = x1
        u = modulated(x1.astype(F32), vec_ref, b, SHIFT2, SCALE2)
        if b == batch - 1:
            tu_ref[...] = u
            return
        t_u[b] = u
        t_out(T_OUT_FIRST, b, bit1, bit2, first).start()
        t_out(T_OUT_SECOND, b, bit1, bit2, second).start()
        t_out(T_CORE_OWN, b, bit1, bit2, partner).start()
        t_local(b).start()

    def text_relay(b):
        t_out(T_OUT_FIRST, b, not1, bit2, first).wait_recv()
        t_out(T_OUT_RELAY, b, not1, bit2, second).start()
        t_out(T_CORE_FIRST, b, not1, bit2, partner).start()
        t_out(T_OUT_SECOND, b, bit1, not2, second).wait_recv()
        t_out(T_CORE_SECOND, b, bit1, not2, partner).start()

    def text_last(b):
        t_out(T_OUT_RELAY, b, not1, not2, second).wait_recv()
        t_out(T_CORE_RELAY, b, not1, not2, partner).start()

    def g_rows(m, who):
        return o_all.at[rows_at((batch + m) * rows + who * half, half), :]

    def g_mine(m):
        return og_hbm.at[m, :, rows_at(me * width, width)]

    def g_local(m):
        return pltpu.make_async_copy(g_rows(m, core), g_mine(m), gsem.at[m])

    def g_core(m):
        return remote(gsend, grecv, G_CORE, m, g_rows(m, far), g_mine(m), partner)

    def g_copy(kind, m, owner, dev):
        ref = og_hbm.at[m, :, rows_at(owner // 2 * (2 * width), 2 * width)]
        return remote(gsend, grecv, kind, m, ref, ref, dev)

    def gather_start(m):
        g_local(m).start()
        g_core(m).start()

    def gather_send(m):
        g_local(m).wait()
        g_core(m).wait()
        g_copy(G_FIRST, m, me, first).start()
        g_copy(G_SECOND, m, me, second).start()

    def gather_relay(m):
        g_copy(G_FIRST, m, first, first).wait_recv()
        g_copy(G_RELAY, m, first, second).start()

    qkv_first, attend_first = (batch + per_img) // 2, 1 + EARLY
    resume = blocks // 2 + attend_first
    steps = blocks // 2 + done_here
    known = dict(locals())

    def run(calls):
        for call in calls:
            name, *args = call.split()
            known[name](*map(int, args))

    def attended(a):
        early = ((a >= 1) & (a <= EARLY)).astype(jnp.int32)
        return a + early - EARLY * (a == attend_first).astype(jnp.int32)

    def attention_step(a, begins):
        n = attended(a)

        @pl.when(begins)
        def _():
            scores(n, 0, s0)

        scores(n, 1, s1)
        weigh(n, 0, s0)
        scores(n, 2, s2)
        weigh(n, 1, s1)
        scores(attended(jnp.minimum(a + 1, done_here - 1)), 0, s0)
        weigh(n, 2, s2)

    def step(i):
        for when, calls in enumerate(HOOKS[:steps]):
            if calls:
                @pl.when(i == when)
                def _():
                    run(calls)

        in_first = i < qkv_first
        in_second = (i >= qkv_first + attend_first) & (i < resume)

        @pl.when(in_first | in_second)
        def _():
            qkv_step(i - attend_first * in_second.astype(jnp.int32))

        @pl.when(jnp.logical_not(in_first | in_second))
        def _():
            late = (i >= resume).astype(jnp.int32)
            attention_step(i - late * (blocks // 2) - (1 - late) * qkv_first, (i == qkv_first) | (i == resume))

    loop(steps, step)

    o_out = pltpu.make_async_copy(o_all.at[batch * rows:, :], o_hbm, osem)
    o_out.start()
    run(HOOKS[steps])
    o_out.wait()
    kv_store.wait()
    t_local(0).wait()
    for kind, b1, b2, dev in ((T_OUT_FIRST, bit1, bit2, first), (T_OUT_SECOND, bit1, bit2, second), (T_OUT_RELAY, not1, bit2, second)):
        t_out(kind, 0, b1, b2, dev).wait_send()
    for kind, b1, b2 in ((T_CORE_OWN, bit1, bit2), (T_CORE_FIRST, not1, bit2), (T_CORE_SECOND, bit1, not2), (T_CORE_RELAY, not1, not2)):
        t_out(kind, 0, b1, b2, partner).wait()
    for j in SHARED:
        for kind, owner, dev in ((W_FIRST, me, first), (W_SECOND, me, second), (W_RELAY, first, second)):
            p_copy(kind, j, owner, dev).wait_send()
    w_own().wait()
    for kind, owner, core_kind in from_beside:
        for j in SHARED:
            z_copy(kind, owner, j, j).wait_send()
        for j in range(PIECES):
            p_copy(core_kind, j, owner, partner).wait()
    for m in range(READY):
        g_copy(G_FIRST, m, me, first).wait_send()
        g_copy(G_SECOND, m, me, second).wait_send()
        g_copy(G_RELAY, m, first, second).wait_send()
        g_copy(G_SECOND, m, second, second).wait_recv()
        g_copy(G_RELAY, m, diagonal, second).wait_recv()


HOOKS = (
    (),
    (),
    ('w_relay 0',),
    (),
    ('w_relay 1',),
    ('late_send 0',),
    ('text_partial 0',),
    ('text_sum 0', 'w_last 1', 'gather_start 0'),
    ('w_last 0', 'gather_start 1'),
    ('w_beside 0', 'gather_send 0'),
    ('gather_start 2', 'gather_start 3', 'gather_send 1'),
    ('w_second 0', 'text_quarter 0', 'gather_start 4'),
    ('gather_send 3', 'gather_send 2'),
    ('gather_relay 1', 'gather_send 4'),
    ('late_send 1', 'w_beside 2', 'gather_relay 0'),
    ('kv_send', 'late_rows 0', 'gather_relay 4', 'w_second 1', 'w_beside 5', 'text_finish 0'),
    ('text_partial 1', 'gather_relay 2', 'text_sum 1'),
    ('w_beside 1', 'text_relay 0', 'w_beside 3', 'gather_relay 3', 'w_core'),
    ('text_quarter 1', 'w_beside 4'),
    ('late_rows 1', 'text_last 0', 'text_finish 1'),
)


def front_call(txt, img, wt, wi, mt, mi, pw, tw, cond, small_t, small_i, ids_t, table, n_dev, rows):
    batch, txt_len, dim = txt.shape
    img_len = img.shape[1]
    total = txt_len + img_len
    width = pw.shape[0]
    heads = width // HEAD
    half, quarter, eighth = rows // 2, rows // 4, rows // 8
    assert heads == HEADS_HERE and batch == 2
    cfg = (batch, txt_len, img_len, rows)
    blocks = batch * (1 + img_len // rows)
    vmem = pl.BlockSpec(memory_space=pltpu.VMEM)
    anywhere = pl.BlockSpec(memory_space=pl.ANY)
    tall = [pltpu.VMEM((half, dim), BF16), pltpu.VMEM((batch, half, dim), BF16), pltpu.VMEM((half, dim), F32), pltpu.VMEM((batch, half, dim), BF16), pltpu.VMEM((batch, quarter, dim), BF16)]
    short = [pltpu.VMEM((batch, eighth, dim), dtype) for dtype in (BF16, BF16, F32, BF16, BF16)]
    return pl.pallas_call(
        functools.partial(front_kernel, cfg),
        in_specs=[anywhere] * 8 + [vmem, (vmem,) * len(small_t), (vmem,) * len(small_i), vmem, vmem],
        out_specs=[anywhere] * 5 + [vmem] * 4,
        out_shape=[
            jax.ShapeDtypeStruct((img_len, width), BF16),
            jax.ShapeDtypeStruct((3 * heads, total, HEAD), BF16),
            jax.ShapeDtypeStruct((n_dev, width, dim), BF16),
            jax.ShapeDtypeStruct((batch, txt_len, dim), BF16),
            jax.ShapeDtypeStruct((READY, half, dim), BF16),
            jax.ShapeDtypeStruct((batch, eighth, dim), BF16),
            jax.ShapeDtypeStruct((eighth, dim), BF16),
            jax.ShapeDtypeStruct((2 * batch, FC2_B + 1, dim), F32),
            jax.ShapeDtypeStruct((2, FC1_B + 1, dim), F32),
        ],
        scratch_shapes=[
            pltpu.VMEM((2, dim, 3 * width), BF16),
            pltpu.VMEM((2, dim, width), BF16),
            pltpu.VMEM((2, PROJ_B, width), F32),
            pltpu.VMEM((n_dev, 4 * batch, width), BF16),
            pltpu.VMEM((n_dev, blocks // 2, batch, width), F32),
            pltpu.VMEM((4, rows, dim), BF16),
            pltpu.VMEM((batch, half, dim), BF16),
            pltpu.VMEM((batch, half, dim), BF16),
            pltpu.VMEM((3 * heads, batch * total, HEAD), BF16),
            pltpu.VMEM((total, rows), F32),
            pltpu.VMEM((total, rows), F32),
            pltpu.VMEM((total, rows), F32),
            pltpu.VMEM((total, rows), BF16),
            pltpu.VMEM((batch * txt_len + img_len, width), BF16),
            pltpu.VMEM((width, dim), BF16),
            *tall,
            *short,
            pltpu.SemaphoreType.DMA((2, 3)),
            pltpu.SemaphoreType.DMA((2,)),
            pltpu.SemaphoreType.DMA((4,)),
            pltpu.SemaphoreType.DMA,
            pltpu.SemaphoreType.DMA((6,)),
            pltpu.SemaphoreType.DMA((READY,)),
            *[pltpu.SemaphoreType.DMA((10, PIECES))] * 2,
            *[pltpu.SemaphoreType.DMA((10, batch))] * 2,
            *[pltpu.SemaphoreType.DMA((4, READY))] * 2,
            *[pltpu.SemaphoreType.DMA((3, n_dev))] * 2,
        ],
        compiler_params=pltpu.CompilerParams(collective_id=2, has_side_effects=True, vmem_limit_bytes=VMEM_BYTES),
        name="front",
    )(txt, img, wt, wi, mt, mi, pw, tw, cond, small_t, small_i, ids_t, table)


(O_CORE, O_FIRST, O_SECOND, O_RELAY, U_CORE, PART_CORE, RS_FIRST, RS_SECOND, OUT_FIRST, OUT_SECOND, OUT_RELAY, CORE_OWN, CORE_FIRST, CORE_SECOND, CORE_RELAY,
 U_FIRST, U_SECOND, U_RELAY, U_OWN, U_CORE_FIRST, U_CORE_SECOND, U_CORE_RELAY) = range(22)
(L_O, L_X, L_OUT) = range(3)
SLOTS = 4
O_SLOTS = 10
OPENED = 1
SEMS = 12


def two(n):
    return n % 2


def block_kernel(cfg, o_hbm, og_hbm, kv_hbm, x_hbm, ut_hbm, x1t_hbm, tu_hbm, wp_hbm, pw_hbm, w1t_hbm, w2t_hbm, w1i_hbm, w2i_hbm, vec_ref, fb_ref, out_hbm, o2_hbm,
                 kv, qs, os, wp, w1, w2, obuf, xbuf, x1keep, u2, hid, psend, precv, own, chip_sum, rs1, keep2, rs2_out, rs2_in, outb,
                 asem, wsem, lsem, tsem, ssem, rsem):
    batch, txt_chunks, img_chunks, per_img, rows, tile = cfg
    half, quarter, eighth = rows // 2, rows // 4, rows // 8
    dim = wp.shape[0]
    ff = w1.shape[1]
    cols = o_hbm.shape[1]
    heads = cols // HEAD
    total = txt_chunks + img_chunks
    per_txt = txt_chunks // batch

    place = Place()
    me, core, partner, first, second, bit1, bit2 = place.me, place.core, place.partner, place.first, place.second, place.bit1, place.bit2
    not1, not2, far = place.not1, place.not2, place.far
    txt_len = ut_hbm.shape[1]
    place.enter([partner, first, second])

    def remote(kind, g, src, dst, dev):
        return pltpu.make_async_remote_copy(src_ref=src, dst_ref=dst, send_sem=ssem.at[kind, g % SEMS], recv_sem=rsem.at[kind, g % SEMS], device_id={'tp': dev}, device_id_type=MESH)

    def img_pos(g):
        k = g - txt_chunks
        return k // per_img, (k % per_img) * rows

    def chip_cols(dev):
        return rows_at((dev // 2) * (2 * cols), 2 * cols)

    def own_rows(b1, b2):
        return core * half + b1 * quarter + b2 * eighth

    def o_from(b):
        return (o_hbm, o2_hbm)[b]

    first_open = txt_chunks + og_hbm.shape[0]

    def o_ready(g):
        return pltpu.make_async_copy(og_hbm.at[g - txt_chunks], obuf.at[g % O_SLOTS], lsem.at[L_O, g % SEMS])

    def o_local(g, b):
        r0 = img_pos(g)[1]
        return pltpu.make_async_copy(o_from(b).at[rows_at(r0 + core * half, half), :], obuf.at[g % O_SLOTS, :, rows_at(me * cols, cols)], lsem.at[L_O, g % SEMS])

    def o_core(g, b):
        r0 = img_pos(g)[1]
        return remote(O_CORE, g, o_from(b).at[rows_at(r0 + far * half, half), :], obuf.at[g % O_SLOTS, :, rows_at(me * cols, cols)], partner)

    units = per_img * heads

    def q_load(u):
        r0 = txt_len + u // heads * rows
        return pltpu.make_async_copy(kv_hbm.at[u % heads, rows_at(r0, rows), :], qs.at[two(u)], asem.at[two(u)])

    def o_store(u):
        return pltpu.make_async_copy(os.at[two(u)], o2_hbm.at[rows_at(u // heads * rows, rows), rows_at(u % heads * HEAD, HEAD)], asem.at[2 + two(u)])

    def kv_load():
        return pltpu.make_async_copy(kv_hbm.at[heads:], kv, asem.at[4])

    def attend(u, carry):
        @pl.when(u == 0)
        def _():
            kv_load().wait()

        q_load(u).wait()

        @pl.when(u + 1 < units)
        def _():
            q_load(u + 1).start()

        @pl.when(u >= 2)
        def _():
            o_store(u - 2).wait()

        k = kv[u % heads]
        v = kv[heads + u % heads]
        for r in range(0, rows, half):
            os[two(u), r:r + half, :] = weighted(scores_of(qs[two(u), r:r + half, :], k), v)
        o_store(u).start()

        @pl.when(u == units - 1)
        def _():
            o_store(u - 1).wait()
            o_store(u).wait()
        return carry

    def attended(i):
        return sum(count * (i > n).astype(jnp.int32) for n, count in enumerate(ATTEND) if count)

    def o_send(kind, g, owner, dev):
        ref = obuf.at[g % O_SLOTS, :, chip_cols(owner)]
        return remote(kind, g, ref, ref, dev)

    def x_load(g):
        b, r0 = img_pos(g)
        return pltpu.make_async_copy(x_hbm.at[b, rows_at(r0 + core * half, half), :], xbuf.at[two(g)], lsem.at[L_X, g % SEMS])

    def u_core(g):
        return remote(U_CORE, g, u2.at[two(g), :half, :], u2.at[two(g), half:, :], partner)

    def part_core(g):
        return remote(PART_CORE, g, psend, precv.at[two(g)], partner)

    def rs_first(g):
        return remote(RS_FIRST, g, chip_sum.at[rows_at(not1 * quarter, quarter), :], rs1.at[two(g)], first)

    def rs_second(g):
        return remote(RS_SECOND, g, rs2_out.at[two(g)], rs2_in.at[g % SLOTS], second)

    def out_ref(g, b1, b2):
        return out_hbm.at[rows_at(g * rows + own_rows(b1, b2), eighth), :]

    def out_send(kind, g, b1, b2, dev):
        ref = out_ref(g, b1, b2)
        mine = kind in (OUT_FIRST, OUT_SECOND, CORE_OWN)
        return remote(kind, g, outb.at[g % SLOTS] if mine else ref, ref, dev)

    def out_local(g):
        return pltpu.make_async_copy(outb.at[g % SLOTS], out_ref(g, bit1, bit2), lsem.at[L_OUT, g % SEMS])

    last_txt = txt_chunks - 1

    def txt_load(g, who):
        mine = who is core
        return pltpu.make_async_copy(ut_hbm.at[g, rows_at(who * half, half), :], u2.at[two(g), slice(half) if mine else slice(half, rows), :], tsem.at[0 if mine else 2, g])

    def x1_load(g):
        return pltpu.make_async_copy(x1t_hbm.at[g], x1keep.at[g], tsem.at[1, g])

    def u_rows(b1, b2, base=0):
        return u2.at[two(last_txt), rows_at(base + b1 * quarter + b2 * eighth, eighth), :]

    def u_local():
        return pltpu.make_async_copy(tu_hbm, u_rows(bit1, bit2), tsem.at[0, last_txt])

    def u_send(kind, b1, b2, dev):
        src = tu_hbm if kind in (U_FIRST, U_SECOND, U_OWN) else u_rows(b1, b2)
        return remote(kind, last_txt, src, u_rows(b1, b2, 0 if dev is not partner else half), dev)

    def u_start():
        u_local().start()
        u_send(U_FIRST, bit1, bit2, first).start()
        u_send(U_SECOND, bit1, bit2, second).start()
        u_send(U_OWN, bit1, bit2, partner).start()

    def u_relay():
        u_send(U_FIRST, not1, bit2, first).wait_recv()
        u_send(U_RELAY, not1, bit2, second).start()
        u_send(U_CORE_FIRST, not1, bit2, partner).start()
        u_send(U_SECOND, bit1, not2, second).wait_recv()
        u_send(U_CORE_SECOND, bit1, not2, partner).start()

    def u_last():
        u_send(U_RELAY, not1, not2, second).wait_recv()
        u_send(U_CORE_RELAY, not1, not2, partner).start()

    def u_wait():
        u_local().wait()
        u_send(U_FIRST, bit1, bit2, first).wait_send()
        u_send(U_SECOND, bit1, bit2, second).wait_send()
        u_send(U_RELAY, not1, bit2, second).wait_send()
        for kind, b1, b2 in ((U_OWN, bit1, bit2), (U_CORE_FIRST, not1, bit2), (U_CORE_SECOND, bit1, not2), (U_CORE_RELAY, not1, not2)):
            u_send(kind, b1, b2, partner).wait()

    def w_load(k, src, dst):
        return pltpu.make_async_copy(src, dst, wsem.at[k])

    def wp_load(j, src):
        return pltpu.make_async_copy(src, wp.at[j * cols:(j + 1) * cols, :], wsem.at[2 + j])

    def select(g):
        txt = (g < txt_chunks).astype(jnp.int32)
        return txt * (g // per_txt) + (1 - txt) * (batch + (g - txt_chunks) // per_img)

    def start_o(g):
        @pl.when(g < first_open)
        def _():
            o_ready(g).start()

        for b in range(batch):
            @pl.when((g >= first_open) & (img_pos(g)[0] == b))
            def _():
                o_local(g, b).start()
                o_core(g, b).start()

    def send_o(g):
        o_local(g, 0).wait()
        o_core(g, 0).wait()
        o_send(O_FIRST, g, me, first).start()
        o_send(O_SECOND, g, me, second).start()

    def relay_o(g):
        o_send(O_FIRST, g, first, first).wait_recv()
        o_send(O_RELAY, g, first, second).start()

    def start_x(g):
        x_load(g).start()

    wide = 2 * tile

    def project(g):
        @pl.when(g < first_open)
        def _():
            o_ready(g).wait()

        @pl.when(g >= first_open)
        def _():
            o_send(O_FIRST, g, me, first).wait_send()
            o_send(O_SECOND, g, me, second).wait_send()
            o_send(O_RELAY, g, first, second).wait_send()
            o_send(O_SECOND, g, second, second).wait_recv()
            o_send(O_RELAY, g, second, second).wait_recv()

        x_load(g).wait()

        @pl.when(g == txt_chunks)
        def _():
            for j in range(wp_hbm.shape[0]):
                wp_load(j, wp_hbm.at[j]).wait()

        sel = select(g)
        slot = g % SLOTS

        def columns(n):
            at = rows_at(n * wide, wide)
            acc = jnp.dot(obuf[g % O_SLOTS], wp[:, at], preferred_element_type=F32)
            branch = acc + row_of(vec_ref, sel, PROJ_B, at)
            xbuf[two(g), :, at] = (xbuf[two(g), :, at].astype(F32) + row_of(vec_ref, sel, GATE1, at) * branch).astype(BF16)

        loop(dim // wide, columns)

        def norm(n):
            at = rows_at(n * STRIP, STRIP)
            u2[two(g), at, :] = modulated(xbuf[two(g), at, :].astype(F32), vec_ref, sel, SHIFT2, SCALE2)

        loop(half // STRIP, norm)
        u_core(g).start()
        x1keep[slot] = xbuf[two(g), rows_at(bit1 * quarter + bit2 * eighth, eighth), :]

    def mlp_hidden(g):
        @pl.when(g < last_txt)
        def _():
            for who in (core, far):
                txt_load(g, who).wait()

        @pl.when(g == last_txt)
        def _():
            u_wait()

        @pl.when(g < txt_chunks)
        def _():
            x1_load(g).wait()

        @pl.when(g >= txt_chunks)
        def _():
            u_core(g).wait()

        @pl.when(g == 0)
        def _():
            w_load(0, w1t_hbm, w1).wait()
            w_load(1, w2t_hbm, w2).wait()
            for j in range(wp_hbm.shape[0]):
                @pl.when(j != me)
                def _():
                    wp_load(j, wp_hbm.at[j]).start()

                @pl.when(j == me)
                def _():
                    wp_load(j, pw_hbm).start()

        @pl.when(g == txt_chunks)
        def _():
            w_load(0, w1i_hbm, w1).wait()
            w_load(1, w2i_hbm, w2).wait()

        path = (g >= txt_chunks).astype(jnp.int32)

        def hidden(n):
            at = rows_at(n * tile, tile)
            acc = jnp.dot(u2[two(g)], w1[:, at], preferred_element_type=F32)
            pre = acc + row_of(fb_ref, path, FC1_B, at)
            hid[:, at] = jax.nn.gelu(pre, approximate=True).astype(BF16)

        loop(ff // tile, hidden)

    def mlp_out(g):
        def columns(n):
            at = rows_at(n * tile, tile)
            acc = jnp.dot(hid[...], w2[:, at], preferred_element_type=F32)
            own[:, at] = acc[:half]
            psend[:, at] = acc[half:].astype(BF16)

        loop(dim // tile, columns)
        part_core(g).start()

        @pl.when(g == txt_chunks - 1)
        def _():
            w_load(0, w1i_hbm, w1).start()
            w_load(1, w2i_hbm, w2).start()

    def mlp_sum(g):
        part_core(g).wait()

        def add(n):
            at = rows_at(n * STRIP, STRIP)
            chip_sum[at, :] = (own[at, :] + precv[two(g), at, :].astype(F32)).astype(BF16)

        loop(half // STRIP, add)
        rs_first(g).start()

    def add_first(g):
        rs_first(g).wait()
        rs2_out[two(g)] = (chip_sum[rows_at(bit1 * quarter + not2 * eighth, eighth), :].astype(F32) + rs1[two(g), rows_at(not2 * eighth, eighth), :].astype(F32)).astype(BF16)
        rs_second(g).start()
        keep2[two(g)] = chip_sum[rows_at(bit1 * quarter + bit2 * eighth, eighth), :].astype(F32) + rs1[two(g), rows_at(bit2 * eighth, eighth), :].astype(F32)

    def finish(g):
        rs_second(g).wait()
        sel = select(g)
        branch = keep2[two(g)] + rs2_in[g % SLOTS].astype(F32) + row_of(vec_ref, sel, FC2_B)
        outb[g % SLOTS] = (x1keep[g % SLOTS].astype(F32) + row_of(vec_ref, sel, GATE2) * branch).astype(BF16)
        out_send(OUT_FIRST, g, bit1, bit2, first).start()
        out_send(OUT_SECOND, g, bit1, bit2, second).start()
        out_send(CORE_OWN, g, bit1, bit2, partner).start()
        out_local(g).start()

    def relay_out(g):
        out_send(OUT_FIRST, g, not1, bit2, first).wait_recv()
        out_send(OUT_RELAY, g, not1, bit2, second).start()
        out_send(CORE_FIRST, g, not1, bit2, partner).start()

    def second_out(g):
        out_send(OUT_SECOND, g, bit1, not2, second).wait_recv()
        out_send(CORE_SECOND, g, bit1, not2, partner).start()

    def relay_core(g):
        out_send(OUT_RELAY, g, not1, not2, second).wait_recv()
        out_send(CORE_RELAY, g, not1, not2, partner).start()

    def drain(g):
        out_local(g).wait()
        out_send(OUT_FIRST, g, bit1, bit2, first).wait_send()
        out_send(OUT_SECOND, g, bit1, bit2, second).wait_send()
        out_send(OUT_RELAY, g, not1, bit2, second).wait_send()
        out_send(CORE_OWN, g, bit1, bit2, partner).wait()
        out_send(CORE_FIRST, g, not1, bit2, partner).wait()
        out_send(CORE_SECOND, g, bit1, not2, partner).wait()
        out_send(CORE_RELAY, g, not1, not2, partner).wait()

    u_start()
    opened = first_open + OPENED
    for g in range(txt_chunks, opened):
        start_o(jnp.int32(g))
    w_load(0, w1t_hbm, w1).start()
    w_load(1, w2t_hbm, w2).start()
    for g in range(txt_chunks):
        x1_load(g).start()
        if g < last_txt:
            for who in (core, far):
                txt_load(g, who).start()
    kv_load().start()
    q_load(0).start()
    for g in range(first_open, opened):
        send_o(jnp.int32(g))

    stages = ((finish, -3, 0), (start_o, 8, opened), (relay_out, -4, 0), (second_out, -5, 0), (mlp_hidden, 0, 0), (relay_o, 7, first_open), (start_x, 2, txt_chunks), (send_o, 8, opened),
              (mlp_out, 0, 0), (project, 1, txt_chunks), (add_first, -1, 0), (drain, -6, 0), (relay_core, -5, 0), (mlp_sum, 0, 0), (attend, 0, 0))
    most = max(ahead for _, ahead, _ in stages)
    least = min(ahead for _, ahead, _ in stages)

    def step(i):
        @pl.when(i == U_RELAY_STEP)
        def _():
            u_relay()

        for stage, ahead, lowest in stages:
            if stage is attend:
                lax.fori_loop(attended(i), attended(i + 1), attend, 0)
                continue
            g = i + txt_chunks - most + ahead

            @pl.when((g >= lowest) & (g < total))
            def _():
                stage(g)

        @pl.when(i == U_RELAY_STEP + 1)
        def _():
            u_last()

    loop(total - txt_chunks + most - least, step)


ATTEND = (2, 2, 2, 0, 0, 0, 0, 1, 2, 2, 3, 3, 3, 3, 1)
U_RELAY_STEP = 2


def block_call(img_o, og, kv, x, u_txt, x1_txt, tu, wp, pw, w1t, w2t, w1i, w2i, vecs, fb, rows):
    batch, img_len, dim = x.shape
    txt_len = u_txt.shape[1]
    ff = w1t.shape[1]
    txt_chunks = batch * (txt_len // rows)
    per_img = img_len // rows
    img_chunks = batch * per_img
    assert txt_chunks == 2
    half, quarter, eighth = rows // 2, rows // 4, rows // 8
    cfg = (batch, txt_chunks, img_chunks, per_img, rows, 512)
    total = txt_chunks + img_chunks
    anywhere = pl.BlockSpec(memory_space=pl.ANY)
    return pl.pallas_call(
        functools.partial(block_kernel, cfg),
        in_specs=[anywhere] * 13 + [pl.BlockSpec(memory_space=pltpu.VMEM)] * 2,
        out_specs=[anywhere, anywhere],
        out_shape=[jax.ShapeDtypeStruct((total * rows, dim), BF16), jax.ShapeDtypeStruct(img_o.shape, BF16)],
        scratch_shapes=[
            pltpu.VMEM((kv.shape[0] // 3 * 2,) + kv.shape[1:], BF16),
            pltpu.VMEM((2, rows, HEAD), BF16),
            pltpu.VMEM((2, rows, HEAD), BF16),
            pltpu.VMEM((dim, dim), BF16),
            pltpu.VMEM((dim, ff), BF16),
            pltpu.VMEM((ff, dim), BF16),
            pltpu.VMEM((O_SLOTS, half, dim), BF16),
            pltpu.VMEM((2, half, dim), BF16),
            pltpu.VMEM((SLOTS, eighth, dim), BF16),
            pltpu.VMEM((2, rows, dim), BF16),
            pltpu.VMEM((rows, ff), BF16),
            pltpu.VMEM((half, dim), BF16),
            pltpu.VMEM((2, half, dim), BF16),
            pltpu.VMEM((half, dim), F32),
            pltpu.VMEM((half, dim), BF16),
            pltpu.VMEM((2, quarter, dim), BF16),
            pltpu.VMEM((2, eighth, dim), F32),
            pltpu.VMEM((2, eighth, dim), BF16),
            pltpu.VMEM((SLOTS, eighth, dim), BF16),
            pltpu.VMEM((SLOTS, eighth, dim), BF16),
            pltpu.SemaphoreType.DMA((5,)),
            pltpu.SemaphoreType.DMA((10,)),
            pltpu.SemaphoreType.DMA((3, SEMS)),
            pltpu.SemaphoreType.DMA((3, 2)),
            *[pltpu.SemaphoreType.DMA((22, SEMS))] * 2,
        ],
        compiler_params=pltpu.CompilerParams(collective_id=0, has_side_effects=True, vmem_limit_bytes=VMEM_BYTES),
        name="block",
    )(img_o, og, kv, x, u_txt, x1_txt, tu, wp, pw, w1t, w2t, w1i, w2i, vecs, fb)


def copy_kernel(pieces, flat_hbm, *rest):
    outs, (buf, isem, osem) = rest[:-3], rest[-3:]
    rows = buf.shape[1]
    loads = []
    for n, (which, b, r) in enumerate(pieces):
        load = pltpu.make_async_copy(flat_hbm.at[n * rows:(n + 1) * rows, :], buf.at[n], isem.at[n])
        load.start()
        loads.append(load)
    stores = []
    for n, (which, b, r) in enumerate(pieces):
        loads[n].wait()
        store = pltpu.make_async_copy(buf.at[n], outs[which].at[b, r:r + rows, :], osem.at[n])
        store.start()
        stores.append(store)
    for store in stores:
        store.wait()


def copy_call(flat, shapes, rows):
    pieces = [(which, b, r) for which, shape in enumerate(shapes) for b in range(shape[0]) for r in range(0, shape[1], rows)]
    anywhere = pl.BlockSpec(memory_space=pl.ANY)
    dim = flat.shape[1]
    return pl.pallas_call(
        functools.partial(copy_kernel, pieces),
        in_specs=[anywhere],
        out_specs=[anywhere] * len(shapes),
        out_shape=[jax.ShapeDtypeStruct(shape, flat.dtype) for shape in shapes],
        scratch_shapes=[
            pltpu.VMEM((len(pieces), rows, dim), flat.dtype),
            pltpu.SemaphoreType.DMA((len(pieces),)),
            pltpu.SemaphoreType.DMA((len(pieces),)),
        ],
        compiler_params=pltpu.CompilerParams(vmem_limit_bytes=VMEM_BYTES),
        name="copy_out",
    )(flat)


def local_block(img, txt, vec, ids, img_w, txt_w):
    n_dev = 8
    batch, txt_len = txt.shape[:2]
    rows = txt_len

    def by_kind(weight):
        return jnp.transpose(weight, (1, 0, 2))

    def small_of(w):
        return w[1], w[3], w[4], w[5], w[7], w[9], w[11]

    table = jnp.asarray(rope_table())
    ids_t = jnp.transpose(ids, (2, 0, 1))
    o, kv, proj_w, txt_u, og, txt_x1, txt_tu, vecs, small = front_call(txt, img, by_kind(txt_w[2]), by_kind(img_w[2]), by_kind(txt_w[0]), by_kind(img_w[0]), img_w[6], txt_w[6], vec, small_of(txt_w), small_of(img_w), ids_t, table, n_dev, rows)
    flat, _ = block_call(o, og, kv, img, txt_u, txt_x1, txt_tu, proj_w, img_w[6], txt_w[8], txt_w[10], img_w[8], img_w[10], vecs, small, rows)
    txt_out, img_out = copy_call(flat, (txt.shape, img.shape), rows)
    return img_out, txt_out


def solution(mesh):
    act_spec = P('dp', WHOLE, WHOLE)
    mapped = jax.shard_map(local_block, mesh=mesh, in_specs=(act_spec, act_spec, P('dp', WHOLE), act_spec, PATH_SPECS, PATH_SPECS), out_specs=(act_spec, act_spec), check_vma=False)

    def forward(img, txt, vec, ids, *weights):
        return mapped(img, txt, vec, ids, weights[:12], weights[12:])

    return forward
```

```python
import functools

import jax
import jax.numpy as jnp
import numpy as np
from jax import lax
from jax.experimental import pallas as pl
from jax.experimental.pallas import tpu as pltpu
from jax.sharding import PartitionSpec as P

HEAD = 128
NORM_EPS = 1e-6
ROPE_THETA = 10000.0
AXES_DIM = (16, 56, 56)
N_IDS = 64
WHOLE = None
PATH_SPECS = (P(WHOLE, WHOLE, 'tp'), P(WHOLE, 'tp'), P(WHOLE, WHOLE, 'tp'), P(WHOLE, 'tp'), P(WHOLE), P(WHOLE), P('tp', WHOLE), P(WHOLE), P(WHOLE, 'tp'), P('tp'), P('tp', WHOLE), P(WHOLE))
F32 = jnp.float32
BF16 = jnp.bfloat16


def rope_table():
    cos = np.zeros((3 * N_IDS, HEAD), np.float32)
    sin = np.zeros((3 * N_IDS, HEAD), np.float32)
    lane = 0
    for axis, dim in enumerate(AXES_DIM):
        inv_freq = np.float32(ROPE_THETA) ** (-np.arange(0, dim, 2, dtype=np.float32) / np.float32(dim))
        angles = np.arange(N_IDS, dtype=np.float32)[:, None] * inv_freq.astype(np.float32)
        rows = slice(axis * N_IDS, (axis + 1) * N_IDS)
        c = np.cos(angles.astype(np.float64)).astype(np.float32)
        s = np.sin(angles.astype(np.float64)).astype(np.float32)
        cos[rows, lane:lane + dim:2] = c
        cos[rows, lane + 1:lane + dim:2] = c
        sin[rows, lane:lane + dim:2] = -s
        sin[rows, lane + 1:lane + dim:2] = s
        lane += dim
    parts = []
    for table in (cos, sin):
        rest = table
        for _ in range(3):
            part = rest.astype(jnp.bfloat16)
            parts.append(np.asarray(part))
            rest = rest - np.asarray(part).astype(np.float32)
    return np.concatenate(parts, axis=1)


MESH = pl.DeviceIdType.MESH


SHIFT1, SCALE1, GATE1, SHIFT2, SCALE2, GATE2, PROJ_B, FC2_B = range(8)
QKV_B, Q_GAIN, K_GAIN, FC1_B = range(4)
VMEM_BYTES = 67043328


def row_of(ref, sel, row, at=slice(None)):
    return ref[sel, pl.ds(row, 1), at]


STRIP = 16
PATHS = range(2)


def loop(count, body):
    lax.fori_loop(0, count, lambda i, carry: (body(i), carry)[-1], 0)


def row_mean(x):
    return jnp.mean(x, axis=-1, keepdims=True)


def normalize(x):
    centered = x - row_mean(x)
    return centered * lax.rsqrt(row_mean(centered * centered) + NORM_EPS)


def softened(s):
    top = jnp.max(s, axis=-1, keepdims=True)
    p = jnp.exp2((s - top) * (HEAD ** -0.5 * LOG2E))
    return p.astype(BF16), jnp.sum(p, axis=-1, keepdims=True)


def weighted(s, v):
    p, total = softened(s)
    return (jnp.dot(p, v, preferred_element_type=F32) * (1.0 / total)).astype(BF16)


def scores_of(q, k):
    return lax.dot_general(q, k, (((1,), (1,)), ((), ())), preferred_element_type=F32)


def modulated(x, vec_ref, sel, shift, scale):
    return ((1.0 + row_of(vec_ref, sel, scale)) * normalize(x) + row_of(vec_ref, sel, shift)).astype(BF16)


LOG2E = 1.4426950408889634
(W_FIRST, W_SECOND, W_RELAY, W_CORE, W_CORE_FIRST, W_CORE_SECOND, W_CORE_RELAY, Z_FIRST, Z_SECOND, Z_RELAY) = range(10)
(G_CORE, G_FIRST, G_SECOND, G_RELAY) = range(4)
(T_CORE, T_FIRST, T_SECOND, T_OUT_FIRST, T_OUT_SECOND, T_OUT_RELAY, T_CORE_OWN, T_CORE_FIRST, T_CORE_SECOND, T_CORE_RELAY) = range(10)
PIECES = 4
SHARED = range(2)
READY = 4
EARLY = 4
FIRST_LATE = 5
HEADS_HERE = 3


def ident(dev):
    return dev if isinstance(dev, dict) else {'tp': dev}


class Place:
    def __init__(self):
        me = lax.axis_index('tp')
        core = me % 2
        xi = (me // 2) % 2
        yi = me // 4
        x_next = me + 2 - 4 * xi
        y_next = me + 4 - 8 * yi
        self.me, self.core = me, core
        self.partner = me + 1 - 2 * core
        self.first = x_next * (1 - core) + y_next * core
        self.second = x_next * core + y_next * (1 - core)
        self.diagonal = x_next + y_next - me
        self.bit1 = xi * (1 - core) + yi * core
        self.bit2 = xi * core + yi * (1 - core)
        self.not1, self.not2, self.far = 1 - self.bit1, 1 - self.bit2, 1 - core

    def enter(self, others):
        barrier = pltpu.get_barrier_semaphore()
        for dev in others:
            pl.semaphore_signal(barrier, inc=1, device_id=ident(dev), device_id_type=MESH)
        pl.semaphore_wait(barrier, len(others))


def rows_at(start, size):
    return pl.ds(pl.multiple_of(start, size), size)


def front_kernel(cfg, txt_hbm, img_hbm, wt_hbm, wi_hbm, mt_hbm, mi_hbm, pw_hbm, tw_hbm, cond_ref, small_t, small_i, ids_ref, tab_ref,
                 o_hbm, kv_hbm, wp_hbm, ut_hbm, og_hbm, x1_ref, tu_ref, vec_ref, small_ref,
                 w, m_w, m_b, m_early, m_late, xs, ua, ub, qkv, s0, s1, s2, probs, o_all, tw, t_send, t_recv, t_own, t_sum, t_rs1, t_rs2_out, t_rs2_in, t_keep, t_x, t_u,
                 wsem, msem, xsem, osem, tsem, gsem, psend, precv, tsend, trecv, gsend, grecv, msend, mrecv):
    batch, txt_len, img_len, rows = cfg
    half, quarter, eighth = rows // 2, rows // 4, rows // 8
    total = txt_len + img_len
    per_img = img_len // rows
    blocks = batch * (per_img + 1)
    n_dev = m_early.shape[0]
    others = range(1, n_dev)
    dim = w.shape[1]
    width = o_all.shape[1]
    heads = width // HEAD
    place = Place()
    me, core, partner, first, second, diagonal, bit1, bit2 = place.me, place.core, place.partner, place.first, place.second, place.diagonal, place.bit1, place.bit2
    not1, not2, far = place.not1, place.not2, place.far
    piece = width // PIECES
    plane = lax.axis_index('dp')
    odd = plane % 2
    beside = {'dp': plane + 1 - 2 * odd}

    def position(n):
        n = jnp.int32(n)
        img = (n >= batch).astype(jnp.int32)
        m = n - batch
        b = (1 - img) * n + img * (m // per_img)
        r = img * (1 + m % per_img)
        return b, r * rows

    def x_copy(n, source):
        b, r0 = position(n)
        ref = txt_hbm.at[b] if source == 0 else img_hbm.at[b, rows_at(r0 - rows, rows), :]
        return pltpu.make_async_copy(ref, xs.at[n % 4], xsem.at[n % 4])

    def x_start(n):
        @pl.when(n < batch)
        def _():
            x_copy(n, 0).start()

        @pl.when((n >= batch) & (n < blocks))
        def _():
            x_copy(n, 1).start()

    def x_wait(n):
        @pl.when(n < blocks)
        def _():
            pltpu.make_async_copy(txt_hbm.at[0], xs.at[n % 4], xsem.at[n % 4]).wait()

    def w_columns(path, j):
        return w.at[path, :, j * width:(j + 1) * width]

    def w_load(path, j):
        return pltpu.make_async_copy((wt_hbm, wi_hbm)[path].at[j], w_columns(path, j), wsem.at[path, j])

    def early_place(path, k):
        return m_w.at[k] if path == 0 else w_columns(path, k)

    def early_load(path, k):
        return pltpu.make_async_copy((mt_hbm, mi_hbm)[path].at[k], early_place(path, k), (msem if path == 0 else wsem.at[path]).at[k])

    def late_load(c, path):
        return pltpu.make_async_copy((mt_hbm, mi_hbm)[path].at[GATE1 + c // 2], m_w.at[c % 2], msem.at[c % 2])

    def late_start(c):
        for path in PATHS:
            @pl.when(c % 2 == path)
            def _():
                late_load(c, path).start()

    def m_copy(part, d, send):
        buf, at = ((m_early, slice(None)), (m_late, slice(FIRST_LATE)), (m_late, slice(FIRST_LATE, 8)))[part]
        ref = buf.at[me if send else (me + n_dev - d) % n_dev, at]
        return pltpu.make_async_remote_copy(src_ref=ref, dst_ref=ref, send_sem=msend.at[part, d], recv_sem=mrecv.at[part, d], device_id={'tp': (me + d) % n_dev}, device_id_type=MESH)

    def m_send(part):
        for d in others:
            m_copy(part, d, True).start()

    def m_wait(part):
        for d in others:
            m_copy(part, d, True).wait_send()
            m_copy(part, d, False).wait_recv()

    for k in (SHIFT1, SCALE1):
        for path in PATHS:
            early_load(path, k).start()
    for n in range(3):
        x_copy(n, 0 if n < batch else 1).start()
    for j in range(3):
        w_load(0, j).start()
    v = cond_ref[...].astype(F32)
    silu = (v * (1.0 / (1.0 + jnp.exp(-v)))).astype(BF16)
    for path, (mod_b, qkv_b, q_gain, k_gain, proj_b, fc1_b, fc2_b) in enumerate((small_t, small_i)):
        m_b[path] = mod_b[...].astype(F32)
        for row, ref in ((PROJ_B, proj_b), (FC2_B, fc2_b)):
            vector = ref[...].astype(F32)[None, :]
            for b in range(batch):
                vec_ref[path * batch + b, row:row + 1, :] = vector
        for row, ref in ((Q_GAIN, q_gain), (K_GAIN, k_gain), (FC1_B, fc1_b)):
            vector = ref[...].astype(F32)[None, :]
            small_ref[path, row:row + 1, :vector.shape[1]] = vector
        for j in range(qkv_b.shape[0]):
            small_ref[path, QKV_B:Q_GAIN, j * width:(j + 1) * width] = qkv_b[j:j + 1, :].astype(F32)
    place.enter([(me + d) % n_dev for d in others] + [beside])

    def early_chunk(k, path):
        early_load(path, k).wait()
        acc = jnp.dot(silu, early_place(path, k)[...], preferred_element_type=F32)
        return (acc + m_b[path, k:k + 1, :]).astype(BF16)

    m_early[me] = jnp.concatenate([early_chunk(k, path) for k in (SHIFT1, SCALE1) for path in PATHS], axis=0)
    m_send(0)
    tw_load = pltpu.make_async_copy(tw_hbm, tw, tsem.at[1])

    def late_chunk(t):
        c = jnp.minimum(t, 7)
        path, k = c % 2, GATE1 + c // 2
        acc = jnp.dot(silu, m_w[c % 2], preferred_element_type=F32) + m_b[path, pl.ds(k, 1), :]
        m_late[me, t] = acc.astype(BF16).astype(F32)

    def late_rows(part):
        m_wait(1 + part)
        for j in range(n_dev):
            for c in range(8)[slice(FIRST_LATE) if part == 0 else slice(FIRST_LATE, 8)]:
                for b in range(batch):
                    vec_ref[c % 2 * batch + b, pl.ds(GATE1 + c // 2, 1), j * width:(j + 1) * width] = m_late[j, c, b:b + 1, :]

    def piece_at(j):
        return rows_at((j + 2 * odd) % PIECES * piece, piece)

    def remote(sends, recvs, kind, j, src, dst, dev):
        return pltpu.make_async_remote_copy(src_ref=src, dst_ref=dst, send_sem=sends.at[kind, j], recv_sem=recvs.at[kind, j], device_id=ident(dev), device_id_type=MESH)

    def p_copy(kind, j, owner, dev):
        dst = wp_hbm.at[owner, piece_at(j), :]
        src = pw_hbm.at[piece_at(j), :] if kind in (W_FIRST, W_SECOND) else dst
        return remote(psend, precv, kind, j, src, dst, dev)

    def w_own():
        return remote(psend, precv, W_CORE, 0, pw_hbm, wp_hbm.at[me], partner)

    def w_core():
        w_own().start()

    def z_copy(kind, owner, j, at):
        ref = wp_hbm.at[owner, piece_at(at), :]
        return remote(psend, precv, kind, j, ref, ref, beside)

    def w_relay(j):
        p_copy(W_FIRST, j, first, first).wait_recv()
        p_copy(W_RELAY, j, first, second).start()
        p_copy(W_CORE_FIRST, j, first, partner).start()
        z_copy(Z_FIRST, first, j, j).start()
        if j == 0:
            p_copy(W_SECOND, 1, me, second).start()

    def w_second(j):
        p_copy(W_SECOND, j, second, second).wait_recv()
        p_copy(W_CORE_SECOND, j, second, partner).start()
        z_copy(Z_SECOND, second, j, j).start()

    def w_last(j):
        p_copy(W_RELAY, j, diagonal, second).wait_recv()
        p_copy(W_CORE_RELAY, j, diagonal, partner).start()
        z_copy(Z_RELAY, diagonal, j, j).start()

    from_beside = ((Z_FIRST, first, W_CORE_FIRST), (Z_SECOND, second, W_CORE_SECOND), (Z_RELAY, diagonal, W_CORE_RELAY))

    def w_beside(n):
        kind, owner, core_kind = from_beside[n % 3]
        j = n // 3
        z_copy(kind, owner, j, j + 2).wait_recv()
        p_copy(core_kind, j + 2, owner, partner).start()

    p_copy(W_FIRST, 0, me, first).start()
    p_copy(W_SECOND, 0, me, second).start()
    p_copy(W_FIRST, 1, me, first).start()

    even = lax.broadcasted_iota(jnp.int32, (rows, HEAD), 1) % 2 == 0
    code = lax.broadcasted_iota(jnp.int32, (N_IDS, rows), 0)

    def select(n):
        n = jnp.int32(n)
        img = (n >= batch).astype(jnp.int32)
        return (1 - img) * n + img * (batch + (n - batch) // per_img)

    def norm(n, u):
        sel = select(n)
        for r in range(0, rows, STRIP):
            u[r // half, r % half:r % half + STRIP, :] = modulated(xs[n % 4, r:r + STRIP, :].astype(F32), vec_ref, sel, SHIFT1, SCALE1)

    def heads_of(n, u):
        b, r0 = position(n)
        path = (jnp.int32(n) >= batch).astype(jnp.int32)
        hot = jnp.concatenate([(ids_ref[axis, pl.ds(b, 1), rows_at(r0, rows)] == code).astype(F32).astype(BF16) for axis in range(3)], axis=0)
        parts = lax.dot_general(hot, tab_ref[...], (((0,), (0,)), ((), ())), preferred_element_type=F32)
        cos_t, sin_t = (sum(parts[:, (3 * i + j) * HEAD:(3 * i + j + 1) * HEAD] for j in range(3)) for i in range(2))
        at = rows_at(b * total + r0, rows)
        for c0 in range(0, 3 * heads, 4):
            c1 = min(c0 + 4, 3 * heads)
            a = jnp.dot(u[...].reshape(rows, dim), w[path, :, c0 * HEAD:c1 * HEAD], preferred_element_type=F32) + row_of(small_ref, path, QKV_B, slice(c0 * HEAD, c1 * HEAD))
            for c in range(c0, c1):
                t = a[:, (c - c0) * HEAD:(c - c0 + 1) * HEAD]
                kind = c // heads
                if kind < 2:
                    t = t * lax.rsqrt(row_mean(t * t) + NORM_EPS) * row_of(small_ref, path, Q_GAIN + kind, slice(HEAD))
                    swapped = jnp.where(even, pltpu.roll(t, HEAD - 1, 1), pltpu.roll(t, 1, 1))
                    t = t * cos_t + swapped * sin_t
                qkv[c, at, :] = t.astype(BF16)

    m_wait(0)
    for j in range(n_dev):
        rows_here = m_early[j].astype(F32)
        for n in range(2 * 2 * batch):
            k, sel = n // (2 * batch), n % (2 * batch)
            vec_ref[sel, k:k + 1, j * width:(j + 1) * width] = rows_here[n:n + 1, :]
    x_wait(0)
    norm(0, ua)
    for j in range(3):
        w_load(0, j).wait()
    for c in range(2):
        late_load(c, c).start()
    for j in range(3):
        w_load(1, j).start()
    tw_load.start()

    def qkv_step(t):
        x_start(2 * t + 3)
        x_start(2 * t + 4)
        x_wait(2 * t + 1)
        x_wait(2 * t + 2)
        @pl.when(t == 1)
        def _():
            for j in range(3):
                w_load(1, j).wait()

        @pl.when(t < 8)
        def _():
            late_load(t, 0).wait()

        late_chunk(t)
        norm(2 * t + 1, ub)
        heads_of(2 * t, ua)
        norm(jnp.minimum(2 * t + 2, blocks - 1), ua)
        heads_of(2 * t + 1, ub)

        @pl.when(t < 6)
        def _():
            late_start(t + 2)

    kv_store = pltpu.make_async_copy(qkv.at[:, total:, :], kv_hbm, tsem.at[0])

    def late_send(part):
        m_send(1 + part)

    def kv_send():
        kv_store.start()

    done_here = batch + per_img

    def rows_of(n, c, size, r0):
        return qkv[c, rows_at(position(n)[0] * total + r0, size), :]

    def scores(n, h, s):
        s[...] = scores_of(rows_of(n, heads + h, total, 0), rows_of(n, h, rows, position(n)[1]))

    def weigh(n, h, s):
        top = jnp.max(s[...], axis=0, keepdims=True)
        keys = total // 9
        sums = 0.0
        for r in range(0, total, keys):
            p = jnp.exp2((s[r:r + keys, :] - top) * (HEAD ** -0.5 * LOG2E))
            sums += jnp.sum(p, axis=0, keepdims=True)
            probs[r:r + keys, :] = p.astype(BF16)
        o = lax.dot_general(rows_of(n, 2 * heads + h, total, 0), probs[...], (((0,), (0,)), ((), ())), preferred_element_type=F32)
        o_all[rows_at(n * rows, rows), h * HEAD:(h + 1) * HEAD] = (o * (1.0 / sums)).T.astype(BF16)

    def t_copy(kind, b, src, dst, dev):
        return remote(tsend, trecv, kind, b, src, dst, dev)

    def t_core(b):
        return t_copy(T_CORE, b, t_send, t_recv.at[b], partner)

    def t_first(b):
        return t_copy(T_FIRST, b, t_sum.at[b, rows_at(not1 * quarter, quarter), :], t_rs1.at[b], first)

    def t_second(b):
        return t_copy(T_SECOND, b, t_rs2_out.at[b], t_rs2_in.at[b], second)

    def own_rows(b1, b2):
        return rows_at(core * half + b1 * quarter + b2 * eighth, eighth)

    def t_parts(b):
        return [t_copy(kind, b, t_sum.at[b, rows_at(b1 * quarter + b2 * eighth, eighth), :], dst, dev) for kind, b1, b2, dst, dev in (
            (T_FIRST, not1, bit2, t_rs1.at[b, :eighth], first), (T_SECOND, bit1, not2, t_rs2_in.at[b], second), (T_OUT_FIRST, not1, not2, t_rs1.at[b, eighth:], diagonal))]

    def t_out(kind, b, b1, b2, dev):
        ref = ut_hbm.at[b, own_rows(b1, b2), :]
        return t_copy(kind, b, t_u.at[b] if kind in (T_OUT_FIRST, T_OUT_SECOND, T_CORE_OWN) else ref, ref, dev)

    def t_local(b):
        return pltpu.make_async_copy(t_u.at[b], ut_hbm.at[b, own_rows(bit1, bit2), :], tsem.at[2 + b])

    def t_load(b):
        return pltpu.make_async_copy(txt_hbm.at[b, own_rows(bit1, bit2), :], t_x.at[b], tsem.at[2 + batch + b])

    tile = min(512, dim)

    def text_product(b, who, store):
        def columns(n):
            at = rows_at(n * tile, tile)
            store(at, jnp.dot(o_all[rows_at(b * rows + who * half, half), :], tw[:, at], preferred_element_type=F32))

        loop(dim // tile, columns)

    def text_partial(b):
        if b == 0:
            tw_load.wait()
        t_load(b).start()

        def to_send(at, value):
            t_send[:, at] = value.astype(BF16)

        def to_own(at, value):
            t_own[:, at] = value

        text_product(b, far, to_send)
        t_core(b).start()
        text_product(b, core, to_own)

    def text_sum(b):
        t_core(b).wait()

        def add(n):
            at = rows_at(n * STRIP, STRIP)
            t_sum[b, at, :] = (t_own[at, :] + t_recv[b, at, :].astype(F32)).astype(BF16)

        loop(half // STRIP, add)
        if b < batch - 1:
            t_first(b).start()
            return
        for part in t_parts(b):
            part.start()

    def text_quarter(b):
        t_first(b).wait()
        t_rs2_out[b] = (t_sum[b, rows_at(bit1 * quarter + not2 * eighth, eighth), :].astype(F32) + t_rs1[b, rows_at(not2 * eighth, eighth), :].astype(F32)).astype(BF16)
        t_keep[b] = t_sum[b, rows_at(bit1 * quarter + bit2 * eighth, eighth), :].astype(F32) + t_rs1[b, rows_at(bit2 * eighth, eighth), :].astype(F32)
        t_second(b).start()

    def text_finish(b):
        for part in [t_second(b)] if b < batch - 1 else t_parts(b):
            part.wait()
        t_load(b).wait()
        if b == batch - 1:
            t_keep[b] = t_sum[b, rows_at(bit1 * quarter + bit2 * eighth, eighth), :].astype(F32) + t_rs1[b, :eighth].astype(F32) + t_rs1[b, eighth:].astype(F32)
        branch = t_keep[b] + t_rs2_in[b].astype(F32) + row_of(vec_ref, b, PROJ_B)
        x1 = (t_x[b].astype(F32) + row_of(vec_ref, b, GATE1) * branch).astype(BF16)
        x1_ref[b] = x1
        u = modulated(x1.astype(F32), vec_ref, b, SHIFT2, SCALE2)
        if b == batch - 1:
            tu_ref[...] = u
            return
        t_u[b] = u
        t_out(T_OUT_FIRST, b, bit1, bit2, first).start()
        t_out(T_OUT_SECOND, b, bit1, bit2, second).start()
        t_out(T_CORE_OWN, b, bit1, bit2, partner).start()
        t_local(b).start()

    def text_relay(b):
        t_out(T_OUT_FIRST, b, not1, bit2, first).wait_recv()
        t_out(T_OUT_RELAY, b, not1, bit2, second).start()
        t_out(T_CORE_FIRST, b, not1, bit2, partner).start()
        t_out(T_OUT_SECOND, b, bit1, not2, second).wait_recv()
        t_out(T_CORE_SECOND, b, bit1, not2, partner).start()

    def text_last(b):
        t_out(T_OUT_RELAY, b, not1, not2, second).wait_recv()
        t_out(T_CORE_RELAY, b, not1, not2, partner).start()

    def g_rows(m, who):
        return o_all.at[rows_at((batch + m) * rows + who * half, half), :]

    def g_mine(m):
        return og_hbm.at[m, :, rows_at(me * width, width)]

    def g_local(m):
        return pltpu.make_async_copy(g_rows(m, core), g_mine(m), gsem.at[m])

    def g_core(m):
        return remote(gsend, grecv, G_CORE, m, g_rows(m, far), g_mine(m), partner)

    def g_copy(kind, m, owner, dev):
        ref = og_hbm.at[m, :, rows_at(owner // 2 * (2 * width), 2 * width)]
        return remote(gsend, grecv, kind, m, ref, ref, dev)

    def gather_start(m):
        g_local(m).start()
        g_core(m).start()

    def gather_send(m):
        g_local(m).wait()
        g_core(m).wait()
        g_copy(G_FIRST, m, me, first).start()
        g_copy(G_SECOND, m, me, second).start()

    def gather_relay(m):
        g_copy(G_FIRST, m, first, first).wait_recv()
        g_copy(G_RELAY, m, first, second).start()

    qkv_first, attend_first = (batch + per_img) // 2, 1 + EARLY
    resume = blocks // 2 + attend_first
    steps = blocks // 2 + done_here
    known = dict(locals())

    def run(calls):
        for call in calls:
            name, *args = call.split()
            known[name](*map(int, args))

    def attended(a):
        early = ((a >= 1) & (a <= EARLY)).astype(jnp.int32)
        return a + early - EARLY * (a == attend_first).astype(jnp.int32)

    def attention_step(a, begins):
        n = attended(a)

        @pl.when(begins)
        def _():
            scores(n, 0, s0)

        scores(n, 1, s1)
        weigh(n, 0, s0)
        scores(n, 2, s2)
        weigh(n, 1, s1)
        scores(attended(jnp.minimum(a + 1, done_here - 1)), 0, s0)
        weigh(n, 2, s2)

    def step(i):
        for start, stop in ((0, resume), (resume, steps)):
            @pl.when((i >= start) & (i < stop))
            def _():
                for when, calls in enumerate(HOOKS[start:stop], start):
                    if calls:
                        pl.when(i == when)(functools.partial(run, calls))

        in_first = i < qkv_first
        in_second = (i >= qkv_first + attend_first) & (i < resume)

        @pl.when(in_first | in_second)
        def _():
            qkv_step(i - attend_first * in_second.astype(jnp.int32))

        @pl.when(jnp.logical_not(in_first | in_second))
        def _():
            late = (i >= resume).astype(jnp.int32)
            attention_step(i - late * (blocks // 2) - (1 - late) * qkv_first, (i == qkv_first) | (i == resume))

    loop(steps, step)

    o_out = pltpu.make_async_copy(o_all.at[batch * rows:, :], o_hbm, osem)
    o_out.start()
    run(HOOKS[steps])
    o_out.wait()
    kv_store.wait()
    t_local(0).wait()
    for kind, b1, b2, dev in ((T_OUT_FIRST, bit1, bit2, first), (T_OUT_SECOND, bit1, bit2, second), (T_OUT_RELAY, not1, bit2, second)):
        t_out(kind, 0, b1, b2, dev).wait_send()
    for kind, b1, b2 in ((T_CORE_OWN, bit1, bit2), (T_CORE_FIRST, not1, bit2), (T_CORE_SECOND, bit1, not2), (T_CORE_RELAY, not1, not2)):
        t_out(kind, 0, b1, b2, partner).wait()
    for j in SHARED:
        for kind, owner, dev in ((W_FIRST, me, first), (W_SECOND, me, second), (W_RELAY, first, second)):
            p_copy(kind, j, owner, dev).wait_send()
    w_own().wait()
    for kind, owner, core_kind in from_beside:
        for j in SHARED:
            z_copy(kind, owner, j, j).wait_send()
        for j in range(PIECES):
            p_copy(core_kind, j, owner, partner).wait()
    for m in range(READY):
        g_copy(G_FIRST, m, me, first).wait_send()
        g_copy(G_SECOND, m, me, second).wait_send()
        g_copy(G_RELAY, m, first, second).wait_send()
        g_copy(G_SECOND, m, second, second).wait_recv()
        g_copy(G_RELAY, m, diagonal, second).wait_recv()


HOOKS = (
    (),
    (),
    ('w_relay 0',),
    ('w_second 0',),
    ('w_relay 1',),
    ('late_send 0',),
    (),
    ('gather_start 0',),
    ('gather_send 0', 'w_beside 0'),
    ('gather_start 2', 'gather_start 1'),
    ('gather_send 2', 'gather_start 3', 'text_partial 0', 'w_beside 1', 'w_last 0', 'gather_send 3'),
    ('text_sum 0', 'gather_send 1', 'w_second 1', 'gather_relay 2'),
    ('w_core',),
    ('late_send 1', 'text_quarter 0', 'gather_relay 0', 'w_beside 3', 'w_last 1'),
    ('kv_send', 'late_rows 0', 'gather_relay 3', 'text_finish 0'),
    ('gather_relay 1',),
    ('text_partial 1', 'text_relay 0', 'text_sum 1', 'w_beside 2'),
    ('text_last 0',),
    ('w_beside 4',),
    ('late_rows 1', 'w_beside 5', 'text_finish 1'),
)


def front_call(txt, img, wt, wi, mt, mi, pw, tw, cond, small_t, small_i, ids_t, table, n_dev, rows):
    batch, txt_len, dim = txt.shape
    img_len = img.shape[1]
    total = txt_len + img_len
    width = pw.shape[0]
    heads = width // HEAD
    half, quarter, eighth = rows // 2, rows // 4, rows // 8
    assert heads == HEADS_HERE and batch == 2
    cfg = (batch, txt_len, img_len, rows)
    blocks = batch * (1 + img_len // rows)
    vmem = pl.BlockSpec(memory_space=pltpu.VMEM)
    anywhere = pl.BlockSpec(memory_space=pl.ANY)
    tall = [pltpu.VMEM((half, dim), BF16), pltpu.VMEM((batch, half, dim), BF16), pltpu.VMEM((half, dim), F32), pltpu.VMEM((batch, half, dim), BF16), pltpu.VMEM((batch, quarter, dim), BF16)]
    short = [pltpu.VMEM((batch, eighth, dim), dtype) for dtype in (BF16, BF16, F32, BF16, BF16)]
    return pl.pallas_call(
        functools.partial(front_kernel, cfg),
        in_specs=[anywhere] * 8 + [vmem, (vmem,) * len(small_t), (vmem,) * len(small_i), vmem, vmem],
        out_specs=[anywhere] * 5 + [vmem] * 4,
        out_shape=[
            jax.ShapeDtypeStruct((img_len, width), BF16),
            jax.ShapeDtypeStruct((3 * heads, total, HEAD), BF16),
            jax.ShapeDtypeStruct((n_dev, width, dim), BF16),
            jax.ShapeDtypeStruct((batch, txt_len, dim), BF16),
            jax.ShapeDtypeStruct((READY, half, dim), BF16),
            jax.ShapeDtypeStruct((batch, eighth, dim), BF16),
            jax.ShapeDtypeStruct((eighth, dim), BF16),
            jax.ShapeDtypeStruct((2 * batch, FC2_B + 1, dim), F32),
            jax.ShapeDtypeStruct((2, FC1_B + 1, dim), F32),
        ],
        scratch_shapes=[
            pltpu.VMEM((2, dim, 3 * width), BF16),
            pltpu.VMEM((2, dim, width), BF16),
            pltpu.VMEM((2, PROJ_B, width), F32),
            pltpu.VMEM((n_dev, 4 * batch, width), BF16),
            pltpu.VMEM((n_dev, blocks // 2, batch, width), F32),
            pltpu.VMEM((4, rows, dim), BF16),
            pltpu.VMEM((batch, half, dim), BF16),
            pltpu.VMEM((batch, half, dim), BF16),
            pltpu.VMEM((3 * heads, batch * total, HEAD), BF16),
            pltpu.VMEM((total, rows), F32),
            pltpu.VMEM((total, rows), F32),
            pltpu.VMEM((total, rows), F32),
            pltpu.VMEM((total, rows), BF16),
            pltpu.VMEM((batch * txt_len + img_len, width), BF16),
            pltpu.VMEM((width, dim), BF16),
            *tall,
            *short,
            pltpu.SemaphoreType.DMA((2, 3)),
            pltpu.SemaphoreType.DMA((2,)),
            pltpu.SemaphoreType.DMA((4,)),
            pltpu.SemaphoreType.DMA,
            pltpu.SemaphoreType.DMA((6,)),
            pltpu.SemaphoreType.DMA((READY,)),
            *[pltpu.SemaphoreType.DMA((10, PIECES))] * 2,
            *[pltpu.SemaphoreType.DMA((10, batch))] * 2,
            *[pltpu.SemaphoreType.DMA((4, READY))] * 2,
            *[pltpu.SemaphoreType.DMA((3, n_dev))] * 2,
        ],
        compiler_params=pltpu.CompilerParams(collective_id=2, has_side_effects=True, vmem_limit_bytes=VMEM_BYTES),
        name="front",
    )(txt, img, wt, wi, mt, mi, pw, tw, cond, small_t, small_i, ids_t, table)


(O_CORE, O_FIRST, O_SECOND, O_RELAY, U_CORE, PART_CORE, RS_FIRST, RS_SECOND, OUT_FIRST, OUT_SECOND, OUT_RELAY, CORE_OWN, CORE_FIRST, CORE_SECOND, CORE_RELAY,
 U_FIRST, U_SECOND, U_RELAY, U_OWN, U_CORE_FIRST, U_CORE_SECOND, U_CORE_RELAY) = range(22)
(L_O, L_X, L_OUT) = range(3)
SLOTS = 4
O_SLOTS = 10
OPENED = 1
SEMS = 12


def two(n):
    return n % 2


def block_kernel(cfg, o_hbm, og_hbm, kv_hbm, x_hbm, ut_hbm, x1t_hbm, tu_hbm, wp_hbm, pw_hbm, w1t_hbm, w2t_hbm, w1i_hbm, w2i_hbm, vec_ref, fb_ref, out_hbm, o2_hbm,
                 kv, qs, os, wp, w1, w2, obuf, xbuf, x1keep, u2, hid, psend, precv, own, chip_sum, rs1, keep2, rs2_out, rs2_in, outb,
                 asem, wsem, lsem, tsem, ssem, rsem):
    batch, txt_chunks, img_chunks, per_img, rows, tile = cfg
    half, quarter, eighth = rows // 2, rows // 4, rows // 8
    dim = wp.shape[0]
    ff = w1.shape[1]
    cols = o_hbm.shape[1]
    heads = cols // HEAD
    total = txt_chunks + img_chunks
    per_txt = txt_chunks // batch

    place = Place()
    me, core, partner, first, second, bit1, bit2 = place.me, place.core, place.partner, place.first, place.second, place.bit1, place.bit2
    not1, not2, far = place.not1, place.not2, place.far
    txt_len = ut_hbm.shape[1]
    place.enter([partner, first, second])

    def remote(kind, g, src, dst, dev):
        return pltpu.make_async_remote_copy(src_ref=src, dst_ref=dst, send_sem=ssem.at[kind, g % SEMS], recv_sem=rsem.at[kind, g % SEMS], device_id={'tp': dev}, device_id_type=MESH)

    def img_pos(g):
        k = g - txt_chunks
        return k // per_img, (k % per_img) * rows

    def chip_cols(dev):
        return rows_at((dev // 2) * (2 * cols), 2 * cols)

    def own_rows(b1, b2):
        return core * half + b1 * quarter + b2 * eighth

    def o_from(b):
        return (o_hbm, o2_hbm)[b]

    first_open = txt_chunks + og_hbm.shape[0]

    def o_ready(g):
        return pltpu.make_async_copy(og_hbm.at[g - txt_chunks], obuf.at[g % O_SLOTS], lsem.at[L_O, g % SEMS])

    def o_local(g, b):
        r0 = img_pos(g)[1]
        return pltpu.make_async_copy(o_from(b).at[rows_at(r0 + core * half, half), :], obuf.at[g % O_SLOTS, :, rows_at(me * cols, cols)], lsem.at[L_O, g % SEMS])

    def o_core(g, b):
        r0 = img_pos(g)[1]
        return remote(O_CORE, g, o_from(b).at[rows_at(r0 + far * half, half), :], obuf.at[g % O_SLOTS, :, rows_at(me * cols, cols)], partner)

    units = per_img * heads

    def q_load(u):
        r0 = txt_len + u // heads * rows
        return pltpu.make_async_copy(kv_hbm.at[u % heads, rows_at(r0, rows), :], qs.at[two(u)], asem.at[two(u)])

    def o_store(u):
        return pltpu.make_async_copy(os.at[two(u)], o2_hbm.at[rows_at(u // heads * rows, rows), rows_at(u % heads * HEAD, HEAD)], asem.at[2 + two(u)])

    def kv_load():
        return pltpu.make_async_copy(kv_hbm.at[heads:], kv, asem.at[4])

    def attend(u, carry):
        @pl.when(u == 0)
        def _():
            kv_load().wait()

        q_load(u).wait()

        @pl.when(u + 1 < units)
        def _():
            q_load(u + 1).start()

        @pl.when(u >= 2)
        def _():
            o_store(u - 2).wait()

        k = kv[u % heads]
        v = kv[heads + u % heads]
        for r in range(0, rows, half):
            os[two(u), r:r + half, :] = weighted(scores_of(qs[two(u), r:r + half, :], k), v)
        o_store(u).start()

        @pl.when(u == units - 1)
        def _():
            o_store(u - 1).wait()
            o_store(u).wait()
        return carry

    def attended(i):
        return sum(count * (i > n).astype(jnp.int32) for n, count in enumerate(ATTEND) if count)

    def o_send(kind, g, owner, dev):
        ref = obuf.at[g % O_SLOTS, :, chip_cols(owner)]
        return remote(kind, g, ref, ref, dev)

    def x_load(g):
        b, r0 = img_pos(g)
        return pltpu.make_async_copy(x_hbm.at[b, rows_at(r0 + core * half, half), :], xbuf.at[two(g)], lsem.at[L_X, g % SEMS])

    def u_core(g):
        return remote(U_CORE, g, u2.at[two(g), :half, :], u2.at[two(g), half:, :], partner)

    def part_core(g):
        return remote(PART_CORE, g, psend, precv.at[two(g)], partner)

    def rs_first(g):
        return remote(RS_FIRST, g, chip_sum.at[rows_at(not1 * quarter, quarter), :], rs1.at[two(g)], first)

    def rs_second(g):
        return remote(RS_SECOND, g, rs2_out.at[two(g)], rs2_in.at[g % SLOTS], second)

    def out_ref(g, b1, b2):
        return out_hbm.at[rows_at(g * rows + own_rows(b1, b2), eighth), :]

    def out_send(kind, g, b1, b2, dev):
        ref = out_ref(g, b1, b2)
        mine = kind in (OUT_FIRST, OUT_SECOND, CORE_OWN)
        return remote(kind, g, outb.at[g % SLOTS] if mine else ref, ref, dev)

    def out_local(g):
        return pltpu.make_async_copy(outb.at[g % SLOTS], out_ref(g, bit1, bit2), lsem.at[L_OUT, g % SEMS])

    last_txt = txt_chunks - 1

    def txt_load(g, who):
        mine = who is core
        return pltpu.make_async_copy(ut_hbm.at[g, rows_at(who * half, half), :], u2.at[two(g), slice(half) if mine else slice(half, rows), :], tsem.at[0 if mine else 2, g])

    def x1_load(g):
        return pltpu.make_async_copy(x1t_hbm.at[g], x1keep.at[g], tsem.at[1, g])

    def u_rows(b1, b2, base=0):
        return u2.at[two(last_txt), rows_at(base + b1 * quarter + b2 * eighth, eighth), :]

    def u_local():
        return pltpu.make_async_copy(tu_hbm, u_rows(bit1, bit2), tsem.at[0, last_txt])

    def u_send(kind, b1, b2, dev):
        src = tu_hbm if kind in (U_FIRST, U_SECOND, U_OWN) else u_rows(b1, b2)
        return remote(kind, last_txt, src, u_rows(b1, b2, 0 if dev is not partner else half), dev)

    def u_start():
        u_local().start()
        u_send(U_FIRST, bit1, bit2, first).start()
        u_send(U_SECOND, bit1, bit2, second).start()
        u_send(U_OWN, bit1, bit2, partner).start()

    def u_relay():
        u_send(U_FIRST, not1, bit2, first).wait_recv()
        u_send(U_RELAY, not1, bit2, second).start()
        u_send(U_CORE_FIRST, not1, bit2, partner).start()
        u_send(U_SECOND, bit1, not2, second).wait_recv()
        u_send(U_CORE_SECOND, bit1, not2, partner).start()

    def u_last():
        u_send(U_RELAY, not1, not2, second).wait_recv()
        u_send(U_CORE_RELAY, not1, not2, partner).start()

    def u_wait():
        u_local().wait()
        u_send(U_FIRST, bit1, bit2, first).wait_send()
        u_send(U_SECOND, bit1, bit2, second).wait_send()
        u_send(U_RELAY, not1, bit2, second).wait_send()
        for kind, b1, b2 in ((U_OWN, bit1, bit2), (U_CORE_FIRST, not1, bit2), (U_CORE_SECOND, bit1, not2), (U_CORE_RELAY, not1, not2)):
            u_send(kind, b1, b2, partner).wait()

    def w_load(k, src, dst):
        return pltpu.make_async_copy(src, dst, wsem.at[k])

    def wp_load(j, src):
        return pltpu.make_async_copy(src, wp.at[j * cols:(j + 1) * cols, :], wsem.at[2 + j])

    def select(g):
        txt = (g < txt_chunks).astype(jnp.int32)
        return txt * (g // per_txt) + (1 - txt) * (batch + (g - txt_chunks) // per_img)

    def start_o(g):
        @pl.when(g < first_open)
        def _():
            o_ready(g).start()

        for b in range(batch):
            @pl.when((g >= first_open) & (img_pos(g)[0] == b))
            def _():
                o_local(g, b).start()
                o_core(g, b).start()

    def send_o(g):
        o_local(g, 0).wait()
        o_core(g, 0).wait()
        o_send(O_FIRST, g, me, first).start()
        o_send(O_SECOND, g, me, second).start()

    def relay_o(g):
        o_send(O_FIRST, g, first, first).wait_recv()
        o_send(O_RELAY, g, first, second).start()

    def start_x(g):
        x_load(g).start()

    wide = 2 * tile

    def project(g):
        @pl.when(g < first_open)
        def _():
            o_ready(g).wait()

        @pl.when(g >= first_open)
        def _():
            o_send(O_FIRST, g, me, first).wait_send()
            o_send(O_SECOND, g, me, second).wait_send()
            o_send(O_RELAY, g, first, second).wait_send()
            o_send(O_SECOND, g, second, second).wait_recv()
            o_send(O_RELAY, g, second, second).wait_recv()

        x_load(g).wait()

        @pl.when(g == txt_chunks)
        def _():
            for j in range(wp_hbm.shape[0]):
                wp_load(j, wp_hbm.at[j]).wait()

        sel = select(g)
        slot = g % SLOTS

        def columns(n):
            at = rows_at(n * wide, wide)
            acc = jnp.dot(obuf[g % O_SLOTS], wp[:, at], preferred_element_type=F32)
            branch = acc + row_of(vec_ref, sel, PROJ_B, at)
            xbuf[two(g), :, at] = (xbuf[two(g), :, at].astype(F32) + row_of(vec_ref, sel, GATE1, at) * branch).astype(BF16)

        loop(dim // wide, columns)

        def norm(n):
            at = rows_at(n * STRIP, STRIP)
            u2[two(g), at, :] = modulated(xbuf[two(g), at, :].astype(F32), vec_ref, sel, SHIFT2, SCALE2)

        loop(half // STRIP, norm)
        u_core(g).start()
        x1keep[slot] = xbuf[two(g), rows_at(bit1 * quarter + bit2 * eighth, eighth), :]

    def mlp_hidden(g):
        @pl.when(g < last_txt)
        def _():
            for who in (core, far):
                txt_load(g, who).wait()

        @pl.when(g == last_txt)
        def _():
            u_wait()

        @pl.when(g < txt_chunks)
        def _():
            x1_load(g).wait()

        @pl.when(g >= txt_chunks)
        def _():
            u_core(g).wait()

        @pl.when(g == 0)
        def _():
            w_load(0, w1t_hbm, w1).wait()
            w_load(1, w2t_hbm, w2).wait()
            for j in range(wp_hbm.shape[0]):
                @pl.when(j != me)
                def _():
                    wp_load(j, wp_hbm.at[j]).start()

                @pl.when(j == me)
                def _():
                    wp_load(j, pw_hbm).start()

        @pl.when(g == txt_chunks)
        def _():
            w_load(0, w1i_hbm, w1).wait()
            w_load(1, w2i_hbm, w2).wait()

        path = (g >= txt_chunks).astype(jnp.int32)

        def hidden(n):
            at = rows_at(n * tile, tile)
            acc = jnp.dot(u2[two(g)], w1[:, at], preferred_element_type=F32)
            pre = acc + row_of(fb_ref, path, FC1_B, at)
            hid[:, at] = jax.nn.gelu(pre, approximate=True).astype(BF16)

        loop(ff // tile, hidden)

    def mlp_out(g):
        def columns(n):
            at = rows_at(n * tile, tile)
            acc = jnp.dot(hid[...], w2[:, at], preferred_element_type=F32)
            own[:, at] = acc[:half]
            psend[:, at] = acc[half:].astype(BF16)

        loop(dim // tile, columns)
        part_core(g).start()

        @pl.when(g == txt_chunks - 1)
        def _():
            w_load(0, w1i_hbm, w1).start()
            w_load(1, w2i_hbm, w2).start()

    def mlp_sum(g):
        part_core(g).wait()

        def add(n):
            at = rows_at(n * STRIP, STRIP)
            chip_sum[at, :] = (own[at, :] + precv[two(g), at, :].astype(F32)).astype(BF16)

        loop(half // STRIP, add)
        rs_first(g).start()

    def add_first(g):
        rs_first(g).wait()
        rs2_out[two(g)] = (chip_sum[rows_at(bit1 * quarter + not2 * eighth, eighth), :].astype(F32) + rs1[two(g), rows_at(not2 * eighth, eighth), :].astype(F32)).astype(BF16)
        rs_second(g).start()
        keep2[two(g)] = chip_sum[rows_at(bit1 * quarter + bit2 * eighth, eighth), :].astype(F32) + rs1[two(g), rows_at(bit2 * eighth, eighth), :].astype(F32)

    def finish(g):
        rs_second(g).wait()
        sel = select(g)
        branch = keep2[two(g)] + rs2_in[g % SLOTS].astype(F32) + row_of(vec_ref, sel, FC2_B)
        outb[g % SLOTS] = (x1keep[g % SLOTS].astype(F32) + row_of(vec_ref, sel, GATE2) * branch).astype(BF16)
        out_send(OUT_FIRST, g, bit1, bit2, first).start()
        out_send(OUT_SECOND, g, bit1, bit2, second).start()
        out_send(CORE_OWN, g, bit1, bit2, partner).start()
        out_local(g).start()

    def relay_out(g):
        out_send(OUT_FIRST, g, not1, bit2, first).wait_recv()
        out_send(OUT_RELAY, g, not1, bit2, second).start()
        out_send(CORE_FIRST, g, not1, bit2, partner).start()

    def second_out(g):
        out_send(OUT_SECOND, g, bit1, not2, second).wait_recv()
        out_send(CORE_SECOND, g, bit1, not2, partner).start()

    def relay_core(g):
        out_send(OUT_RELAY, g, not1, not2, second).wait_recv()
        out_send(CORE_RELAY, g, not1, not2, partner).start()

    def drain(g):
        out_local(g).wait()
        out_send(OUT_FIRST, g, bit1, bit2, first).wait_send()
        out_send(OUT_SECOND, g, bit1, bit2, second).wait_send()
        out_send(OUT_RELAY, g, not1, bit2, second).wait_send()
        out_send(CORE_OWN, g, bit1, bit2, partner).wait()
        out_send(CORE_FIRST, g, not1, bit2, partner).wait()
        out_send(CORE_SECOND, g, bit1, not2, partner).wait()
        out_send(CORE_RELAY, g, not1, not2, partner).wait()

    u_start()
    opened = first_open + OPENED
    for g in range(txt_chunks, opened):
        start_o(jnp.int32(g))
    w_load(0, w1t_hbm, w1).start()
    w_load(1, w2t_hbm, w2).start()
    for g in range(txt_chunks):
        x1_load(g).start()
        if g < last_txt:
            for who in (core, far):
                txt_load(g, who).start()
    kv_load().start()
    q_load(0).start()
    for g in range(first_open, opened):
        send_o(jnp.int32(g))

    stages = ((finish, -3, 0), (start_o, 8, opened), (relay_out, -4, 0), (mlp_hidden, 0, 0), (send_o, 8, opened), (relay_core, -6, 0), (mlp_out, 0, 0), (relay_o, 7, first_open),
              (start_x, 2, txt_chunks), (project, 1, txt_chunks), (second_out, -4, 0), (add_first, -1, 0), (mlp_sum, 0, 0), (drain, -6, 0), (attend, 0, 0))
    most = max(ahead for _, ahead, _ in stages)
    least = min(ahead for _, ahead, _ in stages)

    def step(i):
        @pl.when(i == U_RELAY_STEP)
        def _():
            u_relay()

        for stage, ahead, lowest in stages:
            if stage is attend:
                lax.fori_loop(attended(i), attended(i + 1), attend, 0)
                continue
            g = i + txt_chunks - most + ahead

            @pl.when((g >= lowest) & (g < total))
            def _():
                stage(g)

        @pl.when(i == U_RELAY_STEP + 1)
        def _():
            u_last()

    loop(total - txt_chunks + most - least, step)


ATTEND = (2, 2, 2, 0, 0, 0, 0, 1, 2, 2, 3, 3, 3, 3, 1)
U_RELAY_STEP = 2


def block_call(img_o, og, kv, x, u_txt, x1_txt, tu, wp, pw, w1t, w2t, w1i, w2i, vecs, fb, rows):
    batch, img_len, dim = x.shape
    txt_len = u_txt.shape[1]
    ff = w1t.shape[1]
    txt_chunks = batch * (txt_len // rows)
    per_img = img_len // rows
    img_chunks = batch * per_img
    assert txt_chunks == 2
    half, quarter, eighth = rows // 2, rows // 4, rows // 8
    cfg = (batch, txt_chunks, img_chunks, per_img, rows, 512)
    total = txt_chunks + img_chunks
    anywhere = pl.BlockSpec(memory_space=pl.ANY)
    return pl.pallas_call(
        functools.partial(block_kernel, cfg),
        in_specs=[anywhere] * 13 + [pl.BlockSpec(memory_space=pltpu.VMEM)] * 2,
        out_specs=[anywhere, anywhere],
        out_shape=[jax.ShapeDtypeStruct((total * rows, dim), BF16), jax.ShapeDtypeStruct(img_o.shape, BF16)],
        scratch_shapes=[
            pltpu.VMEM((kv.shape[0] // 3 * 2,) + kv.shape[1:], BF16),
            pltpu.VMEM((2, rows, HEAD), BF16),
            pltpu.VMEM((2, rows, HEAD), BF16),
            pltpu.VMEM((dim, dim), BF16),
            pltpu.VMEM((dim, ff), BF16),
            pltpu.VMEM((ff, dim), BF16),
            pltpu.VMEM((O_SLOTS, half, dim), BF16),
            pltpu.VMEM((2, half, dim), BF16),
            pltpu.VMEM((SLOTS, eighth, dim), BF16),
            pltpu.VMEM((2, rows, dim), BF16),
            pltpu.VMEM((rows, ff), BF16),
            pltpu.VMEM((half, dim), BF16),
            pltpu.VMEM((2, half, dim), BF16),
            pltpu.VMEM((half, dim), F32),
            pltpu.VMEM((half, dim), BF16),
            pltpu.VMEM((2, quarter, dim), BF16),
            pltpu.VMEM((2, eighth, dim), F32),
            pltpu.VMEM((2, eighth, dim), BF16),
            pltpu.VMEM((SLOTS, eighth, dim), BF16),
            pltpu.VMEM((SLOTS, eighth, dim), BF16),
            pltpu.SemaphoreType.DMA((5,)),
            pltpu.SemaphoreType.DMA((10,)),
            pltpu.SemaphoreType.DMA((3, SEMS)),
            pltpu.SemaphoreType.DMA((3, 2)),
            *[pltpu.SemaphoreType.DMA((22, SEMS))] * 2,
        ],
        compiler_params=pltpu.CompilerParams(collective_id=0, has_side_effects=True, vmem_limit_bytes=VMEM_BYTES),
        name="block",
    )(img_o, og, kv, x, u_txt, x1_txt, tu, wp, pw, w1t, w2t, w1i, w2i, vecs, fb)


def copy_kernel(pieces, flat_hbm, *rest):
    outs, (buf, isem, osem) = rest[:-3], rest[-3:]
    rows = buf.shape[1]
    loads = []
    for n, (which, b, r) in enumerate(pieces):
        load = pltpu.make_async_copy(flat_hbm.at[n * rows:(n + 1) * rows, :], buf.at[n], isem.at[n])
        load.start()
        loads.append(load)
    stores = []
    for n, (which, b, r) in enumerate(pieces):
        loads[n].wait()
        store = pltpu.make_async_copy(buf.at[n], outs[which].at[b, r:r + rows, :], osem.at[n])
        store.start()
        stores.append(store)
    for store in stores:
        store.wait()


def copy_call(flat, shapes, rows):
    pieces = [(which, b, r) for which, shape in enumerate(shapes) for b in range(shape[0]) for r in range(0, shape[1], rows)]
    anywhere = pl.BlockSpec(memory_space=pl.ANY)
    dim = flat.shape[1]
    return pl.pallas_call(
        functools.partial(copy_kernel, pieces),
        in_specs=[anywhere],
        out_specs=[anywhere] * len(shapes),
        out_shape=[jax.ShapeDtypeStruct(shape, flat.dtype) for shape in shapes],
        scratch_shapes=[
            pltpu.VMEM((len(pieces), rows, dim), flat.dtype),
            pltpu.SemaphoreType.DMA((len(pieces),)),
            pltpu.SemaphoreType.DMA((len(pieces),)),
        ],
        compiler_params=pltpu.CompilerParams(vmem_limit_bytes=VMEM_BYTES),
        name="copy_out",
    )(flat)


def local_block(img, txt, vec, ids, img_w, txt_w):
    n_dev = 8
    batch, txt_len = txt.shape[:2]
    rows = txt_len

    def by_kind(weight):
        return jnp.transpose(weight, (1, 0, 2))

    def small_of(w):
        return w[1], w[3], w[4], w[5], w[7], w[9], w[11]

    table = jnp.asarray(rope_table())
    ids_t = jnp.transpose(ids, (2, 0, 1))
    o, kv, proj_w, txt_u, og, txt_x1, txt_tu, vecs, small = front_call(txt, img, by_kind(txt_w[2]), by_kind(img_w[2]), by_kind(txt_w[0]), by_kind(img_w[0]), img_w[6], txt_w[6], vec, small_of(txt_w), small_of(img_w), ids_t, table, n_dev, rows)
    flat, _ = block_call(o, og, kv, img, txt_u, txt_x1, txt_tu, proj_w, img_w[6], txt_w[8], txt_w[10], img_w[8], img_w[10], vecs, small, rows)
    txt_out, img_out = copy_call(flat, (txt.shape, img.shape), rows)
    return img_out, txt_out


def solution(mesh):
    act_spec = P('dp', WHOLE, WHOLE)
    mapped = jax.shard_map(local_block, mesh=mesh, in_specs=(act_spec, act_spec, P('dp', WHOLE), act_spec, PATH_SPECS, PATH_SPECS), out_specs=(act_spec, act_spec), check_vma=False)

    def forward(img, txt, vec, ids, *weights):
        return mapped(img, txt, vec, ids, weights[:12], weights[12:])

    return forward
```

```python
import functools

import jax
import jax.numpy as jnp
import numpy as np
from jax import lax
from jax.experimental import pallas as pl
from jax.experimental.pallas import tpu as pltpu
from jax.sharding import PartitionSpec as P

HEAD = 128
NORM_EPS = 1e-6
ROPE_THETA = 10000.0
AXES_DIM = (16, 56, 56)
N_IDS = 64
WHOLE = None
PATH_SPECS = (P(WHOLE, WHOLE, 'tp'), P(WHOLE, 'tp'), P(WHOLE, WHOLE, 'tp'), P(WHOLE, 'tp'), P(WHOLE), P(WHOLE), P('tp', WHOLE), P(WHOLE), P(WHOLE, 'tp'), P('tp'), P('tp', WHOLE), P(WHOLE))
F32 = jnp.float32
BF16 = jnp.bfloat16


def rope_table():
    cos = np.zeros((3 * N_IDS, HEAD), np.float32)
    sin = np.zeros((3 * N_IDS, HEAD), np.float32)
    lane = 0
    for axis, dim in enumerate(AXES_DIM):
        inv_freq = np.float32(ROPE_THETA) ** (-np.arange(0, dim, 2, dtype=np.float32) / np.float32(dim))
        angles = np.arange(N_IDS, dtype=np.float32)[:, None] * inv_freq.astype(np.float32)
        rows = slice(axis * N_IDS, (axis + 1) * N_IDS)
        c = np.cos(angles.astype(np.float64)).astype(np.float32)
        s = np.sin(angles.astype(np.float64)).astype(np.float32)
        cos[rows, lane:lane + dim:2] = c
        cos[rows, lane + 1:lane + dim:2] = c
        sin[rows, lane:lane + dim:2] = -s
        sin[rows, lane + 1:lane + dim:2] = s
        lane += dim
    parts = []
    for table in (cos, sin):
        rest = table
        for _ in range(3):
            part = rest.astype(jnp.bfloat16)
            parts.append(np.asarray(part))
            rest = rest - np.asarray(part).astype(np.float32)
    return np.concatenate(parts, axis=1)


MESH = pl.DeviceIdType.MESH


SHIFT1, SCALE1, GATE1, SHIFT2, SCALE2, GATE2, PROJ_B, FC2_B = range(8)
QKV_B, Q_GAIN, K_GAIN, FC1_B = range(4)
VMEM_BYTES = 67043328


def row_of(ref, sel, row, at=slice(None)):
    return ref[sel, pl.ds(row, 1), at]


STRIP = 16
PATHS = range(2)


def loop(count, body):
    lax.fori_loop(0, count, lambda i, carry: (body(i), carry)[-1], 0)


def row_mean(x):
    return jnp.mean(x, axis=-1, keepdims=True)


def normalize(x):
    centered = x - row_mean(x)
    return centered * lax.rsqrt(row_mean(centered * centered) + NORM_EPS)


def softened(s):
    top = jnp.max(s, axis=-1, keepdims=True)
    p = jnp.exp2((s - top) * (HEAD ** -0.5 * LOG2E))
    return p.astype(BF16), jnp.sum(p, axis=-1, keepdims=True)


def weighted(s, v):
    p, total = softened(s)
    return (jnp.dot(p, v, preferred_element_type=F32) * (1.0 / total)).astype(BF16)


def scores_of(q, k):
    return lax.dot_general(q, k, (((1,), (1,)), ((), ())), preferred_element_type=F32)


def modulated(x, vec_ref, sel, shift, scale):
    return ((1.0 + row_of(vec_ref, sel, scale)) * normalize(x) + row_of(vec_ref, sel, shift)).astype(BF16)


LOG2E = 1.4426950408889634
(W_FIRST, W_SECOND, W_RELAY, W_CORE, W_CORE_FIRST, W_CORE_SECOND, W_CORE_RELAY, Z_FIRST, Z_SECOND, Z_RELAY) = range(10)
(G_CORE, G_FIRST, G_SECOND, G_RELAY) = range(4)
(T_CORE, T_FIRST, T_SECOND, T_OUT_FIRST, T_OUT_SECOND, T_OUT_RELAY, T_CORE_OWN, T_CORE_FIRST, T_CORE_SECOND, T_CORE_RELAY) = range(10)
PIECES = 4
SHARED = range(2)
READY = 4
EARLY = 4
FIRST_LATE = 5
HEADS_HERE = 3


def ident(dev):
    return dev if isinstance(dev, dict) else {'tp': dev}


class Place:
    def __init__(self):
        me = lax.axis_index('tp')
        core = me % 2
        xi = (me // 2) % 2
        yi = me // 4
        x_next = me + 2 - 4 * xi
        y_next = me + 4 - 8 * yi
        self.me, self.core = me, core
        self.partner = me + 1 - 2 * core
        self.first = x_next * (1 - core) + y_next * core
        self.second = x_next * core + y_next * (1 - core)
        self.diagonal = x_next + y_next - me
        self.bit1 = xi * (1 - core) + yi * core
        self.bit2 = xi * core + yi * (1 - core)
        self.not1, self.not2, self.far = 1 - self.bit1, 1 - self.bit2, 1 - core

    def enter(self, others):
        barrier = pltpu.get_barrier_semaphore()
        for dev in others:
            pl.semaphore_signal(barrier, inc=1, device_id=ident(dev), device_id_type=MESH)
        pl.semaphore_wait(barrier, len(others))


def rows_at(start, size):
    return pl.ds(pl.multiple_of(start, size), size)


def front_kernel(cfg, txt_hbm, img_hbm, wt_hbm, wi_hbm, mt_hbm, mi_hbm, pw_hbm, tw_hbm, cond_ref, small_t, small_i, ids_ref, tab_ref,
                 o_hbm, kv_hbm, wp_hbm, ut_hbm, og_hbm, x1_ref, tu_ref, vec_ref, small_ref,
                 w, m_w, m_b, m_early, m_late, xs, ua, ub, qkv, s0, s1, s2, probs, o_all, tw, t_send, t_recv, t_own, t_sum, t_rs1, t_rs2_out, t_rs2_in, t_keep, t_x, t_u,
                 wsem, msem, xsem, osem, tsem, gsem, psend, precv, tsend, trecv, gsend, grecv, msend, mrecv):
    batch, txt_len, img_len, rows = cfg
    half, quarter, eighth = rows // 2, rows // 4, rows // 8
    total = txt_len + img_len
    per_img = img_len // rows
    blocks = batch * (per_img + 1)
    n_dev = m_early.shape[0]
    others = range(1, n_dev)
    dim = w.shape[1]
    width = o_all.shape[1]
    heads = width // HEAD
    place = Place()
    me, core, partner, first, second, diagonal, bit1, bit2 = place.me, place.core, place.partner, place.first, place.second, place.diagonal, place.bit1, place.bit2
    not1, not2, far = place.not1, place.not2, place.far
    piece = width // PIECES
    plane = lax.axis_index('dp')
    odd = plane % 2
    beside = {'dp': plane + 1 - 2 * odd}

    def position(n):
        n = jnp.int32(n)
        img = (n >= batch).astype(jnp.int32)
        m = n - batch
        b = (1 - img) * n + img * (m // per_img)
        r = img * (1 + m % per_img)
        return b, r * rows

    def x_copy(n, source):
        b, r0 = position(n)
        ref = txt_hbm.at[b] if source == 0 else img_hbm.at[b, rows_at(r0 - rows, rows), :]
        return pltpu.make_async_copy(ref, xs.at[n % 4], xsem.at[n % 4])

    def x_start(n):
        @pl.when(n < batch)
        def _():
            x_copy(n, 0).start()

        @pl.when((n >= batch) & (n < blocks))
        def _():
            x_copy(n, 1).start()

    def x_wait(n):
        @pl.when(n < blocks)
        def _():
            pltpu.make_async_copy(txt_hbm.at[0], xs.at[n % 4], xsem.at[n % 4]).wait()

    def w_columns(path, j):
        return w.at[path, :, j * width:(j + 1) * width]

    def w_load(path, j):
        return pltpu.make_async_copy((wt_hbm, wi_hbm)[path].at[j], w_columns(path, j), wsem.at[path, j])

    def early_place(path, k):
        return m_w.at[k] if path == 0 else w_columns(path, k)

    def early_load(path, k):
        return pltpu.make_async_copy((mt_hbm, mi_hbm)[path].at[k], early_place(path, k), (msem if path == 0 else wsem.at[path]).at[k])

    def late_load(c, path):
        return pltpu.make_async_copy((mt_hbm, mi_hbm)[path].at[GATE1 + c // 2], m_w.at[c % 2], msem.at[c % 2])

    def late_start(c):
        for path in PATHS:
            @pl.when(c % 2 == path)
            def _():
                late_load(c, path).start()

    def m_copy(part, d, send):
        buf, at = ((m_early, slice(None)), (m_late, slice(FIRST_LATE)), (m_late, slice(FIRST_LATE, 8)))[part]
        ref = buf.at[me if send else (me + n_dev - d) % n_dev, at]
        return pltpu.make_async_remote_copy(src_ref=ref, dst_ref=ref, send_sem=msend.at[part, d], recv_sem=mrecv.at[part, d], device_id={'tp': (me + d) % n_dev}, device_id_type=MESH)

    def m_send(part):
        for d in others:
            m_copy(part, d, True).start()

    def m_wait(part):
        for d in others:
            m_copy(part, d, True).wait_send()
            m_copy(part, d, False).wait_recv()

    for k in (SHIFT1, SCALE1):
        for path in PATHS:
            early_load(path, k).start()
    for n in range(3):
        x_copy(n, 0 if n < batch else 1).start()
    for j in range(3):
        w_load(0, j).start()
    v = cond_ref[...].astype(F32)
    silu = (v * (1.0 / (1.0 + jnp.exp(-v)))).astype(BF16)
    for path, (mod_b, qkv_b, q_gain, k_gain, proj_b, fc1_b, fc2_b) in enumerate((small_t, small_i)):
        m_b[path] = mod_b[...].astype(F32)
        for row, ref in ((PROJ_B, proj_b), (FC2_B, fc2_b)):
            vector = ref[...].astype(F32)[None, :]
            for b in range(batch):
                vec_ref[path * batch + b, row:row + 1, :] = vector
        for row, ref in ((Q_GAIN, q_gain), (K_GAIN, k_gain), (FC1_B, fc1_b)):
            vector = ref[...].astype(F32)[None, :]
            small_ref[path, row:row + 1, :vector.shape[1]] = vector
        for j in range(qkv_b.shape[0]):
            small_ref[path, QKV_B:Q_GAIN, j * width:(j + 1) * width] = qkv_b[j:j + 1, :].astype(F32)
    place.enter([(me + d) % n_dev for d in others] + [beside])

    def early_chunk(k, path):
        early_load(path, k).wait()
        acc = jnp.dot(silu, early_place(path, k)[...], preferred_element_type=F32)
        return (acc + m_b[path, k:k + 1, :]).astype(BF16)

    m_early[me] = jnp.concatenate([early_chunk(k, path) for k in (SHIFT1, SCALE1) for path in PATHS], axis=0)
    m_send(0)
    tw_load = pltpu.make_async_copy(tw_hbm, tw, tsem.at[1])

    def late_chunk(t):
        c = jnp.minimum(t, 7)
        path, k = c % 2, GATE1 + c // 2
        acc = jnp.dot(silu, m_w[c % 2], preferred_element_type=F32) + m_b[path, pl.ds(k, 1), :]
        m_late[me, t] = acc.astype(BF16).astype(F32)

    def late_rows(part):
        m_wait(1 + part)
        for j in range(n_dev):
            for c in range(8)[slice(FIRST_LATE) if part == 0 else slice(FIRST_LATE, 8)]:
                for b in range(batch):
                    vec_ref[c % 2 * batch + b, pl.ds(GATE1 + c // 2, 1), j * width:(j + 1) * width] = m_late[j, c, b:b + 1, :]

    def piece_at(j):
        return rows_at((j + 2 * odd) % PIECES * piece, piece)

    def remote(sends, recvs, kind, j, src, dst, dev):
        return pltpu.make_async_remote_copy(src_ref=src, dst_ref=dst, send_sem=sends.at[kind, j], recv_sem=recvs.at[kind, j], device_id=ident(dev), device_id_type=MESH)

    def p_copy(kind, j, owner, dev):
        dst = wp_hbm.at[owner, piece_at(j), :]
        src = pw_hbm.at[piece_at(j), :] if kind in (W_FIRST, W_SECOND) else dst
        return remote(psend, precv, kind, j, src, dst, dev)

    def w_own():
        return remote(psend, precv, W_CORE, 0, pw_hbm, wp_hbm.at[me], partner)

    def w_core():
        w_own().start()

    def z_copy(kind, owner, j, at):
        ref = wp_hbm.at[owner, piece_at(at), :]
        return remote(psend, precv, kind, j, ref, ref, beside)

    def w_relay(j):
        p_copy(W_FIRST, j, first, first).wait_recv()
        p_copy(W_RELAY, j, first, second).start()
        p_copy(W_CORE_FIRST, j, first, partner).start()
        z_copy(Z_FIRST, first, j, j).start()
        if j == 0:
            p_copy(W_SECOND, 1, me, second).start()

    def w_second(j):
        p_copy(W_SECOND, j, second, second).wait_recv()
        p_copy(W_CORE_SECOND, j, second, partner).start()
        z_copy(Z_SECOND, second, j, j).start()

    def w_last(j):
        p_copy(W_RELAY, j, diagonal, second).wait_recv()
        p_copy(W_CORE_RELAY, j, diagonal, partner).start()
        z_copy(Z_RELAY, diagonal, j, j).start()

    from_beside = ((Z_FIRST, first, W_CORE_FIRST), (Z_SECOND, second, W_CORE_SECOND), (Z_RELAY, diagonal, W_CORE_RELAY))

    def w_beside(n):
        kind, owner, core_kind = from_beside[n % 3]
        j = n // 3
        z_copy(kind, owner, j, j + 2).wait_recv()
        p_copy(core_kind, j + 2, owner, partner).start()

    p_copy(W_FIRST, 0, me, first).start()
    p_copy(W_SECOND, 0, me, second).start()
    p_copy(W_FIRST, 1, me, first).start()

    even = lax.broadcasted_iota(jnp.int32, (rows, HEAD), 1) % 2 == 0
    code = lax.broadcasted_iota(jnp.int32, (N_IDS, rows), 0)

    def select(n):
        n = jnp.int32(n)
        img = (n >= batch).astype(jnp.int32)
        return (1 - img) * n + img * (batch + (n - batch) // per_img)

    def norm(n, u):
        sel = select(n)
        for r in range(0, rows, STRIP):
            u[r // half, r % half:r % half + STRIP, :] = modulated(xs[n % 4, r:r + STRIP, :].astype(F32), vec_ref, sel, SHIFT1, SCALE1)

    def heads_of(n, u):
        b, r0 = position(n)
        path = (jnp.int32(n) >= batch).astype(jnp.int32)
        hot = jnp.concatenate([(ids_ref[axis, pl.ds(b, 1), rows_at(r0, rows)] == code).astype(F32).astype(BF16) for axis in range(3)], axis=0)
        parts = lax.dot_general(hot, tab_ref[...], (((0,), (0,)), ((), ())), preferred_element_type=F32)
        cos_t, sin_t = (sum(parts[:, (3 * i + j) * HEAD:(3 * i + j + 1) * HEAD] for j in range(3)) for i in range(2))
        at = rows_at(b * total + r0, rows)
        for c0 in range(0, 3 * heads, 4):
            c1 = min(c0 + 4, 3 * heads)
            a = jnp.dot(u[...].reshape(rows, dim), w[path, :, c0 * HEAD:c1 * HEAD], preferred_element_type=F32) + row_of(small_ref, path, QKV_B, slice(c0 * HEAD, c1 * HEAD))
            for c in range(c0, c1):
                t = a[:, (c - c0) * HEAD:(c - c0 + 1) * HEAD]
                kind = c // heads
                if kind < 2:
                    t = t * lax.rsqrt(row_mean(t * t) + NORM_EPS) * row_of(small_ref, path, Q_GAIN + kind, slice(HEAD))
                    swapped = jnp.where(even, pltpu.roll(t, HEAD - 1, 1), pltpu.roll(t, 1, 1))
                    t = t * cos_t + swapped * sin_t
                qkv[c, at, :] = t.astype(BF16)

    m_wait(0)
    for j in range(n_dev):
        rows_here = m_early[j].astype(F32)
        for n in range(2 * 2 * batch):
            k, sel = n // (2 * batch), n % (2 * batch)
            vec_ref[sel, k:k + 1, j * width:(j + 1) * width] = rows_here[n:n + 1, :]
    x_wait(0)
    norm(0, ua)
    for j in range(3):
        w_load(0, j).wait()
    for c in range(2):
        late_load(c, c).start()
    for j in range(3):
        w_load(1, j).start()
    tw_load.start()

    def qkv_step(t):
        x_start(2 * t + 3)
        x_start(2 * t + 4)
        x_wait(2 * t + 1)
        x_wait(2 * t + 2)
        @pl.when(t == 1)
        def _():
            for j in range(3):
                w_load(1, j).wait()

        @pl.when(t < 8)
        def _():
            late_load(t, 0).wait()

        late_chunk(t)
        norm(2 * t + 1, ub)
        heads_of(2 * t, ua)
        norm(jnp.minimum(2 * t + 2, blocks - 1), ua)
        heads_of(2 * t + 1, ub)

        @pl.when(t < 6)
        def _():
            late_start(t + 2)

    kv_store = pltpu.make_async_copy(qkv.at[:, total:, :], kv_hbm, tsem.at[0])

    def late_send(part):
        m_send(1 + part)

    def kv_send():
        kv_store.start()

    done_here = batch + per_img

    def rows_of(n, c, size, r0):
        return qkv[c, rows_at(position(n)[0] * total + r0, size), :]

    def scores(n, h, s):
        s[...] = scores_of(rows_of(n, heads + h, total, 0), rows_of(n, h, rows, position(n)[1]))

    def weigh(n, h, s):
        top = jnp.max(s[...], axis=0, keepdims=True)
        keys = total // 9
        sums = 0.0
        for r in range(0, total, keys):
            p = jnp.exp2((s[r:r + keys, :] - top) * (HEAD ** -0.5 * LOG2E))
            sums += jnp.sum(p, axis=0, keepdims=True)
            probs[r:r + keys, :] = p.astype(BF16)
        o = lax.dot_general(rows_of(n, 2 * heads + h, total, 0), probs[...], (((0,), (0,)), ((), ())), preferred_element_type=F32)
        o_all[rows_at(n * rows, rows), h * HEAD:(h + 1) * HEAD] = (o * (1.0 / sums)).T.astype(BF16)

    def t_copy(kind, b, src, dst, dev):
        return remote(tsend, trecv, kind, b, src, dst, dev)

    def t_core(b):
        return t_copy(T_CORE, b, t_send, t_recv.at[b], partner)

    def t_first(b):
        return t_copy(T_FIRST, b, t_sum.at[b, rows_at(not1 * quarter, quarter), :], t_rs1.at[b], first)

    def t_second(b):
        return t_copy(T_SECOND, b, t_rs2_out.at[b], t_rs2_in.at[b], second)

    def own_rows(b1, b2):
        return rows_at(core * half + b1 * quarter + b2 * eighth, eighth)

    def t_parts(b):
        return [t_copy(kind, b, t_sum.at[b, rows_at(b1 * quarter + b2 * eighth, eighth), :], dst, dev) for kind, b1, b2, dst, dev in (
            (T_FIRST, not1, bit2, t_rs1.at[b, :eighth], first), (T_SECOND, bit1, not2, t_rs2_in.at[b], second), (T_OUT_FIRST, not1, not2, t_rs1.at[b, eighth:], diagonal))]

    def t_out(kind, b, b1, b2, dev):
        ref = ut_hbm.at[b, own_rows(b1, b2), :]
        return t_copy(kind, b, t_u.at[b] if kind in (T_OUT_FIRST, T_OUT_SECOND, T_CORE_OWN) else ref, ref, dev)

    def t_local(b):
        return pltpu.make_async_copy(t_u.at[b], ut_hbm.at[b, own_rows(bit1, bit2), :], tsem.at[2 + b])

    def t_load(b):
        return pltpu.make_async_copy(txt_hbm.at[b, own_rows(bit1, bit2), :], t_x.at[b], tsem.at[2 + batch + b])

    tile = min(512, dim)

    def text_product(b, who, store):
        def columns(n):
            at = rows_at(n * tile, tile)
            store(at, jnp.dot(o_all[rows_at(b * rows + who * half, half), :], tw[:, at], preferred_element_type=F32))

        loop(dim // tile, columns)

    def text_partial(b):
        if b == 0:
            tw_load.wait()
        t_load(b).start()

        def to_send(at, value):
            t_send[:, at] = value.astype(BF16)

        def to_own(at, value):
            t_own[:, at] = value

        text_product(b, far, to_send)
        t_core(b).start()
        text_product(b, core, to_own)

    def text_sum(b):
        t_core(b).wait()

        def add(n):
            at = rows_at(n * STRIP, STRIP)
            t_sum[b, at, :] = (t_own[at, :] + t_recv[b, at, :].astype(F32)).astype(BF16)

        loop(half // STRIP, add)
        if b < batch - 1:
            t_first(b).start()
            return
        for part in t_parts(b):
            part.start()

    def text_quarter(b):
        t_first(b).wait()
        t_rs2_out[b] = (t_sum[b, rows_at(bit1 * quarter + not2 * eighth, eighth), :].astype(F32) + t_rs1[b, rows_at(not2 * eighth, eighth), :].astype(F32)).astype(BF16)
        t_keep[b] = t_sum[b, rows_at(bit1 * quarter + bit2 * eighth, eighth), :].astype(F32) + t_rs1[b, rows_at(bit2 * eighth, eighth), :].astype(F32)
        t_second(b).start()

    def text_finish(b):
        for part in [t_second(b)] if b < batch - 1 else t_parts(b):
            part.wait()
        t_load(b).wait()
        if b == batch - 1:
            t_keep[b] = t_sum[b, rows_at(bit1 * quarter + bit2 * eighth, eighth), :].astype(F32) + t_rs1[b, :eighth].astype(F32) + t_rs1[b, eighth:].astype(F32)
        branch = t_keep[b] + t_rs2_in[b].astype(F32) + row_of(vec_ref, b, PROJ_B)
        x1 = (t_x[b].astype(F32) + row_of(vec_ref, b, GATE1) * branch).astype(BF16)
        x1_ref[b] = x1
        u = modulated(x1.astype(F32), vec_ref, b, SHIFT2, SCALE2)
        if b == batch - 1:
            tu_ref[...] = u
            return
        t_u[b] = u
        t_out(T_OUT_FIRST, b, bit1, bit2, first).start()
        t_out(T_OUT_SECOND, b, bit1, bit2, second).start()
        t_out(T_CORE_OWN, b, bit1, bit2, partner).start()
        t_local(b).start()

    def text_relay(b):
        t_out(T_OUT_FIRST, b, not1, bit2, first).wait_recv()
        t_out(T_OUT_RELAY, b, not1, bit2, second).start()
        t_out(T_CORE_FIRST, b, not1, bit2, partner).start()
        t_out(T_OUT_SECOND, b, bit1, not2, second).wait_recv()
        t_out(T_CORE_SECOND, b, bit1, not2, partner).start()

    def text_last(b):
        t_out(T_OUT_RELAY, b, not1, not2, second).wait_recv()
        t_out(T_CORE_RELAY, b, not1, not2, partner).start()

    def g_rows(m, who):
        return o_all.at[rows_at((batch + m) * rows + who * half, half), :]

    def g_mine(m):
        return og_hbm.at[m, :, rows_at(me * width, width)]

    def g_local(m):
        return pltpu.make_async_copy(g_rows(m, core), g_mine(m), gsem.at[m])

    def g_core(m):
        return remote(gsend, grecv, G_CORE, m, g_rows(m, far), g_mine(m), partner)

    def g_copy(kind, m, owner, dev):
        ref = og_hbm.at[m, :, rows_at(owner // 2 * (2 * width), 2 * width)]
        return remote(gsend, grecv, kind, m, ref, ref, dev)

    def gather_start(m):
        g_local(m).start()
        g_core(m).start()

    def gather_send(m):
        g_local(m).wait()
        g_core(m).wait()
        g_copy(G_FIRST, m, me, first).start()
        g_copy(G_SECOND, m, me, second).start()

    def gather_relay(m):
        g_copy(G_FIRST, m, first, first).wait_recv()
        g_copy(G_RELAY, m, first, second).start()

    qkv_first, attend_first = (batch + per_img) // 2, 1 + EARLY
    resume = blocks // 2 + attend_first
    steps = blocks // 2 + done_here
    known = dict(locals())

    def run(calls):
        for call in calls:
            name, *args = call.split()
            known[name](*map(int, args))

    def attended(a):
        early = ((a >= 1) & (a <= EARLY)).astype(jnp.int32)
        return a + early - EARLY * (a == attend_first).astype(jnp.int32)

    def attention_step(a, begins):
        n = attended(a)

        @pl.when(begins)
        def _():
            scores(n, 0, s0)

        scores(n, 1, s1)
        weigh(n, 0, s0)
        scores(n, 2, s2)
        weigh(n, 1, s1)
        scores(attended(jnp.minimum(a + 1, done_here - 1)), 0, s0)
        weigh(n, 2, s2)

    def step(i):
        for start, stop in ((0, resume), (resume, steps)):
            @pl.when((i >= start) & (i < stop))
            def _():
                for when, calls in enumerate(HOOKS[start:stop], start):
                    if calls:
                        pl.when(i == when)(functools.partial(run, calls))

        in_first = i < qkv_first
        in_second = (i >= qkv_first + attend_first) & (i < resume)

        @pl.when(in_first | in_second)
        def _():
            qkv_step(i - attend_first * in_second.astype(jnp.int32))

        @pl.when(jnp.logical_not(in_first | in_second))
        def _():
            late = (i >= resume).astype(jnp.int32)
            attention_step(i - late * (blocks // 2) - (1 - late) * qkv_first, (i == qkv_first) | (i == resume))

    loop(steps, step)

    o_out = pltpu.make_async_copy(o_all.at[batch * rows:, :], o_hbm, osem)
    o_out.start()
    run(HOOKS[steps])
    o_out.wait()
    kv_store.wait()
    t_local(0).wait()
    for kind, b1, b2, dev in ((T_OUT_FIRST, bit1, bit2, first), (T_OUT_SECOND, bit1, bit2, second), (T_OUT_RELAY, not1, bit2, second)):
        t_out(kind, 0, b1, b2, dev).wait_send()
    for kind, b1, b2 in ((T_CORE_OWN, bit1, bit2), (T_CORE_FIRST, not1, bit2), (T_CORE_SECOND, bit1, not2), (T_CORE_RELAY, not1, not2)):
        t_out(kind, 0, b1, b2, partner).wait()
    for j in SHARED:
        for kind, owner, dev in ((W_FIRST, me, first), (W_SECOND, me, second), (W_RELAY, first, second)):
            p_copy(kind, j, owner, dev).wait_send()
    w_own().wait()
    for kind, owner, core_kind in from_beside:
        for j in SHARED:
            z_copy(kind, owner, j, j).wait_send()
        for j in range(PIECES):
            p_copy(core_kind, j, owner, partner).wait()
    for m in range(READY):
        g_copy(G_FIRST, m, me, first).wait_send()
        g_copy(G_SECOND, m, me, second).wait_send()
        g_copy(G_RELAY, m, first, second).wait_send()
        g_copy(G_SECOND, m, second, second).wait_recv()
        g_copy(G_RELAY, m, diagonal, second).wait_recv()


HOOKS = (
    (),
    (),
    ('w_relay 0',),
    ('w_second 0',),
    ('w_relay 1',),
    ('late_send 0', 'w_last 0'),
    (),
    ('gather_start 0', 'w_second 1'),
    ('gather_send 0', 'w_beside 0', 'w_last 1'),
    ('gather_start 2', 'gather_start 1'),
    ('gather_send 2', 'gather_start 3', 'text_partial 0', 'w_beside 1', 'gather_send 3'),
    ('text_sum 0', 'gather_send 1', 'gather_relay 2'),
    ('w_core', 'w_beside 3'),
    ('late_send 1', 'text_quarter 0', 'gather_relay 0'),
    ('kv_send', 'late_rows 0', 'gather_relay 3', 'text_finish 0', 'w_beside 2'),
    ('gather_relay 1',),
    ('text_partial 1', 'text_relay 0', 'text_sum 1', 'w_beside 4'),
    ('text_last 0', 'late_rows 1'),
    (),
    ('w_beside 5', 'text_finish 1'),
)


def front_call(txt, img, wt, wi, mt, mi, pw, tw, cond, small_t, small_i, ids_t, table, n_dev, rows):
    batch, txt_len, dim = txt.shape
    img_len = img.shape[1]
    total = txt_len + img_len
    width = pw.shape[0]
    heads = width // HEAD
    half, quarter, eighth = rows // 2, rows // 4, rows // 8
    assert heads == HEADS_HERE and batch == 2
    cfg = (batch, txt_len, img_len, rows)
    blocks = batch * (1 + img_len // rows)
    vmem = pl.BlockSpec(memory_space=pltpu.VMEM)
    anywhere = pl.BlockSpec(memory_space=pl.ANY)
    tall = [pltpu.VMEM((half, dim), BF16), pltpu.VMEM((batch, half, dim), BF16), pltpu.VMEM((half, dim), F32), pltpu.VMEM((batch, half, dim), BF16), pltpu.VMEM((batch, quarter, dim), BF16)]
    short = [pltpu.VMEM((batch, eighth, dim), dtype) for dtype in (BF16, BF16, F32, BF16, BF16)]
    return pl.pallas_call(
        functools.partial(front_kernel, cfg),
        in_specs=[anywhere] * 8 + [vmem, (vmem,) * len(small_t), (vmem,) * len(small_i), vmem, vmem],
        out_specs=[anywhere] * 5 + [vmem] * 4,
        out_shape=[
            jax.ShapeDtypeStruct((img_len, width), BF16),
            jax.ShapeDtypeStruct((3 * heads, total, HEAD), BF16),
            jax.ShapeDtypeStruct((n_dev, width, dim), BF16),
            jax.ShapeDtypeStruct((batch, txt_len, dim), BF16),
            jax.ShapeDtypeStruct((READY, half, dim), BF16),
            jax.ShapeDtypeStruct((batch, eighth, dim), BF16),
            jax.ShapeDtypeStruct((eighth, dim), BF16),
            jax.ShapeDtypeStruct((2 * batch, FC2_B + 1, dim), F32),
            jax.ShapeDtypeStruct((2, FC1_B + 1, dim), F32),
        ],
        scratch_shapes=[
            pltpu.VMEM((2, dim, 3 * width), BF16),
            pltpu.VMEM((2, dim, width), BF16),
            pltpu.VMEM((2, PROJ_B, width), F32),
            pltpu.VMEM((n_dev, 4 * batch, width), BF16),
            pltpu.VMEM((n_dev, blocks // 2, batch, width), F32),
            pltpu.VMEM((4, rows, dim), BF16),
            pltpu.VMEM((batch, half, dim), BF16),
            pltpu.VMEM((batch, half, dim), BF16),
            pltpu.VMEM((3 * heads, batch * total, HEAD), BF16),
            pltpu.VMEM((total, rows), F32),
            pltpu.VMEM((total, rows), F32),
            pltpu.VMEM((total, rows), F32),
            pltpu.VMEM((total, rows), BF16),
            pltpu.VMEM((batch * txt_len + img_len, width), BF16),
            pltpu.VMEM((width, dim), BF16),
            *tall,
            *short,
            pltpu.SemaphoreType.DMA((2, 3)),
            pltpu.SemaphoreType.DMA((2,)),
            pltpu.SemaphoreType.DMA((4,)),
            pltpu.SemaphoreType.DMA,
            pltpu.SemaphoreType.DMA((6,)),
            pltpu.SemaphoreType.DMA((READY,)),
            *[pltpu.SemaphoreType.DMA((10, PIECES))] * 2,
            *[pltpu.SemaphoreType.DMA((10, batch))] * 2,
            *[pltpu.SemaphoreType.DMA((4, READY))] * 2,
            *[pltpu.SemaphoreType.DMA((3, n_dev))] * 2,
        ],
        compiler_params=pltpu.CompilerParams(collective_id=2, has_side_effects=True, vmem_limit_bytes=VMEM_BYTES),
        name="front",
    )(txt, img, wt, wi, mt, mi, pw, tw, cond, small_t, small_i, ids_t, table)


(O_CORE, O_FIRST, O_SECOND, O_RELAY, U_CORE, PART_CORE, RS_FIRST, RS_SECOND, OUT_FIRST, OUT_SECOND, OUT_RELAY, CORE_OWN, CORE_FIRST, CORE_SECOND, CORE_RELAY,
 U_FIRST, U_SECOND, U_RELAY, U_OWN, U_CORE_FIRST, U_CORE_SECOND, U_CORE_RELAY) = range(22)
(L_O, L_X, L_OUT) = range(3)
SLOTS = 4
O_SLOTS = 10
OPENED = 1
SEMS = 12


def two(n):
    return n % 2


def block_kernel(cfg, o_hbm, og_hbm, kv_hbm, x_hbm, ut_hbm, x1t_hbm, tu_hbm, wp_hbm, pw_hbm, w1t_hbm, w2t_hbm, w1i_hbm, w2i_hbm, vec_ref, fb_ref, out_hbm, o2_hbm,
                 kv, qs, os, wp, w1, w2, obuf, xbuf, x1keep, u2, hid, psend, precv, own, chip_sum, rs1, keep2, rs2_out, rs2_in, outb,
                 asem, wsem, lsem, tsem, ssem, rsem):
    batch, txt_chunks, img_chunks, per_img, rows, tile = cfg
    half, quarter, eighth = rows // 2, rows // 4, rows // 8
    dim = wp.shape[0]
    ff = w1.shape[1]
    cols = o_hbm.shape[1]
    heads = cols // HEAD
    total = txt_chunks + img_chunks
    per_txt = txt_chunks // batch

    place = Place()
    me, core, partner, first, second, bit1, bit2 = place.me, place.core, place.partner, place.first, place.second, place.bit1, place.bit2
    not1, not2, far = place.not1, place.not2, place.far
    txt_len = ut_hbm.shape[1]
    place.enter([partner, first, second])

    def remote(kind, g, src, dst, dev):
        return pltpu.make_async_remote_copy(src_ref=src, dst_ref=dst, send_sem=ssem.at[kind, g % SEMS], recv_sem=rsem.at[kind, g % SEMS], device_id={'tp': dev}, device_id_type=MESH)

    def img_pos(g):
        k = g - txt_chunks
        return k // per_img, (k % per_img) * rows

    def chip_cols(dev):
        return rows_at((dev // 2) * (2 * cols), 2 * cols)

    def own_rows(b1, b2):
        return core * half + b1 * quarter + b2 * eighth

    def o_from(b):
        return (o_hbm, o2_hbm)[b]

    first_open = txt_chunks + og_hbm.shape[0]

    def o_ready(g):
        return pltpu.make_async_copy(og_hbm.at[g - txt_chunks], obuf.at[g % O_SLOTS], lsem.at[L_O, g % SEMS])

    def o_local(g, b):
        r0 = img_pos(g)[1]
        return pltpu.make_async_copy(o_from(b).at[rows_at(r0 + core * half, half), :], obuf.at[g % O_SLOTS, :, rows_at(me * cols, cols)], lsem.at[L_O, g % SEMS])

    def o_core(g, b):
        r0 = img_pos(g)[1]
        return remote(O_CORE, g, o_from(b).at[rows_at(r0 + far * half, half), :], obuf.at[g % O_SLOTS, :, rows_at(me * cols, cols)], partner)

    units = per_img * heads

    def q_load(u):
        r0 = txt_len + u // heads * rows
        return pltpu.make_async_copy(kv_hbm.at[u % heads, rows_at(r0, rows), :], qs.at[two(u)], asem.at[two(u)])

    def o_store(u):
        return pltpu.make_async_copy(os.at[two(u)], o2_hbm.at[rows_at(u // heads * rows, rows), rows_at(u % heads * HEAD, HEAD)], asem.at[2 + two(u)])

    def kv_load():
        return pltpu.make_async_copy(kv_hbm.at[heads:], kv, asem.at[4])

    def attend(u, carry):
        @pl.when(u == 0)
        def _():
            kv_load().wait()

        q_load(u).wait()

        @pl.when(u + 1 < units)
        def _():
            q_load(u + 1).start()

        @pl.when(u >= 2)
        def _():
            o_store(u - 2).wait()

        k = kv[u % heads]
        v = kv[heads + u % heads]
        for r in range(0, rows, half):
            os[two(u), r:r + half, :] = weighted(scores_of(qs[two(u), r:r + half, :], k), v)
        o_store(u).start()

        @pl.when(u == units - 1)
        def _():
            o_store(u - 1).wait()
            o_store(u).wait()
        return carry

    def attended(i):
        return sum(count * (i > n).astype(jnp.int32) for n, count in enumerate(ATTEND) if count)

    def o_send(kind, g, owner, dev):
        ref = obuf.at[g % O_SLOTS, :, chip_cols(owner)]
        return remote(kind, g, ref, ref, dev)

    def x_load(g):
        b, r0 = img_pos(g)
        return pltpu.make_async_copy(x_hbm.at[b, rows_at(r0 + core * half, half), :], xbuf.at[two(g)], lsem.at[L_X, g % SEMS])

    def u_core(g):
        return remote(U_CORE, g, u2.at[two(g), :half, :], u2.at[two(g), half:, :], partner)

    def part_core(g):
        return remote(PART_CORE, g, psend, precv.at[two(g)], partner)

    def rs_first(g):
        return remote(RS_FIRST, g, chip_sum.at[rows_at(not1 * quarter, quarter), :], rs1.at[two(g)], first)

    def rs_second(g):
        return remote(RS_SECOND, g, rs2_out.at[two(g)], rs2_in.at[g % SLOTS], second)

    def out_ref(g, b1, b2):
        return out_hbm.at[rows_at(g * rows + own_rows(b1, b2), eighth), :]

    def out_send(kind, g, b1, b2, dev):
        ref = out_ref(g, b1, b2)
        mine = kind in (OUT_FIRST, OUT_SECOND, CORE_OWN)
        return remote(kind, g, outb.at[g % SLOTS] if mine else ref, ref, dev)

    def out_local(g):
        return pltpu.make_async_copy(outb.at[g % SLOTS], out_ref(g, bit1, bit2), lsem.at[L_OUT, g % SEMS])

    last_txt = txt_chunks - 1

    def txt_load(g, who):
        mine = who is core
        return pltpu.make_async_copy(ut_hbm.at[g, rows_at(who * half, half), :], u2.at[two(g), slice(half) if mine else slice(half, rows), :], tsem.at[0 if mine else 2, g])

    def x1_load(g):
        return pltpu.make_async_copy(x1t_hbm.at[g], x1keep.at[g], tsem.at[1, g])

    def u_rows(b1, b2, base=0):
        return u2.at[two(last_txt), rows_at(base + b1 * quarter + b2 * eighth, eighth), :]

    def u_local():
        return pltpu.make_async_copy(tu_hbm, u_rows(bit1, bit2), tsem.at[0, last_txt])

    def u_send(kind, b1, b2, dev):
        src = tu_hbm if kind in (U_FIRST, U_SECOND, U_OWN) else u_rows(b1, b2)
        return remote(kind, last_txt, src, u_rows(b1, b2, 0 if dev is not partner else half), dev)

    def u_start():
        u_local().start()
        u_send(U_FIRST, bit1, bit2, first).start()
        u_send(U_SECOND, bit1, bit2, second).start()
        u_send(U_OWN, bit1, bit2, partner).start()

    def u_relay():
        u_send(U_FIRST, not1, bit2, first).wait_recv()
        u_send(U_RELAY, not1, bit2, second).start()
        u_send(U_CORE_FIRST, not1, bit2, partner).start()
        u_send(U_SECOND, bit1, not2, second).wait_recv()
        u_send(U_CORE_SECOND, bit1, not2, partner).start()

    def u_last():
        u_send(U_RELAY, not1, not2, second).wait_recv()
        u_send(U_CORE_RELAY, not1, not2, partner).start()

    def u_wait():
        u_local().wait()
        u_send(U_FIRST, bit1, bit2, first).wait_send()
        u_send(U_SECOND, bit1, bit2, second).wait_send()
        u_send(U_RELAY, not1, bit2, second).wait_send()
        for kind, b1, b2 in ((U_OWN, bit1, bit2), (U_CORE_FIRST, not1, bit2), (U_CORE_SECOND, bit1, not2), (U_CORE_RELAY, not1, not2)):
            u_send(kind, b1, b2, partner).wait()

    def w_load(k, src, dst):
        return pltpu.make_async_copy(src, dst, wsem.at[k])

    def wp_load(j, src):
        return pltpu.make_async_copy(src, wp.at[j * cols:(j + 1) * cols, :], wsem.at[2 + j])

    def select(g):
        txt = (g < txt_chunks).astype(jnp.int32)
        return txt * (g // per_txt) + (1 - txt) * (batch + (g - txt_chunks) // per_img)

    def start_o(g):
        @pl.when(g < first_open)
        def _():
            o_ready(g).start()

        for b in range(batch):
            @pl.when((g >= first_open) & (img_pos(g)[0] == b))
            def _():
                o_local(g, b).start()
                o_core(g, b).start()

    def send_o(g):
        o_local(g, 0).wait()
        o_core(g, 0).wait()
        o_send(O_FIRST, g, me, first).start()
        o_send(O_SECOND, g, me, second).start()

    def relay_o(g):
        o_send(O_FIRST, g, first, first).wait_recv()
        o_send(O_RELAY, g, first, second).start()

    def start_x(g):
        x_load(g).start()

    wide = 2 * tile

    def project(g):
        @pl.when(g < first_open)
        def _():
            o_ready(g).wait()

        @pl.when(g >= first_open)
        def _():
            o_send(O_FIRST, g, me, first).wait_send()
            o_send(O_SECOND, g, me, second).wait_send()
            o_send(O_RELAY, g, first, second).wait_send()
            o_send(O_SECOND, g, second, second).wait_recv()
            o_send(O_RELAY, g, second, second).wait_recv()

        x_load(g).wait()

        @pl.when(g == txt_chunks)
        def _():
            for j in range(wp_hbm.shape[0]):
                wp_load(j, wp_hbm.at[j]).wait()

        sel = select(g)
        slot = g % SLOTS

        def columns(n):
            at = rows_at(n * wide, wide)
            acc = jnp.dot(obuf[g % O_SLOTS], wp[:, at], preferred_element_type=F32)
            branch = acc + row_of(vec_ref, sel, PROJ_B, at)
            xbuf[two(g), :, at] = (xbuf[two(g), :, at].astype(F32) + row_of(vec_ref, sel, GATE1, at) * branch).astype(BF16)

        loop(dim // wide, columns)

        def norm(n):
            at = rows_at(n * STRIP, STRIP)
            u2[two(g), at, :] = modulated(xbuf[two(g), at, :].astype(F32), vec_ref, sel, SHIFT2, SCALE2)

        loop(half // STRIP, norm)
        u_core(g).start()
        x1keep[slot] = xbuf[two(g), rows_at(bit1 * quarter + bit2 * eighth, eighth), :]

    def mlp_hidden(g):
        @pl.when(g < last_txt)
        def _():
            for who in (core, far):
                txt_load(g, who).wait()

        @pl.when(g == last_txt)
        def _():
            u_wait()

        @pl.when(g < txt_chunks)
        def _():
            x1_load(g).wait()

        @pl.when(g >= txt_chunks)
        def _():
            u_core(g).wait()

        @pl.when(g == 0)
        def _():
            w_load(0, w1t_hbm, w1).wait()
            w_load(1, w2t_hbm, w2).wait()
            for j in range(wp_hbm.shape[0]):
                @pl.when(j != me)
                def _():
                    wp_load(j, wp_hbm.at[j]).start()

                @pl.when(j == me)
                def _():
                    wp_load(j, pw_hbm).start()

        @pl.when(g == txt_chunks)
        def _():
            w_load(0, w1i_hbm, w1).wait()
            w_load(1, w2i_hbm, w2).wait()

        path = (g >= txt_chunks).astype(jnp.int32)

        def hidden(n):
            at = rows_at(n * tile, tile)
            acc = jnp.dot(u2[two(g)], w1[:, at], preferred_element_type=F32)
            pre = acc + row_of(fb_ref, path, FC1_B, at)
            hid[:, at] = jax.nn.gelu(pre, approximate=True).astype(BF16)

        loop(ff // tile, hidden)

    def mlp_out(g):
        def columns(n):
            at = rows_at(n * tile, tile)
            acc = jnp.dot(hid[...], w2[:, at], preferred_element_type=F32)
            own[:, at] = acc[:half]
            psend[:, at] = acc[half:].astype(BF16)

        loop(dim // tile, columns)
        part_core(g).start()

        @pl.when(g == txt_chunks - 1)
        def _():
            w_load(0, w1i_hbm, w1).start()
            w_load(1, w2i_hbm, w2).start()

    def mlp_sum(g):
        part_core(g).wait()

        def add(n):
            at = rows_at(n * STRIP, STRIP)
            chip_sum[at, :] = (own[at, :] + precv[two(g), at, :].astype(F32)).astype(BF16)

        loop(half // STRIP, add)
        rs_first(g).start()

    def add_first(g):
        rs_first(g).wait()
        rs2_out[two(g)] = (chip_sum[rows_at(bit1 * quarter + not2 * eighth, eighth), :].astype(F32) + rs1[two(g), rows_at(not2 * eighth, eighth), :].astype(F32)).astype(BF16)
        rs_second(g).start()
        keep2[two(g)] = chip_sum[rows_at(bit1 * quarter + bit2 * eighth, eighth), :].astype(F32) + rs1[two(g), rows_at(bit2 * eighth, eighth), :].astype(F32)

    def finish(g):
        rs_second(g).wait()
        sel = select(g)
        branch = keep2[two(g)] + rs2_in[g % SLOTS].astype(F32) + row_of(vec_ref, sel, FC2_B)
        outb[g % SLOTS] = (x1keep[g % SLOTS].astype(F32) + row_of(vec_ref, sel, GATE2) * branch).astype(BF16)
        out_send(OUT_FIRST, g, bit1, bit2, first).start()
        out_send(OUT_SECOND, g, bit1, bit2, second).start()
        out_send(CORE_OWN, g, bit1, bit2, partner).start()
        out_local(g).start()

    def relay_out(g):
        out_send(OUT_FIRST, g, not1, bit2, first).wait_recv()
        out_send(OUT_RELAY, g, not1, bit2, second).start()
        out_send(CORE_FIRST, g, not1, bit2, partner).start()

    def second_out(g):
        out_send(OUT_SECOND, g, bit1, not2, second).wait_recv()
        out_send(CORE_SECOND, g, bit1, not2, partner).start()

    def relay_core(g):
        out_send(OUT_RELAY, g, not1, not2, second).wait_recv()
        out_send(CORE_RELAY, g, not1, not2, partner).start()

    def drain(g):
        out_local(g).wait()
        out_send(OUT_FIRST, g, bit1, bit2, first).wait_send()
        out_send(OUT_SECOND, g, bit1, bit2, second).wait_send()
        out_send(OUT_RELAY, g, not1, bit2, second).wait_send()
        out_send(CORE_OWN, g, bit1, bit2, partner).wait()
        out_send(CORE_FIRST, g, not1, bit2, partner).wait()
        out_send(CORE_SECOND, g, bit1, not2, partner).wait()
        out_send(CORE_RELAY, g, not1, not2, partner).wait()

    u_start()
    opened = first_open + OPENED
    for g in range(txt_chunks, opened):
        start_o(jnp.int32(g))
    w_load(0, w1t_hbm, w1).start()
    w_load(1, w2t_hbm, w2).start()
    for g in range(txt_chunks):
        x1_load(g).start()
        if g < last_txt:
            for who in (core, far):
                txt_load(g, who).start()
    kv_load().start()
    q_load(0).start()
    for g in range(first_open, opened):
        send_o(jnp.int32(g))

    stages = ((finish, -3, 0), (start_o, 8, opened), (relay_out, -4, 0), (mlp_hidden, 0, 0), (send_o, 8, opened), (relay_core, -6, 0), (mlp_out, 0, 0), (relay_o, 7, first_open),
              (start_x, 2, txt_chunks), (project, 1, txt_chunks), (second_out, -4, 0), (add_first, -1, 0), (mlp_sum, 0, 0), (drain, -6, 0), (attend, 0, 0))
    most = max(ahead for _, ahead, _ in stages)
    least = min(ahead for _, ahead, _ in stages)

    def step(i):
        @pl.when(i == U_RELAY_STEP)
        def _():
            u_relay()

        for stage, ahead, lowest in stages:
            if stage is attend:
                lax.fori_loop(attended(i), attended(i + 1), attend, 0)
                continue
            g = i + txt_chunks - most + ahead

            @pl.when((g >= lowest) & (g < total))
            def _():
                stage(g)

        @pl.when(i == U_RELAY_STEP + 1)
        def _():
            u_last()

    loop(total - txt_chunks + most - least, step)


ATTEND = (2, 2, 2, 0, 0, 0, 0, 1, 2, 2, 3, 3, 3, 3, 1)
U_RELAY_STEP = 2


def block_call(img_o, og, kv, x, u_txt, x1_txt, tu, wp, pw, w1t, w2t, w1i, w2i, vecs, fb, rows):
    batch, img_len, dim = x.shape
    txt_len = u_txt.shape[1]
    ff = w1t.shape[1]
    txt_chunks = batch * (txt_len // rows)
    per_img = img_len // rows
    img_chunks = batch * per_img
    assert txt_chunks == 2
    half, quarter, eighth = rows // 2, rows // 4, rows // 8
    cfg = (batch, txt_chunks, img_chunks, per_img, rows, 512)
    total = txt_chunks + img_chunks
    anywhere = pl.BlockSpec(memory_space=pl.ANY)
    return pl.pallas_call(
        functools.partial(block_kernel, cfg),
        in_specs=[anywhere] * 13 + [pl.BlockSpec(memory_space=pltpu.VMEM)] * 2,
        out_specs=[anywhere, anywhere],
        out_shape=[jax.ShapeDtypeStruct((total * rows, dim), BF16), jax.ShapeDtypeStruct(img_o.shape, BF16)],
        scratch_shapes=[
            pltpu.VMEM((kv.shape[0] // 3 * 2,) + kv.shape[1:], BF16),
            pltpu.VMEM((2, rows, HEAD), BF16),
            pltpu.VMEM((2, rows, HEAD), BF16),
            pltpu.VMEM((dim, dim), BF16),
            pltpu.VMEM((dim, ff), BF16),
            pltpu.VMEM((ff, dim), BF16),
            pltpu.VMEM((O_SLOTS, half, dim), BF16),
            pltpu.VMEM((2, half, dim), BF16),
            pltpu.VMEM((SLOTS, eighth, dim), BF16),
            pltpu.VMEM((2, rows, dim), BF16),
            pltpu.VMEM((rows, ff), BF16),
            pltpu.VMEM((half, dim), BF16),
            pltpu.VMEM((2, half, dim), BF16),
            pltpu.VMEM((half, dim), F32),
            pltpu.VMEM((half, dim), BF16),
            pltpu.VMEM((2, quarter, dim), BF16),
            pltpu.VMEM((2, eighth, dim), F32),
            pltpu.VMEM((2, eighth, dim), BF16),
            pltpu.VMEM((SLOTS, eighth, dim), BF16),
            pltpu.VMEM((SLOTS, eighth, dim), BF16),
            pltpu.SemaphoreType.DMA((5,)),
            pltpu.SemaphoreType.DMA((10,)),
            pltpu.SemaphoreType.DMA((3, SEMS)),
            pltpu.SemaphoreType.DMA((3, 2)),
            *[pltpu.SemaphoreType.DMA((22, SEMS))] * 2,
        ],
        compiler_params=pltpu.CompilerParams(collective_id=0, has_side_effects=True, vmem_limit_bytes=VMEM_BYTES),
        name="block",
    )(img_o, og, kv, x, u_txt, x1_txt, tu, wp, pw, w1t, w2t, w1i, w2i, vecs, fb)


def copy_kernel(pieces, flat_hbm, *rest):
    outs, (buf, isem, osem) = rest[:-3], rest[-3:]
    rows = buf.shape[1]
    loads = []
    for n, (which, b, r) in enumerate(pieces):
        load = pltpu.make_async_copy(flat_hbm.at[n * rows:(n + 1) * rows, :], buf.at[n], isem.at[n])
        load.start()
        loads.append(load)
    stores = []
    for n, (which, b, r) in enumerate(pieces):
        loads[n].wait()
        store = pltpu.make_async_copy(buf.at[n], outs[which].at[b, r:r + rows, :], osem.at[n])
        store.start()
        stores.append(store)
    for store in stores:
        store.wait()


def copy_call(flat, shapes, rows):
    pieces = [(which, b, r) for which, shape in enumerate(shapes) for b in range(shape[0]) for r in range(0, shape[1], rows)]
    anywhere = pl.BlockSpec(memory_space=pl.ANY)
    dim = flat.shape[1]
    return pl.pallas_call(
        functools.partial(copy_kernel, pieces),
        in_specs=[anywhere],
        out_specs=[anywhere] * len(shapes),
        out_shape=[jax.ShapeDtypeStruct(shape, flat.dtype) for shape in shapes],
        scratch_shapes=[
            pltpu.VMEM((len(pieces), rows, dim), flat.dtype),
            pltpu.SemaphoreType.DMA((len(pieces),)),
            pltpu.SemaphoreType.DMA((len(pieces),)),
        ],
        compiler_params=pltpu.CompilerParams(vmem_limit_bytes=VMEM_BYTES),
        name="copy_out",
    )(flat)


def local_block(img, txt, vec, ids, img_w, txt_w):
    n_dev = 8
    batch, txt_len = txt.shape[:2]
    rows = txt_len

    def by_kind(weight):
        return jnp.transpose(weight, (1, 0, 2))

    def small_of(w):
        return w[1], w[3], w[4], w[5], w[7], w[9], w[11]

    table = jnp.asarray(rope_table())
    ids_t = jnp.transpose(ids, (2, 0, 1))
    o, kv, proj_w, txt_u, og, txt_x1, txt_tu, vecs, small = front_call(txt, img, by_kind(txt_w[2]), by_kind(img_w[2]), by_kind(txt_w[0]), by_kind(img_w[0]), img_w[6], txt_w[6], vec, small_of(txt_w), small_of(img_w), ids_t, table, n_dev, rows)
    flat, _ = block_call(o, og, kv, img, txt_u, txt_x1, txt_tu, proj_w, img_w[6], txt_w[8], txt_w[10], img_w[8], img_w[10], vecs, small, rows)
    txt_out, img_out = copy_call(flat, (txt.shape, img.shape), rows)
    return img_out, txt_out


def solution(mesh):
    act_spec = P('dp', WHOLE, WHOLE)
    mapped = jax.shard_map(local_block, mesh=mesh, in_specs=(act_spec, act_spec, P('dp', WHOLE), act_spec, PATH_SPECS, PATH_SPECS), out_specs=(act_spec, act_spec), check_vma=False)

    def forward(img, txt, vec, ids, *weights):
        return mapped(img, txt, vec, ids, weights[:12], weights[12:])

    return forward
```
